16 devices in a mesh: tp: 4 (over z, y), dp: 4 (over x, core).
Axes of the slice: x: 2, y: 2, z: 2, core: 2. Of those that a mesh axis runs over, the one named last changes fastest.
Arguments:
- tok_ids: int32 [32, 1024], P('dp')
- emb_table: bfloat16 [50272, 1024], P('tp')
- pos_table: bfloat16 [2050, 1024], replicated
- ln1_gain: bfloat16 [1024], replicated
- ln1_bias: bfloat16 [1024], replicated
- w_qkv: bfloat16 [1024, 3, 16, 64], P(None, None, 'tp')
- b_qkv: bfloat16 [3, 16, 64], P(None, 'tp')
- w_out: bfloat16 [16, 64, 1024], P('tp')
- b_out: bfloat16 [1024], replicated
- ln2_gain: bfloat16 [1024], replicated
- ln2_bias: bfloat16 [1024], replicated
- w_up: bfloat16 [1024, 4096], P(None, 'tp')
- b_up: bfloat16 [4096], P('tp')
- w_down: bfloat16 [4096, 1024], P('tp')
- b_down: bfloat16 [1024], replicated
- out_grad: bfloat16 [32, 1024, 1024], P('dp', 'tp')
Outputs:
- output 1: bfloat16 [32, 1024, 1024], P('dp', 'tp')
- output 2: float32 [50272, 1024], P('tp')
- output 3: float32 [2050, 1024], replicated
- output 4: float32 [1024], replicated
- output 5: float32 [1024], replicated
- output 6: float32 [1024, 3, 16, 64], P(None, None, 'tp')
- output 7: float32 [3, 16, 64], P(None, 'tp')
- output 8: float32 [16, 64, 1024], P('tp')
- output 9: float32 [1024], replicated
- output 10: float32 [1024], replicated
- output 11: float32 [1024], replicated
- output 12: float32 [1024, 4096], P(None, 'tp')
- output 13: float32 [4096], P('tp')
- output 14: float32 [4096, 1024], P('tp')
- output 15: float32 [1024], replicated
All inputs are finite; a program needn't handle non-finite values.
Results may differ from the reference program's by a relative error of at most 0.0153794.
Values are sent between devices in bfloat16 or wider.
A program may use at most 1 GiB of HBM per device.

```python
import jax
import jax.numpy as jnp
from jax import lax

D = 1024
HEADS = 16
HEAD = 64
FF = 4096
VOCAB = 50272
POS_ROWS = 2050
SEQ = 1024
BATCH = 32
HOT = 512


def draw_ids(id_key):
    key_pool, key_left, key_right, key_flat, key_pick = jax.random.split(id_key, 5)
    pool_ids = jax.random.randint(key_pool, (HOT,), 0, VOCAB)
    left_idx = jax.random.randint(key_left, (BATCH, SEQ), 0, 22)
    right_idx = jax.random.randint(key_right, (BATCH, SEQ), 0, 22)
    hot_ids = jnp.take(pool_ids, left_idx * right_idx)
    flat_ids = jax.random.randint(key_flat, (BATCH, SEQ), 0, VOCAB)
    pick_flat = jax.random.randint(key_pick, (BATCH, SEQ), 0, 2)
    tok_ids = jnp.where(pick_flat == 0, flat_ids, hot_ids)
    tok_ids = tok_ids.at[0, 0].set(0).at[0, 1].set(VOCAB - 1)
    return tok_ids.astype(jnp.int32)


def setup_inputs(seed: int = 0) -> dict:
    keys = jax.random.split(jax.random.key(seed), 16)

    def draw_normal(key_idx, arr_shape, std_dev, center):
        values = center + std_dev * jax.random.normal(keys[key_idx], arr_shape, jnp.float32)
        return values.astype(jnp.bfloat16)

    return {
        "tok_ids": draw_ids(keys[0]),
        "emb_table": draw_normal(1, (VOCAB, D), 1.0, 0.0),
        "pos_table": draw_normal(2, (POS_ROWS, D), 0.5, 0.0),
        "ln1_gain": draw_normal(3, (D,), 0.2, 1.0),
        "ln1_bias": draw_normal(4, (D,), 0.2, 0.0),
        "w_qkv": draw_normal(5, (D, 3, HEADS, HEAD), D ** -0.5, 0.0),
        "b_qkv": draw_normal(6, (3, HEADS, HEAD), 0.2, 0.0),
        "w_out": draw_normal(7, (HEADS, HEAD, D), (HEADS * HEAD) ** -0.5, 0.0),
        "b_out": draw_normal(8, (D,), 0.3, 0.0),
        "ln2_gain": draw_normal(9, (D,), 0.2, 1.0),
        "ln2_bias": draw_normal(10, (D,), 0.2, 0.0),
        "w_up": draw_normal(11, (D, FF), D ** -0.5, 0.0),
        "b_up": draw_normal(12, (FF,), 0.3, 0.0),
        "w_down": draw_normal(13, (FF, D), FF ** -0.5, 0.0),
        "b_down": draw_normal(14, (D,), 0.3, 0.0),
        "out_grad": draw_normal(15, (BATCH, SEQ, D), (BATCH * SEQ) ** -0.5, 0.0),
    }


def as_bf16(values):
    return values.astype(jnp.bfloat16).astype(jnp.float32)


def layer_norm(x_in, ln_gain, ln_shift):
    row_mean = jnp.mean(x_in, axis=-1, keepdims=True)
    centered = x_in - row_mean
    variance = jnp.mean(centered * centered, axis=-1, keepdims=True)
    return centered * lax.rsqrt(variance + 1e-5) * ln_gain + ln_shift


def seq_forward(params, row_ids):
    (emb_table, pos_table, ln1_gain, ln1_bias, w_qkv, b_qkv, w_out, b_out,
     ln2_gain, ln2_bias, w_up, b_up, w_down, b_down) = params
    resid_x = jnp.take(emb_table, row_ids, axis=0) + pos_table[2:SEQ + 2]
    hid1 = as_bf16(layer_norm(resid_x, ln1_gain, ln1_bias))
    qkv_heads = as_bf16(jnp.einsum("sd,djhe->jhse", hid1, w_qkv) + b_qkv[:, :, None, :])
    scores = jnp.einsum("hqe,hke->hqk", qkv_heads[0], qkv_heads[1]) * HEAD ** -0.5
    causal = jnp.arange(SEQ)[:, None] >= jnp.arange(SEQ)[None, :]
    attn_probs = as_bf16(jax.nn.softmax(jnp.where(causal[None], scores, -1e30), axis=-1))
    context = as_bf16(jnp.einsum("hqk,hke->qhe", attn_probs, qkv_heads[2]))
    resid_x1 = resid_x + as_bf16(jnp.einsum("qhe,hed->qd", context, w_out)) + b_out
    hid2 = as_bf16(layer_norm(resid_x1, ln2_gain, ln2_bias))
    act_out = as_bf16(jax.nn.gelu(jnp.dot(hid2, w_up) + b_up, approximate=True))
    return as_bf16(resid_x1 + as_bf16(jnp.dot(act_out, w_down)) + b_down)


def reference(tok_ids, emb_table, pos_table, ln1_gain, ln1_bias, w_qkv, b_qkv, w_out, b_out,
              ln2_gain, ln2_bias, w_up, b_up, w_down, b_down, out_grad):
    params = tuple(weight.astype(jnp.float32) for weight in (
        emb_table, pos_table, ln1_gain, ln1_bias, w_qkv, b_qkv, w_out, b_out,
        ln2_gain, ln2_bias, w_up, b_up, w_down, b_down))
    seq_body = jax.checkpoint(seq_forward)

    def whole_batch(prm_all):
        return lax.map(lambda row_ids: seq_body(prm_all, row_ids), tok_ids)

    layer_out, pull_back = jax.vjp(whole_batch, params)
    (param_grads,) = pull_back(out_grad.astype(jnp.float32))
    return (layer_out.astype(jnp.bfloat16), param_grads[0], param_grads[1], param_grads[2],
            param_grads[3], param_grads[4], param_grads[5], param_grads[6], param_grads[7],
            param_grads[8], param_grads[9], param_grads[10], param_grads[11], param_grads[12],
            param_grads[13])
```

```python
import functools

import jax
import jax.numpy as jnp
from jax import lax
from jax.experimental import pallas as pl
from jax.experimental.pallas import tpu as pltpu
from jax.sharding import Mesh, PartitionSpec as P

F32 = jnp.float32
BF16 = jnp.bfloat16

BLK = 256


def dot_nt(a, b):
    return lax.dot_general(a, b, (((1,), (1,)), ((), ())), preferred_element_type=F32)


def dot_nn(a, b):
    return lax.dot_general(a, b, (((1,), (0,)), ((), ())), preferred_element_type=F32)


def head_only(x, head):
    half = x.shape[1] // 2
    lane = lax.broadcasted_iota(jnp.int32, x.shape, 1)
    keep = (lane < half) if head == 0 else (lane >= half)
    return jnp.where(keep, x, jnp.zeros((), x.dtype))


def attn_fwd_kernel(qkv_ref, ctx_ref, lse_ref, ctx_t):
    seq, width = ctx_ref.shape
    half = width // 2
    scale = half ** -0.5
    q2 = qkv_ref[:, 0:width] * jnp.asarray(scale, BF16)
    v_t = qkv_ref[:, 2 * width:3 * width].T
    for head in range(2):
        q_h = head_only(q2, head)
        v_h = v_t[head * half:(head + 1) * half, :]
        for i in range(seq // BLK):
            lo, hi = i * BLK, (i + 1) * BLK
            s = dot_nt(qkv_ref[0:hi, width:2 * width], q_h[lo:hi, :])
            diag = s[lo:hi]
            key = lax.broadcasted_iota(jnp.int32, (BLK, BLK), 0)
            qry = lax.broadcasted_iota(jnp.int32, (BLK, BLK), 1)
            diag = jnp.where(key <= qry, diag, -1e30)
            top = jnp.max(diag, axis=0, keepdims=True)
            if i:
                top = jnp.maximum(top, jnp.max(s[0:lo], axis=0, keepdims=True))
            p_diag = jnp.exp(diag - top)
            total = jnp.sum(p_diag, axis=0, keepdims=True)
            if i:
                p_left = jnp.exp(s[0:lo] - top)
                total = total + jnp.sum(p_left, axis=0, keepdims=True)
            inv = 1.0 / total
            acc = dot_nn(v_h[:, lo:hi], (p_diag * inv).astype(BF16))
            if i:
                acc = acc + dot_nn(v_h[:, 0:lo], (p_left * inv).astype(BF16))
            ctx_t[head * half:(head + 1) * half, lo:hi] = acc
            lse_ref[head:head + 1, lo:hi] = top + jnp.log(total)
    ctx_ref[...] = ctx_t[...].T.astype(BF16)


def attn_fwd(qkv, n_seq, seq, n_pair):
    width = 128
    return pl.pallas_call(
        attn_fwd_kernel,
        grid=(n_seq, n_pair),
        in_specs=[pl.BlockSpec((seq, 3 * width), lambda b, p: (b, p))],
        out_specs=[pl.BlockSpec((seq, width), lambda b, p: (b, p)),
                   pl.BlockSpec((None, None, 2, seq), lambda b, p: (b, p, 0, 0))],
        out_shape=[jax.ShapeDtypeStruct((n_seq * seq, n_pair * width), BF16),
                   jax.ShapeDtypeStruct((n_seq, n_pair, 2, seq), F32)],
        scratch_shapes=[pltpu.VMEM((width, seq), F32)],
        name="attn_fwd",
        cost_estimate=pl.CostEstimate(flops=n_seq * n_pair * 8 * seq * seq * 256 * 10 // 16, bytes_accessed=n_seq * seq * n_pair * width * 8,
                                      transcendentals=n_seq * n_pair * seq * seq),
        compiler_params=pltpu.CompilerParams(vmem_limit_bytes=48 * 1024 * 1024),
    )(qkv)


def attn_bwd_kernel(qkv_ref, ctx_ref, dctx_ref, lse_ref, dqkv_ref, dk_t, dv_t):
    seq, width = ctx_ref.shape
    half = width // 2
    scale = half ** -0.5
    q2 = qkv_ref[:, 0:width] * jnp.asarray(scale, BF16)
    q_t = q2.T
    do_t = dctx_ref[...].T
    lse_c = jnp.concatenate([lse_ref[...], jnp.zeros((6, seq), F32)], axis=0).T
    prod = dctx_ref[...].astype(F32) * ctx_ref[...].astype(F32)
    for i in range(seq // BLK):
        lo, hi = i * BLK, (i + 1) * BLK
        dq = []
        for head in range(2):
            rows = slice(head * half, (head + 1) * half)
            mean = jnp.sum(head_only(prod[lo:hi], head), axis=1, keepdims=True)
            lse = lse_c[lo:hi, head:head + 1]
            q_h = head_only(q2[lo:hi], head)
            do_h = head_only(dctx_ref[lo:hi, :], head)
            s = dot_nt(q_h, qkv_ref[0:hi, width:2 * width])
            dp = dot_nt(do_h, qkv_ref[0:hi, 2 * width:3 * width])
            qry = lax.broadcasted_iota(jnp.int32, (BLK, BLK), 0)
            key = lax.broadcasted_iota(jnp.int32, (BLK, BLK), 1)
            p_diag = jnp.where(key <= qry, jnp.exp(s[:, lo:hi] - lse), 0.0)
            ds_diag = (p_diag * (dp[:, lo:hi] - mean)).astype(BF16)
            pb_diag = p_diag.astype(BF16)
            dv_t[rows, lo:hi] = dot_nn(do_t[rows, lo:hi], pb_diag)
            dk_t[rows, lo:hi] = dot_nn(q_t[rows, lo:hi], ds_diag)
            dq_h = dot_nn(ds_diag, qkv_ref[lo:hi, width:2 * width])
            if i:
                p_left = jnp.exp(s[:, 0:lo] - lse)
                ds_left = (p_left * (dp[:, 0:lo] - mean)).astype(BF16)
                pb_left = p_left.astype(BF16)
                dv_t[rows, 0:lo] += dot_nn(do_t[rows, lo:hi], pb_left)
                dk_t[rows, 0:lo] += dot_nn(q_t[rows, lo:hi], ds_left)
                dq_h = dq_h + dot_nn(ds_left, qkv_ref[0:lo, width:2 * width])
            dq.append(dq_h)
        lane = lax.broadcasted_iota(jnp.int32, (BLK, width), 1)
        dqkv_ref[lo:hi, 0:width] = (jnp.where(lane < half, dq[0], dq[1]) * scale).astype(BF16)
    dqkv_ref[:, width:2 * width] = dk_t[...].T.astype(BF16)
    dqkv_ref[:, 2 * width:3 * width] = dv_t[...].T.astype(BF16)


def attn_bwd(qkv, ctx, dctx, lse, n_seq, seq, n_pair):
    width = 128
    return pl.pallas_call(
        attn_bwd_kernel,
        grid=(n_seq, n_pair),
        in_specs=[pl.BlockSpec((seq, 3 * width), lambda b, p: (b, p)),
                  pl.BlockSpec((seq, width), lambda b, p: (b, p)),
                  pl.BlockSpec((seq, width), lambda b, p: (b, p)),
                  pl.BlockSpec((None, None, 2, seq), lambda b, p: (b, p, 0, 0))],
        out_specs=pl.BlockSpec((seq, 3 * width), lambda b, p: (b, p)),
        out_shape=jax.ShapeDtypeStruct((n_seq * seq, n_pair * 3 * width), BF16),
        scratch_shapes=[pltpu.VMEM((width, seq), F32), pltpu.VMEM((width, seq), F32)],
        name="attn_bwd",
        cost_estimate=pl.CostEstimate(flops=n_seq * n_pair * 20 * seq * seq * 256 * 10 // 16, bytes_accessed=n_seq * seq * n_pair * width * 16,
                                      transcendentals=n_seq * n_pair * seq * seq),
        compiler_params=pltpu.CompilerParams(vmem_limit_bytes=48 * 1024 * 1024),
    )(qkv, ctx, dctx, lse)


LANES = 128


def accum_kernel(n_block, cap, sub_rows, width, pos_ref, first_ref, *refs):
    tok_refs = refs[:n_block]
    out_ref = refs[n_block]
    n_sub = len(sub_rows)
    acc = refs[n_block + 1:n_block + 1 + n_sub]
    buf, stage, in_sem, out_sem = refs[n_block + 1 + n_sub:]
    tiles = width // LANES
    group = 8 * tiles

    def fetch(block):
        return pltpu.make_async_copy(tok_refs[block], buf.at[block % 2], in_sem.at[block % 2])

    fetch(0).start()
    for s in range(n_sub):
        def clear(i, _, s=s):
            acc[s][pl.ds(pl.multiple_of(i * group, group), group), :] = jnp.zeros((group, LANES), F32)
            return 0
        lax.fori_loop(0, sub_rows[s] // 8, clear, 0)
    for block in range(n_block):
        if block + 1 < n_block:
            fetch(block + 1).start()
        fetch(block).wait()

        def widen(g, _, block=block):
            rows = buf[block % 2, pl.ds(pl.multiple_of(g * 16, 16), 16), :].astype(F32)
            base = pl.multiple_of(g * 2 * group, 2 * group)
            for h in range(2):
                for c in range(tiles):
                    stage[pl.ds(base + h * group + c * 8, 8), :] = rows[h * 8:(h + 1) * 8, c * LANES:(c + 1) * LANES]
            return 0
        lax.fori_loop(0, cap // 16, widen, 0)

        starts = [first_ref[block * (n_sub + 1) + s] for s in range(n_sub + 1)]
        counts = [starts[s + 1] - starts[s] for s in range(n_sub)]
        longest = functools.reduce(jnp.maximum, counts)

        def add_rows(i, _, block=block, starts=starts, counts=counts):
            for s in range(n_sub):
                valid = i < counts[s]
                slot = jnp.where(valid, starts[s] + i, 0)
                at = jnp.where(valid, pos_ref[block * cap + slot], 0)
                src = (slot >> 3) * group + (slot & 7)
                row = stage[pl.ds(src, tiles, stride=8), :]
                row = jnp.where(valid, row, 0.0)
                acc[s][pl.ds(at, tiles, stride=8), :] += row
            return 0
        lax.fori_loop(0, longest, add_rows, 0)
    done = 0
    copies = []
    for s in range(n_sub):
        n = sub_rows[s] * tiles
        copies.append(pltpu.make_async_copy(acc[s], out_ref.at[pl.ds(done, n), :], out_sem.at[s]))
        copies[-1].start()
        done += n
    for c in copies:
        c.wait()


def accum(tok_blocks, pos, first, sub_rows, width):
    n_block = len(tok_blocks)
    cap = tok_blocks[0].shape[0]
    n_sub = len(sub_rows)
    tiles = width // LANES
    return pl.pallas_call(
        functools.partial(accum_kernel, n_block, cap, sub_rows, width),
        in_specs=[pl.BlockSpec(memory_space=pltpu.SMEM), pl.BlockSpec(memory_space=pltpu.SMEM)]
        + [pl.BlockSpec(memory_space=pl.ANY)] * n_block,
        out_specs=pl.BlockSpec(memory_space=pl.ANY),
        out_shape=jax.ShapeDtypeStruct((sum(sub_rows) * tiles, LANES), F32),
        scratch_shapes=[pltpu.VMEM((r * tiles, LANES), F32) for r in sub_rows]
        + [pltpu.VMEM((2, cap, width), BF16), pltpu.VMEM((cap * tiles, LANES), F32),
           pltpu.SemaphoreType.DMA((2,)), pltpu.SemaphoreType.DMA((n_sub,))],
        name="table_accum",
        compiler_params=pltpu.CompilerParams(vmem_limit_bytes=63 * 1024 * 1024),
    )(pos, first, *tok_blocks)


POS_OFFSET = 2
LN_EPS = 1e-5
SLOTS = 768
LOW = 32
GELU_S = 0.7978845608028654
GELU_A = 0.044715


def dot_tn(a, b):
    return lax.dot_general(a, b, (((0,), (0,)), ((), ())), preferred_element_type=F32)


def norm_forward(x_in, gain, shift):
    mean = jnp.mean(x_in, axis=-1, keepdims=True)
    centered = x_in - mean
    inv_std = lax.rsqrt(jnp.mean(centered * centered, axis=-1, keepdims=True) + LN_EPS)
    normed = centered * inv_std
    return normed * gain + shift, normed, inv_std


def norm_backward(d_y, normed, inv_std, gain):
    d_norm = d_y * gain
    d_x = inv_std * (d_norm - jnp.mean(d_norm, axis=-1, keepdims=True)
                     - normed * jnp.mean(d_norm * normed, axis=-1, keepdims=True))
    return d_x, jnp.sum(d_y * normed, axis=0), jnp.sum(d_y, axis=0)


def before(n):
    return (lax.broadcasted_iota(jnp.int32, (n, n), 1) < lax.broadcasted_iota(jnp.int32, (n, n), 0)).astype(BF16)


def rank_in_class(hot):
    n_blk, n_tok, n_cls = hot.shape
    ones = hot.astype(BF16).reshape(n_blk, n_tok // 128, 128, n_cls)
    within = jnp.einsum("ij,bnjk->bnik", before(128), ones, preferred_element_type=F32)
    sums = jnp.sum(ones.astype(F32), axis=2)
    ahead = jnp.einsum("mn,bnk->bmk", before(n_tok // 128), sums.astype(BF16), preferred_element_type=F32)
    rank = jnp.sum((within + ahead[:, :, None, :]) * ones.astype(F32), axis=3)
    return rank.reshape(n_blk, n_tok).astype(jnp.int32), jnp.sum(sums, axis=1).astype(jnp.int32)


def compact(rank, valid, value):
    n_high = SLOTS // LOW
    high = ((rank // LOW)[:, :, None] == jnp.arange(n_high)) & valid[:, :, None]
    low = ((rank % LOW)[:, :, None] == jnp.arange(LOW)).astype(F32)
    parts = jnp.concatenate([low * (value // 128).astype(F32)[:, :, None], low * (value % 128).astype(F32)[:, :, None]], axis=2)
    out = jnp.einsum("bjh,bjl->bhl", high.astype(BF16), parts.astype(BF16), preferred_element_type=F32).astype(jnp.int32)
    return (out[:, :, :LOW] * 128 + out[:, :, LOW:]).reshape(rank.shape[0], SLOTS)


def solution(mesh):
    n_tp, n_dp = mesh.shape["tp"], mesh.shape["dp"]
    n_core = 2
    n_x = n_dp // n_core
    mesh3 = Mesh(mesh.devices.reshape(n_tp, n_x, n_core), ("tp", "xx", "cc"))
    dp = ("xx", "cc")
    tp_swap = [[(i, i ^ k) for i in range(n_tp)] for k in range(n_tp)]
    pair = [(0, 1), (1, 0)]

    def local_step(tok_ids, emb_table, pos_table, ln1_gain, ln1_bias, w_qkv, b_qkv, w_out, b_out,
                   ln2_gain, ln2_bias, w_up, b_up, w_down, b_down, out_grad):
        tp_index, x_index, c_index = lax.axis_index("tp"), lax.axis_index("xx"), lax.axis_index("cc")
        dp_index = x_index * n_core + c_index
        n_seq_dp, seq = tok_ids.shape
        n_seq = n_seq_dp // n_tp
        n_tok = n_seq * seq
        rows, width = emb_table.shape
        n_sub = 4
        sub = -(-rows // n_sub // 8) * 8
        sub_rows = (sub,) * (n_sub - 1) + (rows - (n_sub - 1) * sub,)
        seq_local = seq // n_tp
        ff = w_up.shape[1]
        gain1, bias1 = ln1_gain.astype(F32), ln1_bias.astype(F32)
        gain2, bias2 = ln2_gain.astype(F32), ln2_bias.astype(F32)

        def half(w, axis):
            n = w.shape[axis] // n_core
            return lax.dynamic_slice_in_dim(w, c_index * n, n, axis)

        def gather_rows(w):
            return lax.all_gather(w, ("tp", "cc"), axis=0, tiled=True)

        def swap(v, axis, k=1):
            return lax.ppermute(v, axis, tp_swap[k] if axis == "tp" else pair)

        wqkv_t = gather_rows(jnp.transpose(half(w_qkv, 2), (1, 2, 3, 0)).reshape(-1, width))
        wout_w = gather_rows(half(w_out, 0).reshape(-1, width))
        wup_t = gather_rows(half(w_up, 1).T)
        wdown_w = gather_rows(half(w_down, 0))
        n_pair = wout_w.shape[0] // 128
        biases = lax.all_gather(jnp.concatenate([
            b_qkv.reshape(3, n_core, -1, b_qkv.shape[2]).transpose(1, 0, 2, 3).reshape(-1), b_up]), "tp", axis=0)
        bqkv_w = biases[:, :-ff].reshape(-1).astype(F32)
        bup_w = biases[:, -ff:].reshape(-1).astype(F32)

        ids_all = lax.all_gather(tok_ids, dp, axis=0, tiled=True).reshape(n_dp * n_tp, n_tok)
        local = ids_all - tp_index * rows
        sub_of = sum(((local >= s * sub).astype(jnp.int32) for s in range(1, n_sub)), jnp.zeros_like(local))
        owned = (local >= 0) & (local < rows)
        hot = owned[:, :, None] & (sub_of[:, :, None] == jnp.arange(n_sub))
        rank, counts = rank_in_class(hot)
        first = jnp.concatenate([jnp.zeros_like(counts[:, :1]), jnp.cumsum(counts, axis=1)], axis=1)
        rank = rank + jnp.sum(jnp.where(hot, first[:, None, :-1], 0), axis=2)
        most = jnp.stack([jnp.max(jnp.sum(((ids_all >= o * rows) & (ids_all < (o + 1) * rows)).astype(jnp.int32), axis=1))
                          for o in range(n_tp)])
        rounds = (jnp.max(most) + SLOTS - 1) // SLOTS

        def lists(r):
            at = rank - r * SLOTS
            return compact(at, owned & (at >= 0) & (at < SLOTS), jnp.where(owned, local, 0))

        own_ids = lax.dynamic_index_in_dim(ids_all, dp_index * n_tp + tp_index, 0, keepdims=True)
        own_owner = sum(((own_ids >= o * rows).astype(jnp.int32) for o in range(1, n_tp)), jnp.zeros_like(own_ids))
        own_local = own_ids - own_owner * rows
        own_sub = sum(((own_local >= s * sub).astype(jnp.int32) for s in range(1, n_sub)), jnp.zeros_like(own_ids))
        own_hot = (own_owner * n_sub + own_sub)[:, :, None] == jnp.arange(n_tp * n_sub)
        own_rank, own_counts = rank_in_class(own_hot)
        own_first = jnp.cumsum(own_counts.reshape(n_tp, n_sub), axis=1) - own_counts.reshape(n_tp, n_sub)
        own_rank = (own_rank + jnp.sum(jnp.where(own_hot, own_first.reshape(1, 1, -1), 0), axis=2))[0]
        own_owner = own_owner[0]

        def own_lists(r):
            at = jnp.broadcast_to(own_rank - r * SLOTS, (n_tp, n_tok))
            mine = own_owner == jnp.arange(n_tp)[:, None]
            return compact(at, mine & (at >= 0) & (at < SLOTS), jnp.broadcast_to(jnp.arange(n_tok), (n_tp, n_tok)))

        def fetch_rows(r, my_lists):
            sent = [jnp.take(emb_table, lax.dynamic_index_in_dim(my_lists, tp_index ^ k, 0, keepdims=False), axis=0)
                    for k in range(n_tp)]
            got = jnp.concatenate([sent[0]] + [swap(sent[k], "tp", k) for k in range(1, n_tp)], axis=0)
            at = own_rank - r * SLOTS
            valid = (at >= 0) & (at < SLOTS)
            place = jnp.where(valid, (own_owner ^ tp_index) * SLOTS + at, 0)
            return jnp.take(got, place, axis=0), valid

        lists0 = lists(0)
        my_lists0 = lax.dynamic_slice_in_dim(lists0, dp_index * n_tp, n_tp, 0)
        emb_rows, _ = fetch_rows(0, my_lists0)

        def more_rows(carry):
            r, emb = carry
            got, valid = fetch_rows(r, lax.dynamic_slice_in_dim(lists(r), dp_index * n_tp, n_tp, 0))
            return r + 1, jnp.where(valid[:, None], got, emb)

        _, emb_rows = lax.while_loop(lambda c: c[0] < rounds, more_rows, (jnp.int32(1), emb_rows))

        og_parts = out_grad.reshape(n_tp, n_seq, seq_local, width)
        og = jnp.zeros((n_seq, seq, width), BF16)
        for k in range(n_tp):
            part = lax.dynamic_index_in_dim(og_parts, tp_index ^ k, 0, keepdims=False)
            part = swap(part, "tp", k) if k else part
            og = lax.dynamic_update_slice_in_dim(og, part, (tp_index ^ k) * seq_local, 1)
        og = og.reshape(n_tok, width)

        pos_rows = lax.slice_in_dim(pos_table, POS_OFFSET, POS_OFFSET + seq, axis=0)
        resid_x = (emb_rows.reshape(n_seq, seq, width).astype(F32) + pos_rows.astype(F32)[None]).reshape(n_tok, width)
        y1, normed1, inv_std1 = norm_forward(resid_x, gain1, bias1)
        hid1 = y1.astype(BF16)
        qkv = (dot_nt(hid1, wqkv_t) + bqkv_w).astype(BF16)
        ctx, lse = attn_fwd(qkv, n_seq, seq, n_pair)
        resid_x1 = resid_x + dot_nn(ctx, wout_w).astype(BF16).astype(F32) + b_out.astype(F32)
        y2, normed2, inv_std2 = norm_forward(resid_x1, gain2, bias2)
        hid2 = y2.astype(BF16)
        d_act = dot_nt(og, wdown_w).astype(BF16)
        z = dot_nt(hid2, wup_t) + bup_w
        th = jnp.tanh(GELU_S * (z + GELU_A * z * z * z))
        act = (0.5 * z * (1.0 + th)).astype(BF16)
        d_up = d_act.astype(F32) * (0.5 * (1.0 + th) + 0.5 * z * (1.0 - th * th) * (GELU_S * (1.0 + 3.0 * GELU_A * z * z)))
        d_b_up = jnp.sum(d_up, axis=0)
        d_up = d_up.astype(BF16)
        out = (resid_x1 + dot_nn(act, wdown_w).astype(BF16).astype(F32) + b_down.astype(F32)).astype(BF16)

        out4 = out.reshape(n_seq, seq, width)
        layer_out = jnp.zeros((n_tp, n_seq, seq_local, width), BF16)
        for k in range(n_tp):
            part = lax.dynamic_slice_in_dim(out4, (tp_index ^ k) * seq_local, seq_local, 1)
            part = swap(part, "tp", k) if k else part
            layer_out = lax.dynamic_update_slice_in_dim(layer_out, part[None], tp_index ^ k, 0)
        layer_out = layer_out.reshape(n_seq_dp, seq_local, width)

        def reduce_rows(g):
            g = lax.psum_scatter(g, ("tp", "cc"), scatter_dimension=0, tiled=True)
            g = g + swap(g, "xx")
            return g

        def share_core(g):
            return lax.all_gather(g, "cc", axis=0, tiled=True)

        d_wdown = reduce_rows(dot_tn(act, og))
        d_wup = reduce_rows(dot_tn(d_up, hid2))
        d_y2 = dot_nn(d_up, wup_t).astype(BF16).astype(F32)
        d_ln2, d_gain2, d_bias2 = norm_backward(d_y2, normed2, inv_std2, gain2)
        d_resid1 = og.astype(F32) + d_ln2
        d_attn = d_resid1.astype(BF16)
        d_wout = reduce_rows(dot_tn(ctx, d_attn))
        d_ctx = dot_nt(d_attn, wout_w).astype(BF16)
        d_qkv = attn_bwd(qkv, ctx, d_ctx, lse, n_seq, seq, n_pair)
        d_wqkv = reduce_rows(dot_tn(d_qkv, hid1))
        d_y1 = dot_nn(d_qkv, wqkv_t).astype(BF16).astype(F32)
        d_ln1, d_gain1, d_bias1 = norm_backward(d_y1, normed1, inv_std1, gain1)
        d_resid = d_resid1 + d_ln1

        def token_blocks(r):
            own = own_lists(r)
            d_tok = d_resid.astype(BF16)
            blocks = []
            for k in range(n_tp):
                part = jnp.take(d_tok, lax.dynamic_index_in_dim(own, tp_index ^ k, 0, keepdims=False), axis=0)
                blocks.append(swap(part, "tp", k) if k else part)
            other = [swap(b, "xx") for b in blocks]
            here = blocks + other
            return here + [swap(b, "cc") for b in here]

        def in_block_order(table):
            out = []
            for dc in range(n_core):
                for dx in range(n_x):
                    for k in range(n_tp):
                        d = (x_index ^ dx) * n_core + (c_index ^ dc)
                        out.append(lax.dynamic_index_in_dim(table, d * n_tp + (tp_index ^ k), 0, keepdims=False))
            return jnp.stack(out)

        block_rows = in_block_order(lists0)
        in_sub = sum(((block_rows >= s * sub).astype(jnp.int32) for s in range(1, n_sub)), jnp.zeros_like(block_rows))
        in_sub = block_rows - in_sub * sub
        pos_at = (in_sub // 8) * (width // 16) + in_sub % 8
        block_first = jnp.minimum(in_block_order(first), SLOTS)
        image = accum(token_blocks(0), pos_at.reshape(-1), block_first.reshape(-1), sub_rows, width)
        tiles = width // 128
        d_emb = image.reshape(rows // 8, tiles, 8, 128).transpose(0, 2, 1, 3).reshape(rows, width)

        def more_grads(carry):
            r, table = carry
            at = rank - r * SLOTS
            there = owned & (at >= 0) & (at < SLOTS)
            dest = compact(at, there, jnp.where(owned, local, 0) + 1)
            dest = jnp.where(dest == 0, rows, dest - 1)
            grads = jnp.concatenate(token_blocks(r), axis=0).astype(F32)
            return r + 1, table.at[in_block_order(dest).reshape(-1)].add(grads, mode="drop")

        _, d_emb = lax.while_loop(lambda c: c[0] < rounds, more_grads, (jnp.int32(1), d_emb))

        d_pos_sum = jnp.sum(d_resid.reshape(n_seq, seq, width), axis=0)
        d_pos_seq = gather_rows(reduce_rows(d_pos_sum))
        d_pos = jnp.pad(d_pos_seq, ((POS_OFFSET, pos_table.shape[0] - seq - POS_OFFSET), (0, 0)))

        small = lax.psum(jnp.concatenate([
            jnp.sum(d_qkv.astype(F32), axis=0), d_b_up, d_gain1, d_bias1, jnp.sum(d_resid1, axis=0),
            d_gain2, d_bias2, jnp.sum(og.astype(F32), axis=0)]), ("tp", "xx", "cc"))
        n_b = b_qkv.size
        d_b_qkv = lax.dynamic_slice_in_dim(small, tp_index * n_b, n_b).reshape(n_core, 3, -1, b_qkv.shape[2])
        d_b_qkv = d_b_qkv.transpose(1, 0, 2, 3).reshape(b_qkv.shape)
        d_b_up = lax.dynamic_slice_in_dim(small, n_tp * n_b + tp_index * ff, ff)
        vec = small[n_tp * (n_b + ff):].reshape(6, width)

        d_w_qkv = share_core(d_wqkv).reshape(n_core, 3, -1, w_qkv.shape[3], width).transpose(4, 1, 0, 2, 3).reshape(w_qkv.shape)
        d_w_out = share_core(d_wout).reshape(w_out.shape)
        d_w_up = share_core(d_wup).T
        d_w_down = share_core(d_wdown)
        return (layer_out, d_emb, d_pos, vec[0], vec[1], d_w_qkv, d_b_qkv, d_w_out,
                vec[2], vec[3], vec[4], d_w_up, d_b_up, d_w_down, vec[5])

    rep = P()
    in_specs = (P(dp, None), P("tp", None), rep, rep, rep,
                P(None, None, "tp", None), P(None, "tp", None), P("tp", None, None), rep,
                rep, rep, P(None, "tp"), P("tp"), P("tp", None), rep,
                P(dp, "tp", None))
    out_specs = (P(dp, "tp", None), P("tp", None), rep, rep, rep,
                 P(None, None, "tp", None), P(None, "tp", None), P("tp", None, None), rep,
                 rep, rep, P(None, "tp"), P("tp"), P("tp", None), rep)
    return jax.shard_map(local_step, mesh=mesh3, in_specs=in_specs, out_specs=out_specs, check_vma=False)
```

```python
import functools

import jax
import jax.numpy as jnp
from jax import lax
from jax.experimental import pallas as pl
from jax.experimental.pallas import tpu as pltpu
from jax.sharding import Mesh, PartitionSpec as P


F32 = jnp.float32
BF16 = jnp.bfloat16
MIB = 1024 * 1024
WIDEN = 32

BLK = 256


def dot_nt(a, b):
    return lax.dot_general(a, b, (((1,), (1,)), ((), ())), preferred_element_type=F32)


def dot_nn(a, b):
    return lax.dot_general(a, b, (((1,), (0,)), ((), ())), preferred_element_type=F32)


def head_only(x, head):
    half = x.shape[1] // 2
    lane = lax.broadcasted_iota(jnp.int32, x.shape, 1)
    keep = (lane < half) if head == 0 else (lane >= half)
    return jnp.where(keep, x, jnp.zeros((), x.dtype))


def attn_fwd_kernel(qkv_ref, ctx_ref, lse_ref, ctx_t):
    seq, width = ctx_ref.shape
    half = width // 2
    scale = half ** -0.5
    q2 = qkv_ref[:, 0:width] * jnp.asarray(scale, BF16)
    v_t = qkv_ref[:, 2 * width:3 * width].T
    tasks = [(head, i) for i in range(seq // BLK) for head in range(2)]

    def scores(head, i):
        return dot_nt(qkv_ref[0:(i + 1) * BLK, width:2 * width], head_only(q2[i * BLK:(i + 1) * BLK], head))

    ready = scores(*tasks[0])
    for n, (head, i) in enumerate(tasks):
        s = ready
        if n + 1 < len(tasks):
            ready = scores(*tasks[n + 1])
        lo, hi = i * BLK, (i + 1) * BLK
        v_h = v_t[head * half:(head + 1) * half, :]
        key = lax.broadcasted_iota(jnp.int32, (BLK, BLK), 0)
        qry = lax.broadcasted_iota(jnp.int32, (BLK, BLK), 1)
        diag = jnp.where(key <= qry, s[lo:hi], -1e30)
        top = jnp.max(diag, axis=0, keepdims=True)
        if i:
            top = jnp.maximum(top, jnp.max(s[0:lo], axis=0, keepdims=True))
        p_diag = jnp.exp(diag - top)
        total = jnp.sum(p_diag, axis=0, keepdims=True)
        if i:
            p_left = jnp.exp(s[0:lo] - top)
            total = total + jnp.sum(p_left, axis=0, keepdims=True)
        inv = 1.0 / total
        acc = dot_nn(v_h[:, lo:hi], (p_diag * inv).astype(BF16))
        if i:
            acc = acc + dot_nn(v_h[:, 0:lo], (p_left * inv).astype(BF16))
        ctx_t[head * half:(head + 1) * half, lo:hi] = acc
        lse_ref[head:head + 1, lo:hi] = top + jnp.log(total)
    ctx_ref[...] = ctx_t[...].T.astype(BF16)


def attn_fwd(qkv, n_seq, seq, n_pair):
    width = 128
    return pl.pallas_call(
        attn_fwd_kernel,
        grid=(n_seq, n_pair),
        in_specs=[pl.BlockSpec((seq, 3 * width), lambda b, p: (b, p))],
        out_specs=[pl.BlockSpec((seq, width), lambda b, p: (b, p)),
                   pl.BlockSpec((None, None, 2, seq), lambda b, p: (b, p, 0, 0))],
        out_shape=[jax.ShapeDtypeStruct((n_seq * seq, n_pair * width), BF16),
                   jax.ShapeDtypeStruct((n_seq, n_pair, 2, seq), F32)],
        scratch_shapes=[pltpu.VMEM((width, seq), F32)],
        name="attn_fwd",
        cost_estimate=pl.CostEstimate(flops=n_seq * n_pair * 8 * seq * seq * 256 * 10 // 16, bytes_accessed=n_seq * seq * n_pair * width * 8,
                                      transcendentals=n_seq * n_pair * seq * seq),
        compiler_params=pltpu.CompilerParams(vmem_limit_bytes=48 * 1024 * 1024),
    )(qkv)


def attn_bwd_kernel(qkv_ref, ctx_ref, dctx_ref, lse_ref, dqkv_ref, dk_t, dv_t):
    seq, width = ctx_ref.shape
    half = width // 2
    scale = half ** -0.5
    q2 = qkv_ref[:, 0:width] * jnp.asarray(scale, BF16)
    q_t = q2.T
    do_t = dctx_ref[...].T
    lse_c = jnp.concatenate([lse_ref[...], jnp.zeros((6, seq), F32)], axis=0).T
    prod = dctx_ref[...].astype(F32) * ctx_ref[...].astype(F32)
    tasks = [(head, i) for i in range(seq // BLK) for head in range(2)]

    def scores(head, i):
        lo, hi = i * BLK, (i + 1) * BLK
        return (dot_nt(head_only(q2[lo:hi], head), qkv_ref[0:hi, width:2 * width]),
                dot_nt(head_only(dctx_ref[lo:hi, :], head), qkv_ref[0:hi, 2 * width:3 * width]))

    dq = []
    ready = scores(*tasks[0])
    for n, (head, i) in enumerate(tasks):
        s, dp = ready
        if n + 1 < len(tasks):
            ready = scores(*tasks[n + 1])
        lo, hi = i * BLK, (i + 1) * BLK
        rows = slice(head * half, (head + 1) * half)
        mean = jnp.sum(head_only(prod[lo:hi], head), axis=1, keepdims=True)
        lse = lse_c[lo:hi, head:head + 1]
        qry = lax.broadcasted_iota(jnp.int32, (BLK, BLK), 0)
        key = lax.broadcasted_iota(jnp.int32, (BLK, BLK), 1)
        p_diag = jnp.where(key <= qry, jnp.exp(s[:, lo:hi] - lse), 0.0)
        ds_diag = (p_diag * (dp[:, lo:hi] - mean)).astype(BF16)
        dv_t[rows, lo:hi] = dot_nn(do_t[rows, lo:hi], p_diag.astype(BF16))
        dk_t[rows, lo:hi] = dot_nn(q_t[rows, lo:hi], ds_diag)
        dq_h = dot_nn(ds_diag, qkv_ref[lo:hi, width:2 * width])
        if i:
            p_left = jnp.exp(s[:, 0:lo] - lse)
            ds_left = (p_left * (dp[:, 0:lo] - mean)).astype(BF16)
            dv_t[rows, 0:lo] += dot_nn(do_t[rows, lo:hi], p_left.astype(BF16))
            dk_t[rows, 0:lo] += dot_nn(q_t[rows, lo:hi], ds_left)
            dq_h = dq_h + dot_nn(ds_left, qkv_ref[0:lo, width:2 * width])
        dq.append(dq_h)
        if head == 1:
            lane = lax.broadcasted_iota(jnp.int32, (BLK, width), 1)
            dqkv_ref[lo:hi, 0:width] = (jnp.where(lane < half, dq[0], dq[1]) * scale).astype(BF16)
            dq = []
    dqkv_ref[:, width:2 * width] = dk_t[...].T.astype(BF16)
    dqkv_ref[:, 2 * width:3 * width] = dv_t[...].T.astype(BF16)


def attn_bwd(qkv, ctx, dctx, lse, n_seq, seq, n_pair):
    width = 128
    return pl.pallas_call(
        attn_bwd_kernel,
        grid=(n_seq, n_pair),
        in_specs=[pl.BlockSpec((seq, 3 * width), lambda b, p: (b, p)),
                  pl.BlockSpec((seq, width), lambda b, p: (b, p)),
                  pl.BlockSpec((seq, width), lambda b, p: (b, p)),
                  pl.BlockSpec((None, None, 2, seq), lambda b, p: (b, p, 0, 0))],
        out_specs=pl.BlockSpec((seq, 3 * width), lambda b, p: (b, p)),
        out_shape=jax.ShapeDtypeStruct((n_seq * seq, n_pair * 3 * width), BF16),
        scratch_shapes=[pltpu.VMEM((width, seq), F32), pltpu.VMEM((width, seq), F32)],
        name="attn_bwd",
        cost_estimate=pl.CostEstimate(flops=n_seq * n_pair * 20 * seq * seq * 256 * 10 // 16, bytes_accessed=n_seq * seq * n_pair * width * 16,
                                      transcendentals=n_seq * n_pair * seq * seq),
        compiler_params=pltpu.CompilerParams(vmem_limit_bytes=48 * 1024 * 1024),
    )(qkv, ctx, dctx, lse)


LN_EPS = 1e-5
GELU_S = 0.7978845608028654
GELU_A = 0.044715


def row_mean(v):
    return jnp.sum(v, axis=1, keepdims=True) * (1.0 / v.shape[1])


def row_stats(v):
    centered = v - row_mean(v)
    inv_std = lax.rsqrt(row_mean(centered * centered) + LN_EPS)
    return centered * inv_std, inv_std


def norm_back(d_y, x_in, gain):
    normed, inv_std = row_stats(x_in)
    d_norm = d_y * gain
    d_x = inv_std * (d_norm - row_mean(d_norm) - normed * row_mean(d_norm * normed))
    return d_x, d_y * normed


def col_sum(v):
    return jnp.sum(v, axis=0, keepdims=True)


def to_image(rows, image, base):
    tiles = rows.shape[1] // 128
    for h in range(rows.shape[0] // 8):
        for c in range(tiles):
            image[pl.ds(base + (h * tiles + c) * 8, 8), :] = rows[h * 8:(h + 1) * 8, c * 128:(c + 1) * 128]


def from_image(image, base, n_rows, width):
    tiles = width // 128
    return jnp.concatenate([jnp.concatenate([image[pl.ds(base + (h * tiles + c) * 8, 8), :] for c in range(tiles)], axis=1)
                            for h in range(n_rows // 8)], axis=0)


def pick_rows(code_ref, first, stage, image, n_rows, tiles):
    def pick(g, _):
        base = pl.multiple_of(g * 16 * tiles, 16 * tiles)
        for j in range(16):
            row = stage[pl.ds(code_ref[first + g * 16 + j], tiles, stride=8), :]
            image[pl.ds(base + (j // 8) * 8 * tiles + j % 8, tiles, stride=8), :] = row
        return 0

    lax.fori_loop(0, n_rows // 16, pick, 0)


def embed_kernel(n_blk, cap, code_ref, *refs):
    tok_refs = refs[:n_blk]
    pos_ref, gain_ref, bias_ref, x_ref, hid_ref, stage, image = refs[n_blk:]
    rows, width = x_ref.shape
    tiles = width // 128

    @pl.when(pl.program_id(0) == 0)
    def _():
        for b in range(n_blk):
            def widen(g, _, b=b):
                part = tok_refs[b][pl.ds(pl.multiple_of(g * WIDEN, WIDEN), WIDEN), :].astype(F32)
                to_image(part, stage, pl.multiple_of((b * cap + g * WIDEN) * tiles, WIDEN * tiles))
                return 0

            lax.fori_loop(0, cap // WIDEN, widen, 0)

    pick_rows(code_ref, pl.program_id(0) * rows, stage, image, rows, tiles)
    part = 64
    for i in range(rows // part):
        at = slice(i * part, (i + 1) * part)
        x = from_image(image, i * part * tiles, part, width) + pos_ref[at, :].astype(F32)
        x_ref[at, :] = x
        normed, _ = row_stats(x)
        hid_ref[at, :] = (normed * gain_ref[...] + bias_ref[...]).astype(BF16)


def embed(code, blocks, pos_rows, gain, bias, n_tok):
    cap, width = blocks[0].shape
    seq = pos_rows.shape[0]
    rows = 256
    per_seq = seq // rows
    n_blk = len(blocks)
    vec = pl.BlockSpec((1, width), lambda i: (0, 0))
    return pl.pallas_call(
        functools.partial(embed_kernel, n_blk, cap),
        grid=(n_tok // rows,),
        in_specs=[pl.BlockSpec(memory_space=pltpu.SMEM)]
        + [pl.BlockSpec((cap, width), lambda i: (0, 0), pipeline_mode=pl.Buffered(1))] * n_blk
        + [pl.BlockSpec((rows, width), lambda i: (i % per_seq, 0)), vec, vec],
        out_specs=[pl.BlockSpec((rows, width), lambda i: (i, 0))] * 2,
        out_shape=[jax.ShapeDtypeStruct((n_tok, width), F32), jax.ShapeDtypeStruct((n_tok, width), BF16)],
        scratch_shapes=[pltpu.VMEM((n_blk * cap * width // 128, 128), F32), pltpu.VMEM((rows * width // 128, 128), F32)],
        name="embed_norm",
        cost_estimate=pl.CostEstimate(flops=15_000_000_000, bytes_accessed=n_tok * width * 10, transcendentals=0),
        compiler_params=pltpu.CompilerParams(vmem_limit_bytes=48 * MIB),
    )(code, *blocks, pos_rows, gain, bias)


def pack_kernel(n_blk, code_ref, tok_ref, *refs):
    out_refs = refs[:n_blk]
    stage, image = refs[n_blk:]
    n_tok, width = tok_ref.shape
    cap = out_refs[0].shape[0]
    tiles = width // 128

    def widen(g, _):
        part = tok_ref[pl.ds(pl.multiple_of(g * WIDEN, WIDEN), WIDEN), :].astype(F32)
        to_image(part, stage, pl.multiple_of(g * WIDEN * tiles, WIDEN * tiles))
        return 0

    lax.fori_loop(0, n_tok // WIDEN, widen, 0)
    for b in range(n_blk):
        pick_rows(code_ref, b * cap, stage, image, cap, tiles)

        def narrow(g, _, b=b):
            part = from_image(image, pl.multiple_of(g * WIDEN * tiles, WIDEN * tiles), WIDEN, width)
            out_refs[b][pl.ds(pl.multiple_of(g * WIDEN, WIDEN), WIDEN), :] = part.astype(BF16)
            return 0

        lax.fori_loop(0, cap // WIDEN, narrow, 0)


def pack(code, tok, cap):
    n_tok, width = tok.shape
    n_blk = code.shape[0] // cap
    return pl.pallas_call(
        functools.partial(pack_kernel, n_blk),
        in_specs=[pl.BlockSpec(memory_space=pltpu.SMEM), pl.BlockSpec(memory_space=pltpu.VMEM)],
        out_specs=[pl.BlockSpec(memory_space=pltpu.VMEM)] * n_blk,
        out_shape=[jax.ShapeDtypeStruct((cap, width), BF16)] * n_blk,
        scratch_shapes=[pltpu.VMEM((n_tok * width // 128, 128), F32), pltpu.VMEM((cap * width // 128, 128), F32)],
        name="token_pack",
        cost_estimate=pl.CostEstimate(flops=15_000_000_000, bytes_accessed=n_tok * width * 5, transcendentals=0),
        compiler_params=pltpu.CompilerParams(vmem_limit_bytes=40 * MIB),
    )(code, tok)


def proj_kernel(c_ref, w_ref, x_ref, b_ref, gain_ref, bias_ref, x1_ref, hid_ref):
    part = x_ref.shape[0] // 2
    for i in range(2):
        at = slice(i * part, (i + 1) * part)
        x1 = x_ref[at, :] + dot_nn(c_ref[at, :], w_ref[...].reshape(c_ref.shape[1], -1)).astype(BF16).astype(F32) + b_ref[...]
        x1_ref[at, :] = x1
        normed, _ = row_stats(x1)
        hid_ref[at, :] = (normed * gain_ref[...] + bias_ref[...]).astype(BF16)


def proj_norm(ctx, w, start, x, b, gain, bias):
    n_tok, width = x.shape
    n_row = ctx.shape[1] // w.shape[0]
    rows = 512
    vec = pl.BlockSpec((1, width), lambda i: (0, 0))
    mat = pl.BlockSpec((rows, width), lambda i: (i, 0))
    return pl.pallas_call(
        proj_kernel,
        grid=(n_tok // rows,),
        in_specs=[pl.BlockSpec((rows, ctx.shape[1]), lambda i: (i, 0)), pl.BlockSpec((w.shape[0], n_row, width), lambda i: (0, start // n_row, 0)), mat, vec, vec, vec],
        out_specs=[mat, mat],
        out_shape=[jax.ShapeDtypeStruct((n_tok, width), F32), jax.ShapeDtypeStruct((n_tok, width), BF16)],
        name="proj_norm",
        cost_estimate=pl.CostEstimate(flops=2 * n_tok * ctx.shape[1] * width, bytes_accessed=n_tok * width * 12, transcendentals=0),
        compiler_params=pltpu.CompilerParams(vmem_limit_bytes=40 * MIB),
    )(ctx, w, x, b, gain, bias)


def ffn_kernel(part, h_ref, og_ref, wu_ref, wd_ref, b_ref, act_ref, dup_ref, db_ref):
    total = jnp.zeros(db_ref.shape, F32)
    for i in range(h_ref.shape[0] // part):
        at = slice(i * part, (i + 1) * part)
        z = dot_nt(h_ref[at, :], wu_ref[0]) + b_ref[...]
        d_act = dot_nt(og_ref[at, :], wd_ref[0])
        z2 = z * z
        gate = 0.5 * jnp.tanh(z * (GELU_S + (GELU_S * GELU_A) * z2)) + 0.5
        act = z * gate
        d_up = d_act * (gate + act * (1.0 - gate) * (2.0 * GELU_S + (6.0 * GELU_S * GELU_A) * z2))
        act_ref[at, :] = act.astype(BF16)
        dup_ref[at, :] = d_up.astype(BF16)
        total = total + col_sum(d_up)
    db_ref[...] = total


def ffn(hid, og, w, b_up, part=1024):
    n_tok, width = hid.shape
    ff = b_up.shape[1]
    n_piece = w.shape[0]
    bn = ff // n_piece
    whole = pl.BlockSpec((n_tok, width), lambda i: (0, 0), pipeline_mode=pl.Buffered(1))
    ospec = pl.BlockSpec((n_tok, bn), lambda i: (0, i))
    vec = pl.BlockSpec((1, bn), lambda i: (0, i))
    return pl.pallas_call(
        functools.partial(ffn_kernel, part),
        grid=(n_piece,),
        in_specs=[whole, whole, pl.BlockSpec((1, bn, width), lambda i: (i, 0, 0)), pl.BlockSpec((1, bn, width), lambda i: (i, 1, 0)), vec],
        out_specs=[ospec, ospec, vec],
        out_shape=[jax.ShapeDtypeStruct((n_tok, ff), BF16), jax.ShapeDtypeStruct((n_tok, ff), BF16), jax.ShapeDtypeStruct((1, ff), F32)],
        name="ffn",
        cost_estimate=pl.CostEstimate(flops=4 * n_tok * ff * width, bytes_accessed=4 * n_tok * ff + 4 * ff * width, transcendentals=n_tok * ff),
        compiler_params=pltpu.CompilerParams(vmem_limit_bytes=48 * MIB),
    )(hid, og, w, w, b_up)


def back2_kernel(dup_ref, w_ref, x1_ref, og_ref, gain_ref, dr_ref, da_ref, sums_ref):
    @pl.when(pl.program_id(0) == 0)
    def _():
        sums_ref[...] = jnp.zeros(sums_ref.shape, F32)

    n_part = 2
    part = dr_ref.shape[0] // n_part
    w = w_ref[...].reshape(dup_ref.shape[1], -1)
    d_ys = [dot_nn(dup_ref[i * part:(i + 1) * part, :], w) for i in range(n_part)]
    for i in range(n_part):
        at = slice(i * part, (i + 1) * part)
        d_y = d_ys[i].astype(BF16).astype(F32)
        d_x, d_gain = norm_back(d_y, x1_ref[at, :], gain_ref[...])
        og = og_ref[at, :].astype(F32)
        d_resid = og + d_x
        dr_ref[at, :] = d_resid
        da_ref[at, :] = d_resid.astype(BF16)
        sums_ref[0:1, :] += col_sum(d_gain)
        sums_ref[1:2, :] += col_sum(d_y)
        sums_ref[2:3, :] += col_sum(d_resid)
        sums_ref[3:4, :] += col_sum(og)


def back2(d_up, w, x1, og, gain):
    n_tok, width = x1.shape
    ff = d_up.shape[1]
    rows = 256
    mat = pl.BlockSpec((rows, width), lambda i: (i, 0))
    return pl.pallas_call(
        back2_kernel,
        grid=(n_tok // rows,),
        in_specs=[pl.BlockSpec((rows, ff), lambda i: (i, 0)), pl.BlockSpec((w.shape[0], ff // w.shape[0], width), lambda i: (0, 0, 0), pipeline_mode=pl.Buffered(1)),
                  mat, mat, pl.BlockSpec((1, width), lambda i: (0, 0))],
        out_specs=[mat, mat, pl.BlockSpec((8, width), lambda i: (0, 0))],
        out_shape=[jax.ShapeDtypeStruct((n_tok, width), F32), jax.ShapeDtypeStruct((n_tok, width), BF16), jax.ShapeDtypeStruct((8, width), F32)],
        name="ffn_back",
        cost_estimate=pl.CostEstimate(flops=2 * n_tok * ff * width, bytes_accessed=2 * n_tok * ff + n_tok * width * 12, transcendentals=0),
        compiler_params=pltpu.CompilerParams(vmem_limit_bytes=48 * MIB),
    )(d_up, w, x1, og, gain)


def back1_kernel(dq_ref, w_ref, x_ref, dr_ref, gain_ref, tok_ref, pos_ref, sums_ref, bsum_ref):
    @pl.when((pl.program_id(0) == 0) & (pl.program_id(1) == 0))
    def _():
        sums_ref[...] = jnp.zeros(sums_ref.shape, F32)
        bsum_ref[...] = jnp.zeros(bsum_ref.shape, F32)

    @pl.when(pl.program_id(1) == 0)
    def _():
        pos_ref[...] = jnp.zeros(pos_ref.shape, F32)

    n_part = 2
    part = tok_ref.shape[0] // n_part
    d_ys = [dot_nn(dq_ref[i * part:(i + 1) * part, :], w_ref[...]) for i in range(n_part)]
    for i in range(n_part):
        at = slice(i * part, (i + 1) * part)
        d_y = d_ys[i].astype(BF16).astype(F32)
        d_x, d_gain = norm_back(d_y, x_ref[at, :], gain_ref[...])
        d_resid = dr_ref[at, :] + d_x
        tok_ref[at, :] = d_resid.astype(BF16)
        pos_ref[at, :] += d_resid
        sums_ref[0:1, :] += col_sum(d_gain)
        sums_ref[1:2, :] += col_sum(d_y)
        bsum_ref[0:1, :] += col_sum(dq_ref[at, :].astype(F32))


def back1(d_qkv, w_qkv, x, d_resid1, gain, n_seq, pos_rows):
    n_tok, width = x.shape
    n_cols = d_qkv.shape[1]
    rows = 256
    per_seq = n_tok // n_seq // rows
    mat = pl.BlockSpec((rows, width), lambda i, b: (b * per_seq + i, 0))
    return pl.pallas_call(
        back1_kernel,
        grid=(per_seq, n_seq),
        in_specs=[pl.BlockSpec((rows, n_cols), lambda i, b: (b * per_seq + i, 0)),
                  pl.BlockSpec((n_cols, width), lambda i, b: (0, 0), pipeline_mode=pl.Buffered(1)),
                  mat, mat, pl.BlockSpec((1, width), lambda i, b: (0, 0))],
        out_specs=[mat, pl.BlockSpec((rows, width), lambda i, b: (i, 0)), pl.BlockSpec((8, width), lambda i, b: (0, 0)),
                   pl.BlockSpec((8, n_cols), lambda i, b: (0, 0))],
        out_shape=[jax.ShapeDtypeStruct((n_tok, width), BF16), jax.ShapeDtypeStruct((pos_rows, width), F32),
                   jax.ShapeDtypeStruct((8, width), F32), jax.ShapeDtypeStruct((8, n_cols), F32)],
        name="qkv_back",
        cost_estimate=pl.CostEstimate(flops=2 * n_tok * n_cols * width, bytes_accessed=2 * n_tok * n_cols + n_tok * width * 12, transcendentals=0),
        compiler_params=pltpu.CompilerParams(vmem_limit_bytes=48 * MIB),
    )(d_qkv, w_qkv, x, d_resid1, gain)


def assemble_kernel(n, me_ref, *refs):
    out_ref = refs[n]
    k = me_ref[0] ^ pl.program_id(0)
    for j in range(n):
        @pl.when(k == j)
        def _(j=j):
            out_ref[...] = refs[j][...].reshape(out_ref.shape)


def assemble(me, parts, out_shape, block):
    at = 1 if len(out_shape) == 4 else 0
    return pl.pallas_call(
        functools.partial(assemble_kernel, len(parts)),
        grid_spec=pltpu.PrefetchScalarGridSpec(
            num_scalar_prefetch=1, grid=(len(parts),),
            in_specs=[pl.BlockSpec(p.shape, lambda i, m: (0, 0, 0), pipeline_mode=pl.Buffered(1)) for p in parts],
            out_specs=pl.BlockSpec(block, lambda i, m: tuple(i if d == at else 0 for d in range(len(block))))),
        out_shape=jax.ShapeDtypeStruct(out_shape, parts[0].dtype),
        name="assemble",
        cost_estimate=pl.CostEstimate(flops=4_000_000_000, bytes_accessed=16 * MIB, transcendentals=0),
        compiler_params=pltpu.CompilerParams(vmem_limit_bytes=24 * MIB),
    )(me, *parts)


LANES = 128


def accum_kernel(n_block, cap, sub_rows, width, where_ref, first_ref, *refs):
    tok_refs = refs[:n_block]
    out_ref = refs[n_block]
    n_sub = len(sub_rows)
    acc = refs[n_block + 1:n_block + 1 + n_sub]
    buf, stage, in_sem, out_sem = refs[n_block + 1 + n_sub:]
    tiles = width // LANES
    group = 8 * tiles

    def fetch(block):
        return pltpu.make_async_copy(tok_refs[block], buf.at[block % 2], in_sem.at[block % 2])

    fetch(0).start()
    for s in range(n_sub):
        def clear(i, _, s=s):
            acc[s][pl.ds(pl.multiple_of(i * group, group), group), :] = jnp.zeros((group, LANES), F32)
            return 0

        lax.fori_loop(0, sub_rows[s] // 8, clear, 0)

    def add_rows(s, slot, n):
        codes = [where_ref[slot + j] for j in range(n)]
        at = [code >> 16 for code in codes]
        rows = [stage[pl.ds(code & 0xffff, tiles, stride=8), :] for code in codes]
        sums = [acc[s][pl.ds(a, tiles, stride=8), :] for a in at]
        for j in range(n):
            for i in range(j):
                sums[j] = jnp.where(at[i] == at[j], sums[i], sums[j])
            sums[j] = sums[j] + rows[j]
        for j in range(n):
            acc[s][pl.ds(at[j], tiles, stride=8), :] = sums[j]

    for block in range(n_block):
        if block + 1 < n_block:
            fetch(block + 1).start()
        fetch(block).wait()

        def widen(g, _, block=block):
            rows = buf[block % 2, pl.ds(pl.multiple_of(g * WIDEN, WIDEN), WIDEN), :].astype(F32)
            base = pl.multiple_of(g * (WIDEN // 8) * group, (WIDEN // 8) * group)
            for h in range(WIDEN // 8):
                for c in range(tiles):
                    stage[pl.ds(base + h * group + c * 8, 8), :] = rows[h * 8:(h + 1) * 8, c * LANES:(c + 1) * LANES]
            return 0

        lax.fori_loop(0, cap // WIDEN, widen, 0)

        starts = [first_ref[block * (n_sub + 1) + s] for s in range(n_sub + 1)]
        counts = [starts[s + 1] - starts[s] for s in range(n_sub)]
        both = functools.reduce(jnp.minimum, counts) // 2
        begin = [block * cap + starts[s] for s in range(n_sub)]

        def together(i, _, begin=begin):
            for s in range(n_sub):
                add_rows(s, begin[s] + 2 * i, 2)
            return 0

        lax.fori_loop(0, both, together, 0)
        for s in range(n_sub):
            fours = (counts[s] - 2 * both) // 4

            def alone(i, _, s=s, begin=begin, both=both):
                add_rows(s, begin[s] + 2 * both + 4 * i, 4)
                return 0

            lax.fori_loop(0, fours, alone, 0)

            def single(i, _, s=s, begin=begin):
                add_rows(s, begin[s] + i, 1)
                return 0

            lax.fori_loop(2 * both + 4 * fours, counts[s], single, 0)
    done = 0
    copies = []
    for s in range(n_sub):
        n = sub_rows[s] * tiles
        copies.append(pltpu.make_async_copy(acc[s], out_ref.at[pl.ds(done, n), :], out_sem.at[s]))
        copies[-1].start()
        done += n
    for c in copies:
        c.wait()


def accum(tok_blocks, code, first, sub_rows, width):
    n_block = len(tok_blocks)
    cap = tok_blocks[0].shape[0]
    n_sub = len(sub_rows)
    tiles = width // LANES
    return pl.pallas_call(
        functools.partial(accum_kernel, n_block, cap, sub_rows, width),
        in_specs=[pl.BlockSpec(memory_space=pltpu.SMEM), pl.BlockSpec(memory_space=pltpu.SMEM)]
        + [pl.BlockSpec(memory_space=pl.ANY)] * n_block,
        out_specs=pl.BlockSpec(memory_space=pl.ANY),
        out_shape=jax.ShapeDtypeStruct((sum(sub_rows) * tiles, LANES), F32),
        scratch_shapes=[pltpu.VMEM((r * tiles, LANES), F32) for r in sub_rows]
        + [pltpu.VMEM((2, cap, width), BF16), pltpu.VMEM((cap * tiles, LANES), F32),
           pltpu.SemaphoreType.DMA((2,)), pltpu.SemaphoreType.DMA((n_sub,))],
        name="table_accum",
        cost_estimate=pl.CostEstimate(flops=50_000_000_000, bytes_accessed=100_000_000, transcendentals=0),
        compiler_params=pltpu.CompilerParams(vmem_limit_bytes=63 * 1024 * 1024),
    )(code, first, *tok_blocks)


def dot_tn(a, b):
    return lax.dot_general(a, b, (((0,), (0,)), ((), ())), preferred_element_type=F32)


def grad_kernel(has_plus, core_ref, a_ref, b_ref, *refs):
    out_ref = refs[-1]
    n = a_ref.shape[1]
    g = dot_tn(a_ref[...], b_ref[...])
    out_ref[0:n, :] = g + refs[0][0:n, :] if has_plus else g
    if out_ref.shape[0] > n:
        out_ref[n:, :] = jnp.zeros((out_ref.shape[0] - n, out_ref.shape[1]), F32)


def grad_pieces(core, a, b, n_tp, piece, which, n_which, plus=None, into=None):
    n_tok, n_cols = a.shape
    width = b.shape[1]
    bn = n_cols // (4 * n_tp)
    out_spec = pl.BlockSpec((piece, width), lambda p, c: (n_which * p + which, 0))
    in_specs = [pl.BlockSpec((n_tok, bn), lambda p, c: (0, 4 * (p // 2) + 2 * c[0] + p % 2)),
                pl.BlockSpec((n_tok, width), lambda p, c: (0, 0), pipeline_mode=pl.Buffered(1))]
    args = [a, b]
    if plus is not None:
        in_specs.append(pl.BlockSpec((piece, width), lambda p, c: (p, 0)))
        args.append(plus)
    if into is not None:
        in_specs.append(pl.BlockSpec(memory_space=pl.ANY))
        args.append(into)
    return pl.pallas_call(
        functools.partial(grad_kernel, plus is not None),
        grid_spec=pltpu.PrefetchScalarGridSpec(num_scalar_prefetch=1, grid=(2 * n_tp,), in_specs=in_specs, out_specs=out_spec),
        out_shape=jax.ShapeDtypeStruct((2 * n_tp * n_which * piece, width), F32),
        input_output_aliases={} if into is None else {len(args): 0},
        name="weight_grad",
        cost_estimate=pl.CostEstimate(flops=n_tok * n_cols * width, bytes_accessed=n_tok * (n_cols + 2 * width) + 2 * n_cols * width,
                                      transcendentals=0),
        compiler_params=pltpu.CompilerParams(vmem_limit_bytes=32 * MIB),
    )(core, *args)


def grad_rest_kernel(spans, last, core_ref, a1_ref, b1_ref, a2_ref, b2_ref, *refs):
    out_ref = refs[-1]
    plus = refs[0] if len(refs) > 1 else None
    piece, piece_in = out_ref.shape[0] // 2, (refs[0].shape[0] // 2 if plus is not None else 0)
    for (a_ref, b_ref), (start, stop) in zip(((a1_ref, b1_ref), (a2_ref, b2_ref)), spans):
        half = a_ref.shape[1] // 2
        for i in range(0, 2 * half, 128):
            g = dot_tn(a_ref[:, i:i + 128], b_ref[...])
            for x in range(2):
                lo, hi = max(i, x * half), min(i + 128, (x + 1) * half)
                if lo < hi:
                    to = lo - x * half + start
                    part = g[lo - i:hi - i]
                    if plus is not None:
                        part = part + plus[x * piece_in + to:x * piece_in + to + hi - lo, :]
                    out_ref[x * piece + to:x * piece + to + hi - lo, :] = part
        for x in range(2):
            if stop > start + half:
                out_ref[x * piece + start + half:x * piece + stop, :] = jnp.zeros((stop - start - half, out_ref.shape[1]), F32)
    if last:
        for x in range(2):
            out_ref[x * piece + spans[-1][1]:(x + 1) * piece, :] = refs[1][x, 0] + refs[2][x * last:(x + 1) * last, :]


def grad_rest(core, a1, b1, a2, b2, n_tp, spans, plus=None, tail=None):
    n_tok, width = b1.shape
    last = tail[0].shape[2] if tail else 0
    piece = spans[-1][1] + last
    whole = pl.BlockSpec((n_tok, width), lambda t, c: (0, 0), pipeline_mode=pl.Buffered(1))
    in_specs, args = [], []
    for a, b in ((a1, b1), (a2, b2)):
        in_specs += [pl.BlockSpec((n_tok, a.shape[1] // (2 * n_tp)), lambda t, c: (0, 2 * t + c[0])), whole]
        args += [a, b]
    if plus is not None:
        in_specs.append(pl.BlockSpec((plus.shape[0] // n_tp, width), lambda t, c: (t, 0)))
        args.append(plus)
    if tail:
        in_specs.append(pl.BlockSpec((2, 1, last, width), lambda t, c: (t, c[0], 0, 0)))
        in_specs.append(pl.BlockSpec((2 * last, width), lambda t, c: (t, 0)))
        args += tail
    n_cols = a1.shape[1] + a2.shape[1]
    return pl.pallas_call(
        functools.partial(grad_rest_kernel, spans, last),
        grid_spec=pltpu.PrefetchScalarGridSpec(num_scalar_prefetch=1, grid=(n_tp,), in_specs=in_specs,
                                               out_specs=pl.BlockSpec((2 * piece, width), lambda t, c: (t, 0))),
        out_shape=jax.ShapeDtypeStruct((2 * n_tp * piece, width), F32),
        name="weight_grads",
        cost_estimate=pl.CostEstimate(flops=n_tok * n_cols * width, bytes_accessed=n_tok * (n_cols + 4 * width) + 2 * n_cols * width,
                                      transcendentals=0),
        compiler_params=pltpu.CompilerParams(vmem_limit_bytes=40 * MIB),
    )(core, *args)


POS_OFFSET = 2
SLOTS = 704
LOW = 32


def before(n):
    return (lax.broadcasted_iota(jnp.int32, (n, n), 1) < lax.broadcasted_iota(jnp.int32, (n, n), 0)).astype(BF16)


def rank_in_class(hot):
    n_blk, n_tok, n_cls = hot.shape
    ones = hot.astype(BF16).reshape(n_blk, n_tok // 128, 128, n_cls)
    within = jnp.einsum("ij,bnjk->bnik", before(128), ones, preferred_element_type=F32)
    sums = jnp.sum(ones.astype(F32), axis=2)
    ahead = jnp.einsum("mn,bnk->bmk", before(n_tok // 128), sums.astype(BF16), preferred_element_type=F32)
    rank = jnp.sum((within + ahead[:, :, None, :]) * ones.astype(F32), axis=3)
    return rank.reshape(n_blk, n_tok).astype(jnp.int32), jnp.sum(sums, axis=1).astype(jnp.int32)


def compact(rank, valid, value):
    n_high = SLOTS // LOW
    high = ((rank // LOW)[:, :, None] == jnp.arange(n_high)) & valid[:, :, None]
    low = ((rank % LOW)[:, :, None] == jnp.arange(LOW)).astype(F32)
    parts = jnp.concatenate([low * (value // 128).astype(F32)[:, :, None], low * (value % 128).astype(F32)[:, :, None]], axis=2)
    out = jnp.einsum("bjh,bjl->bhl", high.astype(BF16), parts.astype(BF16), preferred_element_type=F32).astype(jnp.int32)
    return (out[:, :, :LOW] * 128 + out[:, :, LOW:]).reshape(rank.shape[0], SLOTS)


def solution(mesh):
    n_tp, n_dp = mesh.shape["tp"], mesh.shape["dp"]
    n_core = 2
    n_x = n_dp // n_core
    mesh3 = Mesh(mesh.devices.reshape(n_tp, n_x, n_core), ("tp", "xx", "cc"))
    dp = ("xx", "cc")
    tp_swap = [[(i, i ^ k) for i in range(n_tp)] for k in range(n_tp)]
    pair = [(0, 1), (1, 0)]

    def local_step(tok_ids, emb_table, pos_table, ln1_gain, ln1_bias, w_qkv, b_qkv, w_out, b_out,
                   ln2_gain, ln2_bias, w_up, b_up, w_down, b_down, out_grad):
        tp_index, x_index, c_index = lax.axis_index("tp"), lax.axis_index("xx"), lax.axis_index("cc")
        dp_index = x_index * n_core + c_index
        n_seq_dp, seq = tok_ids.shape
        n_seq = n_seq_dp // n_tp
        n_tok = n_seq * seq
        rows, width = emb_table.shape
        n_sub = 4
        sub = -(-rows // n_sub // 8) * 8
        sub_rows = (sub,) * (n_sub - 1) + (rows - (n_sub - 1) * sub,)
        seq_local = seq // n_tp
        ff = w_up.shape[1]
        gain1, bias1 = ln1_gain.astype(F32)[None], ln1_bias.astype(F32)[None]
        gain2, bias2 = ln2_gain.astype(F32)[None], ln2_bias.astype(F32)[None]

        def half(w, axis):
            n = w.shape[axis] // n_core
            return lax.dynamic_slice_in_dim(w, c_index * n, n, axis)

        def gather_rows(w):
            return lax.all_gather(w, ("tp", "cc"), axis=0, tiled=True)

        def swap(v, axis, k=1):
            return lax.ppermute(v, axis, tp_swap[k] if axis == "tp" else pair)

        def by_owner(parts):
            out = []
            for p in range(n_tp):
                k = tp_index ^ p
                out.append(jnp.where(k < 2, jnp.where(k == 0, parts[0], parts[1]), jnp.where(k == 2, parts[2], parts[3])))
            return out

        wqkv_t = gather_rows(jnp.transpose(half(w_qkv, 2), (1, 2, 3, 0)).reshape(-1, width))
        n_ff, n_out = ff // n_dp, w_out.shape[0] * w_out.shape[1] // n_dp

        def quarter(w, axis):
            n = w.shape[axis] // n_dp
            return lax.dynamic_slice_in_dim(w, dp_index * n, n, axis)

        w_all = lax.all_gather(jnp.concatenate([quarter(w_up, 1).T, quarter(w_down, 0), quarter(w_out.reshape(-1, width), 0)]),
                               ("tp", "xx", "cc"), axis=0, tiled=True).reshape(n_tp * n_dp, 2 * n_ff + n_out, width)
        wdown_w = w_all[:, n_ff:2 * n_ff].reshape(-1, width)
        wout_w = w_all[:, 2 * n_ff:].reshape(-1, width)
        n_pair = wqkv_t.shape[0] // (3 * 128)
        own_bias = jnp.concatenate([b_qkv.reshape(3, n_core, -1, b_qkv.shape[2]).transpose(1, 0, 2, 3).reshape(-1), b_up])
        biases = jnp.stack(by_owner([swap(own_bias, "tp", k) if k else own_bias for k in range(n_tp)]))
        bqkv_w = biases[:, :-ff].reshape(-1).astype(F32)
        bup_w = biases[:, -ff:].reshape(1, -1).astype(F32)
        pos_rows = lax.slice_in_dim(pos_table, POS_OFFSET, POS_OFFSET + seq, axis=0)

        ids_all = lax.all_gather(tok_ids, dp, axis=0, tiled=True).reshape(n_dp * n_tp, n_tok)
        local = ids_all - tp_index * rows
        sub_of = sum(((local >= s * sub).astype(jnp.int32) for s in range(1, n_sub)), jnp.zeros_like(local))
        owned = (local >= 0) & (local < rows)
        hot = owned[:, :, None] & (sub_of[:, :, None] == jnp.arange(n_sub))
        rank, counts = rank_in_class(hot)
        first = jnp.concatenate([jnp.zeros_like(counts[:, :1]), jnp.cumsum(counts, axis=1)], axis=1)
        rank = rank + jnp.sum(jnp.where(hot, first[:, None, :-1], 0), axis=2)
        most = jnp.stack([jnp.max(jnp.sum(((ids_all >= o * rows) & (ids_all < (o + 1) * rows)).astype(jnp.int32), axis=1))
                          for o in range(n_tp)])
        rounds = (jnp.max(most) + SLOTS - 1) // SLOTS

        def lists(r):
            at = rank - r * SLOTS
            return compact(at, owned & (at >= 0) & (at < SLOTS), jnp.where(owned, local, 0))

        own_ids = lax.dynamic_index_in_dim(ids_all, dp_index * n_tp + tp_index, 0, keepdims=True)
        own_owner = sum(((own_ids >= o * rows).astype(jnp.int32) for o in range(1, n_tp)), jnp.zeros_like(own_ids))
        own_local = own_ids - own_owner * rows
        own_sub = sum(((own_local >= s * sub).astype(jnp.int32) for s in range(1, n_sub)), jnp.zeros_like(own_ids))
        own_hot = (own_owner * n_sub + own_sub)[:, :, None] == jnp.arange(n_tp * n_sub)
        own_rank, own_counts = rank_in_class(own_hot)
        own_first = jnp.cumsum(own_counts.reshape(n_tp, n_sub), axis=1) - own_counts.reshape(n_tp, n_sub)
        own_rank = (own_rank + jnp.sum(jnp.where(own_hot, own_first.reshape(1, 1, -1), 0), axis=2))[0]
        own_owner = own_owner[0]

        def own_lists(r):
            at = jnp.broadcast_to(own_rank - r * SLOTS, (n_tp, n_tok))
            mine = own_owner == jnp.arange(n_tp)[:, None]
            return compact(at, mine & (at >= 0) & (at < SLOTS), jnp.broadcast_to(jnp.arange(n_tok), (n_tp, n_tok)))

        tiles = width // 128

        def rows_here(r, my_lists):
            index = [lax.dynamic_index_in_dim(my_lists, tp_index ^ k, 0, keepdims=False) for k in range(n_tp)]
            first_two = jnp.take(emb_table, jnp.concatenate([index[3], index[1]]), axis=0, mode="clip")
            rest, first_two = lax.optimization_barrier((jnp.concatenate([index[2], index[0]]), first_two))
            last_two = jnp.take(emb_table, rest, axis=0, mode="clip")
            sent = [last_two[SLOTS:], first_two[SLOTS:], last_two[:SLOTS], first_two[:SLOTS]]
            got = list(sent)
            for k in range(1, n_tp):
                got[k] = swap(sent[k], "tp", k)
            at = own_rank - r * SLOTS
            valid = (at >= 0) & (at < SLOTS)
            return got, jnp.where(valid, (own_owner ^ tp_index) * SLOTS + at, 0), valid

        def norm_rows(x):
            normed, _ = row_stats(x)
            return (normed * gain1 + bias1).astype(BF16)

        lists0 = lists(0)
        my_lists0 = lax.dynamic_slice_in_dim(lists0, dp_index * n_tp, n_tp, 0)
        got0, place0, _ = rows_here(0, my_lists0)
        code0 = (place0 // 8) * (8 * tiles) + place0 % 8
        got0, out_grad = lax.optimization_barrier((got0, out_grad))
        resid_x, hid1 = embed(code0, got0, pos_rows, gain1, bias1, n_tok)

        def more_rows(carry):
            r, x, _ = carry
            got, place, valid = rows_here(r, lax.dynamic_slice_in_dim(lists(r), dp_index * n_tp, n_tp, 0))
            new = jnp.take(jnp.concatenate(got), place, axis=0, mode="clip").astype(F32) + jnp.tile(pos_rows.astype(F32), (n_seq, 1))
            x = jnp.where(valid[:, None], new, x)
            return r + 1, x, norm_rows(x)

        _, resid_x, hid1 = lax.while_loop(lambda c: c[0] < rounds, more_rows, (jnp.int32(1), resid_x, hid1))

        og_parts = out_grad.reshape(n_tp, n_seq, seq_local, width)
        parts = [lax.dynamic_index_in_dim(og_parts, tp_index ^ k, 0, keepdims=False) for k in range(n_tp)]
        parts = [swap(part, "tp", k) if k else part for k, part in enumerate(parts)]
        me = jnp.reshape(tp_index, (1,))
        og = assemble(me, parts, (n_seq, n_tp, seq_local, width), (n_seq, 1, seq_local, width)).reshape(n_tok, width)

        qkv = (dot_nt(hid1, wqkv_t) + bqkv_w).astype(BF16)
        ctx, lse = attn_fwd(qkv, n_seq, seq, n_pair)
        resid_x1, hid2 = proj_norm(ctx, w_all, 2 * n_ff, resid_x, b_out.astype(F32)[None], gain2, bias2)
        act, d_up, d_b_up = ffn(hid2, og, w_all, bup_w)
        out = (resid_x1 + dot_nn(act, wdown_w).astype(BF16).astype(F32) + b_down.astype(F32)).astype(BF16)

        out4 = out.reshape(n_seq, seq, width)
        parts = [lax.dynamic_slice_in_dim(out4, (tp_index ^ k) * seq_local, seq_local, 1) for k in range(n_tp)]
        parts = [swap(part, "tp", k) if k else part for k, part in enumerate(parts)]
        layer_out = assemble(me, parts, (n_seq_dp, seq_local, width), (n_seq, seq_local, width))

        core = jnp.reshape(c_index, (1,))

        def piece_of(n_rows):
            return -(-n_rows // (4 * n_tp) // 24) * 24

        def pick_pieces(g, start, n_rows):
            n = n_rows // (n_x * n_core)
            g = g.reshape(n_x, n_core, -1, width)[:, :, start:start + n]
            return g.transpose(1, 0, 2, 3).reshape(n_rows, width)

        p_ff = piece_of(n_tp * ff)
        down_theirs = swap(grad_pieces(1 - core, act, og, n_tp, p_ff, 0, 1), "cc")
        up_theirs = swap(grad_pieces(1 - core, d_up, hid2, n_tp, p_ff, 0, 1), "cc")
        ff_grads = grad_pieces(core, act, og, n_tp, p_ff, 0, 2, plus=down_theirs)
        ff_grads = grad_pieces(core, d_up, hid2, n_tp, p_ff, 1, 2, plus=up_theirs, into=ff_grads)
        ff_grads = lax.psum_scatter(ff_grads, ("tp", "xx"), scatter_dimension=0, tiled=True)
        ff_grads = lax.all_gather(ff_grads, dp, axis=0, tiled=True)

        d_resid1, d_attn, sums2 = back2(d_up, w_all, resid_x1, og, gain2)
        d_ctx = dot_nt(d_attn, wout_w).astype(BF16)
        d_qkv = attn_bwd(qkv, ctx, d_ctx, lse, n_seq, seq, n_pair)
        p_out = piece_of(wout_w.shape[0])
        spans = ((0, p_out), (p_out, p_out + piece_of(wqkv_t.shape[0])))
        n_small = n_tp * (b_qkv.size + ff) // width + 6
        p_pos = -(-(seq + n_small) // (24 * n_tp * n_dp)) * 24
        rest_theirs = swap(grad_rest(1 - core, ctx, d_attn, d_qkv, hid1, n_tp, spans), "cc")
        d_tok, pos_all, sums1, sums_qkv = back1(d_qkv, wqkv_t, resid_x, d_resid1, gain1, n_seq, p_pos * n_tp * n_dp)

        def token_blocks(r):
            own = own_lists(r)
            place = jnp.concatenate([lax.dynamic_index_in_dim(own, tp_index ^ k, 0, keepdims=False) for k in range(n_tp)])
            parts = pack((place // 8) * (8 * tiles) + place % 8, d_tok, SLOTS)
            blocks = [swap(part, "tp", k) if k else part for k, part in enumerate(parts)]
            other = []
            for b in blocks:
                other.append(swap(b, "xx"))
            return blocks + other + [swap(b, "cc") for b in blocks + other]

        def in_block_order(table):
            out = []
            for dc in range(n_core):
                for dx in range(n_x):
                    for k in range(n_tp):
                        d = (x_index ^ dx) * n_core + (c_index ^ dc)
                        out.append(lax.dynamic_index_in_dim(table, d * n_tp + (tp_index ^ k), 0, keepdims=False))
            return jnp.stack(out)

        block_rows = in_block_order(lists0)
        in_sub = sum(((block_rows >= s * sub).astype(jnp.int32) for s in range(1, n_sub)), jnp.zeros_like(block_rows))
        in_sub = block_rows - in_sub * sub
        slot = jnp.arange(SLOTS)
        code = (((in_sub // 8) * (8 * tiles) + in_sub % 8) << 16) | ((slot // 8) * (8 * tiles) + slot % 8)
        block_first = jnp.minimum(in_block_order(first), SLOTS)
        d_w_down = pick_pieces(ff_grads, 0, ff)
        d_w_up = pick_pieces(ff_grads, p_ff, ff).T
        blocks0, d_w_down, d_w_up = lax.optimization_barrier((token_blocks(0), d_w_down, d_w_up))
        image = accum(blocks0, code.reshape(-1), block_first.reshape(-1), sub_rows, width)
        d_emb = image.reshape(rows // 8, tiles, 8, 128).transpose(0, 2, 1, 3).reshape(rows, width)

        def more_grads(carry):
            r, table = carry
            at = rank - r * SLOTS
            there = owned & (at >= 0) & (at < SLOTS)
            dest = compact(at, there, jnp.where(owned, local, 0) + 1)
            dest = jnp.where(dest == 0, rows, dest - 1)
            grads = jnp.concatenate(token_blocks(r), axis=0).astype(F32)
            return r + 1, table.at[in_block_order(dest).reshape(-1)].add(grads, mode="drop")

        _, d_emb = lax.while_loop(lambda c: c[0] < rounds, more_grads, (jnp.int32(1), d_emb))

        small = jnp.concatenate([sums_qkv[0], d_b_up[0], sums1[:2].reshape(-1), sums2[:4].reshape(-1)]).reshape(-1, width)
        small = jnp.concatenate([small, jnp.zeros((pos_all.shape[0] - seq - n_small, width), F32)])
        pos_all = lax.dynamic_update_slice_in_dim(pos_all, small, seq, 0).reshape(n_tp * n_x, n_core, p_pos, width)
        pos_theirs = swap(lax.dynamic_index_in_dim(pos_all, 1 - c_index, 1, keepdims=False).reshape(-1, width), "cc")
        rest = grad_rest(core, ctx, d_attn, d_qkv, hid1, n_tp, spans, plus=rest_theirs, tail=(pos_all, pos_theirs))
        rest = lax.psum_scatter(rest, ("tp", "xx"), scatter_dimension=0, tiled=True)
        rest_w = lax.all_gather(rest[:spans[1][1]], dp, axis=0, tiled=True)
        whole = lax.all_gather(rest[spans[1][1]:], ("tp", "xx", "cc"), axis=0, tiled=True)
        d_pos = jnp.pad(whole[:seq], ((POS_OFFSET, pos_table.shape[0] - seq - POS_OFFSET), (0, 0)))
        small = whole[seq:seq + n_small].reshape(-1)
        n_b = b_qkv.size
        d_b_qkv = lax.dynamic_slice_in_dim(small, tp_index * n_b, n_b).reshape(n_core, 3, -1, b_qkv.shape[2])
        d_b_qkv = d_b_qkv.transpose(1, 0, 2, 3).reshape(b_qkv.shape)
        d_b_up = lax.dynamic_slice_in_dim(small, n_tp * n_b + tp_index * ff, ff)
        d_gain1, d_bias1, d_gain2, d_bias2, d_b_out, d_b_down = small[n_tp * (n_b + ff):].reshape(6, width)

        d_w_out = pick_pieces(rest_w, 0, w_out.shape[0] * w_out.shape[1]).reshape(w_out.shape)
        d_w_qkv = pick_pieces(rest_w, p_out, n_b).reshape(n_core, 3, -1, w_qkv.shape[3], width).transpose(4, 1, 0, 2, 3).reshape(w_qkv.shape)
        return (layer_out, d_emb, d_pos, d_gain1, d_bias1, d_w_qkv, d_b_qkv, d_w_out,
                d_b_out, d_gain2, d_bias2, d_w_up, d_b_up, d_w_down, d_b_down)

    rep = P()
    in_specs = (P(dp, None), P("tp", None), rep, rep, rep,
                P(None, None, "tp", None), P(None, "tp", None), P("tp", None, None), rep,
                rep, rep, P(None, "tp"), P("tp"), P("tp", None), rep,
                P(dp, "tp", None))
    out_specs = (P(dp, "tp", None), P("tp", None), rep, rep, rep,
                 P(None, None, "tp", None), P(None, "tp", None), P("tp", None, None), rep,
                 rep, rep, P(None, "tp"), P("tp"), P("tp", None), rep)

    return jax.shard_map(local_step, mesh=mesh3, in_specs=in_specs, out_specs=out_specs, check_vma=False)
```

```python
import functools

import jax
import jax.numpy as jnp
from jax import lax
from jax.experimental import pallas as pl
from jax.experimental.pallas import tpu as pltpu
from jax.sharding import Mesh, PartitionSpec as P


F32 = jnp.float32
BF16 = jnp.bfloat16
MIB = 1024 * 1024
WIDEN = 32

BLK = 256


def dot_nt(a, b):
    return lax.dot_general(a, b, (((1,), (1,)), ((), ())), preferred_element_type=F32)


def dot_nn(a, b):
    return lax.dot_general(a, b, (((1,), (0,)), ((), ())), preferred_element_type=F32)


def head_only(x, head):
    half = x.shape[1] // 2
    lane = lax.broadcasted_iota(jnp.int32, x.shape, 1)
    keep = (lane < half) if head == 0 else (lane >= half)
    return jnp.where(keep, x, jnp.zeros((), x.dtype))


def attn_fwd_kernel(qkv_ref, ctx_ref, lse_ref, ctx_t):
    seq, width = ctx_ref.shape
    half = width // 2
    scale = half ** -0.5
    q2 = qkv_ref[:, 0:width] * jnp.asarray(scale, BF16)
    v_t = qkv_ref[:, 2 * width:3 * width].T
    tasks = [(head, i) for i in range(seq // BLK) for head in range(2)]

    def scores(head, i):
        return dot_nt(qkv_ref[0:(i + 1) * BLK, width:2 * width], head_only(q2[i * BLK:(i + 1) * BLK], head))

    ready = scores(*tasks[0])
    for n, (head, i) in enumerate(tasks):
        s = ready
        if n + 1 < len(tasks):
            ready = scores(*tasks[n + 1])
        lo, hi = i * BLK, (i + 1) * BLK
        v_h = v_t[head * half:(head + 1) * half, :]
        key = lax.broadcasted_iota(jnp.int32, (BLK, BLK), 0)
        qry = lax.broadcasted_iota(jnp.int32, (BLK, BLK), 1)
        diag = jnp.where(key <= qry, s[lo:hi], -1e30)
        top = jnp.max(diag, axis=0, keepdims=True)
        if i:
            top = jnp.maximum(top, jnp.max(s[0:lo], axis=0, keepdims=True))
        p_diag = jnp.exp(diag - top)
        total = jnp.sum(p_diag, axis=0, keepdims=True)
        if i:
            p_left = jnp.exp(s[0:lo] - top)
            total = total + jnp.sum(p_left, axis=0, keepdims=True)
        inv = 1.0 / total
        acc = dot_nn(v_h[:, lo:hi], (p_diag * inv).astype(BF16))
        if i:
            acc = acc + dot_nn(v_h[:, 0:lo], (p_left * inv).astype(BF16))
        ctx_t[head * half:(head + 1) * half, lo:hi] = acc
        lse_ref[head:head + 1, lo:hi] = top + jnp.log(total)
    ctx_ref[...] = ctx_t[...].T.astype(BF16)


def attn_fwd(qkv, n_seq, seq, n_pair):
    width = 128
    return pl.pallas_call(
        attn_fwd_kernel,
        grid=(n_seq, n_pair),
        in_specs=[pl.BlockSpec((seq, 3 * width), lambda b, p: (b, p))],
        out_specs=[pl.BlockSpec((seq, width), lambda b, p: (b, p)),
                   pl.BlockSpec((None, None, 2, seq), lambda b, p: (b, p, 0, 0))],
        out_shape=[jax.ShapeDtypeStruct((n_seq * seq, n_pair * width), BF16),
                   jax.ShapeDtypeStruct((n_seq, n_pair, 2, seq), F32)],
        scratch_shapes=[pltpu.VMEM((width, seq), F32)],
        name="attn_fwd",
        cost_estimate=pl.CostEstimate(flops=n_seq * n_pair * 8 * seq * seq * 256 * 10 // 16, bytes_accessed=n_seq * seq * n_pair * width * 8,
                                      transcendentals=n_seq * n_pair * seq * seq),
        compiler_params=pltpu.CompilerParams(vmem_limit_bytes=48 * 1024 * 1024),
    )(qkv)


def attn_bwd_kernel(qkv_ref, ctx_ref, dctx_ref, lse_ref, dqkv_ref, dk_t, dv_t):
    seq, width = ctx_ref.shape
    half = width // 2
    scale = half ** -0.5
    q2 = qkv_ref[:, 0:width] * jnp.asarray(scale, BF16)
    q_t = q2.T
    do_t = dctx_ref[...].T
    lse_c = jnp.concatenate([lse_ref[...], jnp.zeros((6, seq), F32)], axis=0).T
    prod = dctx_ref[...].astype(F32) * ctx_ref[...].astype(F32)
    tasks = [(head, i) for i in range(seq // BLK) for head in range(2)]

    def scores(head, i):
        lo, hi = i * BLK, (i + 1) * BLK
        return (dot_nt(head_only(q2[lo:hi], head), qkv_ref[0:hi, width:2 * width]),
                dot_nt(head_only(dctx_ref[lo:hi, :], head), qkv_ref[0:hi, 2 * width:3 * width]))

    dq = []
    ready = scores(*tasks[0])
    for n, (head, i) in enumerate(tasks):
        s, dp = ready
        if n + 1 < len(tasks):
            ready = scores(*tasks[n + 1])
        lo, hi = i * BLK, (i + 1) * BLK
        rows = slice(head * half, (head + 1) * half)
        mean = jnp.sum(head_only(prod[lo:hi], head), axis=1, keepdims=True)
        lse = lse_c[lo:hi, head:head + 1]
        qry = lax.broadcasted_iota(jnp.int32, (BLK, BLK), 0)
        key = lax.broadcasted_iota(jnp.int32, (BLK, BLK), 1)
        p_diag = jnp.where(key <= qry, jnp.exp(s[:, lo:hi] - lse), 0.0)
        ds_diag = (p_diag * (dp[:, lo:hi] - mean)).astype(BF16)
        dv_t[rows, lo:hi] = dot_nn(do_t[rows, lo:hi], p_diag.astype(BF16))
        dk_t[rows, lo:hi] = dot_nn(q_t[rows, lo:hi], ds_diag)
        dq_h = dot_nn(ds_diag, qkv_ref[lo:hi, width:2 * width])
        if i:
            p_left = jnp.exp(s[:, 0:lo] - lse)
            ds_left = (p_left * (dp[:, 0:lo] - mean)).astype(BF16)
            dv_t[rows, 0:lo] += dot_nn(do_t[rows, lo:hi], p_left.astype(BF16))
            dk_t[rows, 0:lo] += dot_nn(q_t[rows, lo:hi], ds_left)
            dq_h = dq_h + dot_nn(ds_left, qkv_ref[0:lo, width:2 * width])
        dq.append(dq_h)
        if head == 1:
            lane = lax.broadcasted_iota(jnp.int32, (BLK, width), 1)
            dqkv_ref[lo:hi, 0:width] = (jnp.where(lane < half, dq[0], dq[1]) * scale).astype(BF16)
            dq = []
    dqkv_ref[:, width:2 * width] = dk_t[...].T.astype(BF16)
    dqkv_ref[:, 2 * width:3 * width] = dv_t[...].T.astype(BF16)


def attn_bwd(qkv, ctx, dctx, lse, at, seq, n_pair):
    width = 128
    return pl.pallas_call(
        attn_bwd_kernel,
        grid=(n_pair,),
        in_specs=[pl.BlockSpec((seq, 3 * width), lambda p: (at, p)),
                  pl.BlockSpec((seq, width), lambda p: (at, p)),
                  pl.BlockSpec((seq, width), lambda p: (at, p)),
                  pl.BlockSpec((None, None, 2, seq), lambda p: (at, p, 0, 0))],
        out_specs=pl.BlockSpec((seq, 3 * width), lambda p: (0, p)),
        out_shape=jax.ShapeDtypeStruct((seq, n_pair * 3 * width), BF16),
        scratch_shapes=[pltpu.VMEM((width, seq), F32), pltpu.VMEM((width, seq), F32)],
        name="attn_bwd",
        cost_estimate=pl.CostEstimate(flops=n_pair * 20 * seq * seq * 256 * 10 // 16, bytes_accessed=seq * n_pair * width * 16,
                                      transcendentals=n_pair * seq * seq),
        compiler_params=pltpu.CompilerParams(vmem_limit_bytes=48 * 1024 * 1024),
    )(qkv, ctx, dctx, lse)


LN_EPS = 1e-5
GELU_S = 0.7978845608028654
GELU_A = 0.044715


def row_mean(v):
    return jnp.sum(v, axis=1, keepdims=True) * (1.0 / v.shape[1])


def row_stats(v):
    centered = v - row_mean(v)
    inv_std = lax.rsqrt(row_mean(centered * centered) + LN_EPS)
    return centered * inv_std, inv_std


def norm_back(d_y, x_in, gain):
    normed, inv_std = row_stats(x_in)
    d_norm = d_y * gain
    d_x = inv_std * (d_norm - row_mean(d_norm) - normed * row_mean(d_norm * normed))
    return d_x, d_y * normed


def col_sum(v):
    return jnp.sum(v, axis=0, keepdims=True)


def to_image(rows, image, base):
    tiles = rows.shape[1] // 128
    for h in range(rows.shape[0] // 8):
        for c in range(tiles):
            image[pl.ds(base + (h * tiles + c) * 8, 8), :] = rows[h * 8:(h + 1) * 8, c * 128:(c + 1) * 128]


def from_image(image, base, n_rows, width):
    tiles = width // 128
    return jnp.concatenate([jnp.concatenate([image[pl.ds(base + (h * tiles + c) * 8, 8), :] for c in range(tiles)], axis=1)
                            for h in range(n_rows // 8)], axis=0)


def pick_rows(code_ref, first, stage, image, n_rows, tiles):
    def pick(g, _):
        base = pl.multiple_of(g * 16 * tiles, 16 * tiles)
        for j in range(16):
            row = stage[pl.ds(code_ref[first + g * 16 + j], tiles, stride=8), :]
            image[pl.ds(base + (j // 8) * 8 * tiles + j % 8, tiles, stride=8), :] = row
        return 0

    lax.fori_loop(0, n_rows // 16, pick, 0)


def embed_kernel(n_blk, cap, code_ref, *refs):
    tok_refs = refs[:n_blk]
    pos_ref, gain_ref, bias_ref, x_ref, hid_ref, stage, image = refs[n_blk:]
    rows, width = x_ref.shape
    tiles = width // 128

    @pl.when(pl.program_id(0) == 0)
    def _():
        for b in range(n_blk):
            def widen(g, _, b=b):
                part = tok_refs[b][pl.ds(pl.multiple_of(g * WIDEN, WIDEN), WIDEN), :].astype(F32)
                to_image(part, stage, pl.multiple_of((b * cap + g * WIDEN) * tiles, WIDEN * tiles))
                return 0

            lax.fori_loop(0, cap // WIDEN, widen, 0)

    pick_rows(code_ref, pl.program_id(0) * rows, stage, image, rows, tiles)
    part = 64
    for i in range(rows // part):
        at = slice(i * part, (i + 1) * part)
        x = from_image(image, i * part * tiles, part, width) + pos_ref[at, :].astype(F32)
        x_ref[at, :] = x
        normed, _ = row_stats(x)
        hid_ref[at, :] = (normed * gain_ref[...] + bias_ref[...]).astype(BF16)


def embed(code, blocks, pos_rows, gain, bias, n_tok):
    cap, width = blocks[0].shape
    seq = pos_rows.shape[0]
    rows = 256
    per_seq = seq // rows
    n_blk = len(blocks)
    vec = pl.BlockSpec((1, width), lambda i: (0, 0))
    return pl.pallas_call(
        functools.partial(embed_kernel, n_blk, cap),
        grid=(n_tok // rows,),
        in_specs=[pl.BlockSpec(memory_space=pltpu.SMEM)]
        + [pl.BlockSpec((cap, width), lambda i: (0, 0), pipeline_mode=pl.Buffered(1))] * n_blk
        + [pl.BlockSpec((rows, width), lambda i: (i % per_seq, 0)), vec, vec],
        out_specs=[pl.BlockSpec((rows, width), lambda i: (i, 0))] * 2,
        out_shape=[jax.ShapeDtypeStruct((n_tok, width), F32), jax.ShapeDtypeStruct((n_tok, width), BF16)],
        scratch_shapes=[pltpu.VMEM((n_blk * cap * width // 128, 128), F32), pltpu.VMEM((rows * width // 128, 128), F32)],
        name="embed_norm",
        cost_estimate=pl.CostEstimate(flops=15_000_000_000, bytes_accessed=n_tok * width * 10, transcendentals=0),
        compiler_params=pltpu.CompilerParams(vmem_limit_bytes=48 * MIB),
    )(code, *blocks, pos_rows, gain, bias)


def pack_kernel(n_blk, code_ref, tok_ref, *refs):
    out_refs = refs[:n_blk]
    stage, image = refs[n_blk:]
    n_tok, width = tok_ref.shape
    cap = out_refs[0].shape[0]
    tiles = width // 128

    def widen(g, _):
        part = tok_ref[pl.ds(pl.multiple_of(g * WIDEN, WIDEN), WIDEN), :].astype(F32)
        to_image(part, stage, pl.multiple_of(g * WIDEN * tiles, WIDEN * tiles))
        return 0

    lax.fori_loop(0, n_tok // WIDEN, widen, 0)
    for b in range(n_blk):
        pick_rows(code_ref, b * cap, stage, image, cap, tiles)

        def narrow(g, _, b=b):
            part = from_image(image, pl.multiple_of(g * WIDEN * tiles, WIDEN * tiles), WIDEN, width)
            out_refs[b][pl.ds(pl.multiple_of(g * WIDEN, WIDEN), WIDEN), :] = part.astype(BF16)
            return 0

        lax.fori_loop(0, cap // WIDEN, narrow, 0)


def pack(code, tok, cap):
    n_tok, width = tok.shape
    n_blk = code.shape[0] // cap
    return pl.pallas_call(
        functools.partial(pack_kernel, n_blk),
        in_specs=[pl.BlockSpec(memory_space=pltpu.SMEM), pl.BlockSpec(memory_space=pltpu.VMEM)],
        out_specs=[pl.BlockSpec(memory_space=pltpu.VMEM)] * n_blk,
        out_shape=[jax.ShapeDtypeStruct((cap, width), BF16)] * n_blk,
        scratch_shapes=[pltpu.VMEM((n_tok * width // 128, 128), F32), pltpu.VMEM((cap * width // 128, 128), F32)],
        name="token_pack",
        cost_estimate=pl.CostEstimate(flops=15_000_000_000, bytes_accessed=n_tok * width * 5, transcendentals=0),
        compiler_params=pltpu.CompilerParams(vmem_limit_bytes=40 * MIB),
    )(code, tok)


def proj_kernel(c_ref, w_ref, x_ref, b_ref, gain_ref, bias_ref, x1_ref, hid_ref):
    part = x_ref.shape[0] // 2
    for i in range(2):
        at = slice(i * part, (i + 1) * part)
        x1 = x_ref[at, :] + dot_nn(c_ref[at, :], w_ref[...].reshape(c_ref.shape[1], -1)).astype(BF16).astype(F32) + b_ref[...]
        x1_ref[at, :] = x1
        normed, _ = row_stats(x1)
        hid_ref[at, :] = (normed * gain_ref[...] + bias_ref[...]).astype(BF16)


def proj_norm(ctx, w, start, x, b, gain, bias):
    n_tok, width = x.shape
    n_row = ctx.shape[1] // w.shape[0]
    rows = 512
    vec = pl.BlockSpec((1, width), lambda i: (0, 0))
    mat = pl.BlockSpec((rows, width), lambda i: (i, 0))
    return pl.pallas_call(
        proj_kernel,
        grid=(n_tok // rows,),
        in_specs=[pl.BlockSpec((rows, ctx.shape[1]), lambda i: (i, 0)), pl.BlockSpec((w.shape[0], n_row, width), lambda i: (0, start // n_row, 0)), mat, vec, vec, vec],
        out_specs=[mat, mat],
        out_shape=[jax.ShapeDtypeStruct((n_tok, width), F32), jax.ShapeDtypeStruct((n_tok, width), BF16)],
        name="proj_norm",
        cost_estimate=pl.CostEstimate(flops=2 * n_tok * ctx.shape[1] * width, bytes_accessed=n_tok * width * 12, transcendentals=0),
        compiler_params=pltpu.CompilerParams(vmem_limit_bytes=40 * MIB),
    )(ctx, w, x, b, gain, bias)


def ffn_kernel(part, h_ref, og_ref, wu_ref, wd_ref, b_ref, act_ref, dup_ref, db_ref):
    total = jnp.zeros(db_ref.shape, F32)
    for i in range(h_ref.shape[0] // part):
        at = slice(i * part, (i + 1) * part)
        z = dot_nt(h_ref[at, :], wu_ref[0]) + b_ref[...]
        d_act = dot_nt(og_ref[at, :], wd_ref[0])
        z2 = z * z
        gate = 0.5 * jnp.tanh(z * (GELU_S + (GELU_S * GELU_A) * z2)) + 0.5
        act = z * gate
        d_up = d_act * (gate + act * (1.0 - gate) * (2.0 * GELU_S + (6.0 * GELU_S * GELU_A) * z2))
        act_ref[at, :] = act.astype(BF16)
        dup_ref[at, :] = d_up.astype(BF16)
        total = total + col_sum(d_up)
    db_ref[...] = total


def ffn(hid, og, w, b_up, part=1024):
    n_tok, width = hid.shape
    ff = b_up.shape[1]
    n_piece = w.shape[0]
    bn = ff // n_piece
    whole = pl.BlockSpec((n_tok, width), lambda i: (0, 0), pipeline_mode=pl.Buffered(1))
    ospec = pl.BlockSpec((n_tok, bn), lambda i: (0, i))
    vec = pl.BlockSpec((1, bn), lambda i: (0, i))
    return pl.pallas_call(
        functools.partial(ffn_kernel, part),
        grid=(n_piece,),
        in_specs=[whole, whole, pl.BlockSpec((1, bn, width), lambda i: (i, 0, 0)), pl.BlockSpec((1, bn, width), lambda i: (i, 1, 0)), vec],
        out_specs=[ospec, ospec, vec],
        out_shape=[jax.ShapeDtypeStruct((n_tok, ff), BF16), jax.ShapeDtypeStruct((n_tok, ff), BF16), jax.ShapeDtypeStruct((1, ff), F32)],
        name="ffn",
        cost_estimate=pl.CostEstimate(flops=4 * n_tok * ff * width, bytes_accessed=4 * n_tok * ff + 4 * ff * width, transcendentals=n_tok * ff),
        compiler_params=pltpu.CompilerParams(vmem_limit_bytes=48 * MIB),
    )(hid, og, w, w, b_up)


def back2_kernel(dup_ref, w_ref, x1_ref, og_ref, gain_ref, dr_ref, da_ref, sums_ref):
    @pl.when(pl.program_id(0) == 0)
    def _():
        sums_ref[...] = jnp.zeros(sums_ref.shape, F32)

    n_part = 2
    part = dr_ref.shape[0] // n_part
    w = w_ref[...].reshape(dup_ref.shape[1], -1)
    d_ys = [dot_nn(dup_ref[i * part:(i + 1) * part, :], w) for i in range(n_part)]
    for i in range(n_part):
        at = slice(i * part, (i + 1) * part)
        d_y = d_ys[i].astype(BF16).astype(F32)
        d_x, d_gain = norm_back(d_y, x1_ref[at, :], gain_ref[...])
        og = og_ref[at, :].astype(F32)
        d_resid = og + d_x
        dr_ref[at, :] = d_resid
        da_ref[at, :] = d_resid.astype(BF16)
        sums_ref[0:1, :] += col_sum(d_gain)
        sums_ref[1:2, :] += col_sum(d_y)
        sums_ref[2:3, :] += col_sum(d_resid)
        sums_ref[3:4, :] += col_sum(og)


def back2(d_up, w, x1, og, gain):
    n_tok, width = x1.shape
    ff = d_up.shape[1]
    rows = 256
    mat = pl.BlockSpec((rows, width), lambda i: (i, 0))
    return pl.pallas_call(
        back2_kernel,
        grid=(n_tok // rows,),
        in_specs=[pl.BlockSpec((rows, ff), lambda i: (i, 0)), pl.BlockSpec((w.shape[0], ff // w.shape[0], width), lambda i: (0, 0, 0), pipeline_mode=pl.Buffered(1)),
                  mat, mat, pl.BlockSpec((1, width), lambda i: (0, 0))],
        out_specs=[mat, mat, pl.BlockSpec((8, width), lambda i: (0, 0))],
        out_shape=[jax.ShapeDtypeStruct((n_tok, width), F32), jax.ShapeDtypeStruct((n_tok, width), BF16), jax.ShapeDtypeStruct((8, width), F32)],
        name="ffn_back",
        cost_estimate=pl.CostEstimate(flops=2 * n_tok * ff * width, bytes_accessed=2 * n_tok * ff + n_tok * width * 12, transcendentals=0),
        compiler_params=pltpu.CompilerParams(vmem_limit_bytes=48 * MIB),
    )(d_up, w, x1, og, gain)


def back1_kernel(dq_ref, w_ref, x_ref, dr_ref, gain_ref, *refs):
    tok_ref, pos_ref, sums_ref, bsum_ref = refs[-4:]
    before_refs = refs[:-4]

    @pl.when(pl.program_id(0) == 0)
    def _():
        sums_ref[...] = before_refs[1][...] if before_refs else jnp.zeros(sums_ref.shape, F32)
        bsum_ref[...] = before_refs[2][...] if before_refs else jnp.zeros(bsum_ref.shape, F32)

    n_part = 2
    part = tok_ref.shape[0] // n_part
    d_ys = [dot_nn(dq_ref[i * part:(i + 1) * part, :], w_ref[...]) for i in range(n_part)]
    for i in range(n_part):
        at = slice(i * part, (i + 1) * part)
        d_y = d_ys[i].astype(BF16).astype(F32)
        d_x, d_gain = norm_back(d_y, x_ref[at, :], gain_ref[...])
        d_resid = dr_ref[at, :] + d_x
        tok_ref[at, :] = d_resid.astype(BF16)
        pos_ref[at, :] = before_refs[0][at, :] + d_resid if before_refs else d_resid
        sums_ref[0:1, :] += col_sum(d_gain)
        sums_ref[1:2, :] += col_sum(d_y)
        bsum_ref[0:1, :] += col_sum(dq_ref[at, :].astype(F32))


def back1(d_qkv, w_qkv, x, d_resid1, gain, at, pos_rows, earlier=None):
    seq, n_cols = d_qkv.shape
    width = x.shape[1]
    rows = 256
    steps = seq // rows
    mat = pl.BlockSpec((rows, width), lambda i: (at * steps + i, 0))
    out = pl.BlockSpec((rows, width), lambda i: (i, 0))
    few = [pl.BlockSpec((8, width), lambda i: (0, 0)), pl.BlockSpec((8, n_cols), lambda i: (0, 0))]
    return pl.pallas_call(
        back1_kernel,
        grid=(steps,),
        in_specs=[pl.BlockSpec((rows, n_cols), lambda i: (i, 0)),
                  pl.BlockSpec((n_cols, width), lambda i: (0, 0), pipeline_mode=pl.Buffered(1)),
                  mat, mat, pl.BlockSpec((1, width), lambda i: (0, 0))] + ([out] + few if earlier else []),
        out_specs=[out, out] + few,
        out_shape=[jax.ShapeDtypeStruct((seq, width), BF16), jax.ShapeDtypeStruct((pos_rows, width), F32),
                   jax.ShapeDtypeStruct((8, width), F32), jax.ShapeDtypeStruct((8, n_cols), F32)],
        name="qkv_back",
        cost_estimate=pl.CostEstimate(flops=2 * seq * n_cols * width, bytes_accessed=2 * seq * n_cols + seq * width * 12, transcendentals=0),
        compiler_params=pltpu.CompilerParams(vmem_limit_bytes=48 * MIB),
    )(d_qkv, w_qkv, x, d_resid1, gain, *(earlier or ()))


def ff_out_kernel(n, start, g_ref, down_ref, up_ref):
    down_ref[...] = g_ref[0, 0:n, :]
    up_ref[...] = g_ref[0, start:start + n, :].T


def ff_out(g, n, start, n_x, n_core):
    n_piece, rows, width = g.shape
    place = lambda p: (p % n_core) * n_x + p // n_core
    return pl.pallas_call(
        functools.partial(ff_out_kernel, n, start),
        grid=(n_piece,),
        in_specs=[pl.BlockSpec((1, rows, width), lambda p: (p, 0, 0))],
        out_specs=[pl.BlockSpec((n, width), lambda p: (place(p), 0)), pl.BlockSpec((width, n), lambda p: (0, place(p)))],
        out_shape=[jax.ShapeDtypeStruct((n_piece * n, width), F32), jax.ShapeDtypeStruct((width, n_piece * n), F32)],
        name="ff_grads_out",
        cost_estimate=pl.CostEstimate(flops=8_000_000_000, bytes_accessed=n_piece * rows * width * 8, transcendentals=0),
        compiler_params=pltpu.CompilerParams(vmem_limit_bytes=24 * MIB),
    )(g)


def assemble_kernel(n, me_ref, *refs):
    out_ref = refs[n]
    k = me_ref[0] ^ pl.program_id(0)
    for j in range(n):
        @pl.when(k == j)
        def _(j=j):
            out_ref[...] = refs[j][...].reshape(out_ref.shape)


def assemble(me, parts, out_shape, block):
    at = 1 if len(out_shape) == 4 else 0
    return pl.pallas_call(
        functools.partial(assemble_kernel, len(parts)),
        grid_spec=pltpu.PrefetchScalarGridSpec(
            num_scalar_prefetch=1, grid=(len(parts),),
            in_specs=[pl.BlockSpec(p.shape, lambda i, m: (0, 0, 0), pipeline_mode=pl.Buffered(1)) for p in parts],
            out_specs=pl.BlockSpec(block, lambda i, m: tuple(i if d == at else 0 for d in range(len(block))))),
        out_shape=jax.ShapeDtypeStruct(out_shape, parts[0].dtype),
        name="assemble",
        cost_estimate=pl.CostEstimate(flops=4_000_000_000, bytes_accessed=16 * MIB, transcendentals=0),
        compiler_params=pltpu.CompilerParams(vmem_limit_bytes=24 * MIB),
    )(me, *parts)


LANES = 128


def accum_kernel(n_block, cap, sub_rows, width, where_ref, first_ref, *refs):
    tok_refs = refs[:n_block]
    out_ref = refs[n_block]
    n_sub = len(sub_rows)
    acc = refs[n_block + 1:n_block + 1 + n_sub]
    buf, stage, in_sem, out_sem = refs[n_block + 1 + n_sub:]
    tiles = width // LANES
    group = 8 * tiles

    def fetch(block, n):
        return pltpu.make_async_copy(tok_refs[n], buf.at[block % 2], in_sem.at[block % 2])

    def fetch_next(block):
        for n in range(n_block):
            @pl.when(block == n)
            def _(n=n):
                fetch(block, n).start()

    fetch_next(0)
    for s in range(n_sub):
        def clear(i, _, s=s):
            acc[s][pl.ds(pl.multiple_of(i * group, group), group), :] = jnp.zeros((group, LANES), F32)
            return 0

        lax.fori_loop(0, sub_rows[s] // 8, clear, 0)

    def add_rows(s, slot, n):
        codes = [where_ref[slot + j] for j in range(n)]
        at = [code >> 16 for code in codes]
        rows = [stage[pl.ds(code & 0xffff, tiles, stride=8), :] for code in codes]
        sums = [acc[s][pl.ds(a, tiles, stride=8), :] for a in at]
        for j in range(n):
            for i in range(j):
                sums[j] = jnp.where(at[i] == at[j], sums[i], sums[j])
            sums[j] = sums[j] + rows[j]
        for j in range(n):
            acc[s][pl.ds(at[j], tiles, stride=8), :] = sums[j]

    def add_block(block, _):
        fetch_next(block + 1)
        fetch(block, 0).wait()

        def widen(g, _):
            rows = buf[block % 2, pl.ds(pl.multiple_of(g * WIDEN, WIDEN), WIDEN), :].astype(F32)
            base = pl.multiple_of(g * (WIDEN // 8) * group, (WIDEN // 8) * group)
            for h in range(WIDEN // 8):
                for c in range(tiles):
                    stage[pl.ds(base + h * group + c * 8, 8), :] = rows[h * 8:(h + 1) * 8, c * LANES:(c + 1) * LANES]
            return 0

        lax.fori_loop(0, cap // WIDEN, widen, 0)

        starts = [first_ref[block * (n_sub + 1) + s] for s in range(n_sub + 1)]
        counts = [starts[s + 1] - starts[s] for s in range(n_sub)]
        both = functools.reduce(jnp.minimum, counts) // 2
        begin = [block * cap + starts[s] for s in range(n_sub)]

        def together(i, _):
            for s in range(n_sub):
                add_rows(s, begin[s] + 2 * i, 2)
            return 0

        lax.fori_loop(0, both, together, 0)
        for s in range(n_sub):
            fours = (counts[s] - 2 * both) // 4

            def alone(i, _, s=s):
                add_rows(s, begin[s] + 2 * both + 4 * i, 4)
                return 0

            lax.fori_loop(0, fours, alone, 0)

            def single(i, _, s=s):
                add_rows(s, begin[s] + i, 1)
                return 0

            lax.fori_loop(2 * both + 4 * fours, counts[s], single, 0)
        return 0

    lax.fori_loop(0, n_block, add_block, 0)
    done = 0
    copies = []
    for s in range(n_sub):
        n = sub_rows[s] * tiles
        copies.append(pltpu.make_async_copy(acc[s], out_ref.at[pl.ds(done, n), :], out_sem.at[s]))
        copies[-1].start()
        done += n
    for c in copies:
        c.wait()


def accum(tok_blocks, code, first, sub_rows, width):
    n_block = len(tok_blocks)
    cap = tok_blocks[0].shape[0]
    n_sub = len(sub_rows)
    tiles = width // LANES
    return pl.pallas_call(
        functools.partial(accum_kernel, n_block, cap, sub_rows, width),
        in_specs=[pl.BlockSpec(memory_space=pltpu.SMEM), pl.BlockSpec(memory_space=pltpu.SMEM)]
        + [pl.BlockSpec(memory_space=pl.ANY)] * n_block,
        out_specs=pl.BlockSpec(memory_space=pl.ANY),
        out_shape=jax.ShapeDtypeStruct((sum(sub_rows) * tiles, LANES), F32),
        scratch_shapes=[pltpu.VMEM((r * tiles, LANES), F32) for r in sub_rows]
        + [pltpu.VMEM((2, cap, width), BF16), pltpu.VMEM((cap * tiles, LANES), F32),
           pltpu.SemaphoreType.DMA((2,)), pltpu.SemaphoreType.DMA((n_sub,))],
        name="table_accum",
        cost_estimate=pl.CostEstimate(flops=50_000_000_000, bytes_accessed=100_000_000, transcendentals=0),
        compiler_params=pltpu.CompilerParams(vmem_limit_bytes=63 * 1024 * 1024),
    )(code, first, *tok_blocks)


def dot_tn(a, b):
    return lax.dot_general(a, b, (((0,), (0,)), ((), ())), preferred_element_type=F32)


def grad_kernel(has_plus, core_ref, a_ref, b_ref, *refs):
    out_ref = refs[-1]
    n = a_ref.shape[1]
    g = dot_tn(a_ref[...], b_ref[...])
    out_ref[0:n, :] = g + refs[0][0:n, :] if has_plus else g
    if out_ref.shape[0] > n:
        out_ref[n:, :] = jnp.zeros((out_ref.shape[0] - n, out_ref.shape[1]), F32)


def grad_pieces(core, a, b, n_tp, piece, which, n_which, plus=None, into=None):
    n_tok, n_cols = a.shape
    width = b.shape[1]
    bn = n_cols // (4 * n_tp)
    out_spec = pl.BlockSpec((piece, width), lambda p, c: (n_which * p + which, 0))
    in_specs = [pl.BlockSpec((n_tok, bn), lambda p, c: (0, 4 * (p // 2) + 2 * c[0] + p % 2)),
                pl.BlockSpec((n_tok, width), lambda p, c: (0, 0), pipeline_mode=pl.Buffered(1))]
    args = [a, b]
    if plus is not None:
        in_specs.append(pl.BlockSpec((piece, width), lambda p, c: (p, 0)))
        args.append(plus)
    if into is not None:
        in_specs.append(pl.BlockSpec(memory_space=pl.ANY))
        args.append(into)
    return pl.pallas_call(
        functools.partial(grad_kernel, plus is not None),
        grid_spec=pltpu.PrefetchScalarGridSpec(num_scalar_prefetch=1, grid=(2 * n_tp,), in_specs=in_specs, out_specs=out_spec),
        out_shape=jax.ShapeDtypeStruct((2 * n_tp * n_which * piece, width), F32),
        input_output_aliases={} if into is None else {len(args): 0},
        name="weight_grad",
        cost_estimate=pl.CostEstimate(flops=n_tok * n_cols * width, bytes_accessed=n_tok * (n_cols + 2 * width) + 2 * n_cols * width,
                                      transcendentals=0),
        compiler_params=pltpu.CompilerParams(vmem_limit_bytes=32 * MIB),
    )(core, *args)


def grad_rest_kernel(spans, last, n_a2, core_ref, a1_ref, b1_ref, b2_ref, *refs):
    a2_refs, refs, out_ref = refs[:n_a2], refs[n_a2:-1], refs[-1]
    plus = refs[0] if refs else None
    piece, piece_in = out_ref.shape[0] // 2, (plus.shape[0] // 2 if refs else 0)
    rows = b2_ref.shape[0] // n_a2
    for which, (start, stop) in enumerate(spans):
        half = (a2_refs[0] if which else a1_ref).shape[1] // 2
        for i in range(0, 2 * half, 128):
            cols = slice(i, i + 128)
            if which:
                g = sum(dot_tn(a_ref[:, cols], b2_ref[n * rows:(n + 1) * rows, :]) for n, a_ref in enumerate(a2_refs))
            else:
                g = dot_tn(a1_ref[:, cols], b1_ref[...])
            for x in range(2):
                lo, hi = max(i, x * half), min(i + 128, (x + 1) * half)
                if lo < hi:
                    to = lo - x * half + start
                    part = g[lo - i:hi - i]
                    if plus is not None:
                        part = part + plus[x * piece_in + to:x * piece_in + to + hi - lo, :]
                    out_ref[x * piece + to:x * piece + to + hi - lo, :] = part
        for x in range(2):
            if stop > start + half:
                out_ref[x * piece + start + half:x * piece + stop, :] = jnp.zeros((stop - start - half, out_ref.shape[1]), F32)
    if last:
        for x in range(2):
            out_ref[x * piece + spans[-1][1]:(x + 1) * piece, :] = refs[1][x, 0] + refs[2][x * last:(x + 1) * last, :]


def grad_rest(core, a1, b1, a2, b2, n_tp, spans, plus=None, tail=None):
    n_tok, width = b1.shape
    last = tail[0].shape[2] if tail else 0
    piece = spans[-1][1] + last
    whole = pl.BlockSpec((n_tok, width), lambda t, c: (0, 0), pipeline_mode=pl.Buffered(1))
    cols = [pl.BlockSpec((a.shape[0], a.shape[1] // (2 * n_tp)), lambda t, c: (0, 2 * t + c[0])) for a in (a1, *a2)]
    in_specs, args = [cols[0], whole, whole] + cols[1:], [a1, b1, b2, *a2]
    if plus is not None:
        in_specs.append(pl.BlockSpec((plus.shape[0] // n_tp, width), lambda t, c: (t, 0)))
        args.append(plus)
    if tail:
        in_specs.append(pl.BlockSpec((2, 1, last, width), lambda t, c: (t, c[0], 0, 0)))
        in_specs.append(pl.BlockSpec((2 * last, width), lambda t, c: (t, 0)))
        args += tail
    n_cols = a1.shape[1] + a2[0].shape[1]
    return pl.pallas_call(
        functools.partial(grad_rest_kernel, spans, last, len(a2)),
        grid_spec=pltpu.PrefetchScalarGridSpec(num_scalar_prefetch=1, grid=(n_tp,), in_specs=in_specs,
                                               out_specs=pl.BlockSpec((2 * piece, width), lambda t, c: (t, 0))),
        out_shape=jax.ShapeDtypeStruct((2 * n_tp * piece, width), F32),
        name="weight_grads",
        cost_estimate=pl.CostEstimate(flops=n_tok * n_cols * width, bytes_accessed=n_tok * (n_cols + 4 * width) + 2 * n_cols * width,
                                      transcendentals=0),
        compiler_params=pltpu.CompilerParams(vmem_limit_bytes=40 * MIB),
    )(core, *args)


POS_OFFSET = 2
SLOTS = 704
GRAD_SLOTS = 384
LOW = 32


def before(n):
    return (lax.broadcasted_iota(jnp.int32, (n, n), 1) < lax.broadcasted_iota(jnp.int32, (n, n), 0)).astype(BF16)


def rank_in_class(hot):
    n_blk, n_tok, n_cls = hot.shape
    ones = hot.astype(BF16).reshape(n_blk, n_tok // 128, 128, n_cls)
    within = jnp.einsum("ij,bnjk->bnik", before(128), ones, preferred_element_type=F32)
    sums = jnp.sum(ones.astype(F32), axis=2)
    ahead = jnp.einsum("mn,bnk->bmk", before(n_tok // 128), sums.astype(BF16), preferred_element_type=F32)
    rank = jnp.sum((within + ahead[:, :, None, :]) * ones.astype(F32), axis=3)
    return rank.reshape(n_blk, n_tok).astype(jnp.int32), jnp.sum(sums, axis=1).astype(jnp.int32)


def compact(rank, valid, value, slots):
    n_high = slots // LOW
    high = ((rank // LOW)[:, :, None] == jnp.arange(n_high)) & valid[:, :, None]
    low = ((rank % LOW)[:, :, None] == jnp.arange(LOW)).astype(F32)
    parts = jnp.concatenate([low * (value // 128).astype(F32)[:, :, None], low * (value % 128).astype(F32)[:, :, None]], axis=2)
    out = jnp.einsum("bjh,bjl->bhl", high.astype(BF16), parts.astype(BF16), preferred_element_type=F32).astype(jnp.int32)
    return (out[:, :, :LOW] * 128 + out[:, :, LOW:]).reshape(rank.shape[0], slots)


def solution(mesh):
    n_tp, n_dp = mesh.shape["tp"], mesh.shape["dp"]
    n_core = 2
    n_x = n_dp // n_core
    mesh3 = Mesh(mesh.devices.reshape(n_tp, n_x, n_core), ("tp", "xx", "cc"))
    dp = ("xx", "cc")
    tp_swap = [[(i, i ^ k) for i in range(n_tp)] for k in range(n_tp)]
    pair = [(0, 1), (1, 0)]

    def local_step(tok_ids, emb_table, pos_table, ln1_gain, ln1_bias, w_qkv, b_qkv, w_out, b_out,
                   ln2_gain, ln2_bias, w_up, b_up, w_down, b_down, out_grad):
        tp_index, x_index, c_index = lax.axis_index("tp"), lax.axis_index("xx"), lax.axis_index("cc")
        dp_index = x_index * n_core + c_index
        n_seq_dp, seq = tok_ids.shape
        n_seq = n_seq_dp // n_tp
        n_tok = n_seq * seq
        rows, width = emb_table.shape
        n_sub = 4
        sub = -(-rows // n_sub // 8) * 8
        sub_rows = (sub,) * (n_sub - 1) + (rows - (n_sub - 1) * sub,)
        seq_local = seq // n_tp
        ff = w_up.shape[1]
        gain1, bias1 = ln1_gain.astype(F32)[None], ln1_bias.astype(F32)[None]
        gain2, bias2 = ln2_gain.astype(F32)[None], ln2_bias.astype(F32)[None]

        def half(w, axis):
            n = w.shape[axis] // n_core
            return lax.dynamic_slice_in_dim(w, c_index * n, n, axis)

        def gather_rows(w):
            return lax.all_gather(w, ("tp", "cc"), axis=0, tiled=True)

        def swap(v, axis, k=1):
            return lax.ppermute(v, axis, tp_swap[k] if axis == "tp" else pair)

        def by_owner(parts):
            out = []
            for p in range(n_tp):
                k = tp_index ^ p
                out.append(jnp.where(k < 2, jnp.where(k == 0, parts[0], parts[1]), jnp.where(k == 2, parts[2], parts[3])))
            return out

        ids_all = lax.all_gather(tok_ids, dp, axis=0, tiled=True)
        ids_all, w_up, w_down, w_out, b_qkv, b_up = lax.optimization_barrier((ids_all, w_up, w_down, w_out, b_qkv, b_up))

        wqkv_t = gather_rows(jnp.transpose(half(w_qkv, 2), (1, 2, 3, 0)).reshape(-1, width))
        n_ff, n_out = ff // n_dp, w_out.shape[0] * w_out.shape[1] // n_dp

        def quarter(w, axis):
            n = w.shape[axis] // n_dp
            return lax.dynamic_slice_in_dim(w, dp_index * n, n, axis)

        w_all = lax.all_gather(jnp.concatenate([quarter(w_up, 1).T, quarter(w_down, 0), quarter(w_out.reshape(-1, width), 0)]),
                               ("tp", "xx", "cc"), axis=0, tiled=True).reshape(n_tp * n_dp, 2 * n_ff + n_out, width)
        wdown_w = w_all[:, n_ff:2 * n_ff].reshape(-1, width)
        wout_w = w_all[:, 2 * n_ff:].reshape(-1, width)
        n_pair = wqkv_t.shape[0] // (3 * 128)
        own_bias = jnp.concatenate([b_qkv.reshape(3, n_core, -1, b_qkv.shape[2]).transpose(1, 0, 2, 3).reshape(-1), b_up])
        biases = jnp.stack(by_owner([swap(own_bias, "tp", k) if k else own_bias for k in range(n_tp)]))
        bqkv_w = biases[:, :-ff].reshape(-1).astype(F32)
        bup_w = biases[:, -ff:].reshape(1, -1).astype(F32)
        pos_rows = lax.slice_in_dim(pos_table, POS_OFFSET, POS_OFFSET + seq, axis=0)

        local = ids_all - tp_index * rows
        sub_of = sum(((local >= s * sub).astype(jnp.int32) for s in range(1, n_sub)), jnp.zeros_like(local))
        owned = (local >= 0) & (local < rows)
        hot = owned[:, :, None] & (sub_of[:, :, None] == jnp.arange(n_sub))
        rank, counts = rank_in_class(hot)
        first = jnp.concatenate([jnp.zeros_like(counts[:, :1]), jnp.cumsum(counts, axis=1)], axis=1)
        rank = rank + jnp.sum(jnp.where(hot, first[:, None, :-1], 0), axis=2)
        owner_counts = jnp.stack([jnp.sum(((ids_all >= o * rows) & (ids_all < (o + 1) * rows)).astype(jnp.int32), axis=1)
                                  for o in range(n_tp)])
        grad_rounds = (jnp.max(owner_counts) + GRAD_SLOTS - 1) // GRAD_SLOTS
        rounds = (jnp.max(jnp.sum(owner_counts.reshape(n_tp, -1, n_seq), axis=2)) + SLOTS - 1) // SLOTS

        def after_first(ranks, totals):
            return (ranks + (jnp.cumsum(totals, axis=1) - totals)[:, :, None]).reshape(ranks.shape[0], -1)

        def grad_lists(r):
            at = rank - r * GRAD_SLOTS
            return compact(at, owned & (at >= 0) & (at < GRAD_SLOTS), jnp.where(owned, local, 0), GRAD_SLOTS)

        my_rank = lax.dynamic_slice_in_dim(rank, dp_index * n_seq_dp, n_seq_dp, 0)
        my_total = lax.dynamic_slice_in_dim(first[:, -1], dp_index * n_seq_dp, n_seq_dp, 0)
        my_rank = after_first(my_rank.reshape(n_tp, n_seq, seq), my_total.reshape(n_tp, n_seq))
        my_owned = lax.dynamic_slice_in_dim(owned, dp_index * n_seq_dp, n_seq_dp, 0).reshape(n_tp, n_tok)
        my_local = lax.dynamic_slice_in_dim(local, dp_index * n_seq_dp, n_seq_dp, 0).reshape(n_tp, n_tok)

        def lists(r):
            at = my_rank - r * SLOTS
            return compact(at, my_owned & (at >= 0) & (at < SLOTS), jnp.where(my_owned, my_local, 0), SLOTS)

        own_ids = lax.dynamic_slice_in_dim(ids_all, dp_index * n_seq_dp + tp_index * n_seq, n_seq, 0)
        own_owner = sum(((own_ids >= o * rows).astype(jnp.int32) for o in range(1, n_tp)), jnp.zeros_like(own_ids))
        own_local = own_ids - own_owner * rows
        own_sub = sum(((own_local >= s * sub).astype(jnp.int32) for s in range(1, n_sub)), jnp.zeros_like(own_ids))
        own_hot = (own_owner * n_sub + own_sub)[:, :, None] == jnp.arange(n_tp * n_sub)
        own_rank, own_counts = rank_in_class(own_hot)
        own_counts = own_counts.reshape(n_seq, n_tp, n_sub)
        own_first = jnp.cumsum(own_counts, axis=2) - own_counts
        own_rank = own_rank + jnp.sum(jnp.where(own_hot, own_first.reshape(n_seq, 1, -1), 0), axis=2)
        own_total = jnp.sum(own_counts, axis=2)
        own_shift = jnp.cumsum(own_total, axis=0) - own_total
        own_place = sum(jnp.where(own_owner == o, own_shift[:, o:o + 1], 0) for o in range(n_tp))
        own_place = (own_place + own_rank).reshape(-1)

        def own_lists(r, b):
            at = jnp.broadcast_to(own_rank[b] - r * GRAD_SLOTS, (n_tp, seq))
            mine = own_owner[b] == jnp.arange(n_tp)[:, None]
            return compact(at, mine & (at >= 0) & (at < GRAD_SLOTS), jnp.broadcast_to(jnp.arange(seq), (n_tp, seq)), GRAD_SLOTS)

        tiles = width // 128

        def rows_here(r, my_lists):
            index = [lax.dynamic_index_in_dim(my_lists, tp_index ^ k, 0, keepdims=False) for k in range(n_tp)]
            first_two = jnp.take(emb_table, jnp.concatenate([index[3], index[1]]), axis=0, mode="clip")
            rest, first_two = lax.optimization_barrier((jnp.concatenate([index[2], index[0]]), first_two))
            last_two = jnp.take(emb_table, rest, axis=0, mode="clip")
            sent = [last_two[SLOTS:], first_two[SLOTS:], last_two[:SLOTS], first_two[:SLOTS]]
            got = list(sent)
            for k in range(1, n_tp):
                got[k] = swap(sent[k], "tp", k)
            at = own_place - r * SLOTS
            valid = (at >= 0) & (at < SLOTS)
            return got, jnp.where(valid, (own_owner.reshape(-1) ^ tp_index) * SLOTS + at, 0), valid

        def norm_rows(x):
            normed, _ = row_stats(x)
            return (normed * gain1 + bias1).astype(BF16)

        got0, place0, _ = rows_here(0, lists(0))
        code0 = (place0 // 8) * (8 * tiles) + place0 % 8
        got0, out_grad = lax.optimization_barrier((got0, out_grad))
        resid_x, hid1 = embed(code0, got0, pos_rows, gain1, bias1, n_tok)

        def more_rows(carry):
            r, x, _ = carry
            got, place, valid = rows_here(r, lists(r))
            new = jnp.take(jnp.concatenate(got), place, axis=0, mode="clip").astype(F32) + jnp.tile(pos_rows.astype(F32), (n_seq, 1))
            x = jnp.where(valid[:, None], new, x)
            return r + 1, x, norm_rows(x)

        _, resid_x, hid1 = lax.while_loop(lambda c: c[0] < rounds, more_rows, (jnp.int32(1), resid_x, hid1))

        og_parts = out_grad.reshape(n_tp, n_seq, seq_local, width)
        parts = [lax.dynamic_index_in_dim(og_parts, tp_index ^ k, 0, keepdims=False) for k in range(n_tp)]
        parts = [swap(part, "tp", k) if k else part for k, part in enumerate(parts)]
        me = jnp.reshape(tp_index, (1,))
        og = assemble(me, parts, (n_seq, n_tp, seq_local, width), (n_seq, 1, seq_local, width)).reshape(n_tok, width)

        qkv = (dot_nt(hid1, wqkv_t) + bqkv_w).astype(BF16)
        ctx, lse = attn_fwd(qkv, n_seq, seq, n_pair)
        resid_x1, hid2 = proj_norm(ctx, w_all, 2 * n_ff, resid_x, b_out.astype(F32)[None], gain2, bias2)
        act, d_up, d_b_up = ffn(hid2, og, w_all, bup_w)
        out = (resid_x1 + dot_nn(act, wdown_w).astype(BF16).astype(F32) + b_down.astype(F32)).astype(BF16)

        out4 = out.reshape(n_seq, seq, width)
        parts = [lax.dynamic_slice_in_dim(out4, (tp_index ^ k) * seq_local, seq_local, 1) for k in range(n_tp)]
        parts = [swap(part, "tp", k) if k else part for k, part in enumerate(parts)]
        layer_out = assemble(me, parts, (n_seq_dp, seq_local, width), (n_seq, seq_local, width))

        core = jnp.reshape(c_index, (1,))

        def piece_of(n_rows):
            return -(-n_rows // (4 * n_tp) // 24) * 24

        def pick_pieces(g, start, n_rows):
            n = n_rows // (n_x * n_core)
            g = g.reshape(n_x, n_core, -1, width)[:, :, start:start + n]
            return g.transpose(1, 0, 2, 3).reshape(n_rows, width)

        p_ff = piece_of(n_tp * ff)
        down_theirs = swap(grad_pieces(1 - core, act, og, n_tp, p_ff, 0, 1), "cc")
        up_theirs = swap(grad_pieces(1 - core, d_up, hid2, n_tp, p_ff, 0, 1), "cc")
        ff_grads = grad_pieces(core, act, og, n_tp, p_ff, 0, 2, plus=down_theirs)
        ff_grads = grad_pieces(core, d_up, hid2, n_tp, p_ff, 1, 2, plus=up_theirs, into=ff_grads)
        ff_grads = lax.psum_scatter(ff_grads, ("tp", "xx"), scatter_dimension=0, tiled=True)
        ff_grads = lax.all_gather(ff_grads, dp, axis=0, tiled=True)

        d_resid1, d_attn, sums2 = back2(d_up, w_all, resid_x1, og, gain2)
        d_ctx = dot_nt(d_attn, wout_w).astype(BF16)
        n_small = n_tp * (b_qkv.size + ff) // width + 6
        p_pos = -(-(seq + n_small) // (24 * n_tp * n_dp)) * 24
        p_out = piece_of(wout_w.shape[0])
        spans = ((0, p_out), (p_out, p_out + piece_of(wqkv_t.shape[0])))

        def token_blocks(r, b, d_tok):
            own = own_lists(r, b)
            place = jnp.concatenate([lax.dynamic_index_in_dim(own, tp_index ^ k, 0, keepdims=False) for k in range(n_tp)])
            parts = pack((place // 8) * (8 * tiles) + place % 8, d_tok, GRAD_SLOTS)
            blocks = [swap(part, "tp", k) if k else part for k, part in enumerate(parts)]
            other = []
            for block in blocks:
                other.append(swap(block, "xx"))
            return blocks + other + [swap(block, "cc") for block in blocks + other]

        d_qkv0 = attn_bwd(qkv, ctx, d_ctx, lse, 0, seq, n_pair)
        d_tok0, *sums0 = back1(d_qkv0, wqkv_t, resid_x, d_resid1, gain1, 0, p_pos * n_tp * n_dp)
        blocks0 = token_blocks(0, 0, d_tok0)
        d_qkv1 = attn_bwd(qkv, ctx, d_ctx, lse, 1, seq, n_pair)
        d_tok1, pos_all, sums1, sums_qkv = back1(d_qkv1, wqkv_t, resid_x, d_resid1, gain1, 1, p_pos * n_tp * n_dp, earlier=sums0)
        blocks1 = token_blocks(0, 1, d_tok1)
        d_qkvs = [d_qkv0, d_qkv1]
        rest_theirs = swap(grad_rest(1 - core, ctx, d_attn, d_qkvs, hid1, n_tp, spans), "cc")

        def in_block_order(table, b):
            out = []
            for dc in range(n_core):
                for dx in range(n_x):
                    for k in range(n_tp):
                        d = (x_index ^ dx) * n_core + (c_index ^ dc)
                        out.append(lax.dynamic_index_in_dim(table, (d * n_tp + (tp_index ^ k)) * n_seq + b, 0, keepdims=False))
            return out

        def both_orders(table):
            return jnp.stack(in_block_order(table, 0) + in_block_order(table, 1))

        d_w_down, d_w_up = ff_out(ff_grads.reshape(n_dp, -1, width), n_ff, p_ff, n_x, n_core)
        blocks0[0], d_w_down, d_w_up = lax.optimization_barrier((blocks0[0], d_w_down, d_w_up))
        block_rows = both_orders(grad_lists(0))
        in_sub = sum(((block_rows >= s * sub).astype(jnp.int32) for s in range(1, n_sub)), jnp.zeros_like(block_rows))
        in_sub = block_rows - in_sub * sub
        slot = jnp.arange(GRAD_SLOTS)
        code = (((in_sub // 8) * (8 * tiles) + in_sub % 8) << 16) | ((slot // 8) * (8 * tiles) + slot % 8)
        code = code.reshape(-1)
        block_first = jnp.minimum(both_orders(first), GRAD_SLOTS).reshape(-1)
        image = accum(blocks0 + blocks1, code, block_first, sub_rows, width)
        d_emb = image.reshape(rows // 8, tiles, 8, 128).transpose(0, 2, 1, 3).reshape(rows, width)

        def more_grads(carry):
            r, table = carry
            at = rank - r * GRAD_SLOTS
            there = owned & (at >= 0) & (at < GRAD_SLOTS)
            dest = compact(at, there, jnp.where(owned, local, 0) + 1, GRAD_SLOTS)
            dest = jnp.where(dest == 0, rows, dest - 1)
            grads = jnp.concatenate(token_blocks(r, 0, d_tok0) + token_blocks(r, 1, d_tok1), axis=0).astype(F32)
            return r + 1, table.at[both_orders(dest).reshape(-1)].add(grads, mode="drop")

        _, d_emb = lax.while_loop(lambda c: c[0] < grad_rounds, more_grads, (jnp.int32(1), d_emb))

        small = jnp.concatenate([sums_qkv[0], d_b_up[0], sums1[:2].reshape(-1), sums2[:4].reshape(-1)]).reshape(-1, width)
        small = jnp.concatenate([small, jnp.zeros((pos_all.shape[0] - seq - n_small, width), F32)])
        pos_all = lax.dynamic_update_slice_in_dim(pos_all, small, seq, 0).reshape(n_tp * n_x, n_core, p_pos, width)
        pos_theirs = swap(lax.dynamic_index_in_dim(pos_all, 1 - c_index, 1, keepdims=False).reshape(-1, width), "cc")
        rest = grad_rest(core, ctx, d_attn, d_qkvs, hid1, n_tp, spans, plus=rest_theirs, tail=(pos_all, pos_theirs))
        rest = lax.psum_scatter(rest, ("tp", "xx"), scatter_dimension=0, tiled=True)
        rest_w = lax.all_gather(rest[:spans[1][1]], dp, axis=0, tiled=True)
        whole = lax.all_gather(rest[spans[1][1]:], ("tp", "xx", "cc"), axis=0, tiled=True)
        d_pos = jnp.pad(whole[:seq], ((POS_OFFSET, pos_table.shape[0] - seq - POS_OFFSET), (0, 0)))
        small = whole[seq:seq + n_small].reshape(-1)
        n_b = b_qkv.size
        d_b_qkv = lax.dynamic_slice_in_dim(small, tp_index * n_b, n_b).reshape(n_core, 3, -1, b_qkv.shape[2])
        d_b_qkv = d_b_qkv.transpose(1, 0, 2, 3).reshape(b_qkv.shape)
        d_b_up = lax.dynamic_slice_in_dim(small, n_tp * n_b + tp_index * ff, ff)
        d_gain1, d_bias1, d_gain2, d_bias2, d_b_out, d_b_down = small[n_tp * (n_b + ff):].reshape(6, width)

        d_w_out = pick_pieces(rest_w, 0, w_out.shape[0] * w_out.shape[1]).reshape(w_out.shape)
        d_w_qkv = pick_pieces(rest_w, p_out, n_b).reshape(n_core, 3, -1, w_qkv.shape[3], width).transpose(4, 1, 0, 2, 3).reshape(w_qkv.shape)
        return (layer_out, d_emb, d_pos, d_gain1, d_bias1, d_w_qkv, d_b_qkv, d_w_out,
                d_b_out, d_gain2, d_bias2, d_w_up, d_b_up, d_w_down, d_b_down)

    rep = P()
    in_specs = (P(dp, None), P("tp", None), rep, rep, rep,
                P(None, None, "tp", None), P(None, "tp", None), P("tp", None, None), rep,
                rep, rep, P(None, "tp"), P("tp"), P("tp", None), rep,
                P(dp, "tp", None))
    out_specs = (P(dp, "tp", None), P("tp", None), rep, rep, rep,
                 P(None, None, "tp", None), P(None, "tp", None), P("tp", None, None), rep,
                 rep, rep, P(None, "tp"), P("tp"), P("tp", None), rep)

    return jax.shard_map(local_step, mesh=mesh3, in_specs=in_specs, out_specs=out_specs, check_vma=False)
```

```python
import functools

import jax
import jax.numpy as jnp
from jax import lax
from jax.experimental import pallas as pl
from jax.experimental.pallas import tpu as pltpu
from jax.sharding import Mesh, PartitionSpec as P


F32 = jnp.float32
BF16 = jnp.bfloat16
MIB = 1024 * 1024
WIDEN = 32

BLK = 256


def dot_nt(a, b):
    return lax.dot_general(a, b, (((1,), (1,)), ((), ())), preferred_element_type=F32)


def dot_nn(a, b):
    return lax.dot_general(a, b, (((1,), (0,)), ((), ())), preferred_element_type=F32)


def head_only(x, head):
    half = x.shape[1] // 2
    lane = lax.broadcasted_iota(jnp.int32, x.shape, 1)
    keep = (lane < half) if head == 0 else (lane >= half)
    return jnp.where(keep, x, jnp.zeros((), x.dtype))


def attn_fwd_kernel(qkv_ref, ctx_ref, lse_ref, ctx_t):
    seq, width = ctx_ref.shape
    half = width // 2
    scale = half ** -0.5
    q2 = qkv_ref[:, 0:width] * jnp.asarray(scale, BF16)
    v_t = qkv_ref[:, 2 * width:3 * width].T
    tasks = [(head, i) for i in range(seq // BLK) for head in range(2)]

    def scores(head, i):
        return dot_nt(qkv_ref[0:(i + 1) * BLK, width:2 * width], head_only(q2[i * BLK:(i + 1) * BLK], head))

    ready = scores(*tasks[0])
    for n, (head, i) in enumerate(tasks):
        s = ready
        if n + 1 < len(tasks):
            ready = scores(*tasks[n + 1])
        lo, hi = i * BLK, (i + 1) * BLK
        v_h = v_t[head * half:(head + 1) * half, :]
        key = lax.broadcasted_iota(jnp.int32, (BLK, BLK), 0)
        qry = lax.broadcasted_iota(jnp.int32, (BLK, BLK), 1)
        diag = jnp.where(key <= qry, s[lo:hi], -1e30)
        top = jnp.max(diag, axis=0, keepdims=True)
        if i:
            top = jnp.maximum(top, jnp.max(s[0:lo], axis=0, keepdims=True))
        p_diag = jnp.exp(diag - top)
        total = jnp.sum(p_diag, axis=0, keepdims=True)
        if i:
            p_left = jnp.exp(s[0:lo] - top)
            total = total + jnp.sum(p_left, axis=0, keepdims=True)
        inv = 1.0 / total
        acc = dot_nn(v_h[:, lo:hi], (p_diag * inv).astype(BF16))
        if i:
            acc = acc + dot_nn(v_h[:, 0:lo], (p_left * inv).astype(BF16))
        ctx_t[head * half:(head + 1) * half, lo:hi] = acc
        lse_ref[head:head + 1, lo:hi] = top + jnp.log(total)
    ctx_ref[...] = ctx_t[...].T.astype(BF16)


def attn_fwd(qkv, n_seq, seq, n_pair):
    width = 128
    return pl.pallas_call(
        attn_fwd_kernel,
        grid=(n_seq, n_pair),
        in_specs=[pl.BlockSpec((seq, 3 * width), lambda b, p: (b, p))],
        out_specs=[pl.BlockSpec((seq, width), lambda b, p: (b, p)),
                   pl.BlockSpec((None, None, 2, seq), lambda b, p: (b, p, 0, 0))],
        out_shape=[jax.ShapeDtypeStruct((n_seq * seq, n_pair * width), BF16),
                   jax.ShapeDtypeStruct((n_seq, n_pair, 2, seq), F32)],
        scratch_shapes=[pltpu.VMEM((width, seq), F32)],
        name="attn_fwd",
        cost_estimate=pl.CostEstimate(flops=n_seq * n_pair * 8 * seq * seq * 256 * 10 // 16, bytes_accessed=n_seq * seq * n_pair * width * 8,
                                      transcendentals=n_seq * n_pair * seq * seq),
        compiler_params=pltpu.CompilerParams(vmem_limit_bytes=48 * 1024 * 1024),
    )(qkv)


def attn_bwd_kernel(qkv_ref, ctx_ref, dctx_ref, lse_ref, dqkv_ref, dk_t, dv_t):
    seq, width = ctx_ref.shape
    half = width // 2
    scale = half ** -0.5
    q2 = qkv_ref[:, 0:width] * jnp.asarray(scale, BF16)
    q_t = q2.T
    do_t = dctx_ref[...].T
    lse_c = jnp.concatenate([lse_ref[...], jnp.zeros((6, seq), F32)], axis=0).T
    prod = dctx_ref[...].astype(F32) * ctx_ref[...].astype(F32)
    tasks = [(head, i) for i in range(seq // BLK) for head in range(2)]

    def scores(head, i):
        lo, hi = i * BLK, (i + 1) * BLK
        return (dot_nt(head_only(q2[lo:hi], head), qkv_ref[0:hi, width:2 * width]),
                dot_nt(head_only(dctx_ref[lo:hi, :], head), qkv_ref[0:hi, 2 * width:3 * width]))

    dq = []
    ready = scores(*tasks[0])
    for n, (head, i) in enumerate(tasks):
        s, dp = ready
        if n + 1 < len(tasks):
            ready = scores(*tasks[n + 1])
        lo, hi = i * BLK, (i + 1) * BLK
        rows = slice(head * half, (head + 1) * half)
        mean = jnp.sum(head_only(prod[lo:hi], head), axis=1, keepdims=True)
        lse = lse_c[lo:hi, head:head + 1]
        qry = lax.broadcasted_iota(jnp.int32, (BLK, BLK), 0)
        key = lax.broadcasted_iota(jnp.int32, (BLK, BLK), 1)
        p_diag = jnp.where(key <= qry, jnp.exp(s[:, lo:hi] - lse), 0.0)
        ds_diag = (p_diag * (dp[:, lo:hi] - mean)).astype(BF16)
        dv_t[rows, lo:hi] = dot_nn(do_t[rows, lo:hi], p_diag.astype(BF16))
        dk_t[rows, lo:hi] = dot_nn(q_t[rows, lo:hi], ds_diag)
        dq_h = dot_nn(ds_diag, qkv_ref[lo:hi, width:2 * width])
        if i:
            p_left = jnp.exp(s[:, 0:lo] - lse)
            ds_left = (p_left * (dp[:, 0:lo] - mean)).astype(BF16)
            dv_t[rows, 0:lo] += dot_nn(do_t[rows, lo:hi], p_left.astype(BF16))
            dk_t[rows, 0:lo] += dot_nn(q_t[rows, lo:hi], ds_left)
            dq_h = dq_h + dot_nn(ds_left, qkv_ref[0:lo, width:2 * width])
        dq.append(dq_h)
        if head == 1:
            lane = lax.broadcasted_iota(jnp.int32, (BLK, width), 1)
            dqkv_ref[lo:hi, 0:width] = (jnp.where(lane < half, dq[0], dq[1]) * scale).astype(BF16)
            dq = []
    dqkv_ref[:, width:2 * width] = dk_t[...].T.astype(BF16)
    dqkv_ref[:, 2 * width:3 * width] = dv_t[...].T.astype(BF16)


def attn_bwd(qkv, ctx, dctx, lse, at, seq, n_pair):
    width = 128
    return pl.pallas_call(
        attn_bwd_kernel,
        grid=(n_pair,),
        in_specs=[pl.BlockSpec((seq, 3 * width), lambda p: (at, p)),
                  pl.BlockSpec((seq, width), lambda p: (at, p)),
                  pl.BlockSpec((seq, width), lambda p: (at, p)),
                  pl.BlockSpec((None, None, 2, seq), lambda p: (at, p, 0, 0))],
        out_specs=pl.BlockSpec((seq, 3 * width), lambda p: (0, p)),
        out_shape=jax.ShapeDtypeStruct((seq, n_pair * 3 * width), BF16),
        scratch_shapes=[pltpu.VMEM((width, seq), F32), pltpu.VMEM((width, seq), F32)],
        name="attn_bwd",
        cost_estimate=pl.CostEstimate(flops=n_pair * 20 * seq * seq * 256 * 10 // 16, bytes_accessed=seq * n_pair * width * 16,
                                      transcendentals=n_pair * seq * seq),
        compiler_params=pltpu.CompilerParams(vmem_limit_bytes=48 * 1024 * 1024),
    )(qkv, ctx, dctx, lse)


LN_EPS = 1e-5
GELU_S = 0.7978845608028654
GELU_A = 0.044715


def row_mean(v):
    return jnp.sum(v, axis=1, keepdims=True) * (1.0 / v.shape[1])


def row_stats(v):
    centered = v - row_mean(v)
    inv_std = lax.rsqrt(row_mean(centered * centered) + LN_EPS)
    return centered * inv_std, inv_std


def norm_back(d_y, x_in, gain):
    normed, inv_std = row_stats(x_in)
    d_norm = d_y * gain
    d_x = inv_std * (d_norm - row_mean(d_norm) - normed * row_mean(d_norm * normed))
    return d_x, d_y * normed


def col_sum(v):
    return jnp.sum(v, axis=0, keepdims=True)


def to_image(rows, image, base):
    tiles = rows.shape[1] // 128
    for h in range(rows.shape[0] // 8):
        for c in range(tiles):
            image[pl.ds(base + (h * tiles + c) * 8, 8), :] = rows[h * 8:(h + 1) * 8, c * 128:(c + 1) * 128]


def from_image(image, base, n_rows, width):
    tiles = width // 128
    return jnp.concatenate([jnp.concatenate([image[pl.ds(base + (h * tiles + c) * 8, 8), :] for c in range(tiles)], axis=1)
                            for h in range(n_rows // 8)], axis=0)


def pick_rows(code_ref, first, stage, image, n_rows, tiles):
    def pick(g, _):
        base = pl.multiple_of(g * 16 * tiles, 16 * tiles)
        for j in range(16):
            row = stage[pl.ds(code_ref[first + g * 16 + j], tiles, stride=8), :]
            image[pl.ds(base + (j // 8) * 8 * tiles + j % 8, tiles, stride=8), :] = row
        return 0

    lax.fori_loop(0, n_rows // 16, pick, 0)


def embed_kernel(n_blk, cap, code_ref, *refs):
    tok_refs = refs[:n_blk]
    pos_ref, gain_ref, bias_ref, x_ref, hid_ref, stage, image = refs[n_blk:]
    rows, width = x_ref.shape
    tiles = width // 128

    @pl.when(pl.program_id(0) == 0)
    def _():
        for b in range(n_blk):
            def widen(g, _, b=b):
                part = tok_refs[b][pl.ds(pl.multiple_of(g * WIDEN, WIDEN), WIDEN), :].astype(F32)
                to_image(part, stage, pl.multiple_of((b * cap + g * WIDEN) * tiles, WIDEN * tiles))
                return 0

            lax.fori_loop(0, cap // WIDEN, widen, 0)

    pick_rows(code_ref, pl.program_id(0) * rows, stage, image, rows, tiles)
    part = 64
    for i in range(rows // part):
        at = slice(i * part, (i + 1) * part)
        x = from_image(image, i * part * tiles, part, width) + pos_ref[at, :].astype(F32)
        x_ref[at, :] = x
        normed, _ = row_stats(x)
        hid_ref[at, :] = (normed * gain_ref[...] + bias_ref[...]).astype(BF16)


def embed(code, blocks, pos_rows, gain, bias, n_tok):
    cap, width = blocks[0].shape
    seq = pos_rows.shape[0]
    rows = 256
    per_seq = seq // rows
    n_blk = len(blocks)
    vec = pl.BlockSpec((1, width), lambda i: (0, 0))
    return pl.pallas_call(
        functools.partial(embed_kernel, n_blk, cap),
        grid=(n_tok // rows,),
        in_specs=[pl.BlockSpec(memory_space=pltpu.SMEM)]
        + [pl.BlockSpec((cap, width), lambda i: (0, 0), pipeline_mode=pl.Buffered(1))] * n_blk
        + [pl.BlockSpec((rows, width), lambda i: (i % per_seq, 0)), vec, vec],
        out_specs=[pl.BlockSpec((rows, width), lambda i: (i, 0))] * 2,
        out_shape=[jax.ShapeDtypeStruct((n_tok, width), F32), jax.ShapeDtypeStruct((n_tok, width), BF16)],
        scratch_shapes=[pltpu.VMEM((n_blk * cap * width // 128, 128), F32), pltpu.VMEM((rows * width // 128, 128), F32)],
        name="embed_norm",
        cost_estimate=pl.CostEstimate(flops=15_000_000_000, bytes_accessed=n_tok * width * 10, transcendentals=0),
        compiler_params=pltpu.CompilerParams(vmem_limit_bytes=48 * MIB),
    )(code, *blocks, pos_rows, gain, bias)


def pack_kernel(n_blk, code_ref, tok_ref, *refs):
    out_refs = refs[:n_blk]
    stage, image = refs[n_blk:]
    n_tok, width = tok_ref.shape
    cap = out_refs[0].shape[0]
    tiles = width // 128

    def widen(g, _):
        part = tok_ref[pl.ds(pl.multiple_of(g * WIDEN, WIDEN), WIDEN), :].astype(F32)
        to_image(part, stage, pl.multiple_of(g * WIDEN * tiles, WIDEN * tiles))
        return 0

    lax.fori_loop(0, n_tok // WIDEN, widen, 0)
    for b in range(n_blk):
        pick_rows(code_ref, b * cap, stage, image, cap, tiles)

        def narrow(g, _, b=b):
            part = from_image(image, pl.multiple_of(g * WIDEN * tiles, WIDEN * tiles), WIDEN, width)
            out_refs[b][pl.ds(pl.multiple_of(g * WIDEN, WIDEN), WIDEN), :] = part.astype(BF16)
            return 0

        lax.fori_loop(0, cap // WIDEN, narrow, 0)


def pack(code, tok, cap):
    n_tok, width = tok.shape
    n_blk = code.shape[0] // cap
    return pl.pallas_call(
        functools.partial(pack_kernel, n_blk),
        in_specs=[pl.BlockSpec(memory_space=pltpu.SMEM), pl.BlockSpec(memory_space=pltpu.VMEM)],
        out_specs=[pl.BlockSpec(memory_space=pltpu.VMEM)] * n_blk,
        out_shape=[jax.ShapeDtypeStruct((cap, width), BF16)] * n_blk,
        scratch_shapes=[pltpu.VMEM((n_tok * width // 128, 128), F32), pltpu.VMEM((cap * width // 128, 128), F32)],
        name="token_pack",
        cost_estimate=pl.CostEstimate(flops=15_000_000_000, bytes_accessed=n_tok * width * 5, transcendentals=0),
        compiler_params=pltpu.CompilerParams(vmem_limit_bytes=40 * MIB),
    )(code, tok)


def proj_kernel(c_ref, w_ref, x_ref, b_ref, gain_ref, bias_ref, x1_ref, hid_ref):
    part = x_ref.shape[0] // 2
    for i in range(2):
        at = slice(i * part, (i + 1) * part)
        x1 = x_ref[at, :] + dot_nn(c_ref[at, :], w_ref[...].reshape(c_ref.shape[1], -1)).astype(BF16).astype(F32) + b_ref[...]
        x1_ref[at, :] = x1
        normed, _ = row_stats(x1)
        hid_ref[at, :] = (normed * gain_ref[...] + bias_ref[...]).astype(BF16)


def proj_norm(ctx, w, start, x, b, gain, bias):
    n_tok, width = x.shape
    n_row = ctx.shape[1] // w.shape[0]
    rows = 512
    vec = pl.BlockSpec((1, width), lambda i: (0, 0))
    mat = pl.BlockSpec((rows, width), lambda i: (i, 0))
    return pl.pallas_call(
        proj_kernel,
        grid=(n_tok // rows,),
        in_specs=[pl.BlockSpec((rows, ctx.shape[1]), lambda i: (i, 0)), pl.BlockSpec((w.shape[0], n_row, width), lambda i: (0, start // n_row, 0)), mat, vec, vec, vec],
        out_specs=[mat, mat],
        out_shape=[jax.ShapeDtypeStruct((n_tok, width), F32), jax.ShapeDtypeStruct((n_tok, width), BF16)],
        name="proj_norm",
        cost_estimate=pl.CostEstimate(flops=2 * n_tok * ctx.shape[1] * width, bytes_accessed=n_tok * width * 12, transcendentals=0),
        compiler_params=pltpu.CompilerParams(vmem_limit_bytes=40 * MIB),
    )(ctx, w, x, b, gain, bias)


def ffn_kernel(part, h_ref, og_ref, wu_ref, wd_ref, b_ref, act_ref, dup_ref, db_ref):
    total = jnp.zeros(db_ref.shape, F32)
    for i in range(h_ref.shape[0] // part):
        at = slice(i * part, (i + 1) * part)
        z = dot_nt(h_ref[at, :], wu_ref[0]) + b_ref[...]
        d_act = dot_nt(og_ref[at, :], wd_ref[0])
        z2 = z * z
        gate = 0.5 * jnp.tanh(z * (GELU_S + (GELU_S * GELU_A) * z2)) + 0.5
        act = z * gate
        d_up = d_act * (gate + act * (1.0 - gate) * (2.0 * GELU_S + (6.0 * GELU_S * GELU_A) * z2))
        act_ref[at, :] = act.astype(BF16)
        dup_ref[at, :] = d_up.astype(BF16)
        total = total + col_sum(d_up)
    db_ref[...] = total


def ffn(hid, og, w, b_up, part=1024):
    n_tok, width = hid.shape
    ff = b_up.shape[1]
    n_piece = w.shape[0]
    bn = ff // n_piece
    whole = pl.BlockSpec((n_tok, width), lambda i: (0, 0), pipeline_mode=pl.Buffered(1))
    ospec = pl.BlockSpec((n_tok, bn), lambda i: (0, i))
    vec = pl.BlockSpec((1, bn), lambda i: (0, i))
    return pl.pallas_call(
        functools.partial(ffn_kernel, part),
        grid=(n_piece,),
        in_specs=[whole, whole, pl.BlockSpec((1, bn, width), lambda i: (i, 0, 0)), pl.BlockSpec((1, bn, width), lambda i: (i, 1, 0)), vec],
        out_specs=[ospec, ospec, vec],
        out_shape=[jax.ShapeDtypeStruct((n_tok, ff), BF16), jax.ShapeDtypeStruct((n_tok, ff), BF16), jax.ShapeDtypeStruct((1, ff), F32)],
        name="ffn",
        cost_estimate=pl.CostEstimate(flops=4 * n_tok * ff * width, bytes_accessed=4 * n_tok * ff + 4 * ff * width, transcendentals=n_tok * ff),
        compiler_params=pltpu.CompilerParams(vmem_limit_bytes=48 * MIB),
    )(hid, og, w, w, b_up)


def back2_kernel(dup_ref, w_ref, x1_ref, og_ref, gain_ref, dr_ref, da_ref, sums_ref):
    @pl.when(pl.program_id(0) == 0)
    def _():
        sums_ref[...] = jnp.zeros(sums_ref.shape, F32)

    n_part = 2
    part = dr_ref.shape[0] // n_part
    w = w_ref[...].reshape(dup_ref.shape[1], -1)
    d_ys = [dot_nn(dup_ref[i * part:(i + 1) * part, :], w) for i in range(n_part)]
    for i in range(n_part):
        at = slice(i * part, (i + 1) * part)
        d_y = d_ys[i].astype(BF16).astype(F32)
        d_x, d_gain = norm_back(d_y, x1_ref[at, :], gain_ref[...])
        og = og_ref[at, :].astype(F32)
        d_resid = og + d_x
        dr_ref[at, :] = d_resid
        da_ref[at, :] = d_resid.astype(BF16)
        sums_ref[0:1, :] += col_sum(d_gain)
        sums_ref[1:2, :] += col_sum(d_y)
        sums_ref[2:3, :] += col_sum(d_resid)
        sums_ref[3:4, :] += col_sum(og)


def back2(d_up, w, x1, og, gain):
    n_tok, width = x1.shape
    ff = d_up.shape[1]
    rows = 256
    mat = pl.BlockSpec((rows, width), lambda i: (i, 0))
    return pl.pallas_call(
        back2_kernel,
        grid=(n_tok // rows,),
        in_specs=[pl.BlockSpec((rows, ff), lambda i: (i, 0)), pl.BlockSpec((w.shape[0], ff // w.shape[0], width), lambda i: (0, 0, 0), pipeline_mode=pl.Buffered(1)),
                  mat, mat, pl.BlockSpec((1, width), lambda i: (0, 0))],
        out_specs=[mat, mat, pl.BlockSpec((8, width), lambda i: (0, 0))],
        out_shape=[jax.ShapeDtypeStruct((n_tok, width), F32), jax.ShapeDtypeStruct((n_tok, width), BF16), jax.ShapeDtypeStruct((8, width), F32)],
        name="ffn_back",
        cost_estimate=pl.CostEstimate(flops=2 * n_tok * ff * width, bytes_accessed=2 * n_tok * ff + n_tok * width * 12, transcendentals=0),
        compiler_params=pltpu.CompilerParams(vmem_limit_bytes=48 * MIB),
    )(d_up, w, x1, og, gain)


def back1_kernel(dq_ref, w_ref, x_ref, dr_ref, gain_ref, *refs):
    tok_ref, pos_ref, sums_ref, bsum_ref = refs[-4:]
    before_refs = refs[:-4]

    @pl.when(pl.program_id(0) == 0)
    def _():
        sums_ref[...] = before_refs[1][...] if before_refs else jnp.zeros(sums_ref.shape, F32)
        bsum_ref[...] = before_refs[2][...] if before_refs else jnp.zeros(bsum_ref.shape, F32)

    n_part = 2
    part = tok_ref.shape[0] // n_part
    d_ys = [dot_nn(dq_ref[i * part:(i + 1) * part, :], w_ref[...]) for i in range(n_part)]
    for i in range(n_part):
        at = slice(i * part, (i + 1) * part)
        d_y = d_ys[i].astype(BF16).astype(F32)
        d_x, d_gain = norm_back(d_y, x_ref[at, :], gain_ref[...])
        d_resid = dr_ref[at, :] + d_x
        tok_ref[at, :] = d_resid.astype(BF16)
        pos_ref[at, :] = before_refs[0][at, :] + d_resid if before_refs else d_resid
        sums_ref[0:1, :] += col_sum(d_gain)
        sums_ref[1:2, :] += col_sum(d_y)
        bsum_ref[0:1, :] += col_sum(dq_ref[at, :].astype(F32))


def back1(d_qkv, w_qkv, x, d_resid1, gain, at, pos_rows, earlier=None):
    seq, n_cols = d_qkv.shape
    width = x.shape[1]
    rows = 256
    steps = seq // rows
    mat = pl.BlockSpec((rows, width), lambda i: (at * steps + i, 0))
    out = pl.BlockSpec((rows, width), lambda i: (i, 0))
    few = [pl.BlockSpec((8, width), lambda i: (0, 0)), pl.BlockSpec((8, n_cols), lambda i: (0, 0))]
    return pl.pallas_call(
        back1_kernel,
        grid=(steps,),
        in_specs=[pl.BlockSpec((rows, n_cols), lambda i: (i, 0)),
                  pl.BlockSpec((n_cols, width), lambda i: (0, 0), pipeline_mode=pl.Buffered(1)),
                  mat, mat, pl.BlockSpec((1, width), lambda i: (0, 0))] + ([out] + few if earlier else []),
        out_specs=[out, out] + few,
        out_shape=[jax.ShapeDtypeStruct((seq, width), BF16), jax.ShapeDtypeStruct((pos_rows, width), F32),
                   jax.ShapeDtypeStruct((8, width), F32), jax.ShapeDtypeStruct((8, n_cols), F32)],
        name="qkv_back",
        cost_estimate=pl.CostEstimate(flops=2 * seq * n_cols * width, bytes_accessed=2 * seq * n_cols + seq * width * 12, transcendentals=0),
        compiler_params=pltpu.CompilerParams(vmem_limit_bytes=48 * MIB),
    )(d_qkv, w_qkv, x, d_resid1, gain, *(earlier or ()))


def pieces_out_kernel(n_in, spans, me_ref, *refs):
    out_refs = refs[n_in:]
    for p in range(n_in):
        @pl.when(pl.program_id(0) == p)
        def _(p=p):
            for (start, n, turned), out_ref in zip(spans, out_refs):
                part = refs[p][start:start + n, :]
                out_ref[...] = part.T if turned else part


def pieces_out(me, pieces, spans):
    rows, width = pieces[0].shape
    n_in = len(pieces)

    def place(p, m):
        return (m[1] ^ (p // 2)) * 2 + (m[0] ^ (p % 2))

    out_specs, out_shape = [], []
    for start, n, turned in spans:
        if turned:
            out_specs.append(pl.BlockSpec((width, n), lambda p, m: (0, place(p, m))))
            out_shape.append(jax.ShapeDtypeStruct((width, n_in * n), F32))
        else:
            out_specs.append(pl.BlockSpec((n, width), lambda p, m: (place(p, m), 0)))
            out_shape.append(jax.ShapeDtypeStruct((n_in * n, width), F32))
    return pl.pallas_call(
        functools.partial(pieces_out_kernel, n_in, spans),
        grid_spec=pltpu.PrefetchScalarGridSpec(
            num_scalar_prefetch=1, grid=(n_in,),
            in_specs=[pl.BlockSpec((rows, width), lambda p, m: (0, 0), pipeline_mode=pl.Buffered(1))] * n_in,
            out_specs=out_specs),
        out_shape=out_shape,
        name="grads_out",
        cost_estimate=pl.CostEstimate(flops=8_000_000_000, bytes_accessed=n_in * rows * width * 8, transcendentals=0),
        compiler_params=pltpu.CompilerParams(vmem_limit_bytes=32 * MIB),
    )(me, *pieces)


def assemble_kernel(n, me_ref, *refs):
    out_ref = refs[n]
    k = me_ref[0] ^ pl.program_id(0)
    for j in range(n):
        @pl.when(k == j)
        def _(j=j):
            out_ref[...] = refs[j][...].reshape(out_ref.shape)


def assemble(me, parts, out_shape, block):
    at = 1 if len(out_shape) == 4 else 0
    return pl.pallas_call(
        functools.partial(assemble_kernel, len(parts)),
        grid_spec=pltpu.PrefetchScalarGridSpec(
            num_scalar_prefetch=1, grid=(len(parts),),
            in_specs=[pl.BlockSpec(p.shape, lambda i, m: (0, 0, 0), pipeline_mode=pl.Buffered(1)) for p in parts],
            out_specs=pl.BlockSpec(block, lambda i, m: tuple(i if d == at else 0 for d in range(len(block))))),
        out_shape=jax.ShapeDtypeStruct(out_shape, parts[0].dtype),
        name="assemble",
        cost_estimate=pl.CostEstimate(flops=4_000_000_000, bytes_accessed=16 * MIB, transcendentals=0),
        compiler_params=pltpu.CompilerParams(vmem_limit_bytes=24 * MIB),
    )(me, *parts)


LANES = 128


def accum_kernel(n_block, cap, sub_rows, width, where_ref, first_ref, *refs):
    tok_refs = refs[:n_block]
    out_ref = refs[n_block]
    n_sub = len(sub_rows)
    acc = refs[n_block + 1:n_block + 1 + n_sub]
    buf, stage, in_sem, out_sem = refs[n_block + 1 + n_sub:]
    tiles = width // LANES
    group = 8 * tiles

    def fetch(block, n):
        return pltpu.make_async_copy(tok_refs[n], buf.at[block % 2], in_sem.at[block % 2])

    def fetch_next(block):
        for n in range(n_block):
            @pl.when(block == n)
            def _(n=n):
                fetch(block, n).start()

    fetch_next(0)
    for s in range(n_sub):
        def clear(i, _, s=s):
            acc[s][pl.ds(pl.multiple_of(i * group, group), group), :] = jnp.zeros((group, LANES), F32)
            return 0

        lax.fori_loop(0, sub_rows[s] // 8, clear, 0)

    def add_rows(s, slot, n):
        codes = [where_ref[slot + j] for j in range(n)]
        at = [code >> 16 for code in codes]
        rows = [stage[pl.ds(code & 0xffff, tiles, stride=8), :] for code in codes]
        sums = [acc[s][pl.ds(a, tiles, stride=8), :] for a in at]
        for j in range(n):
            for i in range(j):
                sums[j] = jnp.where(at[i] == at[j], sums[i], sums[j])
            sums[j] = sums[j] + rows[j]
        for j in range(n):
            acc[s][pl.ds(at[j], tiles, stride=8), :] = sums[j]

    def add_block(block, _):
        fetch_next(block + 1)
        fetch(block, 0).wait()

        def widen(g, _):
            rows = buf[block % 2, pl.ds(pl.multiple_of(g * WIDEN, WIDEN), WIDEN), :].astype(F32)
            base = pl.multiple_of(g * (WIDEN // 8) * group, (WIDEN // 8) * group)
            for h in range(WIDEN // 8):
                for c in range(tiles):
                    stage[pl.ds(base + h * group + c * 8, 8), :] = rows[h * 8:(h + 1) * 8, c * LANES:(c + 1) * LANES]
            return 0

        lax.fori_loop(0, cap // WIDEN, widen, 0)

        starts = [first_ref[block * (n_sub + 1) + s] for s in range(n_sub + 1)]
        counts = [starts[s + 1] - starts[s] for s in range(n_sub)]
        both = functools.reduce(jnp.minimum, counts) // 2
        begin = [block * cap + starts[s] for s in range(n_sub)]

        def together(i, _):
            for s in range(n_sub):
                add_rows(s, begin[s] + 2 * i, 2)
            return 0

        lax.fori_loop(0, both, together, 0)
        for s in range(n_sub):
            fours = (counts[s] - 2 * both) // 4

            def alone(i, _, s=s):
                add_rows(s, begin[s] + 2 * both + 4 * i, 4)
                return 0

            lax.fori_loop(0, fours, alone, 0)

            def single(i, _, s=s):
                add_rows(s, begin[s] + i, 1)
                return 0

            lax.fori_loop(2 * both + 4 * fours, counts[s], single, 0)
        return 0

    lax.fori_loop(0, n_block, add_block, 0)
    done = 0
    copies = []
    for s in range(n_sub):
        n = sub_rows[s] * tiles
        copies.append(pltpu.make_async_copy(acc[s], out_ref.at[pl.ds(done, n), :], out_sem.at[s]))
        copies[-1].start()
        done += n
    for c in copies:
        c.wait()


def accum(tok_blocks, code, first, sub_rows, width):
    n_block = len(tok_blocks)
    cap = tok_blocks[0].shape[0]
    n_sub = len(sub_rows)
    tiles = width // LANES
    return pl.pallas_call(
        functools.partial(accum_kernel, n_block, cap, sub_rows, width),
        in_specs=[pl.BlockSpec(memory_space=pltpu.SMEM), pl.BlockSpec(memory_space=pltpu.SMEM)]
        + [pl.BlockSpec(memory_space=pl.ANY)] * n_block,
        out_specs=pl.BlockSpec(memory_space=pl.ANY),
        out_shape=jax.ShapeDtypeStruct((sum(sub_rows) * tiles, LANES), F32),
        scratch_shapes=[pltpu.VMEM((r * tiles, LANES), F32) for r in sub_rows]
        + [pltpu.VMEM((2, cap, width), BF16), pltpu.VMEM((cap * tiles, LANES), F32),
           pltpu.SemaphoreType.DMA((2,)), pltpu.SemaphoreType.DMA((n_sub,))],
        name="table_accum",
        cost_estimate=pl.CostEstimate(flops=50_000_000_000, bytes_accessed=100_000_000, transcendentals=0),
        compiler_params=pltpu.CompilerParams(vmem_limit_bytes=63 * 1024 * 1024),
    )(code, first, *tok_blocks)


def dot_tn(a, b):
    return lax.dot_general(a, b, (((0,), (0,)), ((), ())), preferred_element_type=F32)


def grad_kernel(has_plus, core_ref, a_ref, b_ref, *refs):
    out_ref = refs[-1]
    n = a_ref.shape[1]
    g = dot_tn(a_ref[...], b_ref[...])
    out_ref[0:n, :] = g + refs[0][0:n, :] if has_plus else g
    if out_ref.shape[0] > n:
        out_ref[n:, :] = jnp.zeros((out_ref.shape[0] - n, out_ref.shape[1]), F32)


def grad_pieces(core, a, b, n_tp, piece, which, n_which, plus=None, into=None):
    n_tok, n_cols = a.shape
    width = b.shape[1]
    bn = n_cols // (4 * n_tp)
    out_spec = pl.BlockSpec((piece, width), lambda p, c: (n_which * p + which, 0))
    in_specs = [pl.BlockSpec((n_tok, bn), lambda p, c: (0, 4 * (p // 2) + 2 * c[0] + p % 2)),
                pl.BlockSpec((n_tok, width), lambda p, c: (0, 0), pipeline_mode=pl.Buffered(1))]
    args = [a, b]
    if plus is not None:
        in_specs.append(pl.BlockSpec((piece, width), lambda p, c: (p, 0)))
        args.append(plus)
    if into is not None:
        in_specs.append(pl.BlockSpec(memory_space=pl.ANY))
        args.append(into)
    return pl.pallas_call(
        functools.partial(grad_kernel, plus is not None),
        grid_spec=pltpu.PrefetchScalarGridSpec(num_scalar_prefetch=1, grid=(2 * n_tp,), in_specs=in_specs, out_specs=out_spec),
        out_shape=jax.ShapeDtypeStruct((2 * n_tp * n_which * piece, width), F32),
        input_output_aliases={} if into is None else {len(args): 0},
        name="weight_grad",
        cost_estimate=pl.CostEstimate(flops=n_tok * n_cols * width, bytes_accessed=n_tok * (n_cols + 2 * width) + 2 * n_cols * width,
                                      transcendentals=0),
        compiler_params=pltpu.CompilerParams(vmem_limit_bytes=32 * MIB),
    )(core, *args)


def grad_rest_kernel(spans, last, n_a2, core_ref, a1_ref, b1_ref, b2_ref, *refs):
    a2_refs, refs, out_ref = refs[:n_a2], refs[n_a2:-1], refs[-1]
    plus = refs[0] if refs else None
    piece, piece_in = out_ref.shape[0] // 2, (plus.shape[0] // 2 if refs else 0)
    rows = b2_ref.shape[0] // n_a2
    for which, (start, stop) in enumerate(spans):
        half = (a2_refs[0] if which else a1_ref).shape[1] // 2
        for i in range(0, 2 * half, 128):
            cols = slice(i, i + 128)
            if which:
                g = sum(dot_tn(a_ref[:, cols], b2_ref[n * rows:(n + 1) * rows, :]) for n, a_ref in enumerate(a2_refs))
            else:
                g = dot_tn(a1_ref[:, cols], b1_ref[...])
            for x in range(2):
                lo, hi = max(i, x * half), min(i + 128, (x + 1) * half)
                if lo < hi:
                    to = lo - x * half + start
                    part = g[lo - i:hi - i]
                    if plus is not None:
                        part = part + plus[x * piece_in + to:x * piece_in + to + hi - lo, :]
                    out_ref[x * piece + to:x * piece + to + hi - lo, :] = part
        for x in range(2):
            if stop > start + half:
                out_ref[x * piece + start + half:x * piece + stop, :] = jnp.zeros((stop - start - half, out_ref.shape[1]), F32)
    if last:
        for x in range(2):
            out_ref[x * piece + spans[-1][1]:(x + 1) * piece, :] = refs[1][x, 0] + refs[2][x * last:(x + 1) * last, :]


def grad_rest(core, a1, b1, a2, b2, n_tp, spans, plus=None, tail=None):
    n_tok, width = b1.shape
    last = tail[0].shape[2] if tail else 0
    piece = spans[-1][1] + last
    whole = pl.BlockSpec((n_tok, width), lambda t, c: (0, 0), pipeline_mode=pl.Buffered(1))
    cols = [pl.BlockSpec((a.shape[0], a.shape[1] // (2 * n_tp)), lambda t, c: (0, 2 * t + c[0])) for a in (a1, *a2)]
    in_specs, args = [cols[0], whole, whole] + cols[1:], [a1, b1, b2, *a2]
    if plus is not None:
        in_specs.append(pl.BlockSpec((plus.shape[0] // n_tp, width), lambda t, c: (t, 0)))
        args.append(plus)
    if tail:
        in_specs.append(pl.BlockSpec((2, 1, last, width), lambda t, c: (t, c[0], 0, 0)))
        in_specs.append(pl.BlockSpec((2 * last, width), lambda t, c: (t, 0)))
        args += tail
    n_cols = a1.shape[1] + a2[0].shape[1]
    return pl.pallas_call(
        functools.partial(grad_rest_kernel, spans, last, len(a2)),
        grid_spec=pltpu.PrefetchScalarGridSpec(num_scalar_prefetch=1, grid=(n_tp,), in_specs=in_specs,
                                               out_specs=pl.BlockSpec((2 * piece, width), lambda t, c: (t, 0))),
        out_shape=jax.ShapeDtypeStruct((2 * n_tp * piece, width), F32),
        name="weight_grads",
        cost_estimate=pl.CostEstimate(flops=n_tok * n_cols * width, bytes_accessed=n_tok * (n_cols + 4 * width) + 2 * n_cols * width,
                                      transcendentals=0),
        compiler_params=pltpu.CompilerParams(vmem_limit_bytes=40 * MIB),
    )(core, *args)


POS_OFFSET = 2
SLOTS = 704
GRAD_SLOTS = 384
LOW = 32


def before(n):
    return (lax.broadcasted_iota(jnp.int32, (n, n), 1) < lax.broadcasted_iota(jnp.int32, (n, n), 0)).astype(BF16)


def rank_in_class(hot):
    n_blk, n_tok, n_cls = hot.shape
    ones = hot.astype(BF16).reshape(n_blk, n_tok // 128, 128, n_cls)
    within = jnp.einsum("ij,bnjk->bnik", before(128), ones, preferred_element_type=F32)
    sums = jnp.sum(ones.astype(F32), axis=2)
    ahead = jnp.einsum("mn,bnk->bmk", before(n_tok // 128), sums.astype(BF16), preferred_element_type=F32)
    rank = jnp.sum((within + ahead[:, :, None, :]) * ones.astype(F32), axis=3)
    return rank.reshape(n_blk, n_tok).astype(jnp.int32), jnp.sum(sums, axis=1).astype(jnp.int32)


def compact(rank, valid, value, slots):
    n_high = slots // LOW
    high = ((rank // LOW)[:, :, None] == jnp.arange(n_high)) & valid[:, :, None]
    low = ((rank % LOW)[:, :, None] == jnp.arange(LOW)).astype(F32)
    parts = jnp.concatenate([low * (value // 128).astype(F32)[:, :, None], low * (value % 128).astype(F32)[:, :, None]], axis=2)
    out = jnp.einsum("bjh,bjl->bhl", high.astype(BF16), parts.astype(BF16), preferred_element_type=F32).astype(jnp.int32)
    return (out[:, :, :LOW] * 128 + out[:, :, LOW:]).reshape(rank.shape[0], slots)


def solution(mesh):
    n_tp, n_dp = mesh.shape["tp"], mesh.shape["dp"]
    n_core = 2
    n_x = n_dp // n_core
    mesh3 = Mesh(mesh.devices.reshape(n_tp, n_x, n_core), ("tp", "xx", "cc"))
    dp = ("xx", "cc")
    tp_swap = [[(i, i ^ k) for i in range(n_tp)] for k in range(n_tp)]
    pair = [(0, 1), (1, 0)]

    def local_step(tok_ids, emb_table, pos_table, ln1_gain, ln1_bias, w_qkv, b_qkv, w_out, b_out,
                   ln2_gain, ln2_bias, w_up, b_up, w_down, b_down, out_grad):
        tp_index, x_index, c_index = lax.axis_index("tp"), lax.axis_index("xx"), lax.axis_index("cc")
        dp_index = x_index * n_core + c_index
        n_seq_dp, seq = tok_ids.shape
        n_seq = n_seq_dp // n_tp
        n_tok = n_seq * seq
        rows, width = emb_table.shape
        n_sub = 4
        sub = -(-rows // n_sub // 8) * 8
        sub_rows = (sub,) * (n_sub - 1) + (rows - (n_sub - 1) * sub,)
        seq_local = seq // n_tp
        ff = w_up.shape[1]
        gain1, bias1 = ln1_gain.astype(F32)[None], ln1_bias.astype(F32)[None]
        gain2, bias2 = ln2_gain.astype(F32)[None], ln2_bias.astype(F32)[None]

        def half(w, axis):
            n = w.shape[axis] // n_core
            return lax.dynamic_slice_in_dim(w, c_index * n, n, axis)

        def gather_rows(w):
            return lax.all_gather(w, ("tp", "cc"), axis=0, tiled=True)

        def swap(v, axis, k=1):
            return lax.ppermute(v, axis, tp_swap[k] if axis == "tp" else pair)

        def by_owner(parts):
            out = []
            for p in range(n_tp):
                k = tp_index ^ p
                out.append(jnp.where(k < 2, jnp.where(k == 0, parts[0], parts[1]), jnp.where(k == 2, parts[2], parts[3])))
            return out

        ids_all = lax.all_gather(tok_ids, dp, axis=0, tiled=True)
        ids_all, w_up, w_down, w_out, b_qkv, b_up = lax.optimization_barrier((ids_all, w_up, w_down, w_out, b_qkv, b_up))

        wqkv_t = gather_rows(jnp.transpose(half(w_qkv, 2), (1, 2, 3, 0)).reshape(-1, width))
        n_ff, n_out = ff // n_dp, w_out.shape[0] * w_out.shape[1] // n_dp

        def quarter(w, axis):
            n = w.shape[axis] // n_dp
            return lax.dynamic_slice_in_dim(w, dp_index * n, n, axis)

        own_w = jnp.concatenate([quarter(w_up, 1).T, quarter(w_down, 0), quarter(w_out.reshape(-1, width), 0)])
        w_all = lax.all_gather(own_w, ("tp", "xx", "cc"), axis=0, tiled=True)
        w_all = w_all.reshape(n_tp * n_dp, 2 * n_ff + n_out, width)
        wdown_w = w_all[:, n_ff:2 * n_ff].reshape(-1, width)
        wout_w = w_all[:, 2 * n_ff:].reshape(-1, width)
        n_pair = wqkv_t.shape[0] // (3 * 128)
        own_bias = jnp.concatenate([b_qkv.reshape(3, n_core, -1, b_qkv.shape[2]).transpose(1, 0, 2, 3).reshape(-1), b_up])
        biases = jnp.stack(by_owner([swap(own_bias, "tp", k) if k else own_bias for k in range(n_tp)]))
        bqkv_w = biases[:, :-ff].reshape(-1).astype(F32)
        bup_w = biases[:, -ff:].reshape(1, -1).astype(F32)
        pos_rows = lax.slice_in_dim(pos_table, POS_OFFSET, POS_OFFSET + seq, axis=0)

        local = ids_all - tp_index * rows
        sub_of = sum(((local >= s * sub).astype(jnp.int32) for s in range(1, n_sub)), jnp.zeros_like(local))
        owned = (local >= 0) & (local < rows)
        hot = owned[:, :, None] & (sub_of[:, :, None] == jnp.arange(n_sub))
        rank, counts = rank_in_class(hot)
        first = jnp.concatenate([jnp.zeros_like(counts[:, :1]), jnp.cumsum(counts, axis=1)], axis=1)
        rank = rank + jnp.sum(jnp.where(hot, first[:, None, :-1], 0), axis=2)
        owner_counts = jnp.stack([jnp.sum(((ids_all >= o * rows) & (ids_all < (o + 1) * rows)).astype(jnp.int32), axis=1)
                                  for o in range(n_tp)])
        grad_rounds = (jnp.max(owner_counts) + GRAD_SLOTS - 1) // GRAD_SLOTS
        rounds = (jnp.max(jnp.sum(owner_counts.reshape(n_tp, -1, n_seq), axis=2)) + SLOTS - 1) // SLOTS

        def after_first(ranks, totals):
            return (ranks + (jnp.cumsum(totals, axis=1) - totals)[:, :, None]).reshape(ranks.shape[0], -1)

        def grad_lists(r):
            at = rank - r * GRAD_SLOTS
            return compact(at, owned & (at >= 0) & (at < GRAD_SLOTS), jnp.where(owned, local, 0), GRAD_SLOTS)

        my_rank = lax.dynamic_slice_in_dim(rank, dp_index * n_seq_dp, n_seq_dp, 0)
        my_total = lax.dynamic_slice_in_dim(first[:, -1], dp_index * n_seq_dp, n_seq_dp, 0)
        my_rank = after_first(my_rank.reshape(n_tp, n_seq, seq), my_total.reshape(n_tp, n_seq))
        my_owned = lax.dynamic_slice_in_dim(owned, dp_index * n_seq_dp, n_seq_dp, 0).reshape(n_tp, n_tok)
        my_local = lax.dynamic_slice_in_dim(local, dp_index * n_seq_dp, n_seq_dp, 0).reshape(n_tp, n_tok)

        def lists(r):
            at = my_rank - r * SLOTS
            return compact(at, my_owned & (at >= 0) & (at < SLOTS), jnp.where(my_owned, my_local, 0), SLOTS)

        own_ids = lax.dynamic_slice_in_dim(ids_all, dp_index * n_seq_dp + tp_index * n_seq, n_seq, 0)
        own_owner = sum(((own_ids >= o * rows).astype(jnp.int32) for o in range(1, n_tp)), jnp.zeros_like(own_ids))
        own_local = own_ids - own_owner * rows
        own_sub = sum(((own_local >= s * sub).astype(jnp.int32) for s in range(1, n_sub)), jnp.zeros_like(own_ids))
        own_hot = (own_owner * n_sub + own_sub)[:, :, None] == jnp.arange(n_tp * n_sub)
        own_rank, own_counts = rank_in_class(own_hot)
        own_counts = own_counts.reshape(n_seq, n_tp, n_sub)
        own_first = jnp.cumsum(own_counts, axis=2) - own_counts
        own_rank = own_rank + jnp.sum(jnp.where(own_hot, own_first.reshape(n_seq, 1, -1), 0), axis=2)
        own_total = jnp.sum(own_counts, axis=2)
        own_shift = jnp.cumsum(own_total, axis=0) - own_total
        own_place = sum(jnp.where(own_owner == o, own_shift[:, o:o + 1], 0) for o in range(n_tp))
        own_place = (own_place + own_rank).reshape(-1)

        def own_lists(r, b):
            at = jnp.broadcast_to(own_rank[b] - r * GRAD_SLOTS, (n_tp, seq))
            mine = own_owner[b] == jnp.arange(n_tp)[:, None]
            return compact(at, mine & (at >= 0) & (at < GRAD_SLOTS), jnp.broadcast_to(jnp.arange(seq), (n_tp, seq)), GRAD_SLOTS)

        tiles = width // 128

        def rows_here(r, my_lists):
            index = [lax.dynamic_index_in_dim(my_lists, tp_index ^ k, 0, keepdims=False) for k in range(n_tp)]
            first_two = jnp.take(emb_table, jnp.concatenate([index[3], index[1]]), axis=0, mode="clip")
            rest, first_two = lax.optimization_barrier((jnp.concatenate([index[2], index[0]]), first_two))
            last_two = jnp.take(emb_table, rest, axis=0, mode="clip")
            sent = [last_two[SLOTS:], first_two[SLOTS:], last_two[:SLOTS], first_two[:SLOTS]]
            got = list(sent)
            for k in range(1, n_tp):
                got[k] = swap(sent[k], "tp", k)
            at = own_place - r * SLOTS
            valid = (at >= 0) & (at < SLOTS)
            return got, jnp.where(valid, (own_owner.reshape(-1) ^ tp_index) * SLOTS + at, 0), valid

        def norm_rows(x):
            normed, _ = row_stats(x)
            return (normed * gain1 + bias1).astype(BF16)

        got0, place0, _ = rows_here(0, lists(0))
        code0 = (place0 // 8) * (8 * tiles) + place0 % 8
        got0, out_grad = lax.optimization_barrier((got0, out_grad))
        resid_x, hid1 = embed(code0, got0, pos_rows, gain1, bias1, n_tok)

        def more_rows(carry):
            r, x, _ = carry
            got, place, valid = rows_here(r, lists(r))
            new = jnp.take(jnp.concatenate(got), place, axis=0, mode="clip").astype(F32) + jnp.tile(pos_rows.astype(F32), (n_seq, 1))
            x = jnp.where(valid[:, None], new, x)
            return r + 1, x, norm_rows(x)

        _, resid_x, hid1 = lax.while_loop(lambda c: c[0] < rounds, more_rows, (jnp.int32(1), resid_x, hid1))

        og_parts = out_grad.reshape(n_tp, n_seq, seq_local, width)
        parts = [lax.dynamic_index_in_dim(og_parts, tp_index ^ k, 0, keepdims=False) for k in range(n_tp)]
        parts = [swap(part, "tp", k) if k else part for k, part in enumerate(parts)]
        me = jnp.reshape(tp_index, (1,))
        og = assemble(me, parts, (n_seq, n_tp, seq_local, width), (n_seq, 1, seq_local, width)).reshape(n_tok, width)

        qkv = (dot_nt(hid1, wqkv_t) + bqkv_w).astype(BF16)
        ctx, lse = attn_fwd(qkv, n_seq, seq, n_pair)
        resid_x1, hid2 = proj_norm(ctx, w_all, 2 * n_ff, resid_x, b_out.astype(F32)[None], gain2, bias2)
        act, d_up, d_b_up = ffn(hid2, og, w_all, bup_w)
        out = (resid_x1 + dot_nn(act, wdown_w).astype(BF16).astype(F32) + b_down.astype(F32)).astype(BF16)

        out4 = out.reshape(n_seq, seq, width)
        parts = [lax.dynamic_slice_in_dim(out4, (tp_index ^ k) * seq_local, seq_local, 1) for k in range(n_tp)]
        parts = [swap(part, "tp", k) if k else part for k, part in enumerate(parts)]
        layer_out = assemble(me, parts, (n_seq_dp, seq_local, width), (n_seq, seq_local, width))

        core = jnp.reshape(c_index, (1,))

        def piece_of(n_rows):
            return -(-n_rows // (4 * n_tp) // 24) * 24

        def every_piece(g):
            other = swap(g, "xx")
            return [g, other, swap(g, "cc"), swap(other, "cc")]

        x_and_core = jnp.stack([x_index, c_index])

        p_ff = piece_of(n_tp * ff)
        down_theirs = swap(grad_pieces(1 - core, act, og, n_tp, p_ff, 0, 1), "cc")
        up_theirs = swap(grad_pieces(1 - core, d_up, hid2, n_tp, p_ff, 0, 1), "cc")
        ff_grads = grad_pieces(core, act, og, n_tp, p_ff, 0, 2, plus=down_theirs)
        ff_grads = grad_pieces(core, d_up, hid2, n_tp, p_ff, 1, 2, plus=up_theirs, into=ff_grads)
        ff_grads = lax.psum_scatter(ff_grads, ("tp", "xx"), scatter_dimension=0, tiled=True)
        ff_grads = every_piece(ff_grads)

        d_resid1, d_attn, sums2 = back2(d_up, w_all, resid_x1, og, gain2)
        d_ctx = dot_nt(d_attn, wout_w).astype(BF16)
        n_small = n_tp * (b_qkv.size + ff) // width + 6
        p_pos = -(-(seq + n_small) // (24 * n_tp * n_dp)) * 24
        p_out = piece_of(wout_w.shape[0])
        spans = ((0, p_out), (p_out, p_out + piece_of(wqkv_t.shape[0])))

        def token_blocks(r, b, d_tok):
            own = own_lists(r, b)
            place = jnp.concatenate([lax.dynamic_index_in_dim(own, tp_index ^ k, 0, keepdims=False) for k in range(n_tp)])
            parts = pack((place // 8) * (8 * tiles) + place % 8, d_tok, GRAD_SLOTS)
            blocks = [swap(part, "tp", k) if k else part for k, part in enumerate(parts)]
            other = []
            for block in blocks:
                other.append(swap(block, "xx"))
            return blocks + other + [swap(block, "cc") for block in blocks + other]

        d_qkv0 = attn_bwd(qkv, ctx, d_ctx, lse, 0, seq, n_pair)
        d_tok0, *sums0 = back1(d_qkv0, wqkv_t, resid_x, d_resid1, gain1, 0, p_pos * n_tp * n_dp)
        blocks0 = token_blocks(0, 0, d_tok0)
        d_qkv1 = attn_bwd(qkv, ctx, d_ctx, lse, 1, seq, n_pair)
        d_tok1, pos_all, sums1, sums_qkv = back1(d_qkv1, wqkv_t, resid_x, d_resid1, gain1, 1, p_pos * n_tp * n_dp, earlier=sums0)
        blocks1 = token_blocks(0, 1, d_tok1)
        d_qkvs = [d_qkv0, d_qkv1]
        rest_theirs = swap(grad_rest(1 - core, ctx, d_attn, d_qkvs, hid1, n_tp, spans), "cc")

        def in_block_order(table, b):
            out = []
            for dc in range(n_core):
                for dx in range(n_x):
                    for k in range(n_tp):
                        d = (x_index ^ dx) * n_core + (c_index ^ dc)
                        out.append(lax.dynamic_index_in_dim(table, (d * n_tp + (tp_index ^ k)) * n_seq + b, 0, keepdims=False))
            return out

        def both_orders(table):
            return jnp.stack(in_block_order(table, 0) + in_block_order(table, 1))

        d_w_down, d_w_up = pieces_out(x_and_core, ff_grads, ((0, n_ff, False), (p_ff, n_ff, True)))
        block_rows = both_orders(grad_lists(0))
        in_sub = sum(((block_rows >= s * sub).astype(jnp.int32) for s in range(1, n_sub)), jnp.zeros_like(block_rows))
        in_sub = block_rows - in_sub * sub
        slot = jnp.arange(GRAD_SLOTS)
        code = (((in_sub // 8) * (8 * tiles) + in_sub % 8) << 16) | ((slot // 8) * (8 * tiles) + slot % 8)
        code = code.reshape(-1)
        block_first = jnp.minimum(both_orders(first), GRAD_SLOTS).reshape(-1)
        image = accum(blocks0 + blocks1, code, block_first, sub_rows, width)
        d_emb = image.reshape(rows // 8, tiles, 8, 128).transpose(0, 2, 1, 3).reshape(rows, width)

        def more_grads(carry):
            r, table = carry
            at = rank - r * GRAD_SLOTS
            there = owned & (at >= 0) & (at < GRAD_SLOTS)
            dest = compact(at, there, jnp.where(owned, local, 0) + 1, GRAD_SLOTS)
            dest = jnp.where(dest == 0, rows, dest - 1)
            grads = jnp.concatenate(token_blocks(r, 0, d_tok0) + token_blocks(r, 1, d_tok1), axis=0).astype(F32)
            return r + 1, table.at[both_orders(dest).reshape(-1)].add(grads, mode="drop")

        _, d_emb = lax.while_loop(lambda c: c[0] < grad_rounds, more_grads, (jnp.int32(1), d_emb))

        small = jnp.concatenate([sums_qkv[0], d_b_up[0], sums1[:2].reshape(-1), sums2[:4].reshape(-1)]).reshape(-1, width)
        small = jnp.concatenate([small, jnp.zeros((pos_all.shape[0] - seq - n_small, width), F32)])
        pos_all = lax.dynamic_update_slice_in_dim(pos_all, small, seq, 0).reshape(n_tp * n_x, n_core, p_pos, width)
        pos_theirs = swap(lax.dynamic_index_in_dim(pos_all, 1 - c_index, 1, keepdims=False).reshape(-1, width), "cc")
        rest = grad_rest(core, ctx, d_attn, d_qkvs, hid1, n_tp, spans, plus=rest_theirs, tail=(pos_all, pos_theirs))
        rest = lax.psum_scatter(rest, ("tp", "xx"), scatter_dimension=0, tiled=True)
        rest_w = every_piece(rest[:spans[1][1]])
        whole = lax.all_gather(rest[spans[1][1]:], ("tp", "xx", "cc"), axis=0, tiled=True)
        d_pos = jnp.pad(whole[:seq], ((POS_OFFSET, pos_table.shape[0] - seq - POS_OFFSET), (0, 0)))
        small = whole[seq:seq + n_small].reshape(-1)
        n_b = b_qkv.size
        d_b_qkv = lax.dynamic_slice_in_dim(small, tp_index * n_b, n_b).reshape(n_core, 3, -1, b_qkv.shape[2])
        d_b_qkv = d_b_qkv.transpose(1, 0, 2, 3).reshape(b_qkv.shape)
        d_b_up = lax.dynamic_slice_in_dim(small, n_tp * n_b + tp_index * ff, ff)
        d_gain1, d_bias1, d_gain2, d_bias2, d_b_out, d_b_down = small[n_tp * (n_b + ff):].reshape(6, width)

        d_w_out, d_w_qkv = pieces_out(x_and_core, rest_w, ((0, n_out, False), (p_out, n_b // n_dp, False)))
        d_w_out = d_w_out.reshape(w_out.shape)
        d_w_qkv = d_w_qkv.reshape(n_core, 3, -1, w_qkv.shape[3], width).transpose(4, 1, 0, 2, 3).reshape(w_qkv.shape)
        return (layer_out, d_emb, d_pos, d_gain1, d_bias1, d_w_qkv, d_b_qkv, d_w_out,
                d_b_out, d_gain2, d_bias2, d_w_up, d_b_up, d_w_down, d_b_down)

    rep = P()
    in_specs = (P(dp, None), P("tp", None), rep, rep, rep,
                P(None, None, "tp", None), P(None, "tp", None), P("tp", None, None), rep,
                rep, rep, P(None, "tp"), P("tp"), P("tp", None), rep,
                P(dp, "tp", None))
    out_specs = (P(dp, "tp", None), P("tp", None), rep, rep, rep,
                 P(None, None, "tp", None), P(None, "tp", None), P("tp", None, None), rep,
                 rep, rep, P(None, "tp"), P("tp"), P("tp", None), rep)

    return jax.shard_map(local_step, mesh=mesh3, in_specs=in_specs, out_specs=out_specs, check_vma=False)
```

```python
import functools

import jax
import jax.numpy as jnp
from jax import lax
from jax.experimental import pallas as pl
from jax.experimental.pallas import tpu as pltpu
from jax.sharding import Mesh, PartitionSpec as P


F32 = jnp.float32
BF16 = jnp.bfloat16
MIB = 1024 * 1024
WIDEN = 32

BLK = 256


def dot_nt(a, b):
    return lax.dot_general(a, b, (((1,), (1,)), ((), ())), preferred_element_type=F32)


def dot_nn(a, b):
    return lax.dot_general(a, b, (((1,), (0,)), ((), ())), preferred_element_type=F32)


def head_only(x, head):
    half = x.shape[1] // 2
    lane = lax.broadcasted_iota(jnp.int32, x.shape, 1)
    keep = (lane < half) if head == 0 else (lane >= half)
    return jnp.where(keep, x, jnp.zeros((), x.dtype))


def attn_fwd_kernel(qkv_ref, ctx_ref, lse_ref, ctx_t):
    seq, width = ctx_ref.shape
    half = width // 2
    scale = half ** -0.5
    q2 = qkv_ref[:, 0:width] * jnp.asarray(scale, BF16)
    v_t = qkv_ref[:, 2 * width:3 * width].T
    tasks = [(head, i) for i in range(seq // BLK) for head in range(2)]

    def scores(head, i):
        return dot_nt(qkv_ref[0:(i + 1) * BLK, width:2 * width], head_only(q2[i * BLK:(i + 1) * BLK], head))

    ready = scores(*tasks[0])
    for n, (head, i) in enumerate(tasks):
        s = ready
        if n + 1 < len(tasks):
            ready = scores(*tasks[n + 1])
        lo, hi = i * BLK, (i + 1) * BLK
        v_h = v_t[head * half:(head + 1) * half, :]
        key = lax.broadcasted_iota(jnp.int32, (BLK, BLK), 0)
        qry = lax.broadcasted_iota(jnp.int32, (BLK, BLK), 1)
        diag = jnp.where(key <= qry, s[lo:hi], -1e30)
        top = jnp.max(diag, axis=0, keepdims=True)
        if i:
            top = jnp.maximum(top, jnp.max(s[0:lo], axis=0, keepdims=True))
        p_diag = jnp.exp(diag - top)
        total = jnp.sum(p_diag, axis=0, keepdims=True)
        if i:
            p_left = jnp.exp(s[0:lo] - top)
            total = total + jnp.sum(p_left, axis=0, keepdims=True)
        inv = 1.0 / total
        acc = dot_nn(v_h[:, lo:hi], (p_diag * inv).astype(BF16))
        if i:
            acc = acc + dot_nn(v_h[:, 0:lo], (p_left * inv).astype(BF16))
        ctx_t[head * half:(head + 1) * half, lo:hi] = acc
        lse_ref[head:head + 1, lo:hi] = top + jnp.log(total)
    ctx_ref[...] = ctx_t[...].T.astype(BF16)


def attn_fwd(qkv, n_seq, seq, n_pair):
    width = 128
    return pl.pallas_call(
        attn_fwd_kernel,
        grid=(n_seq, n_pair),
        in_specs=[pl.BlockSpec((seq, 3 * width), lambda b, p: (b, p))],
        out_specs=[pl.BlockSpec((seq, width), lambda b, p: (b, p)),
                   pl.BlockSpec((None, None, 2, seq), lambda b, p: (b, p, 0, 0))],
        out_shape=[jax.ShapeDtypeStruct((n_seq * seq, n_pair * width), BF16),
                   jax.ShapeDtypeStruct((n_seq, n_pair, 2, seq), F32)],
        scratch_shapes=[pltpu.VMEM((width, seq), F32)],
        name="attn_fwd",
        cost_estimate=pl.CostEstimate(flops=n_seq * n_pair * 8 * seq * seq * 256 * 10 // 16, bytes_accessed=n_seq * seq * n_pair * width * 8,
                                      transcendentals=n_seq * n_pair * seq * seq),
        compiler_params=pltpu.CompilerParams(vmem_limit_bytes=18 * 1024 * 1024),
    )(qkv)


def attn_bwd_kernel(qkv_ref, ctx_ref, dctx_ref, lse_ref, dqkv_ref, dk_t, dv_t):
    seq, width = ctx_ref.shape
    half = width // 2
    scale = half ** -0.5
    q2 = qkv_ref[:, 0:width] * jnp.asarray(scale, BF16)
    q_t = q2.T
    do_t = dctx_ref[...].T
    lse_c = jnp.concatenate([lse_ref[...], jnp.zeros((6, seq), F32)], axis=0).T
    prod = dctx_ref[...].astype(F32) * ctx_ref[...].astype(F32)
    tasks = [(head, i) for i in range(seq // BLK) for head in range(2)]

    def scores(head, i):
        lo, hi = i * BLK, (i + 1) * BLK
        return (dot_nt(head_only(q2[lo:hi], head), qkv_ref[0:hi, width:2 * width]),
                dot_nt(head_only(dctx_ref[lo:hi, :], head), qkv_ref[0:hi, 2 * width:3 * width]))

    dq = []
    ready = scores(*tasks[0])
    for n, (head, i) in enumerate(tasks):
        s, dp = ready
        if n + 1 < len(tasks):
            ready = scores(*tasks[n + 1])
        lo, hi = i * BLK, (i + 1) * BLK
        rows = slice(head * half, (head + 1) * half)
        mean = jnp.sum(head_only(prod[lo:hi], head), axis=1, keepdims=True)
        lse = lse_c[lo:hi, head:head + 1]
        qry = lax.broadcasted_iota(jnp.int32, (BLK, BLK), 0)
        key = lax.broadcasted_iota(jnp.int32, (BLK, BLK), 1)
        p_diag = jnp.where(key <= qry, jnp.exp(s[:, lo:hi] - lse), 0.0)
        ds_diag = (p_diag * (dp[:, lo:hi] - mean)).astype(BF16)
        dv_t[rows, lo:hi] = dot_nn(do_t[rows, lo:hi], p_diag.astype(BF16))
        dk_t[rows, lo:hi] = dot_nn(q_t[rows, lo:hi], ds_diag)
        dq_h = dot_nn(ds_diag, qkv_ref[lo:hi, width:2 * width])
        if i:
            p_left = jnp.exp(s[:, 0:lo] - lse)
            ds_left = (p_left * (dp[:, 0:lo] - mean)).astype(BF16)
            dv_t[rows, 0:lo] += dot_nn(do_t[rows, lo:hi], p_left.astype(BF16))
            dk_t[rows, 0:lo] += dot_nn(q_t[rows, lo:hi], ds_left)
            dq_h = dq_h + dot_nn(ds_left, qkv_ref[0:lo, width:2 * width])
        dq.append(dq_h)
        if head == 1:
            lane = lax.broadcasted_iota(jnp.int32, (BLK, width), 1)
            dqkv_ref[lo:hi, 0:width] = (jnp.where(lane < half, dq[0], dq[1]) * scale).astype(BF16)
            dq = []
    dqkv_ref[:, width:2 * width] = dk_t[...].T.astype(BF16)
    dqkv_ref[:, 2 * width:3 * width] = dv_t[...].T.astype(BF16)


def attn_bwd(qkv, ctx, dctx, lse, at, seq, n_pair):
    width = 128
    return pl.pallas_call(
        attn_bwd_kernel,
        grid=(n_pair,),
        in_specs=[pl.BlockSpec((seq, 3 * width), lambda p: (at, p)),
                  pl.BlockSpec((seq, width), lambda p: (at, p)),
                  pl.BlockSpec((seq, width), lambda p: (at, p)),
                  pl.BlockSpec((None, None, 2, seq), lambda p: (at, p, 0, 0))],
        out_specs=pl.BlockSpec((seq, 3 * width), lambda p: (0, p)),
        out_shape=jax.ShapeDtypeStruct((seq, n_pair * 3 * width), BF16),
        scratch_shapes=[pltpu.VMEM((width, seq), F32), pltpu.VMEM((width, seq), F32)],
        name="attn_bwd",
        cost_estimate=pl.CostEstimate(flops=n_pair * 20 * seq * seq * 256 * 10 // 16, bytes_accessed=seq * n_pair * width * 16,
                                      transcendentals=n_pair * seq * seq),
        compiler_params=pltpu.CompilerParams(vmem_limit_bytes=22 * 1024 * 1024),
    )(qkv, ctx, dctx, lse)


LN_EPS = 1e-5
GELU_S = 0.7978845608028654
GELU_A = 0.044715


def row_mean(v):
    return jnp.sum(v, axis=1, keepdims=True) * (1.0 / v.shape[1])


def row_stats(v):
    centered = v - row_mean(v)
    inv_std = lax.rsqrt(row_mean(centered * centered) + LN_EPS)
    return centered * inv_std, inv_std


def norm_back(d_y, x_in, gain):
    normed, inv_std = row_stats(x_in)
    d_norm = d_y * gain
    d_x = inv_std * (d_norm - row_mean(d_norm) - normed * row_mean(d_norm * normed))
    return d_x, d_y * normed


def col_sum(v):
    return jnp.sum(v, axis=0, keepdims=True)


def to_image(rows, image, base):
    tiles = rows.shape[1] // 128
    for h in range(rows.shape[0] // 8):
        for c in range(tiles):
            image[pl.ds(base + (h * tiles + c) * 8, 8), :] = rows[h * 8:(h + 1) * 8, c * 128:(c + 1) * 128]


def from_image(image, base, n_rows, width):
    tiles = width // 128
    return jnp.concatenate([jnp.concatenate([image[pl.ds(base + (h * tiles + c) * 8, 8), :] for c in range(tiles)], axis=1)
                            for h in range(n_rows // 8)], axis=0)


def pick_rows(code_ref, first, stage, image, n_rows, tiles):
    def pick(g, _):
        base = pl.multiple_of(g * 16 * tiles, 16 * tiles)
        for j in range(16):
            row = stage[pl.ds(code_ref[first + g * 16 + j], tiles, stride=8), :]
            image[pl.ds(base + (j // 8) * 8 * tiles + j % 8, tiles, stride=8), :] = row
        return 0

    lax.fori_loop(0, n_rows // 16, pick, 0)


def embed_kernel(n_blk, cap, code_ref, *refs):
    tok_refs = refs[:n_blk]
    pos_ref, gain_ref, bias_ref, x_ref, hid_ref, stage, image = refs[n_blk:]
    rows, width = x_ref.shape
    tiles = width // 128

    @pl.when(pl.program_id(0) == 0)
    def _():
        for b in range(n_blk):
            def widen(g, _, b=b):
                part = tok_refs[b][pl.ds(pl.multiple_of(g * WIDEN, WIDEN), WIDEN), :].astype(F32)
                to_image(part, stage, pl.multiple_of((b * cap + g * WIDEN) * tiles, WIDEN * tiles))
                return 0

            lax.fori_loop(0, cap // WIDEN, widen, 0)

    pick_rows(code_ref, pl.program_id(0) * rows, stage, image, rows, tiles)
    part = 64
    for i in range(rows // part):
        at = slice(i * part, (i + 1) * part)
        x = from_image(image, i * part * tiles, part, width) + pos_ref[at, :].astype(F32)
        x_ref[at, :] = x
        normed, _ = row_stats(x)
        hid_ref[at, :] = (normed * gain_ref[...] + bias_ref[...]).astype(BF16)


def embed(code, blocks, pos_rows, gain, bias, n_tok):
    cap, width = blocks[0].shape
    seq = pos_rows.shape[0]
    rows = 256
    per_seq = seq // rows
    n_blk = len(blocks)
    vec = pl.BlockSpec((1, width), lambda i: (0, 0))
    return pl.pallas_call(
        functools.partial(embed_kernel, n_blk, cap),
        grid=(n_tok // rows,),
        in_specs=[pl.BlockSpec(memory_space=pltpu.SMEM)]
        + [pl.BlockSpec((cap, width), lambda i: (0, 0), pipeline_mode=pl.Buffered(1))] * n_blk
        + [pl.BlockSpec((rows, width), lambda i: (i % per_seq, 0)), vec, vec],
        out_specs=[pl.BlockSpec((rows, width), lambda i: (i, 0))] * 2,
        out_shape=[jax.ShapeDtypeStruct((n_tok, width), F32), jax.ShapeDtypeStruct((n_tok, width), BF16)],
        scratch_shapes=[pltpu.VMEM((n_blk * cap * width // 128, 128), F32), pltpu.VMEM((rows * width // 128, 128), F32)],
        name="embed_norm",
        cost_estimate=pl.CostEstimate(flops=15_000_000_000, bytes_accessed=n_tok * width * 10, transcendentals=0),
        compiler_params=pltpu.CompilerParams(vmem_limit_bytes=28 * MIB),
    )(code, *blocks, pos_rows, gain, bias)


def pack_kernel(n_blk, code_ref, tok_ref, *refs):
    out_refs = refs[:n_blk]
    stage, image = refs[n_blk:]
    n_tok, width = tok_ref.shape
    cap = out_refs[0].shape[0]
    tiles = width // 128

    def widen(g, _):
        part = tok_ref[pl.ds(pl.multiple_of(g * WIDEN, WIDEN), WIDEN), :].astype(F32)
        to_image(part, stage, pl.multiple_of(g * WIDEN * tiles, WIDEN * tiles))
        return 0

    lax.fori_loop(0, n_tok // WIDEN, widen, 0)
    for b in range(n_blk):
        pick_rows(code_ref, b * cap, stage, image, cap, tiles)

        def narrow(g, _, b=b):
            part = from_image(image, pl.multiple_of(g * WIDEN * tiles, WIDEN * tiles), WIDEN, width)
            out_refs[b][pl.ds(pl.multiple_of(g * WIDEN, WIDEN), WIDEN), :] = part.astype(BF16)
            return 0

        lax.fori_loop(0, cap // WIDEN, narrow, 0)


def pack(code, tok, cap):
    n_tok, width = tok.shape
    n_blk = code.shape[0] // cap
    return pl.pallas_call(
        functools.partial(pack_kernel, n_blk),
        in_specs=[pl.BlockSpec(memory_space=pltpu.SMEM), pl.BlockSpec(memory_space=pltpu.VMEM)],
        out_specs=[pl.BlockSpec(memory_space=pltpu.VMEM)] * n_blk,
        out_shape=[jax.ShapeDtypeStruct((cap, width), BF16)] * n_blk,
        scratch_shapes=[pltpu.VMEM((n_tok * width // 128, 128), F32), pltpu.VMEM((cap * width // 128, 128), F32)],
        name="token_pack",
        cost_estimate=pl.CostEstimate(flops=15_000_000_000, bytes_accessed=n_tok * width * 5, transcendentals=0),
        compiler_params=pltpu.CompilerParams(vmem_limit_bytes=16 * MIB),
    )(code, tok)


def proj_kernel(c_ref, w_ref, x_ref, b_ref, gain_ref, bias_ref, x1_ref, hid_ref):
    part = x_ref.shape[0] // 2
    for i in range(2):
        at = slice(i * part, (i + 1) * part)
        x1 = x_ref[at, :] + dot_nn(c_ref[at, :], w_ref[...].reshape(c_ref.shape[1], -1)).astype(BF16).astype(F32) + b_ref[...]
        x1_ref[at, :] = x1
        normed, _ = row_stats(x1)
        hid_ref[at, :] = (normed * gain_ref[...] + bias_ref[...]).astype(BF16)


def proj_norm(ctx, w, start, x, b, gain, bias):
    n_tok, width = x.shape
    n_row = ctx.shape[1] // w.shape[0]
    rows = 512
    vec = pl.BlockSpec((1, width), lambda i: (0, 0))
    mat = pl.BlockSpec((rows, width), lambda i: (i, 0))
    return pl.pallas_call(
        proj_kernel,
        grid=(n_tok // rows,),
        in_specs=[pl.BlockSpec((rows, ctx.shape[1]), lambda i: (i, 0)), pl.BlockSpec((w.shape[0], n_row, width), lambda i: (0, start // n_row, 0)), mat, vec, vec, vec],
        out_specs=[mat, mat],
        out_shape=[jax.ShapeDtypeStruct((n_tok, width), F32), jax.ShapeDtypeStruct((n_tok, width), BF16)],
        name="proj_norm",
        cost_estimate=pl.CostEstimate(flops=2 * n_tok * ctx.shape[1] * width, bytes_accessed=n_tok * width * 12, transcendentals=0),
        compiler_params=pltpu.CompilerParams(vmem_limit_bytes=24 * MIB),
    )(ctx, w, x, b, gain, bias)


def ffn_kernel(part, h_ref, og_ref, wu_ref, wd_ref, b_ref, act_ref, dup_ref, db_ref):
    total = jnp.zeros(db_ref.shape, F32)
    for i in range(h_ref.shape[0] // part):
        at = slice(i * part, (i + 1) * part)
        z = dot_nt(h_ref[at, :], wu_ref[0]) + b_ref[...]
        d_act = dot_nt(og_ref[at, :], wd_ref[0])
        z2 = z * z
        gate = 0.5 * jnp.tanh(z * (GELU_S + (GELU_S * GELU_A) * z2)) + 0.5
        act = z * gate
        d_up = d_act * (gate + act * (1.0 - gate) * (2.0 * GELU_S + (6.0 * GELU_S * GELU_A) * z2))
        act_ref[at, :] = act.astype(BF16)
        dup_ref[at, :] = d_up.astype(BF16)
        total = total + col_sum(d_up)
    db_ref[...] = total


def ffn(hid, og, w, b_up, part=1024):
    n_tok, width = hid.shape
    ff = b_up.shape[1]
    n_piece = w.shape[0]
    bn = ff // n_piece
    whole = pl.BlockSpec((n_tok, width), lambda i: (0, 0), pipeline_mode=pl.Buffered(1))
    ospec = pl.BlockSpec((n_tok, bn), lambda i: (0, i))
    vec = pl.BlockSpec((1, bn), lambda i: (0, i))
    return pl.pallas_call(
        functools.partial(ffn_kernel, part),
        grid=(n_piece,),
        in_specs=[whole, whole, pl.BlockSpec((1, bn, width), lambda i: (i, 0, 0)), pl.BlockSpec((1, bn, width), lambda i: (i, 1, 0)), vec],
        out_specs=[ospec, ospec, vec],
        out_shape=[jax.ShapeDtypeStruct((n_tok, ff), BF16), jax.ShapeDtypeStruct((n_tok, ff), BF16), jax.ShapeDtypeStruct((1, ff), F32)],
        name="ffn",
        cost_estimate=pl.CostEstimate(flops=4 * n_tok * ff * width, bytes_accessed=4 * n_tok * ff + 4 * ff * width, transcendentals=n_tok * ff),
        compiler_params=pltpu.CompilerParams(vmem_limit_bytes=26 * MIB),
    )(hid, og, w, w, b_up)


def down_kernel(n_tp, me_ref, act_ref, w_ref, x1_ref, b_ref, *out_refs):
    out = x1_ref[...] + dot_nn(act_ref[...], w_ref[...].reshape(act_ref.shape[1], -1)).astype(BF16).astype(F32) + b_ref[...]
    k = me_ref[0] ^ (pl.program_id(0) % n_tp)
    seq = pl.program_id(0) // n_tp
    for j in range(n_tp):
        @pl.when(k == j)
        def _(j=j):
            out_refs[j][seq] = out.astype(BF16)


def down(me, act, w, x1, b, n_seq, n_tp):
    n_tok, width = x1.shape
    ff = act.shape[1]
    rows = n_tok // n_seq // n_tp
    part = jax.ShapeDtypeStruct((n_seq, rows, width), BF16)
    return pl.pallas_call(
        functools.partial(down_kernel, n_tp),
        grid_spec=pltpu.PrefetchScalarGridSpec(
            num_scalar_prefetch=1, grid=(n_seq * n_tp,),
            in_specs=[pl.BlockSpec((rows, ff), lambda i, m: (i, 0)),
                      pl.BlockSpec((w.shape[0], ff // w.shape[0], width), lambda i, m: (0, 1, 0), pipeline_mode=pl.Buffered(1)),
                      pl.BlockSpec((rows, width), lambda i, m: (i, 0)), pl.BlockSpec((1, width), lambda i, m: (0, 0))],
            out_specs=[pl.BlockSpec(part.shape, lambda i, m: (0, 0, 0))] * n_tp),
        out_shape=[part] * n_tp,
        name="down",
        cost_estimate=pl.CostEstimate(flops=2 * n_tok * ff * width, bytes_accessed=2 * n_tok * ff + n_tok * width * 6, transcendentals=0),
        compiler_params=pltpu.CompilerParams(vmem_limit_bytes=32 * MIB),
    )(me, act, w, x1, b)


def back2_kernel(dup_ref, w_ref, x1_ref, og_ref, gain_ref, dr_ref, da_ref, sums_ref):
    @pl.when(pl.program_id(0) == 0)
    def _():
        sums_ref[...] = jnp.zeros(sums_ref.shape, F32)

    n_part = 2
    part = dr_ref.shape[0] // n_part
    w = w_ref[...].reshape(dup_ref.shape[1], -1)
    d_ys = [dot_nn(dup_ref[i * part:(i + 1) * part, :], w) for i in range(n_part)]
    for i in range(n_part):
        at = slice(i * part, (i + 1) * part)
        d_y = d_ys[i].astype(BF16).astype(F32)
        d_x, d_gain = norm_back(d_y, x1_ref[at, :], gain_ref[...])
        og = og_ref[at, :].astype(F32)
        d_resid = og + d_x
        dr_ref[at, :] = d_resid
        da_ref[at, :] = d_resid.astype(BF16)
        sums_ref[0:1, :] += col_sum(d_gain)
        sums_ref[1:2, :] += col_sum(d_y)
        sums_ref[2:3, :] += col_sum(d_resid)
        sums_ref[3:4, :] += col_sum(og)


def back2(d_up, w, x1, og, gain):
    n_tok, width = x1.shape
    ff = d_up.shape[1]
    rows = 256
    mat = pl.BlockSpec((rows, width), lambda i: (i, 0))
    return pl.pallas_call(
        back2_kernel,
        grid=(n_tok // rows,),
        in_specs=[pl.BlockSpec((rows, ff), lambda i: (i, 0)), pl.BlockSpec((w.shape[0], ff // w.shape[0], width), lambda i: (0, 0, 0), pipeline_mode=pl.Buffered(1)),
                  mat, mat, pl.BlockSpec((1, width), lambda i: (0, 0))],
        out_specs=[mat, mat, pl.BlockSpec((8, width), lambda i: (0, 0))],
        out_shape=[jax.ShapeDtypeStruct((n_tok, width), F32), jax.ShapeDtypeStruct((n_tok, width), BF16), jax.ShapeDtypeStruct((8, width), F32)],
        name="ffn_back",
        cost_estimate=pl.CostEstimate(flops=2 * n_tok * ff * width, bytes_accessed=2 * n_tok * ff + n_tok * width * 12, transcendentals=0),
        compiler_params=pltpu.CompilerParams(vmem_limit_bytes=30 * MIB),
    )(d_up, w, x1, og, gain)


def back1_kernel(dq_ref, w_ref, x_ref, dr_ref, gain_ref, *refs):
    tok_ref, pos_ref, sums_ref, bsum_ref = refs[-4:]
    before_refs = refs[:-4]

    @pl.when(pl.program_id(0) == 0)
    def _():
        sums_ref[...] = before_refs[1][...] if before_refs else jnp.zeros(sums_ref.shape, F32)
        bsum_ref[...] = before_refs[2][...] if before_refs else jnp.zeros(bsum_ref.shape, F32)

    n_part = 2
    part = tok_ref.shape[0] // n_part
    d_ys = [dot_nn(dq_ref[i * part:(i + 1) * part, :], w_ref[...]) for i in range(n_part)]
    for i in range(n_part):
        at = slice(i * part, (i + 1) * part)
        d_y = d_ys[i].astype(BF16).astype(F32)
        d_x, d_gain = norm_back(d_y, x_ref[at, :], gain_ref[...])
        d_resid = dr_ref[at, :] + d_x
        tok_ref[at, :] = d_resid.astype(BF16)
        pos_ref[at, :] = before_refs[0][at, :] + d_resid if before_refs else d_resid
        sums_ref[0:1, :] += col_sum(d_gain)
        sums_ref[1:2, :] += col_sum(d_y)
        bsum_ref[0:1, :] += col_sum(dq_ref[at, :].astype(F32))


def back1(d_qkv, w_qkv, x, d_resid1, gain, at, pos_rows, earlier=None):
    seq, n_cols = d_qkv.shape
    width = x.shape[1]
    rows = 256
    steps = seq // rows
    mat = pl.BlockSpec((rows, width), lambda i: (at * steps + i, 0))
    out = pl.BlockSpec((rows, width), lambda i: (i, 0))
    few = [pl.BlockSpec((8, width), lambda i: (0, 0)), pl.BlockSpec((8, n_cols), lambda i: (0, 0))]
    return pl.pallas_call(
        back1_kernel,
        grid=(steps,),
        in_specs=[pl.BlockSpec((rows, n_cols), lambda i: (i, 0)),
                  pl.BlockSpec((n_cols, width), lambda i: (0, 0), pipeline_mode=pl.Buffered(1)),
                  mat, mat, pl.BlockSpec((1, width), lambda i: (0, 0))] + ([out] + few if earlier else []),
        out_specs=[out, out] + few,
        out_shape=[jax.ShapeDtypeStruct((seq, width), BF16), jax.ShapeDtypeStruct((pos_rows, width), F32),
                   jax.ShapeDtypeStruct((8, width), F32), jax.ShapeDtypeStruct((8, n_cols), F32)],
        name="qkv_back",
        cost_estimate=pl.CostEstimate(flops=2 * seq * n_cols * width, bytes_accessed=2 * seq * n_cols + seq * width * 12, transcendentals=0),
        compiler_params=pltpu.CompilerParams(vmem_limit_bytes=26 * MIB),
    )(d_qkv, w_qkv, x, d_resid1, gain, *(earlier or ()))


def pieces_out_kernel(n_in, spans, me_ref, *refs):
    out_refs = refs[n_in:]
    for p in range(n_in):
        @pl.when(pl.program_id(0) == p)
        def _(p=p):
            for (start, n, turned), out_ref in zip(spans, out_refs):
                part = refs[p][start:start + n, :]
                out_ref[...] = part.T if turned else part


def pieces_out(me, pieces, spans):
    rows, width = pieces[0].shape
    n_in = len(pieces)

    def place(p, m):
        return (m[1] ^ (p // 2)) * 2 + (m[0] ^ (p % 2))

    out_specs, out_shape = [], []
    for start, n, turned in spans:
        if turned:
            out_specs.append(pl.BlockSpec((width, n), lambda p, m: (0, place(p, m))))
            out_shape.append(jax.ShapeDtypeStruct((width, n_in * n), F32))
        else:
            out_specs.append(pl.BlockSpec((n, width), lambda p, m: (place(p, m), 0)))
            out_shape.append(jax.ShapeDtypeStruct((n_in * n, width), F32))
    return pl.pallas_call(
        functools.partial(pieces_out_kernel, n_in, spans),
        grid_spec=pltpu.PrefetchScalarGridSpec(
            num_scalar_prefetch=1, grid=(n_in,),
            in_specs=[pl.BlockSpec((rows, width), lambda p, m: (0, 0), pipeline_mode=pl.Buffered(1))] * n_in,
            out_specs=out_specs),
        out_shape=out_shape,
        name="grads_out",
        cost_estimate=pl.CostEstimate(flops=8_000_000_000, bytes_accessed=n_in * rows * width * 8, transcendentals=0),
        compiler_params=pltpu.CompilerParams(vmem_limit_bytes=20 * MIB),
    )(me, *pieces)


def assemble_kernel(n, me_ref, *refs):
    out_ref = refs[n]
    k = me_ref[0] ^ pl.program_id(0)
    for j in range(n):
        @pl.when(k == j)
        def _(j=j):
            out_ref[...] = refs[j][...].reshape(out_ref.shape)


def assemble(me, parts, out_shape, block):
    at = 1 if len(out_shape) == 4 else 0
    return pl.pallas_call(
        functools.partial(assemble_kernel, len(parts)),
        grid_spec=pltpu.PrefetchScalarGridSpec(
            num_scalar_prefetch=1, grid=(len(parts),),
            in_specs=[pl.BlockSpec(p.shape, lambda i, m: (0, 0, 0), pipeline_mode=pl.Buffered(1)) for p in parts],
            out_specs=pl.BlockSpec(block, lambda i, m: tuple(i if d == at else 0 for d in range(len(block))))),
        out_shape=jax.ShapeDtypeStruct(out_shape, parts[0].dtype),
        name="assemble",
        cost_estimate=pl.CostEstimate(flops=4_000_000_000, bytes_accessed=16 * MIB, transcendentals=0),
        compiler_params=pltpu.CompilerParams(vmem_limit_bytes=10 * MIB),
    )(me, *parts)


LANES = 128


def accum_kernel(n_block, cap, sub_rows, width, where_ref, first_ref, *refs):
    tok_refs = refs[:n_block]
    out_ref = refs[n_block]
    n_sub = len(sub_rows)
    acc = refs[n_block + 1:n_block + 1 + n_sub]
    buf, stage, in_sem, out_sem = refs[n_block + 1 + n_sub:]
    tiles = width // LANES
    group = 8 * tiles

    def fetch(block, n):
        return pltpu.make_async_copy(tok_refs[n], buf.at[block % 2], in_sem.at[block % 2])

    def fetch_next(block):
        for n in range(n_block):
            @pl.when(block == n)
            def _(n=n):
                fetch(block, n).start()

    fetch_next(0)
    for s in range(n_sub):
        def clear(i, _, s=s):
            acc[s][pl.ds(pl.multiple_of(i * group, group), group), :] = jnp.zeros((group, LANES), F32)
            return 0

        lax.fori_loop(0, sub_rows[s] // 8, clear, 0)

    def add_rows(s, slot, n):
        codes = [where_ref[slot + j] for j in range(n)]
        at = [code >> 16 for code in codes]
        rows = [stage[pl.ds(code & 0xffff, tiles, stride=8), :] for code in codes]
        sums = [acc[s][pl.ds(a, tiles, stride=8), :] for a in at]
        for j in range(n):
            for i in range(j):
                sums[j] = jnp.where(at[i] == at[j], sums[i], sums[j])
            sums[j] = sums[j] + rows[j]
        for j in range(n):
            acc[s][pl.ds(at[j], tiles, stride=8), :] = sums[j]

    def add_block(block, _):
        fetch_next(block + 1)
        fetch(block, 0).wait()

        def widen(g, _):
            rows = buf[block % 2, pl.ds(pl.multiple_of(g * WIDEN, WIDEN), WIDEN), :].astype(F32)
            base = pl.multiple_of(g * (WIDEN // 8) * group, (WIDEN // 8) * group)
            for h in range(WIDEN // 8):
                for c in range(tiles):
                    stage[pl.ds(base + h * group + c * 8, 8), :] = rows[h * 8:(h + 1) * 8, c * LANES:(c + 1) * LANES]
            return 0

        lax.fori_loop(0, cap // WIDEN, widen, 0)

        starts = [first_ref[block * (n_sub + 1) + s] for s in range(n_sub + 1)]
        counts = [starts[s + 1] - starts[s] for s in range(n_sub)]
        both = functools.reduce(jnp.minimum, counts) // 2
        begin = [block * cap + starts[s] for s in range(n_sub)]

        def together(i, _):
            for s in range(n_sub):
                add_rows(s, begin[s] + 2 * i, 2)
            return 0

        lax.fori_loop(0, both, together, 0)
        for s in range(n_sub):
            fours = (counts[s] - 2 * both) // 4

            def alone(i, _, s=s):
                add_rows(s, begin[s] + 2 * both + 4 * i, 4)
                return 0

            lax.fori_loop(0, fours, alone, 0)

            def single(i, _, s=s):
                add_rows(s, begin[s] + i, 1)
                return 0

            lax.fori_loop(2 * both + 4 * fours, counts[s], single, 0)
        return 0

    lax.fori_loop(0, n_block, add_block, 0)
    done = 0
    copies = []
    for s in range(n_sub):
        n = sub_rows[s] * tiles
        copies.append(pltpu.make_async_copy(acc[s], out_ref.at[pl.ds(done, n), :], out_sem.at[s]))
        copies[-1].start()
        done += n
    for c in copies:
        c.wait()


def accum(tok_blocks, code, first, sub_rows, width):
    n_block = len(tok_blocks)
    cap = tok_blocks[0].shape[0]
    n_sub = len(sub_rows)
    tiles = width // LANES
    return pl.pallas_call(
        functools.partial(accum_kernel, n_block, cap, sub_rows, width),
        in_specs=[pl.BlockSpec(memory_space=pltpu.SMEM), pl.BlockSpec(memory_space=pltpu.SMEM)]
        + [pl.BlockSpec(memory_space=pl.ANY)] * n_block,
        out_specs=pl.BlockSpec(memory_space=pl.ANY),
        out_shape=jax.ShapeDtypeStruct((sum(sub_rows) * tiles, LANES), F32),
        scratch_shapes=[pltpu.VMEM((r * tiles, LANES), F32) for r in sub_rows]
        + [pltpu.VMEM((2, cap, width), BF16), pltpu.VMEM((cap * tiles, LANES), F32),
           pltpu.SemaphoreType.DMA((2,)), pltpu.SemaphoreType.DMA((n_sub,))],
        name="table_accum",
        cost_estimate=pl.CostEstimate(flops=50_000_000_000, bytes_accessed=100_000_000, transcendentals=0),
        compiler_params=pltpu.CompilerParams(vmem_limit_bytes=63 * 1024 * 1024),
    )(code, first, *tok_blocks)


def dot_tn(a, b):
    return lax.dot_general(a, b, (((0,), (0,)), ((), ())), preferred_element_type=F32)


def grad_kernel(has_plus, core_ref, a_ref, b_ref, *refs):
    out_ref = refs[-1]
    n = a_ref.shape[1]
    g = dot_tn(a_ref[...], b_ref[...])
    out_ref[0:n, :] = g + refs[0][0:n, :] if has_plus else g
    if out_ref.shape[0] > n:
        out_ref[n:, :] = jnp.zeros((out_ref.shape[0] - n, out_ref.shape[1]), F32)


def grad_pieces(core, a, b, n_tp, piece, which, n_which, plus=None, into=None):
    n_tok, n_cols = a.shape
    width = b.shape[1]
    bn = n_cols // (4 * n_tp)
    out_spec = pl.BlockSpec((piece, width), lambda p, c: (n_which * p + which, 0))
    in_specs = [pl.BlockSpec((n_tok, bn), lambda p, c: (0, 4 * (p // 2) + 2 * c[0] + p % 2)),
                pl.BlockSpec((n_tok, width), lambda p, c: (0, 0), pipeline_mode=pl.Buffered(1))]
    args = [a, b]
    if plus is not None:
        in_specs.append(pl.BlockSpec((piece, width), lambda p, c: (p, 0)))
        args.append(plus)
    if into is not None:
        in_specs.append(pl.BlockSpec(memory_space=pl.ANY))
        args.append(into)
    return pl.pallas_call(
        functools.partial(grad_kernel, plus is not None),
        grid_spec=pltpu.PrefetchScalarGridSpec(num_scalar_prefetch=1, grid=(2 * n_tp,), in_specs=in_specs, out_specs=out_spec),
        out_shape=jax.ShapeDtypeStruct((2 * n_tp * n_which * piece, width), F32),
        input_output_aliases={} if into is None else {len(args): 0},
        name="weight_grad",
        cost_estimate=pl.CostEstimate(flops=n_tok * n_cols * width, bytes_accessed=n_tok * (n_cols + 2 * width) + 2 * n_cols * width,
                                      transcendentals=0),
        compiler_params=pltpu.CompilerParams(vmem_limit_bytes=18 * MIB),
    )(core, *args)


def grad_rest_kernel(spans, last, n_a2, core_ref, a1_ref, b1_ref, b2_ref, *refs):
    a2_refs, refs, out_ref = refs[:n_a2], refs[n_a2:-1], refs[-1]
    plus = refs[0] if refs else None
    piece, piece_in = out_ref.shape[0] // 2, (plus.shape[0] // 2 if refs else 0)
    rows = b2_ref.shape[0] // n_a2
    for which, (start, stop) in enumerate(spans):
        half = (a2_refs[0] if which else a1_ref).shape[1] // 2
        for i in range(0, 2 * half, 128):
            cols = slice(i, i + 128)
            if which:
                g = sum(dot_tn(a_ref[:, cols], b2_ref[n * rows:(n + 1) * rows, :]) for n, a_ref in enumerate(a2_refs))
            else:
                g = dot_tn(a1_ref[:, cols], b1_ref[...])
            for x in range(2):
                lo, hi = max(i, x * half), min(i + 128, (x + 1) * half)
                if lo < hi:
                    to = lo - x * half + start
                    part = g[lo - i:hi - i]
                    if plus is not None:
                        part = part + plus[x * piece_in + to:x * piece_in + to + hi - lo, :]
                    out_ref[x * piece + to:x * piece + to + hi - lo, :] = part
        for x in range(2):
            if stop > start + half:
                out_ref[x * piece + start + half:x * piece + stop, :] = jnp.zeros((stop - start - half, out_ref.shape[1]), F32)
    if last:
        for x in range(2):
            out_ref[x * piece + spans[-1][1]:(x + 1) * piece, :] = refs[1][x, 0] + refs[2][x * last:(x + 1) * last, :]


def grad_rest(core, a1, b1, a2, b2, n_tp, spans, plus=None, tail=None):
    n_tok, width = b1.shape
    last = tail[0].shape[2] if tail else 0
    piece = spans[-1][1] + last
    whole = pl.BlockSpec((n_tok, width), lambda t, c: (0, 0), pipeline_mode=pl.Buffered(1))
    cols = [pl.BlockSpec((a.shape[0], a.shape[1] // (2 * n_tp)), lambda t, c: (0, 2 * t + c[0])) for a in (a1, *a2)]
    in_specs, args = [cols[0], whole, whole] + cols[1:], [a1, b1, b2, *a2]
    if plus is not None:
        in_specs.append(pl.BlockSpec((plus.shape[0] // n_tp, width), lambda t, c: (t, 0)))
        args.append(plus)
    if tail:
        in_specs.append(pl.BlockSpec((2, 1, last, width), lambda t, c: (t, c[0], 0, 0)))
        in_specs.append(pl.BlockSpec((2 * last, width), lambda t, c: (t, 0)))
        args += tail
    n_cols = a1.shape[1] + a2[0].shape[1]
    return pl.pallas_call(
        functools.partial(grad_rest_kernel, spans, last, len(a2)),
        grid_spec=pltpu.PrefetchScalarGridSpec(num_scalar_prefetch=1, grid=(n_tp,), in_specs=in_specs,
                                               out_specs=pl.BlockSpec((2 * piece, width), lambda t, c: (t, 0))),
        out_shape=jax.ShapeDtypeStruct((2 * n_tp * piece, width), F32),
        name="weight_grads",
        cost_estimate=pl.CostEstimate(flops=n_tok * n_cols * width, bytes_accessed=n_tok * (n_cols + 4 * width) + 2 * n_cols * width,
                                      transcendentals=0),
        compiler_params=pltpu.CompilerParams(vmem_limit_bytes=32 * MIB),
    )(core, *args)


POS_OFFSET = 2
SLOTS = 704
GRAD_SLOTS = 384
LOW = 32


def before(n):
    return (lax.broadcasted_iota(jnp.int32, (n, n), 1) < lax.broadcasted_iota(jnp.int32, (n, n), 0)).astype(BF16)


def rank_in_class(hot):
    n_blk, n_tok, n_cls = hot.shape
    ones = hot.astype(BF16).reshape(n_blk, n_tok // 128, 128, n_cls)
    within = jnp.einsum("ij,bnjk->bnik", before(128), ones, preferred_element_type=F32)
    sums = jnp.sum(ones.astype(F32), axis=2)
    ahead = jnp.einsum("mn,bnk->bmk", before(n_tok // 128), sums.astype(BF16), preferred_element_type=F32)
    rank = jnp.sum((within + ahead[:, :, None, :]) * ones.astype(F32), axis=3)
    return rank.reshape(n_blk, n_tok).astype(jnp.int32), jnp.sum(sums, axis=1).astype(jnp.int32)


def compact(rank, valid, value, slots):
    n_high = slots // LOW
    high = ((rank // LOW)[:, :, None] == jnp.arange(n_high)) & valid[:, :, None]
    low = ((rank % LOW)[:, :, None] == jnp.arange(LOW)).astype(F32)
    parts = jnp.concatenate([low * (value // 128).astype(F32)[:, :, None], low * (value % 128).astype(F32)[:, :, None]], axis=2)
    out = jnp.einsum("bjh,bjl->bhl", high.astype(BF16), parts.astype(BF16), preferred_element_type=F32).astype(jnp.int32)
    return (out[:, :, :LOW] * 128 + out[:, :, LOW:]).reshape(rank.shape[0], slots)


def solution(mesh):
    n_tp, n_dp = mesh.shape["tp"], mesh.shape["dp"]
    n_core = 2
    n_x = n_dp // n_core
    mesh3 = Mesh(mesh.devices.reshape(n_tp, n_x, n_core), ("tp", "xx", "cc"))
    dp = ("xx", "cc")
    tp_swap = [[(i, i ^ k) for i in range(n_tp)] for k in range(n_tp)]
    pair = [(0, 1), (1, 0)]

    def local_step(tok_ids, emb_table, pos_table, ln1_gain, ln1_bias, w_qkv, b_qkv, w_out, b_out,
                   ln2_gain, ln2_bias, w_up, b_up, w_down, b_down, out_grad):
        tp_index, x_index, c_index = lax.axis_index("tp"), lax.axis_index("xx"), lax.axis_index("cc")
        dp_index = x_index * n_core + c_index
        n_seq_dp, seq = tok_ids.shape
        n_seq = n_seq_dp // n_tp
        n_tok = n_seq * seq
        rows, width = emb_table.shape
        n_sub = 4
        sub = -(-rows // n_sub // 8) * 8
        sub_rows = (sub,) * (n_sub - 1) + (rows - (n_sub - 1) * sub,)
        seq_local = seq // n_tp
        ff = w_up.shape[1]
        gain1, bias1 = ln1_gain.astype(F32)[None], ln1_bias.astype(F32)[None]
        gain2, bias2 = ln2_gain.astype(F32)[None], ln2_bias.astype(F32)[None]

        def half(w, axis):
            n = w.shape[axis] // n_core
            return lax.dynamic_slice_in_dim(w, c_index * n, n, axis)

        def gather_rows(w):
            return lax.all_gather(w, ("tp", "cc"), axis=0, tiled=True)

        def swap(v, axis, k=1):
            return lax.ppermute(v, axis, tp_swap[k] if axis == "tp" else pair)

        def by_owner(parts):
            out = []
            for p in range(n_tp):
                k = tp_index ^ p
                out.append(jnp.where(k < 2, jnp.where(k == 0, parts[0], parts[1]), jnp.where(k == 2, parts[2], parts[3])))
            return out

        ids_all = lax.all_gather(tok_ids, dp, axis=0, tiled=True)
        ids_all, w_up, w_down, w_out, b_qkv, b_up = lax.optimization_barrier((ids_all, w_up, w_down, w_out, b_qkv, b_up))

        wqkv_t = gather_rows(jnp.transpose(half(w_qkv, 2), (1, 2, 3, 0)).reshape(-1, width))
        n_ff, n_out = ff // n_dp, w_out.shape[0] * w_out.shape[1] // n_dp

        def quarter(w, axis):
            n = w.shape[axis] // n_dp
            return lax.dynamic_slice_in_dim(w, dp_index * n, n, axis)

        own_w = jnp.concatenate([quarter(w_up, 1).T, quarter(w_down, 0), quarter(w_out.reshape(-1, width), 0)])
        w_all = lax.all_gather(own_w, ("tp", "xx", "cc"), axis=0, tiled=True)
        w_all = w_all.reshape(n_tp * n_dp, 2 * n_ff + n_out, width)
        wout_w = w_all[:, 2 * n_ff:].reshape(-1, width)
        n_pair = wqkv_t.shape[0] // (3 * 128)
        own_bias = jnp.concatenate([b_qkv.reshape(3, n_core, -1, b_qkv.shape[2]).transpose(1, 0, 2, 3).reshape(-1), b_up])
        biases = jnp.stack(by_owner([swap(own_bias, "tp", k) if k else own_bias for k in range(n_tp)]))
        bqkv_w = biases[:, :-ff].reshape(-1).astype(F32)
        bup_w = biases[:, -ff:].reshape(1, -1).astype(F32)
        pos_rows = lax.slice_in_dim(pos_table, POS_OFFSET, POS_OFFSET + seq, axis=0)

        local = ids_all - tp_index * rows
        sub_of = sum(((local >= s * sub).astype(jnp.int32) for s in range(1, n_sub)), jnp.zeros_like(local))
        owned = (local >= 0) & (local < rows)
        hot = owned[:, :, None] & (sub_of[:, :, None] == jnp.arange(n_sub))
        rank, counts = rank_in_class(hot)
        first = jnp.concatenate([jnp.zeros_like(counts[:, :1]), jnp.cumsum(counts, axis=1)], axis=1)
        rank = rank + jnp.sum(jnp.where(hot, first[:, None, :-1], 0), axis=2)
        owner_counts = jnp.stack([jnp.sum(((ids_all >= o * rows) & (ids_all < (o + 1) * rows)).astype(jnp.int32), axis=1)
                                  for o in range(n_tp)])
        grad_rounds = (jnp.max(owner_counts) + GRAD_SLOTS - 1) // GRAD_SLOTS
        rounds = (jnp.max(jnp.sum(owner_counts.reshape(n_tp, -1, n_seq), axis=2)) + SLOTS - 1) // SLOTS

        def after_first(ranks, totals):
            return (ranks + (jnp.cumsum(totals, axis=1) - totals)[:, :, None]).reshape(ranks.shape[0], -1)

        def grad_lists(r):
            at = rank - r * GRAD_SLOTS
            return compact(at, owned & (at >= 0) & (at < GRAD_SLOTS), jnp.where(owned, local, 0), GRAD_SLOTS)

        my_rank = lax.dynamic_slice_in_dim(rank, dp_index * n_seq_dp, n_seq_dp, 0)
        my_total = lax.dynamic_slice_in_dim(first[:, -1], dp_index * n_seq_dp, n_seq_dp, 0)
        my_rank = after_first(my_rank.reshape(n_tp, n_seq, seq), my_total.reshape(n_tp, n_seq))
        my_owned = lax.dynamic_slice_in_dim(owned, dp_index * n_seq_dp, n_seq_dp, 0).reshape(n_tp, n_tok)
        my_local = lax.dynamic_slice_in_dim(local, dp_index * n_seq_dp, n_seq_dp, 0).reshape(n_tp, n_tok)

        def lists(r):
            at = my_rank - r * SLOTS
            return compact(at, my_owned & (at >= 0) & (at < SLOTS), jnp.where(my_owned, my_local, 0), SLOTS)

        own_ids = lax.dynamic_slice_in_dim(ids_all, dp_index * n_seq_dp + tp_index * n_seq, n_seq, 0)
        own_owner = sum(((own_ids >= o * rows).astype(jnp.int32) for o in range(1, n_tp)), jnp.zeros_like(own_ids))
        own_local = own_ids - own_owner * rows
        own_sub = sum(((own_local >= s * sub).astype(jnp.int32) for s in range(1, n_sub)), jnp.zeros_like(own_ids))
        own_hot = (own_owner * n_sub + own_sub)[:, :, None] == jnp.arange(n_tp * n_sub)
        own_rank, own_counts = rank_in_class(own_hot)
        own_counts = own_counts.reshape(n_seq, n_tp, n_sub)
        own_first = jnp.cumsum(own_counts, axis=2) - own_counts
        own_rank = own_rank + jnp.sum(jnp.where(own_hot, own_first.reshape(n_seq, 1, -1), 0), axis=2)
        own_total = jnp.sum(own_counts, axis=2)
        own_shift = jnp.cumsum(own_total, axis=0) - own_total
        own_place = sum(jnp.where(own_owner == o, own_shift[:, o:o + 1], 0) for o in range(n_tp))
        own_place = (own_place + own_rank).reshape(-1)

        def own_lists(r, b):
            at = jnp.broadcast_to(own_rank[b] - r * GRAD_SLOTS, (n_tp, seq))
            mine = own_owner[b] == jnp.arange(n_tp)[:, None]
            return compact(at, mine & (at >= 0) & (at < GRAD_SLOTS), jnp.broadcast_to(jnp.arange(seq), (n_tp, seq)), GRAD_SLOTS)

        tiles = width // 128

        def own_places(r, b):
            own = own_lists(r, b)
            place = jnp.concatenate([lax.dynamic_index_in_dim(own, tp_index ^ k, 0, keepdims=False) for k in range(n_tp)])
            return (place // 8) * (8 * tiles) + place % 8

        places0 = [own_places(0, b) for b in range(n_seq)]

        def in_block_order(table, b):
            out = []
            for dc in range(n_core):
                for dx in range(n_x):
                    for k in range(n_tp):
                        d = (x_index ^ dx) * n_core + (c_index ^ dc)
                        out.append(lax.dynamic_index_in_dim(table, (d * n_tp + (tp_index ^ k)) * n_seq + b, 0, keepdims=False))
            return out

        def both_orders(table):
            return jnp.stack(in_block_order(table, 0) + in_block_order(table, 1))

        block_rows = both_orders(grad_lists(0))
        in_sub = sum(((block_rows >= s * sub).astype(jnp.int32) for s in range(1, n_sub)), jnp.zeros_like(block_rows))
        in_sub = block_rows - in_sub * sub
        slot = jnp.arange(GRAD_SLOTS)
        code = (((in_sub // 8) * (8 * tiles) + in_sub % 8) << 16) | ((slot // 8) * (8 * tiles) + slot % 8)
        code = code.reshape(-1)
        block_first = jnp.minimum(both_orders(first), GRAD_SLOTS).reshape(-1)

        def rows_here(r, my_lists):
            index = [lax.dynamic_index_in_dim(my_lists, tp_index ^ k, 0, keepdims=False) for k in range(n_tp)]
            first_two = jnp.take(emb_table, jnp.concatenate([index[3], index[1]]), axis=0, mode="clip")
            rest, first_two = lax.optimization_barrier((jnp.concatenate([index[2], index[0]]), first_two))
            last_two = jnp.take(emb_table, rest, axis=0, mode="clip")
            sent = [last_two[SLOTS:], first_two[SLOTS:], last_two[:SLOTS], first_two[:SLOTS]]
            got = list(sent)
            for k in range(1, n_tp):
                got[k] = swap(sent[k], "tp", k)
            at = own_place - r * SLOTS
            valid = (at >= 0) & (at < SLOTS)
            return got, jnp.where(valid, (own_owner.reshape(-1) ^ tp_index) * SLOTS + at, 0), valid

        def norm_rows(x):
            normed, _ = row_stats(x)
            return (normed * gain1 + bias1).astype(BF16)

        got0, place0, _ = rows_here(0, lists(0))
        code0 = (place0 // 8) * (8 * tiles) + place0 % 8
        got0, out_grad = lax.optimization_barrier((got0, out_grad))
        resid_x, hid1 = embed(code0, got0, pos_rows, gain1, bias1, n_tok)

        def more_rows(carry):
            r, x, _ = carry
            got, place, valid = rows_here(r, lists(r))
            new = jnp.take(jnp.concatenate(got), place, axis=0, mode="clip").astype(F32) + jnp.tile(pos_rows.astype(F32), (n_seq, 1))
            x = jnp.where(valid[:, None], new, x)
            return r + 1, x, norm_rows(x)

        _, resid_x, hid1 = lax.while_loop(lambda c: c[0] < rounds, more_rows, (jnp.int32(1), resid_x, hid1))

        og_parts = out_grad.reshape(n_tp, n_seq, seq_local, width)
        parts = [lax.dynamic_index_in_dim(og_parts, tp_index ^ k, 0, keepdims=False) for k in range(n_tp)]
        parts = [swap(part, "tp", k) if k else part for k, part in enumerate(parts)]
        me = jnp.reshape(tp_index, (1,))
        og = assemble(me, parts, (n_seq, n_tp, seq_local, width), (n_seq, 1, seq_local, width)).reshape(n_tok, width)

        qkv = (dot_nt(hid1, wqkv_t) + bqkv_w).astype(BF16)
        ctx, lse = attn_fwd(qkv, n_seq, seq, n_pair)
        resid_x1, hid2 = proj_norm(ctx, w_all, 2 * n_ff, resid_x, b_out.astype(F32)[None], gain2, bias2)
        act, d_up, d_b_up = ffn(hid2, og, w_all, bup_w)
        parts = down(me, act, w_all, resid_x1, b_down.astype(F32)[None], n_seq, n_tp)
        parts = [swap(part, "tp", k) if k else part for k, part in enumerate(parts)]
        layer_out = assemble(me, parts, (n_seq_dp, seq_local, width), (n_seq, seq_local, width))

        core = jnp.reshape(c_index, (1,))

        def piece_of(n_rows):
            return -(-n_rows // (4 * n_tp) // 24) * 24

        def every_piece(g):
            other = swap(g, "xx")
            return [g, other, swap(g, "cc"), swap(other, "cc")]

        x_and_core = jnp.stack([x_index, c_index])

        p_ff = piece_of(n_tp * ff)
        down_theirs = swap(grad_pieces(1 - core, act, og, n_tp, p_ff, 0, 1), "cc")
        up_theirs = swap(grad_pieces(1 - core, d_up, hid2, n_tp, p_ff, 0, 1), "cc")
        ff_grads = grad_pieces(core, act, og, n_tp, p_ff, 0, 2, plus=down_theirs)
        ff_grads = grad_pieces(core, d_up, hid2, n_tp, p_ff, 1, 2, plus=up_theirs, into=ff_grads)
        ff_grads = lax.psum_scatter(ff_grads, ("tp", "xx"), scatter_dimension=0, tiled=True)
        ff_grads = every_piece(ff_grads)

        d_resid1, d_attn, sums2 = back2(d_up, w_all, resid_x1, og, gain2)
        d_ctx = dot_nt(d_attn, wout_w).astype(BF16)
        n_small = n_tp * (b_qkv.size + ff) // width + 6
        p_pos = -(-(seq + n_small) // (24 * n_tp * n_dp)) * 24
        p_out = piece_of(wout_w.shape[0])
        spans = ((0, p_out), (p_out, p_out + piece_of(wqkv_t.shape[0])))

        def token_blocks(places, d_tok):
            parts = pack(places, d_tok, GRAD_SLOTS)
            blocks = [swap(part, "tp", k) if k else part for k, part in enumerate(parts)]
            other = []
            for block in blocks:
                other.append(swap(block, "xx"))
            return blocks + other + [swap(block, "cc") for block in blocks + other]

        d_qkv0 = attn_bwd(qkv, ctx, d_ctx, lse, 0, seq, n_pair)
        d_tok0, *sums0 = back1(d_qkv0, wqkv_t, resid_x, d_resid1, gain1, 0, p_pos * n_tp * n_dp)
        blocks0 = token_blocks(places0[0], d_tok0)
        d_qkv1 = attn_bwd(qkv, ctx, d_ctx, lse, 1, seq, n_pair)
        d_tok1, pos_all, sums1, sums_qkv = back1(d_qkv1, wqkv_t, resid_x, d_resid1, gain1, 1, p_pos * n_tp * n_dp, earlier=sums0)
        blocks1 = token_blocks(places0[1], d_tok1)
        d_qkvs = [d_qkv0, d_qkv1]
        rest_theirs = swap(grad_rest(1 - core, ctx, d_attn, d_qkvs, hid1, n_tp, spans), "cc")

        d_w_down, d_w_up = pieces_out(x_and_core, ff_grads, ((0, n_ff, False), (p_ff, n_ff, True)))
        image = accum(blocks0 + blocks1, code, block_first, sub_rows, width)
        d_emb = image.reshape(rows // 8, tiles, 8, 128).transpose(0, 2, 1, 3).reshape(rows, width)

        def more_grads(carry):
            r, table = carry
            at = rank - r * GRAD_SLOTS
            there = owned & (at >= 0) & (at < GRAD_SLOTS)
            dest = compact(at, there, jnp.where(owned, local, 0) + 1, GRAD_SLOTS)
            dest = jnp.where(dest == 0, rows, dest - 1)
            grads = jnp.concatenate(token_blocks(own_places(r, 0), d_tok0) + token_blocks(own_places(r, 1), d_tok1), axis=0).astype(F32)
            return r + 1, table.at[both_orders(dest).reshape(-1)].add(grads, mode="drop")

        _, d_emb = lax.while_loop(lambda c: c[0] < grad_rounds, more_grads, (jnp.int32(1), d_emb))

        small = jnp.concatenate([sums_qkv[0], d_b_up[0], sums1[:2].reshape(-1), sums2[:4].reshape(-1)]).reshape(-1, width)
        small = jnp.concatenate([small, jnp.zeros((pos_all.shape[0] - seq - n_small, width), F32)])
        pos_all = lax.dynamic_update_slice_in_dim(pos_all, small, seq, 0).reshape(n_tp * n_x, n_core, p_pos, width)
        pos_theirs = swap(lax.dynamic_index_in_dim(pos_all, 1 - c_index, 1, keepdims=False).reshape(-1, width), "cc")
        rest = grad_rest(core, ctx, d_attn, d_qkvs, hid1, n_tp, spans, plus=rest_theirs, tail=(pos_all, pos_theirs))
        rest = lax.psum_scatter(rest, ("tp", "xx"), scatter_dimension=0, tiled=True)
        rest_w = every_piece(rest[:spans[1][1]])
        whole = lax.all_gather(rest[spans[1][1]:], ("tp", "xx", "cc"), axis=0, tiled=True)
        d_pos = jnp.pad(whole[:seq], ((POS_OFFSET, pos_table.shape[0] - seq - POS_OFFSET), (0, 0)))
        small = whole[seq:seq + n_small].reshape(-1)
        n_b = b_qkv.size
        d_b_qkv = lax.dynamic_slice_in_dim(small, tp_index * n_b, n_b).reshape(n_core, 3, -1, b_qkv.shape[2])
        d_b_qkv = d_b_qkv.transpose(1, 0, 2, 3).reshape(b_qkv.shape)
        d_b_up = lax.dynamic_slice_in_dim(small, n_tp * n_b + tp_index * ff, ff)
        d_gain1, d_bias1, d_gain2, d_bias2, d_b_out, d_b_down = small[n_tp * (n_b + ff):].reshape(6, width)

        d_w_out, d_w_qkv = pieces_out(x_and_core, rest_w, ((0, n_out, False), (p_out, n_b // n_dp, False)))
        d_w_out = d_w_out.reshape(w_out.shape)
        d_w_qkv = d_w_qkv.reshape(n_core, 3, -1, w_qkv.shape[3], width).transpose(4, 1, 0, 2, 3).reshape(w_qkv.shape)
        return (layer_out, d_emb, d_pos, d_gain1, d_bias1, d_w_qkv, d_b_qkv, d_w_out,
                d_b_out, d_gain2, d_bias2, d_w_up, d_b_up, d_w_down, d_b_down)

    rep = P()
    in_specs = (P(dp, None), P("tp", None), rep, rep, rep,
                P(None, None, "tp", None), P(None, "tp", None), P("tp", None, None), rep,
                rep, rep, P(None, "tp"), P("tp"), P("tp", None), rep,
                P(dp, "tp", None))
    out_specs = (P(dp, "tp", None), P("tp", None), rep, rep, rep,
                 P(None, None, "tp", None), P(None, "tp", None), P("tp", None, None), rep,
                 rep, rep, P(None, "tp"), P("tp"), P("tp", None), rep)

    return jax.shard_map(local_step, mesh=mesh3, in_specs=in_specs, out_specs=out_specs, check_vma=False)
```

```python
import functools

import jax
import jax.numpy as jnp
from jax import lax
from jax.experimental import pallas as pl
from jax.experimental.pallas import tpu as pltpu
from jax.sharding import Mesh, PartitionSpec as P


F32 = jnp.float32
BF16 = jnp.bfloat16
MIB = 1024 * 1024
WIDEN = 32

BLK = 256


def dot_nt(a, b):
    return lax.dot_general(a, b, (((1,), (1,)), ((), ())), preferred_element_type=F32)


def dot_nn(a, b):
    return lax.dot_general(a, b, (((1,), (0,)), ((), ())), preferred_element_type=F32)


def head_only(x, head):
    half = x.shape[1] // 2
    lane = lax.broadcasted_iota(jnp.int32, x.shape, 1)
    keep = (lane < half) if head == 0 else (lane >= half)
    return jnp.where(keep, x, jnp.zeros((), x.dtype))


def attn_fwd_kernel(qkv_ref, ctx_ref, lse_ref, ctx_t):
    seq, width = ctx_ref.shape
    half = width // 2
    scale = half ** -0.5
    q2 = qkv_ref[:, 0:width] * jnp.asarray(scale, BF16)
    v_t = qkv_ref[:, 2 * width:3 * width].T
    tasks = [(head, i) for i in range(seq // BLK) for head in range(2)]

    def scores(head, i):
        return dot_nt(qkv_ref[0:(i + 1) * BLK, width:2 * width], head_only(q2[i * BLK:(i + 1) * BLK], head))

    ready = scores(*tasks[0])
    for n, (head, i) in enumerate(tasks):
        s = ready
        if n + 1 < len(tasks):
            ready = scores(*tasks[n + 1])
        lo, hi = i * BLK, (i + 1) * BLK
        v_h = v_t[head * half:(head + 1) * half, :]
        key = lax.broadcasted_iota(jnp.int32, (BLK, BLK), 0)
        qry = lax.broadcasted_iota(jnp.int32, (BLK, BLK), 1)
        diag = jnp.where(key <= qry, s[lo:hi], -1e30)
        top = jnp.max(diag, axis=0, keepdims=True)
        if i:
            top = jnp.maximum(top, jnp.max(s[0:lo], axis=0, keepdims=True))
        p_diag = jnp.exp(diag - top)
        total = jnp.sum(p_diag, axis=0, keepdims=True)
        if i:
            p_left = jnp.exp(s[0:lo] - top)
            total = total + jnp.sum(p_left, axis=0, keepdims=True)
        inv = 1.0 / total
        acc = dot_nn(v_h[:, lo:hi], (p_diag * inv).astype(BF16))
        if i:
            acc = acc + dot_nn(v_h[:, 0:lo], (p_left * inv).astype(BF16))
        ctx_t[head * half:(head + 1) * half, lo:hi] = acc
        lse_ref[head:head + 1, lo:hi] = top + jnp.log(total)
    ctx_ref[...] = ctx_t[...].T.astype(BF16)


def attn_fwd(qkv, n_seq, seq, n_pair):
    width = 128
    return pl.pallas_call(
        attn_fwd_kernel,
        grid=(n_seq, n_pair),
        in_specs=[pl.BlockSpec((seq, 3 * width), lambda b, p: (b, p))],
        out_specs=[pl.BlockSpec((seq, width), lambda b, p: (b, p)),
                   pl.BlockSpec((None, None, 2, seq), lambda b, p: (b, p, 0, 0))],
        out_shape=[jax.ShapeDtypeStruct((n_seq * seq, n_pair * width), BF16),
                   jax.ShapeDtypeStruct((n_seq, n_pair, 2, seq), F32)],
        scratch_shapes=[pltpu.VMEM((width, seq), F32)],
        name="attn_fwd",
        cost_estimate=pl.CostEstimate(flops=n_seq * n_pair * 8 * seq * seq * 256 * 10 // 16, bytes_accessed=n_seq * seq * n_pair * width * 8,
                                      transcendentals=n_seq * n_pair * seq * seq),
        compiler_params=pltpu.CompilerParams(vmem_limit_bytes=63 * 1024 * 1024),
    )(qkv)


def attn_bwd_kernel(qkv_ref, ctx_ref, dctx_ref, lse_ref, dqkv_ref, dk_t, dv_t):
    seq, width = ctx_ref.shape
    half = width // 2
    scale = half ** -0.5
    q2 = qkv_ref[:, 0:width] * jnp.asarray(scale, BF16)
    q_t = q2.T
    do_t = dctx_ref[...].T
    lse_c = jnp.concatenate([lse_ref[...], jnp.zeros((6, seq), F32)], axis=0).T
    prod = dctx_ref[...].astype(F32) * ctx_ref[...].astype(F32)
    tasks = [(head, i) for i in range(seq // BLK) for head in range(2)]

    def scores(head, i):
        lo, hi = i * BLK, (i + 1) * BLK
        return (dot_nt(head_only(q2[lo:hi], head), qkv_ref[0:hi, width:2 * width]),
                dot_nt(head_only(dctx_ref[lo:hi, :], head), qkv_ref[0:hi, 2 * width:3 * width]))

    dq = []
    ready = scores(*tasks[0])
    for n, (head, i) in enumerate(tasks):
        s, dp = ready
        if n + 1 < len(tasks):
            ready = scores(*tasks[n + 1])
        lo, hi = i * BLK, (i + 1) * BLK
        rows = slice(head * half, (head + 1) * half)
        mean = jnp.sum(head_only(prod[lo:hi], head), axis=1, keepdims=True)
        lse = lse_c[lo:hi, head:head + 1]
        qry = lax.broadcasted_iota(jnp.int32, (BLK, BLK), 0)
        key = lax.broadcasted_iota(jnp.int32, (BLK, BLK), 1)
        p_diag = jnp.where(key <= qry, jnp.exp(s[:, lo:hi] - lse), 0.0)
        ds_diag = (p_diag * (dp[:, lo:hi] - mean)).astype(BF16)
        dv_t[rows, lo:hi] = dot_nn(do_t[rows, lo:hi], p_diag.astype(BF16))
        dk_t[rows, lo:hi] = dot_nn(q_t[rows, lo:hi], ds_diag)
        dq_h = dot_nn(ds_diag, qkv_ref[lo:hi, width:2 * width])
        if i:
            p_left = jnp.exp(s[:, 0:lo] - lse)
            ds_left = (p_left * (dp[:, 0:lo] - mean)).astype(BF16)
            dv_t[rows, 0:lo] += dot_nn(do_t[rows, lo:hi], p_left.astype(BF16))
            dk_t[rows, 0:lo] += dot_nn(q_t[rows, lo:hi], ds_left)
            dq_h = dq_h + dot_nn(ds_left, qkv_ref[0:lo, width:2 * width])
        dq.append(dq_h)
        if head == 1:
            lane = lax.broadcasted_iota(jnp.int32, (BLK, width), 1)
            dqkv_ref[lo:hi, 0:width] = (jnp.where(lane < half, dq[0], dq[1]) * scale).astype(BF16)
            dq = []
    dqkv_ref[:, width:2 * width] = dk_t[...].T.astype(BF16)
    dqkv_ref[:, 2 * width:3 * width] = dv_t[...].T.astype(BF16)


def attn_bwd(qkv, ctx, dctx, lse, at, seq, n_pair):
    width = 128
    return pl.pallas_call(
        attn_bwd_kernel,
        grid=(n_pair,),
        in_specs=[pl.BlockSpec((seq, 3 * width), lambda p: (at, p)),
                  pl.BlockSpec((seq, width), lambda p: (at, p)),
                  pl.BlockSpec((seq, width), lambda p: (at, p)),
                  pl.BlockSpec((None, None, 2, seq), lambda p: (at, p, 0, 0))],
        out_specs=pl.BlockSpec((seq, 3 * width), lambda p: (0, p)),
        out_shape=jax.ShapeDtypeStruct((seq, n_pair * 3 * width), BF16),
        scratch_shapes=[pltpu.VMEM((width, seq), F32), pltpu.VMEM((width, seq), F32)],
        name="attn_bwd",
        cost_estimate=pl.CostEstimate(flops=n_pair * 20 * seq * seq * 256 * 10 // 16, bytes_accessed=seq * n_pair * width * 16,
                                      transcendentals=n_pair * seq * seq),
        compiler_params=pltpu.CompilerParams(vmem_limit_bytes=63 * 1024 * 1024),
    )(qkv, ctx, dctx, lse)


LN_EPS = 1e-5
GELU_S = 0.7978845608028654
GELU_A = 0.044715


def row_mean(v):
    return jnp.sum(v, axis=1, keepdims=True) * (1.0 / v.shape[1])


def row_stats(v):
    centered = v - row_mean(v)
    inv_std = lax.rsqrt(row_mean(centered * centered) + LN_EPS)
    return centered * inv_std, inv_std


def norm_back(d_y, x_in, gain):
    normed, inv_std = row_stats(x_in)
    d_norm = d_y * gain
    d_x = inv_std * (d_norm - row_mean(d_norm) - normed * row_mean(d_norm * normed))
    return d_x, d_y * normed


def col_sum(v):
    return jnp.sum(v, axis=0, keepdims=True)


def to_image(rows, image, base):
    tiles = rows.shape[1] // 128
    for h in range(rows.shape[0] // 8):
        for c in range(tiles):
            image[pl.ds(base + (h * tiles + c) * 8, 8), :] = rows[h * 8:(h + 1) * 8, c * 128:(c + 1) * 128]


def from_image(image, base, n_rows, width):
    tiles = width // 128
    return jnp.concatenate([jnp.concatenate([image[pl.ds(base + (h * tiles + c) * 8, 8), :] for c in range(tiles)], axis=1)
                            for h in range(n_rows // 8)], axis=0)


def pick_rows(code_ref, first, stage, image, n_rows, tiles):
    def pick(g, _):
        base = pl.multiple_of(g * 16 * tiles, 16 * tiles)
        for j in range(16):
            row = stage[pl.ds(code_ref[first + g * 16 + j], tiles, stride=8), :]
            image[pl.ds(base + (j // 8) * 8 * tiles + j % 8, tiles, stride=8), :] = row
        return 0

    lax.fori_loop(0, n_rows // 16, pick, 0)


def embed_kernel(n_blk, cap, code_ref, *refs):
    tok_refs = refs[:n_blk]
    pos_ref, gain_ref, bias_ref, x_ref, hid_ref, stage, image = refs[n_blk:]
    rows, width = x_ref.shape
    tiles = width // 128

    @pl.when(pl.program_id(0) == 0)
    def _():
        for b in range(n_blk):
            def widen(g, _, b=b):
                part = tok_refs[b][pl.ds(pl.multiple_of(g * WIDEN, WIDEN), WIDEN), :].astype(F32)
                to_image(part, stage, pl.multiple_of((b * cap + g * WIDEN) * tiles, WIDEN * tiles))
                return 0

            lax.fori_loop(0, cap // WIDEN, widen, 0)

    pick_rows(code_ref, pl.program_id(0) * rows, stage, image, rows, tiles)
    part = 64
    for i in range(rows // part):
        at = slice(i * part, (i + 1) * part)
        x = from_image(image, i * part * tiles, part, width) + pos_ref[at, :].astype(F32)
        x_ref[at, :] = x
        normed, _ = row_stats(x)
        hid_ref[at, :] = (normed * gain_ref[...] + bias_ref[...]).astype(BF16)


def embed(code, blocks, pos_rows, gain, bias, n_tok):
    cap, width = blocks[0].shape
    seq = pos_rows.shape[0]
    rows = 256
    per_seq = seq // rows
    n_blk = len(blocks)
    vec = pl.BlockSpec((1, width), lambda i: (0, 0))
    return pl.pallas_call(
        functools.partial(embed_kernel, n_blk, cap),
        grid=(n_tok // rows,),
        in_specs=[pl.BlockSpec(memory_space=pltpu.SMEM)]
        + [pl.BlockSpec((cap, width), lambda i: (0, 0), pipeline_mode=pl.Buffered(1))] * n_blk
        + [pl.BlockSpec((rows, width), lambda i: (i % per_seq, 0)), vec, vec],
        out_specs=[pl.BlockSpec((rows, width), lambda i: (i, 0))] * 2,
        out_shape=[jax.ShapeDtypeStruct((n_tok, width), F32), jax.ShapeDtypeStruct((n_tok, width), BF16)],
        scratch_shapes=[pltpu.VMEM((n_blk * cap * width // 128, 128), F32), pltpu.VMEM((rows * width // 128, 128), F32)],
        name="embed_norm",
        cost_estimate=pl.CostEstimate(flops=15_000_000_000, bytes_accessed=n_tok * width * 10, transcendentals=0),
        compiler_params=pltpu.CompilerParams(vmem_limit_bytes=63 * 1024 * 1024),
    )(code, *blocks, pos_rows, gain, bias)


def pack_kernel(n_blk, code_ref, tok_ref, *refs):
    out_refs = refs[:n_blk]
    stage, image = refs[n_blk:]
    n_tok, width = tok_ref.shape
    cap = out_refs[0].shape[0]
    tiles = width // 128

    def widen(g, _):
        part = tok_ref[pl.ds(pl.multiple_of(g * WIDEN, WIDEN), WIDEN), :].astype(F32)
        to_image(part, stage, pl.multiple_of(g * WIDEN * tiles, WIDEN * tiles))
        return 0

    lax.fori_loop(0, n_tok // WIDEN, widen, 0)
    for b in range(n_blk):
        pick_rows(code_ref, b * cap, stage, image, cap, tiles)

        def narrow(g, _, b=b):
            part = from_image(image, pl.multiple_of(g * WIDEN * tiles, WIDEN * tiles), WIDEN, width)
            out_refs[b][pl.ds(pl.multiple_of(g * WIDEN, WIDEN), WIDEN), :] = part.astype(BF16)
            return 0

        lax.fori_loop(0, cap // WIDEN, narrow, 0)


def pack(code, tok, cap):
    n_tok, width = tok.shape
    n_blk = code.shape[0] // cap
    return pl.pallas_call(
        functools.partial(pack_kernel, n_blk),
        in_specs=[pl.BlockSpec(memory_space=pltpu.SMEM), pl.BlockSpec(memory_space=pltpu.VMEM)],
        out_specs=[pl.BlockSpec(memory_space=pltpu.VMEM)] * n_blk,
        out_shape=[jax.ShapeDtypeStruct((cap, width), BF16)] * n_blk,
        scratch_shapes=[pltpu.VMEM((n_tok * width // 128, 128), F32), pltpu.VMEM((cap * width // 128, 128), F32)],
        name="token_pack",
        cost_estimate=pl.CostEstimate(flops=15_000_000_000, bytes_accessed=n_tok * width * 5, transcendentals=0),
        compiler_params=pltpu.CompilerParams(vmem_limit_bytes=63 * 1024 * 1024),
    )(code, tok)


def proj_kernel(c_ref, w_ref, x_ref, b_ref, gain_ref, bias_ref, x1_ref, hid_ref):
    part = x_ref.shape[0] // 2
    for i in range(2):
        at = slice(i * part, (i + 1) * part)
        x1 = x_ref[at, :] + dot_nn(c_ref[at, :], w_ref[...].reshape(c_ref.shape[1], -1)).astype(BF16).astype(F32) + b_ref[...]
        x1_ref[at, :] = x1
        normed, _ = row_stats(x1)
        hid_ref[at, :] = (normed * gain_ref[...] + bias_ref[...]).astype(BF16)


def proj_norm(ctx, w, start, x, b, gain, bias):
    n_tok, width = x.shape
    n_row = ctx.shape[1] // w.shape[0]
    rows = 512
    vec = pl.BlockSpec((1, width), lambda i: (0, 0))
    mat = pl.BlockSpec((rows, width), lambda i: (i, 0))
    return pl.pallas_call(
        proj_kernel,
        grid=(n_tok // rows,),
        in_specs=[pl.BlockSpec((rows, ctx.shape[1]), lambda i: (i, 0)), pl.BlockSpec((w.shape[0], n_row, width), lambda i: (0, start // n_row, 0)), mat, vec, vec, vec],
        out_specs=[mat, mat],
        out_shape=[jax.ShapeDtypeStruct((n_tok, width), F32), jax.ShapeDtypeStruct((n_tok, width), BF16)],
        name="proj_norm",
        cost_estimate=pl.CostEstimate(flops=2 * n_tok * ctx.shape[1] * width, bytes_accessed=n_tok * width * 12, transcendentals=0),
        compiler_params=pltpu.CompilerParams(vmem_limit_bytes=63 * 1024 * 1024),
    )(ctx, w, x, b, gain, bias)


def ffn_kernel(part, h_ref, og_ref, wu_ref, wd_ref, b_ref, act_ref, dup_ref, db_ref):
    total = jnp.zeros(db_ref.shape, F32)
    for i in range(h_ref.shape[0] // part):
        at = slice(i * part, (i + 1) * part)
        z = dot_nt(h_ref[at, :], wu_ref[0]) + b_ref[...]
        d_act = dot_nt(og_ref[at, :], wd_ref[0])
        z2 = z * z
        gate = 0.5 * jnp.tanh(z * (GELU_S + (GELU_S * GELU_A) * z2)) + 0.5
        act = z * gate
        d_up = d_act * (gate + act * (1.0 - gate) * (2.0 * GELU_S + (6.0 * GELU_S * GELU_A) * z2))
        act_ref[at, :] = act.astype(BF16)
        dup_ref[at, :] = d_up.astype(BF16)
        total = total + col_sum(d_up)
    db_ref[...] = total


def ffn(hid, og, w, b_up, part=1024):
    n_tok, width = hid.shape
    ff = b_up.shape[1]
    n_piece = w.shape[0]
    bn = ff // n_piece
    whole = pl.BlockSpec((n_tok, width), lambda i: (0, 0), pipeline_mode=pl.Buffered(1))
    ospec = pl.BlockSpec((n_tok, bn), lambda i: (0, i))
    vec = pl.BlockSpec((1, bn), lambda i: (0, i))
    return pl.pallas_call(
        functools.partial(ffn_kernel, part),
        grid=(n_piece,),
        in_specs=[whole, whole, pl.BlockSpec((1, bn, width), lambda i: (i, 0, 0)), pl.BlockSpec((1, bn, width), lambda i: (i, 1, 0)), vec],
        out_specs=[ospec, ospec, vec],
        out_shape=[jax.ShapeDtypeStruct((n_tok, ff), BF16), jax.ShapeDtypeStruct((n_tok, ff), BF16), jax.ShapeDtypeStruct((1, ff), F32)],
        name="ffn",
        cost_estimate=pl.CostEstimate(flops=4 * n_tok * ff * width, bytes_accessed=4 * n_tok * ff + 4 * ff * width, transcendentals=n_tok * ff),
        compiler_params=pltpu.CompilerParams(vmem_limit_bytes=63 * 1024 * 1024),
    )(hid, og, w, w, b_up)


def down_kernel(n_tp, me_ref, act_ref, w_ref, x1_ref, b_ref, *out_refs):
    out = x1_ref[...] + dot_nn(act_ref[...], w_ref[...].reshape(act_ref.shape[1], -1)).astype(BF16).astype(F32) + b_ref[...]
    k = me_ref[0] ^ (pl.program_id(0) % n_tp)
    seq = pl.program_id(0) // n_tp
    for j in range(n_tp):
        @pl.when(k == j)
        def _(j=j):
            out_refs[j][seq] = out.astype(BF16)


def down(me, act, w, x1, b, n_seq, n_tp):
    n_tok, width = x1.shape
    ff = act.shape[1]
    rows = n_tok // n_seq // n_tp
    part = jax.ShapeDtypeStruct((n_seq, rows, width), BF16)
    return pl.pallas_call(
        functools.partial(down_kernel, n_tp),
        grid_spec=pltpu.PrefetchScalarGridSpec(
            num_scalar_prefetch=1, grid=(n_seq * n_tp,),
            in_specs=[pl.BlockSpec((rows, ff), lambda i, m: (i, 0)),
                      pl.BlockSpec((w.shape[0], ff // w.shape[0], width), lambda i, m: (0, 1, 0), pipeline_mode=pl.Buffered(1)),
                      pl.BlockSpec((rows, width), lambda i, m: (i, 0)), pl.BlockSpec((1, width), lambda i, m: (0, 0))],
            out_specs=[pl.BlockSpec(part.shape, lambda i, m: (0, 0, 0))] * n_tp),
        out_shape=[part] * n_tp,
        name="down",
        cost_estimate=pl.CostEstimate(flops=2 * n_tok * ff * width, bytes_accessed=2 * n_tok * ff + n_tok * width * 6, transcendentals=0),
        compiler_params=pltpu.CompilerParams(vmem_limit_bytes=63 * 1024 * 1024),
    )(me, act, w, x1, b)


def back2_kernel(dup_ref, w_ref, x1_ref, og_ref, gain_ref, dr_ref, da_ref, sums_ref):
    @pl.when(pl.program_id(0) == 0)
    def _():
        sums_ref[...] = jnp.zeros(sums_ref.shape, F32)

    n_part = 2
    part = dr_ref.shape[0] // n_part
    w = w_ref[...].reshape(dup_ref.shape[1], -1)
    d_ys = [dot_nn(dup_ref[i * part:(i + 1) * part, :], w) for i in range(n_part)]
    for i in range(n_part):
        at = slice(i * part, (i + 1) * part)
        d_y = d_ys[i].astype(BF16).astype(F32)
        d_x, d_gain = norm_back(d_y, x1_ref[at, :], gain_ref[...])
        og = og_ref[at, :].astype(F32)
        d_resid = og + d_x
        dr_ref[at, :] = d_resid
        da_ref[at, :] = d_resid.astype(BF16)
        sums_ref[0:1, :] += col_sum(d_gain)
        sums_ref[1:2, :] += col_sum(d_y)
        sums_ref[2:3, :] += col_sum(d_resid)
        sums_ref[3:4, :] += col_sum(og)


def back2(d_up, w, x1, og, gain):
    n_tok, width = x1.shape
    ff = d_up.shape[1]
    rows = 256
    mat = pl.BlockSpec((rows, width), lambda i: (i, 0))
    return pl.pallas_call(
        back2_kernel,
        grid=(n_tok // rows,),
        in_specs=[pl.BlockSpec((rows, ff), lambda i: (i, 0)), pl.BlockSpec((w.shape[0], ff // w.shape[0], width), lambda i: (0, 0, 0), pipeline_mode=pl.Buffered(1)),
                  mat, mat, pl.BlockSpec((1, width), lambda i: (0, 0))],
        out_specs=[mat, mat, pl.BlockSpec((8, width), lambda i: (0, 0))],
        out_shape=[jax.ShapeDtypeStruct((n_tok, width), F32), jax.ShapeDtypeStruct((n_tok, width), BF16), jax.ShapeDtypeStruct((8, width), F32)],
        name="ffn_back",
        cost_estimate=pl.CostEstimate(flops=2 * n_tok * ff * width, bytes_accessed=2 * n_tok * ff + n_tok * width * 12, transcendentals=0),
        compiler_params=pltpu.CompilerParams(vmem_limit_bytes=63 * 1024 * 1024),
    )(d_up, w, x1, og, gain)


def back1_kernel(dq_ref, w_ref, x_ref, dr_ref, gain_ref, *refs):
    tok_ref, pos_ref, sums_ref, bsum_ref = refs[-4:]
    before_refs = refs[:-4]

    @pl.when(pl.program_id(0) == 0)
    def _():
        sums_ref[...] = before_refs[1][...] if before_refs else jnp.zeros(sums_ref.shape, F32)
        bsum_ref[...] = before_refs[2][...] if before_refs else jnp.zeros(bsum_ref.shape, F32)

    n_part = 2
    part = tok_ref.shape[0] // n_part
    d_ys = [dot_nn(dq_ref[i * part:(i + 1) * part, :], w_ref[...]) for i in range(n_part)]
    for i in range(n_part):
        at = slice(i * part, (i + 1) * part)
        d_y = d_ys[i].astype(BF16).astype(F32)
        d_x, d_gain = norm_back(d_y, x_ref[at, :], gain_ref[...])
        d_resid = dr_ref[at, :] + d_x
        tok_ref[at, :] = d_resid.astype(BF16)
        pos_ref[at, :] = before_refs[0][at, :] + d_resid if before_refs else d_resid
        sums_ref[0:1, :] += col_sum(d_gain)
        sums_ref[1:2, :] += col_sum(d_y)
        bsum_ref[0:1, :] += col_sum(dq_ref[at, :].astype(F32))


def back1(d_qkv, w_qkv, x, d_resid1, gain, at, pos_rows, earlier=None):
    seq, n_cols = d_qkv.shape
    width = x.shape[1]
    rows = 256
    steps = seq // rows
    mat = pl.BlockSpec((rows, width), lambda i: (at * steps + i, 0))
    out = pl.BlockSpec((rows, width), lambda i: (i, 0))
    few = [pl.BlockSpec((8, width), lambda i: (0, 0)), pl.BlockSpec((8, n_cols), lambda i: (0, 0))]
    return pl.pallas_call(
        back1_kernel,
        grid=(steps,),
        in_specs=[pl.BlockSpec((rows, n_cols), lambda i: (i, 0)),
                  pl.BlockSpec((n_cols, width), lambda i: (0, 0), pipeline_mode=pl.Buffered(1)),
                  mat, mat, pl.BlockSpec((1, width), lambda i: (0, 0))] + ([out] + few if earlier else []),
        out_specs=[out, out] + few,
        out_shape=[jax.ShapeDtypeStruct((seq, width), BF16), jax.ShapeDtypeStruct((pos_rows, width), F32),
                   jax.ShapeDtypeStruct((8, width), F32), jax.ShapeDtypeStruct((8, n_cols), F32)],
        name="qkv_back",
        cost_estimate=pl.CostEstimate(flops=2 * seq * n_cols * width, bytes_accessed=2 * seq * n_cols + seq * width * 12, transcendentals=0),
        compiler_params=pltpu.CompilerParams(vmem_limit_bytes=63 * 1024 * 1024),
    )(d_qkv, w_qkv, x, d_resid1, gain, *(earlier or ()))


def pieces_out_kernel(n_in, spans, me_ref, *refs):
    out_refs = refs[n_in:]
    for p in range(n_in):
        @pl.when(pl.program_id(0) == p)
        def _(p=p):
            for (start, n, turned), out_ref in zip(spans, out_refs):
                part = refs[p][start:start + n, :]
                out_ref[...] = part.T if turned else part


def pieces_out(me, pieces, spans):
    rows, width = pieces[0].shape
    n_in = len(pieces)

    def place(p, m):
        return (m[1] ^ (p // 2)) * 2 + (m[0] ^ (p % 2))

    out_specs, out_shape = [], []
    for start, n, turned in spans:
        if turned:
            out_specs.append(pl.BlockSpec((width, n), lambda p, m: (0, place(p, m))))
            out_shape.append(jax.ShapeDtypeStruct((width, n_in * n), F32))
        else:
            out_specs.append(pl.BlockSpec((n, width), lambda p, m: (place(p, m), 0)))
            out_shape.append(jax.ShapeDtypeStruct((n_in * n, width), F32))
    return pl.pallas_call(
        functools.partial(pieces_out_kernel, n_in, spans),
        grid_spec=pltpu.PrefetchScalarGridSpec(
            num_scalar_prefetch=1, grid=(n_in,),
            in_specs=[pl.BlockSpec((rows, width), lambda p, m: (0, 0), pipeline_mode=pl.Buffered(1))] * n_in,
            out_specs=out_specs),
        out_shape=out_shape,
        name="grads_out",
        cost_estimate=pl.CostEstimate(flops=8_000_000_000, bytes_accessed=n_in * rows * width * 8, transcendentals=0),
        compiler_params=pltpu.CompilerParams(vmem_limit_bytes=63 * 1024 * 1024),
    )(me, *pieces)


def assemble_kernel(n, me_ref, *refs):
    out_ref = refs[n]
    k = me_ref[0] ^ pl.program_id(0)
    for j in range(n):
        @pl.when(k == j)
        def _(j=j):
            out_ref[...] = refs[j][...].reshape(out_ref.shape)


def assemble(me, parts, out_shape, block):
    at = 1 if len(out_shape) == 4 else 0
    return pl.pallas_call(
        functools.partial(assemble_kernel, len(parts)),
        grid_spec=pltpu.PrefetchScalarGridSpec(
            num_scalar_prefetch=1, grid=(len(parts),),
            in_specs=[pl.BlockSpec(p.shape, lambda i, m: (0, 0, 0), pipeline_mode=pl.Buffered(1)) for p in parts],
            out_specs=pl.BlockSpec(block, lambda i, m: tuple(i if d == at else 0 for d in range(len(block))))),
        out_shape=jax.ShapeDtypeStruct(out_shape, parts[0].dtype),
        name="assemble",
        cost_estimate=pl.CostEstimate(flops=4_000_000_000, bytes_accessed=16 * MIB, transcendentals=0),
        compiler_params=pltpu.CompilerParams(vmem_limit_bytes=63 * 1024 * 1024),
    )(me, *parts)


LANES = 128


def accum_kernel(n_block, cap, sub_rows, width, where_ref, first_ref, *refs):
    tok_refs = refs[:n_block]
    out_ref = refs[n_block]
    n_sub = len(sub_rows)
    acc = refs[n_block + 1:n_block + 1 + n_sub]
    buf, stage, in_sem, out_sem = refs[n_block + 1 + n_sub:]
    tiles = width // LANES
    group = 8 * tiles

    def fetch(block, n):
        return pltpu.make_async_copy(tok_refs[n], buf.at[block % 2], in_sem.at[block % 2])

    def fetch_next(block):
        for n in range(n_block):
            @pl.when(block == n)
            def _(n=n):
                fetch(block, n).start()

    fetch_next(0)
    for s in range(n_sub):
        def clear(i, _, s=s):
            acc[s][pl.ds(pl.multiple_of(i * group, group), group), :] = jnp.zeros((group, LANES), F32)
            return 0

        lax.fori_loop(0, sub_rows[s] // 8, clear, 0)

    def add_rows(s, slot, n):
        codes = [where_ref[slot + j] for j in range(n)]
        at = [code >> 16 for code in codes]
        rows = [stage[pl.ds(code & 0xffff, tiles, stride=8), :] for code in codes]
        sums = [acc[s][pl.ds(a, tiles, stride=8), :] for a in at]
        for j in range(n):
            for i in range(j):
                sums[j] = jnp.where(at[i] == at[j], sums[i], sums[j])
            sums[j] = sums[j] + rows[j]
        for j in range(n):
            acc[s][pl.ds(at[j], tiles, stride=8), :] = sums[j]

    def add_block(block, _):
        fetch_next(block + 1)
        fetch(block, 0).wait()

        def widen(g, _):
            rows = buf[block % 2, pl.ds(pl.multiple_of(g * WIDEN, WIDEN), WIDEN), :].astype(F32)
            base = pl.multiple_of(g * (WIDEN // 8) * group, (WIDEN // 8) * group)
            for h in range(WIDEN // 8):
                for c in range(tiles):
                    stage[pl.ds(base + h * group + c * 8, 8), :] = rows[h * 8:(h + 1) * 8, c * LANES:(c + 1) * LANES]
            return 0

        lax.fori_loop(0, cap // WIDEN, widen, 0)

        starts = [first_ref[block * (n_sub + 1) + s] for s in range(n_sub + 1)]
        counts = [starts[s + 1] - starts[s] for s in range(n_sub)]
        both = functools.reduce(jnp.minimum, counts) // 2
        begin = [block * cap + starts[s] for s in range(n_sub)]

        def together(i, _):
            for s in range(n_sub):
                add_rows(s, begin[s] + 2 * i, 2)
            return 0

        lax.fori_loop(0, both, together, 0)
        for s in range(n_sub):
            fours = (counts[s] - 2 * both) // 4

            def alone(i, _, s=s):
                add_rows(s, begin[s] + 2 * both + 4 * i, 4)
                return 0

            lax.fori_loop(0, fours, alone, 0)

            def single(i, _, s=s):
                add_rows(s, begin[s] + i, 1)
                return 0

            lax.fori_loop(2 * both + 4 * fours, counts[s], single, 0)
        return 0

    lax.fori_loop(0, n_block, add_block, 0)
    done = 0
    copies = []
    for s in range(n_sub):
        n = sub_rows[s] * tiles
        copies.append(pltpu.make_async_copy(acc[s], out_ref.at[pl.ds(done, n), :], out_sem.at[s]))
        copies[-1].start()
        done += n
    for c in copies:
        c.wait()


def accum(tok_blocks, code, first, sub_rows, width):
    n_block = len(tok_blocks)
    cap = tok_blocks[0].shape[0]
    n_sub = len(sub_rows)
    tiles = width // LANES
    return pl.pallas_call(
        functools.partial(accum_kernel, n_block, cap, sub_rows, width),
        in_specs=[pl.BlockSpec(memory_space=pltpu.SMEM), pl.BlockSpec(memory_space=pltpu.SMEM)]
        + [pl.BlockSpec(memory_space=pl.ANY)] * n_block,
        out_specs=pl.BlockSpec(memory_space=pl.ANY),
        out_shape=jax.ShapeDtypeStruct((sum(sub_rows) * tiles, LANES), F32),
        scratch_shapes=[pltpu.VMEM((r * tiles, LANES), F32) for r in sub_rows]
        + [pltpu.VMEM((2, cap, width), BF16), pltpu.VMEM((cap * tiles, LANES), F32),
           pltpu.SemaphoreType.DMA((2,)), pltpu.SemaphoreType.DMA((n_sub,))],
        name="table_accum",
        cost_estimate=pl.CostEstimate(flops=50_000_000_000, bytes_accessed=100_000_000, transcendentals=0),
        compiler_params=pltpu.CompilerParams(vmem_limit_bytes=63 * 1024 * 1024),
    )(code, first, *tok_blocks)


def dot_tn(a, b):
    return lax.dot_general(a, b, (((0,), (0,)), ((), ())), preferred_element_type=F32)


def grad_kernel(has_plus, core_ref, a_ref, b_ref, *refs):
    out_ref = refs[-1]
    n = a_ref.shape[1]
    g = dot_tn(a_ref[...], b_ref[...])
    out_ref[0:n, :] = g + refs[0][0:n, :] if has_plus else g
    if out_ref.shape[0] > n:
        out_ref[n:, :] = jnp.zeros((out_ref.shape[0] - n, out_ref.shape[1]), F32)


def grad_pieces(core, a, b, n_tp, piece, which, n_which, plus=None, into=None):
    n_tok, n_cols = a.shape
    width = b.shape[1]
    bn = n_cols // (4 * n_tp)
    out_spec = pl.BlockSpec((piece, width), lambda p, c: (n_which * p + which, 0))
    in_specs = [pl.BlockSpec((n_tok, bn), lambda p, c: (0, 4 * (p // 2) + 2 * c[0] + p % 2)),
                pl.BlockSpec((n_tok, width), lambda p, c: (0, 0), pipeline_mode=pl.Buffered(1))]
    args = [a, b]
    if plus is not None:
        in_specs.append(pl.BlockSpec((piece, width), lambda p, c: (p, 0)))
        args.append(plus)
    if into is not None:
        in_specs.append(pl.BlockSpec(memory_space=pl.ANY))
        args.append(into)
    return pl.pallas_call(
        functools.partial(grad_kernel, plus is not None),
        grid_spec=pltpu.PrefetchScalarGridSpec(num_scalar_prefetch=1, grid=(2 * n_tp,), in_specs=in_specs, out_specs=out_spec),
        out_shape=jax.ShapeDtypeStruct((2 * n_tp * n_which * piece, width), F32),
        input_output_aliases={} if into is None else {len(args): 0},
        name="weight_grad",
        cost_estimate=pl.CostEstimate(flops=n_tok * n_cols * width, bytes_accessed=n_tok * (n_cols + 2 * width) + 2 * n_cols * width,
                                      transcendentals=0),
        compiler_params=pltpu.CompilerParams(vmem_limit_bytes=63 * 1024 * 1024),
    )(core, *args)


def grad_rest_kernel(spans, last, n_a2, core_ref, a1_ref, b1_ref, b2_ref, *refs):
    a2_refs, refs, out_ref = refs[:n_a2], refs[n_a2:-1], refs[-1]
    plus = refs[0] if refs else None
    piece, piece_in = out_ref.shape[0] // 2, (plus.shape[0] // 2 if refs else 0)
    rows = b2_ref.shape[0] // n_a2
    for which, (start, stop) in enumerate(spans):
        half = (a2_refs[0] if which else a1_ref).shape[1] // 2
        for i in range(0, 2 * half, 128):
            cols = slice(i, i + 128)
            if which:
                g = sum(dot_tn(a_ref[:, cols], b2_ref[n * rows:(n + 1) * rows, :]) for n, a_ref in enumerate(a2_refs))
            else:
                g = dot_tn(a1_ref[:, cols], b1_ref[...])
            for x in range(2):
                lo, hi = max(i, x * half), min(i + 128, (x + 1) * half)
                if lo < hi:
                    to = lo - x * half + start
                    part = g[lo - i:hi - i]
                    if plus is not None:
                        part = part + plus[x * piece_in + to:x * piece_in + to + hi - lo, :]
                    out_ref[x * piece + to:x * piece + to + hi - lo, :] = part
        for x in range(2):
            if stop > start + half:
                out_ref[x * piece + start + half:x * piece + stop, :] = jnp.zeros((stop - start - half, out_ref.shape[1]), F32)
    if last:
        for x in range(2):
            out_ref[x * piece + spans[-1][1]:(x + 1) * piece, :] = refs[1][x, 0] + refs[2][x * last:(x + 1) * last, :]


def grad_rest(core, a1, b1, a2, b2, n_tp, spans, plus=None, tail=None):
    n_tok, width = b1.shape
    last = tail[0].shape[2] if tail else 0
    piece = spans[-1][1] + last
    whole = pl.BlockSpec((n_tok, width), lambda t, c: (0, 0), pipeline_mode=pl.Buffered(1))
    cols = [pl.BlockSpec((a.shape[0], a.shape[1] // (2 * n_tp)), lambda t, c: (0, 2 * t + c[0])) for a in (a1, *a2)]
    in_specs, args = [cols[0], whole, whole] + cols[1:], [a1, b1, b2, *a2]
    if plus is not None:
        in_specs.append(pl.BlockSpec((plus.shape[0] // n_tp, width), lambda t, c: (t, 0)))
        args.append(plus)
    if tail:
        in_specs.append(pl.BlockSpec((2, 1, last, width), lambda t, c: (t, c[0], 0, 0)))
        in_specs.append(pl.BlockSpec((2 * last, width), lambda t, c: (t, 0)))
        args += tail
    n_cols = a1.shape[1] + a2[0].shape[1]
    return pl.pallas_call(
        functools.partial(grad_rest_kernel, spans, last, len(a2)),
        grid_spec=pltpu.PrefetchScalarGridSpec(num_scalar_prefetch=1, grid=(n_tp,), in_specs=in_specs,
                                               out_specs=pl.BlockSpec((2 * piece, width), lambda t, c: (t, 0))),
        out_shape=jax.ShapeDtypeStruct((2 * n_tp * piece, width), F32),
        name="weight_grads",
        cost_estimate=pl.CostEstimate(flops=n_tok * n_cols * width, bytes_accessed=n_tok * (n_cols + 4 * width) + 2 * n_cols * width,
                                      transcendentals=0),
        compiler_params=pltpu.CompilerParams(vmem_limit_bytes=63 * 1024 * 1024),
    )(core, *args)


POS_OFFSET = 2
SLOTS = 704
GRAD_SLOTS = 384
LOW = 32


def before(n):
    return (lax.broadcasted_iota(jnp.int32, (n, n), 1) < lax.broadcasted_iota(jnp.int32, (n, n), 0)).astype(BF16)


def rank_in_class(hot):
    n_blk, n_tok, n_cls = hot.shape
    ones = hot.astype(BF16).reshape(n_blk, n_tok // 128, 128, n_cls)
    within = jnp.einsum("ij,bnjk->bnik", before(128), ones, preferred_element_type=F32)
    sums = jnp.sum(ones.astype(F32), axis=2)
    ahead = jnp.einsum("mn,bnk->bmk", before(n_tok // 128), sums.astype(BF16), preferred_element_type=F32)
    rank = jnp.sum((within + ahead[:, :, None, :]) * ones.astype(F32), axis=3)
    return rank.reshape(n_blk, n_tok).astype(jnp.int32), jnp.sum(sums, axis=1).astype(jnp.int32)


def compact(rank, valid, value, slots):
    n_high = slots // LOW
    high = ((rank // LOW)[:, :, None] == jnp.arange(n_high)) & valid[:, :, None]
    low = ((rank % LOW)[:, :, None] == jnp.arange(LOW)).astype(F32)
    parts = jnp.concatenate([low * (value // 128).astype(F32)[:, :, None], low * (value % 128).astype(F32)[:, :, None]], axis=2)
    out = jnp.einsum("bjh,bjl->bhl", high.astype(BF16), parts.astype(BF16), preferred_element_type=F32).astype(jnp.int32)
    return (out[:, :, :LOW] * 128 + out[:, :, LOW:]).reshape(rank.shape[0], slots)


def solution(mesh):
    n_tp, n_dp = mesh.shape["tp"], mesh.shape["dp"]
    n_core = 2
    n_x = n_dp // n_core
    mesh3 = Mesh(mesh.devices.reshape(n_tp, n_x, n_core), ("tp", "xx", "cc"))
    dp = ("xx", "cc")
    tp_swap = [[(i, i ^ k) for i in range(n_tp)] for k in range(n_tp)]
    pair = [(0, 1), (1, 0)]

    def local_step(tok_ids, emb_table, pos_table, ln1_gain, ln1_bias, w_qkv, b_qkv, w_out, b_out,
                   ln2_gain, ln2_bias, w_up, b_up, w_down, b_down, out_grad):
        tp_index, x_index, c_index = lax.axis_index("tp"), lax.axis_index("xx"), lax.axis_index("cc")
        dp_index = x_index * n_core + c_index
        n_seq_dp, seq = tok_ids.shape
        n_seq = n_seq_dp // n_tp
        n_tok = n_seq * seq
        rows, width = emb_table.shape
        n_sub = 4
        sub = -(-rows // n_sub // 8) * 8
        sub_rows = (sub,) * (n_sub - 1) + (rows - (n_sub - 1) * sub,)
        seq_local = seq // n_tp
        ff = w_up.shape[1]
        gain1, bias1 = ln1_gain.astype(F32)[None], ln1_bias.astype(F32)[None]
        gain2, bias2 = ln2_gain.astype(F32)[None], ln2_bias.astype(F32)[None]

        def half(w, axis):
            n = w.shape[axis] // n_core
            return lax.dynamic_slice_in_dim(w, c_index * n, n, axis)

        def gather_rows(w):
            return lax.all_gather(w, ("tp", "cc"), axis=0, tiled=True)

        def swap(v, axis, k=1):
            return lax.ppermute(v, axis, tp_swap[k] if axis == "tp" else pair)

        def by_owner(parts):
            out = []
            for p in range(n_tp):
                k = tp_index ^ p
                out.append(jnp.where(k < 2, jnp.where(k == 0, parts[0], parts[1]), jnp.where(k == 2, parts[2], parts[3])))
            return out

        ids_all = lax.all_gather(tok_ids, dp, axis=0, tiled=True)
        ids_all, w_up, w_down, w_out, b_qkv, b_up = lax.optimization_barrier((ids_all, w_up, w_down, w_out, b_qkv, b_up))

        wqkv_t = gather_rows(jnp.transpose(half(w_qkv, 2), (1, 2, 3, 0)).reshape(-1, width))
        n_ff, n_out = ff // n_dp, w_out.shape[0] * w_out.shape[1] // n_dp

        def quarter(w, axis):
            n = w.shape[axis] // n_dp
            return lax.dynamic_slice_in_dim(w, dp_index * n, n, axis)

        own_w = jnp.concatenate([quarter(w_up, 1).T, quarter(w_down, 0), quarter(w_out.reshape(-1, width), 0)])
        w_all = lax.all_gather(own_w, ("tp", "xx", "cc"), axis=0, tiled=True)
        w_all = w_all.reshape(n_tp * n_dp, 2 * n_ff + n_out, width)
        wout_w = w_all[:, 2 * n_ff:].reshape(-1, width)
        n_pair = wqkv_t.shape[0] // (3 * 128)
        own_bias = jnp.concatenate([b_qkv.reshape(3, n_core, -1, b_qkv.shape[2]).transpose(1, 0, 2, 3).reshape(-1), b_up])
        biases = jnp.stack(by_owner([swap(own_bias, "tp", k) if k else own_bias for k in range(n_tp)]))
        bqkv_w = biases[:, :-ff].reshape(-1).astype(F32)
        bup_w = biases[:, -ff:].reshape(1, -1).astype(F32)
        pos_rows = lax.slice_in_dim(pos_table, POS_OFFSET, POS_OFFSET + seq, axis=0)

        local = ids_all - tp_index * rows
        sub_of = sum(((local >= s * sub).astype(jnp.int32) for s in range(1, n_sub)), jnp.zeros_like(local))
        owned = (local >= 0) & (local < rows)
        hot = owned[:, :, None] & (sub_of[:, :, None] == jnp.arange(n_sub))
        rank, counts = rank_in_class(hot)
        first = jnp.concatenate([jnp.zeros_like(counts[:, :1]), jnp.cumsum(counts, axis=1)], axis=1)
        rank = rank + jnp.sum(jnp.where(hot, first[:, None, :-1], 0), axis=2)
        owner_counts = jnp.stack([jnp.sum(((ids_all >= o * rows) & (ids_all < (o + 1) * rows)).astype(jnp.int32), axis=1)
                                  for o in range(n_tp)])
        grad_rounds = (jnp.max(owner_counts) + GRAD_SLOTS - 1) // GRAD_SLOTS
        rounds = (jnp.max(jnp.sum(owner_counts.reshape(n_tp, -1, n_seq), axis=2)) + SLOTS - 1) // SLOTS

        def after_first(ranks, totals):
            return (ranks + (jnp.cumsum(totals, axis=1) - totals)[:, :, None]).reshape(ranks.shape[0], -1)

        def grad_lists(r):
            at = rank - r * GRAD_SLOTS
            return compact(at, owned & (at >= 0) & (at < GRAD_SLOTS), jnp.where(owned, local, 0), GRAD_SLOTS)

        my_rank = lax.dynamic_slice_in_dim(rank, dp_index * n_seq_dp, n_seq_dp, 0)
        my_total = lax.dynamic_slice_in_dim(first[:, -1], dp_index * n_seq_dp, n_seq_dp, 0)
        my_rank = after_first(my_rank.reshape(n_tp, n_seq, seq), my_total.reshape(n_tp, n_seq))
        my_owned = lax.dynamic_slice_in_dim(owned, dp_index * n_seq_dp, n_seq_dp, 0).reshape(n_tp, n_tok)
        my_local = lax.dynamic_slice_in_dim(local, dp_index * n_seq_dp, n_seq_dp, 0).reshape(n_tp, n_tok)

        def lists(r):
            at = my_rank - r * SLOTS
            return compact(at, my_owned & (at >= 0) & (at < SLOTS), jnp.where(my_owned, my_local, 0), SLOTS)

        own_ids = lax.dynamic_slice_in_dim(ids_all, dp_index * n_seq_dp + tp_index * n_seq, n_seq, 0)
        own_owner = sum(((own_ids >= o * rows).astype(jnp.int32) for o in range(1, n_tp)), jnp.zeros_like(own_ids))
        own_local = own_ids - own_owner * rows
        own_sub = sum(((own_local >= s * sub).astype(jnp.int32) for s in range(1, n_sub)), jnp.zeros_like(own_ids))
        own_hot = (own_owner * n_sub + own_sub)[:, :, None] == jnp.arange(n_tp * n_sub)
        own_rank, own_counts = rank_in_class(own_hot)
        own_counts = own_counts.reshape(n_seq, n_tp, n_sub)
        own_first = jnp.cumsum(own_counts, axis=2) - own_counts
        own_rank = own_rank + jnp.sum(jnp.where(own_hot, own_first.reshape(n_seq, 1, -1), 0), axis=2)
        own_total = jnp.sum(own_counts, axis=2)
        own_shift = jnp.cumsum(own_total, axis=0) - own_total
        own_place = sum(jnp.where(own_owner == o, own_shift[:, o:o + 1], 0) for o in range(n_tp))
        own_place = (own_place + own_rank).reshape(-1)

        def own_lists(r, b):
            at = jnp.broadcast_to(own_rank[b] - r * GRAD_SLOTS, (n_tp, seq))
            mine = own_owner[b] == jnp.arange(n_tp)[:, None]
            return compact(at, mine & (at >= 0) & (at < GRAD_SLOTS), jnp.broadcast_to(jnp.arange(seq), (n_tp, seq)), GRAD_SLOTS)

        tiles = width // 128

        def own_places(r, b):
            own = own_lists(r, b)
            place = jnp.concatenate([lax.dynamic_index_in_dim(own, tp_index ^ k, 0, keepdims=False) for k in range(n_tp)])
            return (place // 8) * (8 * tiles) + place % 8

        places0 = [own_places(0, b) for b in range(n_seq)]

        def in_block_order(table, b):
            out = []
            for dc in range(n_core):
                for dx in range(n_x):
                    for k in range(n_tp):
                        d = (x_index ^ dx) * n_core + (c_index ^ dc)
                        out.append(lax.dynamic_index_in_dim(table, (d * n_tp + (tp_index ^ k)) * n_seq + b, 0, keepdims=False))
            return out

        def both_orders(table):
            return jnp.stack(in_block_order(table, 0) + in_block_order(table, 1))

        block_rows = both_orders(grad_lists(0))
        in_sub = sum(((block_rows >= s * sub).astype(jnp.int32) for s in range(1, n_sub)), jnp.zeros_like(block_rows))
        in_sub = block_rows - in_sub * sub
        slot = jnp.arange(GRAD_SLOTS)
        code = (((in_sub // 8) * (8 * tiles) + in_sub % 8) << 16) | ((slot // 8) * (8 * tiles) + slot % 8)
        code = code.reshape(-1)
        block_first = jnp.minimum(both_orders(first), GRAD_SLOTS).reshape(-1)

        def rows_here(r, my_lists):
            index = [lax.dynamic_index_in_dim(my_lists, tp_index ^ k, 0, keepdims=False) for k in range(n_tp)]
            first_two = jnp.take(emb_table, jnp.concatenate([index[3], index[1]]), axis=0, mode="clip")
            rest, first_two = lax.optimization_barrier((jnp.concatenate([index[2], index[0]]), first_two))
            last_two = jnp.take(emb_table, rest, axis=0, mode="clip")
            sent = [last_two[SLOTS:], first_two[SLOTS:], last_two[:SLOTS], first_two[:SLOTS]]
            got = list(sent)
            for k in range(1, n_tp):
                got[k] = swap(sent[k], "tp", k)
            at = own_place - r * SLOTS
            valid = (at >= 0) & (at < SLOTS)
            return got, jnp.where(valid, (own_owner.reshape(-1) ^ tp_index) * SLOTS + at, 0), valid

        def norm_rows(x):
            normed, _ = row_stats(x)
            return (normed * gain1 + bias1).astype(BF16)

        got0, place0, _ = rows_here(0, lists(0))
        code0 = (place0 // 8) * (8 * tiles) + place0 % 8
        got0, out_grad = lax.optimization_barrier((got0, out_grad))
        resid_x, hid1 = embed(code0, got0, pos_rows, gain1, bias1, n_tok)

        def more_rows(carry):
            r, x, _ = carry
            got, place, valid = rows_here(r, lists(r))
            new = jnp.take(jnp.concatenate(got), place, axis=0, mode="clip").astype(F32) + jnp.tile(pos_rows.astype(F32), (n_seq, 1))
            x = jnp.where(valid[:, None], new, x)
            return r + 1, x, norm_rows(x)

        _, resid_x, hid1 = lax.while_loop(lambda c: c[0] < rounds, more_rows, (jnp.int32(1), resid_x, hid1))

        og_parts = out_grad.reshape(n_tp, n_seq, seq_local, width)
        parts = [lax.dynamic_index_in_dim(og_parts, tp_index ^ k, 0, keepdims=False) for k in range(n_tp)]
        parts = [swap(part, "tp", k) if k else part for k, part in enumerate(parts)]
        me = jnp.reshape(tp_index, (1,))
        og = assemble(me, parts, (n_seq, n_tp, seq_local, width), (n_seq, 1, seq_local, width)).reshape(n_tok, width)

        qkv = (dot_nt(hid1, wqkv_t) + bqkv_w).astype(BF16)
        ctx, lse = attn_fwd(qkv, n_seq, seq, n_pair)
        resid_x1, hid2 = proj_norm(ctx, w_all, 2 * n_ff, resid_x, b_out.astype(F32)[None], gain2, bias2)
        act, d_up, d_b_up = ffn(hid2, og, w_all, bup_w)
        parts = down(me, act, w_all, resid_x1, b_down.astype(F32)[None], n_seq, n_tp)
        parts = [swap(part, "tp", k) if k else part for k, part in enumerate(parts)]
        layer_out = assemble(me, parts, (n_seq_dp, seq_local, width), (n_seq, seq_local, width))

        core = jnp.reshape(c_index, (1,))

        def piece_of(n_rows):
            return -(-n_rows // (4 * n_tp) // 24) * 24

        def every_piece(g):
            other = swap(g, "xx")
            return [g, other, swap(g, "cc"), swap(other, "cc")]

        x_and_core = jnp.stack([x_index, c_index])

        p_ff = piece_of(n_tp * ff)
        down_theirs = swap(grad_pieces(1 - core, act, og, n_tp, p_ff, 0, 1), "cc")
        up_theirs = swap(grad_pieces(1 - core, d_up, hid2, n_tp, p_ff, 0, 1), "cc")
        ff_grads = grad_pieces(core, act, og, n_tp, p_ff, 0, 2, plus=down_theirs)
        ff_grads = grad_pieces(core, d_up, hid2, n_tp, p_ff, 1, 2, plus=up_theirs, into=ff_grads)
        ff_grads = lax.psum_scatter(ff_grads, ("tp", "xx"), scatter_dimension=0, tiled=True)
        ff_grads = every_piece(ff_grads)

        d_resid1, d_attn, sums2 = back2(d_up, w_all, resid_x1, og, gain2)
        d_ctx = dot_nt(d_attn, wout_w).astype(BF16)
        n_small = n_tp * (b_qkv.size + ff) // width + 6
        p_pos = -(-(seq + n_small) // (24 * n_tp * n_dp)) * 24
        p_out = piece_of(wout_w.shape[0])
        spans = ((0, p_out), (p_out, p_out + piece_of(wqkv_t.shape[0])))

        def token_blocks(places, d_tok):
            parts = pack(places, d_tok, GRAD_SLOTS)
            blocks = [swap(part, "tp", k) if k else part for k, part in enumerate(parts)]
            other = []
            for block in blocks:
                other.append(swap(block, "xx"))
            return blocks + other + [swap(block, "cc") for block in blocks + other]

        d_qkv0 = attn_bwd(qkv, ctx, d_ctx, lse, 0, seq, n_pair)
        d_tok0, *sums0 = back1(d_qkv0, wqkv_t, resid_x, d_resid1, gain1, 0, p_pos * n_tp * n_dp)
        blocks0 = token_blocks(places0[0], d_tok0)
        d_qkv1 = attn_bwd(qkv, ctx, d_ctx, lse, 1, seq, n_pair)
        d_tok1, pos_all, sums1, sums_qkv = back1(d_qkv1, wqkv_t, resid_x, d_resid1, gain1, 1, p_pos * n_tp * n_dp, earlier=sums0)
        blocks1 = token_blocks(places0[1], d_tok1)
        d_qkvs = [d_qkv0, d_qkv1]
        rest_theirs = swap(grad_rest(1 - core, ctx, d_attn, d_qkvs, hid1, n_tp, spans), "cc")

        d_w_down, d_w_up = pieces_out(x_and_core, ff_grads, ((0, n_ff, False), (p_ff, n_ff, True)))
        image = accum(blocks0 + blocks1, code, block_first, sub_rows, width)
        d_emb = image.reshape(rows // 8, tiles, 8, 128).transpose(0, 2, 1, 3).reshape(rows, width)

        def more_grads(carry):
            r, table = carry
            at = rank - r * GRAD_SLOTS
            there = owned & (at >= 0) & (at < GRAD_SLOTS)
            dest = compact(at, there, jnp.where(owned, local, 0) + 1, GRAD_SLOTS)
            dest = jnp.where(dest == 0, rows, dest - 1)
            grads = jnp.concatenate(token_blocks(own_places(r, 0), d_tok0) + token_blocks(own_places(r, 1), d_tok1), axis=0).astype(F32)
            return r + 1, table.at[both_orders(dest).reshape(-1)].add(grads, mode="drop")

        _, d_emb = lax.while_loop(lambda c: c[0] < grad_rounds, more_grads, (jnp.int32(1), d_emb))

        small = jnp.concatenate([sums_qkv[0], d_b_up[0], sums1[:2].reshape(-1), sums2[:4].reshape(-1)]).reshape(-1, width)
        small = jnp.concatenate([small, jnp.zeros((pos_all.shape[0] - seq - n_small, width), F32)])
        pos_all = lax.dynamic_update_slice_in_dim(pos_all, small, seq, 0).reshape(n_tp * n_x, n_core, p_pos, width)
        pos_theirs = swap(lax.dynamic_index_in_dim(pos_all, 1 - c_index, 1, keepdims=False).reshape(-1, width), "cc")
        rest = grad_rest(core, ctx, d_attn, d_qkvs, hid1, n_tp, spans, plus=rest_theirs, tail=(pos_all, pos_theirs))
        rest = lax.psum_scatter(rest, ("tp", "xx"), scatter_dimension=0, tiled=True)
        rest_w = every_piece(rest[:spans[1][1]])
        whole = lax.all_gather(rest[spans[1][1]:], ("tp", "xx", "cc"), axis=0, tiled=True)
        d_pos = jnp.pad(whole[:seq], ((POS_OFFSET, pos_table.shape[0] - seq - POS_OFFSET), (0, 0)))
        small = whole[seq:seq + n_small].reshape(-1)
        n_b = b_qkv.size
        d_b_qkv = lax.dynamic_slice_in_dim(small, tp_index * n_b, n_b).reshape(n_core, 3, -1, b_qkv.shape[2])
        d_b_qkv = d_b_qkv.transpose(1, 0, 2, 3).reshape(b_qkv.shape)
        d_b_up = lax.dynamic_slice_in_dim(small, n_tp * n_b + tp_index * ff, ff)
        d_gain1, d_bias1, d_gain2, d_bias2, d_b_out, d_b_down = small[n_tp * (n_b + ff):].reshape(6, width)

        d_w_out, d_w_qkv = pieces_out(x_and_core, rest_w, ((0, n_out, False), (p_out, n_b // n_dp, False)))
        d_w_out = d_w_out.reshape(w_out.shape)
        d_w_qkv = d_w_qkv.reshape(n_core, 3, -1, w_qkv.shape[3], width).transpose(4, 1, 0, 2, 3).reshape(w_qkv.shape)
        return (layer_out, d_emb, d_pos, d_gain1, d_bias1, d_w_qkv, d_b_qkv, d_w_out,
                d_b_out, d_gain2, d_bias2, d_w_up, d_b_up, d_w_down, d_b_down)

    rep = P()
    in_specs = (P(dp, None), P("tp", None), rep, rep, rep,
                P(None, None, "tp", None), P(None, "tp", None), P("tp", None, None), rep,
                rep, rep, P(None, "tp"), P("tp"), P("tp", None), rep,
                P(dp, "tp", None))
    out_specs = (P(dp, "tp", None), P("tp", None), rep, rep, rep,
                 P(None, None, "tp", None), P(None, "tp", None), P("tp", None, None), rep,
                 rep, rep, P(None, "tp"), P("tp"), P("tp", None), rep)

    return jax.shard_map(local_step, mesh=mesh3, in_specs=in_specs, out_specs=out_specs, check_vma=False)
```

```python
import functools

import jax
import jax.numpy as jnp
from jax import lax
from jax.experimental import pallas as pl
from jax.experimental.pallas import tpu as pltpu
from jax.sharding import Mesh, PartitionSpec as P


F32 = jnp.float32
BF16 = jnp.bfloat16
MIB = 1024 * 1024
WIDEN = 32

BLK = 256


def dot_nt(a, b):
    return lax.dot_general(a, b, (((1,), (1,)), ((), ())), preferred_element_type=F32)


def dot_nn(a, b):
    return lax.dot_general(a, b, (((1,), (0,)), ((), ())), preferred_element_type=F32)


def head_only(x, head):
    half = x.shape[1] // 2
    lane = lax.broadcasted_iota(jnp.int32, x.shape, 1)
    keep = (lane < half) if head == 0 else (lane >= half)
    return jnp.where(keep, x, jnp.zeros((), x.dtype))


def attn_fwd_kernel(qkv_ref, ctx_ref, lse_ref, ctx_t):
    seq, width = ctx_ref.shape
    half = width // 2
    scale = half ** -0.5
    q2 = qkv_ref[:, 0:width] * jnp.asarray(scale, BF16)
    v_t = qkv_ref[:, 2 * width:3 * width].T
    tasks = [(head, i) for i in range(seq // BLK) for head in range(2)]

    def scores(head, i):
        return dot_nt(qkv_ref[0:(i + 1) * BLK, width:2 * width], head_only(q2[i * BLK:(i + 1) * BLK], head))

    ready = scores(*tasks[0])
    for n, (head, i) in enumerate(tasks):
        s = ready
        if n + 1 < len(tasks):
            ready = scores(*tasks[n + 1])
        lo, hi = i * BLK, (i + 1) * BLK
        v_h = v_t[head * half:(head + 1) * half, :]
        key = lax.broadcasted_iota(jnp.int32, (BLK, BLK), 0)
        qry = lax.broadcasted_iota(jnp.int32, (BLK, BLK), 1)
        diag = jnp.where(key <= qry, s[lo:hi], -1e30)
        top = jnp.max(diag, axis=0, keepdims=True)
        if i:
            top = jnp.maximum(top, jnp.max(s[0:lo], axis=0, keepdims=True))
        p_diag = jnp.exp(diag - top)
        total = jnp.sum(p_diag, axis=0, keepdims=True)
        if i:
            p_left = jnp.exp(s[0:lo] - top)
            total = total + jnp.sum(p_left, axis=0, keepdims=True)
        inv = 1.0 / total
        acc = dot_nn(v_h[:, lo:hi], (p_diag * inv).astype(BF16))
        if i:
            acc = acc + dot_nn(v_h[:, 0:lo], (p_left * inv).astype(BF16))
        ctx_t[head * half:(head + 1) * half, lo:hi] = acc
        lse_ref[head:head + 1, lo:hi] = top + jnp.log(total)
    ctx_ref[...] = ctx_t[...].T.astype(BF16)


def attn_fwd(qkv, n_seq, seq, n_pair):
    width = 128
    return pl.pallas_call(
        attn_fwd_kernel,
        grid=(n_seq, n_pair),
        in_specs=[pl.BlockSpec((seq, 3 * width), lambda b, p: (b, p))],
        out_specs=[pl.BlockSpec((seq, width), lambda b, p: (b, p)),
                   pl.BlockSpec((None, None, 2, seq), lambda b, p: (b, p, 0, 0))],
        out_shape=[jax.ShapeDtypeStruct((n_seq * seq, n_pair * width), BF16),
                   jax.ShapeDtypeStruct((n_seq, n_pair, 2, seq), F32)],
        scratch_shapes=[pltpu.VMEM((width, seq), F32)],
        name="attn_fwd",
        cost_estimate=pl.CostEstimate(flops=n_seq * n_pair * 8 * seq * seq * 256 * 10 // 16, bytes_accessed=n_seq * seq * n_pair * width * 8,
                                      transcendentals=n_seq * n_pair * seq * seq),
        compiler_params=pltpu.CompilerParams(vmem_limit_bytes=63 * 1024 * 1024),
    )(qkv)


def attn_bwd_kernel(qkv_ref, ctx_ref, dctx_ref, lse_ref, dqkv_ref, dk_t, dv_t):
    seq, width = ctx_ref.shape
    half = width // 2
    scale = half ** -0.5
    q2 = qkv_ref[:, 0:width] * jnp.asarray(scale, BF16)
    q_t = q2.T
    do_t = dctx_ref[...].T
    lse_c = jnp.concatenate([lse_ref[...], jnp.zeros((6, seq), F32)], axis=0).T
    prod = dctx_ref[...].astype(F32) * ctx_ref[...].astype(F32)
    tasks = [(head, i) for i in range(seq // BLK) for head in range(2)]

    def scores(head, i):
        lo, hi = i * BLK, (i + 1) * BLK
        return (dot_nt(head_only(q2[lo:hi], head), qkv_ref[0:hi, width:2 * width]),
                dot_nt(head_only(dctx_ref[lo:hi, :], head), qkv_ref[0:hi, 2 * width:3 * width]))

    dq = []
    ready = scores(*tasks[0])
    for n, (head, i) in enumerate(tasks):
        s, dp = ready
        if n + 1 < len(tasks):
            ready = scores(*tasks[n + 1])
        lo, hi = i * BLK, (i + 1) * BLK
        rows = slice(head * half, (head + 1) * half)
        mean = jnp.sum(head_only(prod[lo:hi], head), axis=1, keepdims=True)
        lse = lse_c[lo:hi, head:head + 1]
        qry = lax.broadcasted_iota(jnp.int32, (BLK, BLK), 0)
        key = lax.broadcasted_iota(jnp.int32, (BLK, BLK), 1)
        p_diag = jnp.where(key <= qry, jnp.exp(s[:, lo:hi] - lse), 0.0)
        ds_diag = (p_diag * (dp[:, lo:hi] - mean)).astype(BF16)
        dv_t[rows, lo:hi] = dot_nn(do_t[rows, lo:hi], p_diag.astype(BF16))
        dk_t[rows, lo:hi] = dot_nn(q_t[rows, lo:hi], ds_diag)
        dq_h = dot_nn(ds_diag, qkv_ref[lo:hi, width:2 * width])
        if i:
            p_left = jnp.exp(s[:, 0:lo] - lse)
            ds_left = (p_left * (dp[:, 0:lo] - mean)).astype(BF16)
            dv_t[rows, 0:lo] += dot_nn(do_t[rows, lo:hi], p_left.astype(BF16))
            dk_t[rows, 0:lo] += dot_nn(q_t[rows, lo:hi], ds_left)
            dq_h = dq_h + dot_nn(ds_left, qkv_ref[0:lo, width:2 * width])
        dq.append(dq_h)
        if head == 1:
            lane = lax.broadcasted_iota(jnp.int32, (BLK, width), 1)
            dqkv_ref[lo:hi, 0:width] = (jnp.where(lane < half, dq[0], dq[1]) * scale).astype(BF16)
            dq = []
    dqkv_ref[:, width:2 * width] = dk_t[...].T.astype(BF16)
    dqkv_ref[:, 2 * width:3 * width] = dv_t[...].T.astype(BF16)


def attn_bwd(qkv, ctx, dctx, lse, at, seq, n_pair):
    width = 128
    return pl.pallas_call(
        attn_bwd_kernel,
        grid=(n_pair,),
        in_specs=[pl.BlockSpec((seq, 3 * width), lambda p: (at, p)),
                  pl.BlockSpec((seq, width), lambda p: (at, p)),
                  pl.BlockSpec((seq, width), lambda p: (at, p)),
                  pl.BlockSpec((None, None, 2, seq), lambda p: (at, p, 0, 0))],
        out_specs=pl.BlockSpec((seq, 3 * width), lambda p: (0, p)),
        out_shape=jax.ShapeDtypeStruct((seq, n_pair * 3 * width), BF16),
        scratch_shapes=[pltpu.VMEM((width, seq), F32), pltpu.VMEM((width, seq), F32)],
        name="attn_bwd",
        cost_estimate=pl.CostEstimate(flops=n_pair * 20 * seq * seq * 256 * 10 // 16, bytes_accessed=seq * n_pair * width * 16,
                                      transcendentals=n_pair * seq * seq),
        compiler_params=pltpu.CompilerParams(vmem_limit_bytes=63 * 1024 * 1024),
    )(qkv, ctx, dctx, lse)


LN_EPS = 1e-5
GELU_S = 0.7978845608028654
GELU_A = 0.044715


def row_mean(v):
    return jnp.sum(v, axis=1, keepdims=True) * (1.0 / v.shape[1])


def row_stats(v):
    centered = v - row_mean(v)
    inv_std = lax.rsqrt(row_mean(centered * centered) + LN_EPS)
    return centered * inv_std, inv_std


def norm_back(d_y, x_in, gain):
    normed, inv_std = row_stats(x_in)
    d_norm = d_y * gain
    d_x = inv_std * (d_norm - row_mean(d_norm) - normed * row_mean(d_norm * normed))
    return d_x, d_y * normed


def col_sum(v):
    return jnp.sum(v, axis=0, keepdims=True)


def to_image(rows, image, base):
    tiles = rows.shape[1] // 128
    for h in range(rows.shape[0] // 8):
        for c in range(tiles):
            image[pl.ds(base + (h * tiles + c) * 8, 8), :] = rows[h * 8:(h + 1) * 8, c * 128:(c + 1) * 128]


def from_image(image, base, n_rows, width):
    tiles = width // 128
    return jnp.concatenate([jnp.concatenate([image[pl.ds(base + (h * tiles + c) * 8, 8), :] for c in range(tiles)], axis=1)
                            for h in range(n_rows // 8)], axis=0)


def pick_rows(code_ref, first, stage, image, n_rows, tiles):
    def pick(g, _):
        base = pl.multiple_of(g * 16 * tiles, 16 * tiles)
        for j in range(16):
            row = stage[pl.ds(code_ref[first + g * 16 + j], tiles, stride=8), :]
            image[pl.ds(base + (j // 8) * 8 * tiles + j % 8, tiles, stride=8), :] = row
        return 0

    lax.fori_loop(0, n_rows // 16, pick, 0)


def embed_kernel(n_blk, cap, code_ref, *refs):
    tok_refs = refs[:n_blk]
    pos_ref, gain_ref, bias_ref, x_ref, hid_ref, stage, image = refs[n_blk:]
    rows, width = x_ref.shape
    tiles = width // 128

    @pl.when(pl.program_id(0) == 0)
    def _():
        for b in range(n_blk):
            def widen(g, _, b=b):
                part = tok_refs[b][pl.ds(pl.multiple_of(g * WIDEN, WIDEN), WIDEN), :].astype(F32)
                to_image(part, stage, pl.multiple_of((b * cap + g * WIDEN) * tiles, WIDEN * tiles))
                return 0

            lax.fori_loop(0, cap // WIDEN, widen, 0)

    pick_rows(code_ref, pl.program_id(0) * rows, stage, image, rows, tiles)
    part = 64
    for i in range(rows // part):
        at = slice(i * part, (i + 1) * part)
        x = from_image(image, i * part * tiles, part, width) + pos_ref[at, :].astype(F32)
        x_ref[at, :] = x
        normed, _ = row_stats(x)
        hid_ref[at, :] = (normed * gain_ref[...] + bias_ref[...]).astype(BF16)


def embed(code, blocks, pos_rows, gain, bias, n_tok):
    cap, width = blocks[0].shape
    seq = pos_rows.shape[0]
    rows = 256
    per_seq = seq // rows
    n_blk = len(blocks)
    vec = pl.BlockSpec((1, width), lambda i: (0, 0))
    return pl.pallas_call(
        functools.partial(embed_kernel, n_blk, cap),
        grid=(n_tok // rows,),
        in_specs=[pl.BlockSpec(memory_space=pltpu.SMEM)]
        + [pl.BlockSpec((cap, width), lambda i: (0, 0), pipeline_mode=pl.Buffered(1))] * n_blk
        + [pl.BlockSpec((rows, width), lambda i: (i % per_seq, 0)), vec, vec],
        out_specs=[pl.BlockSpec((rows, width), lambda i: (i, 0))] * 2,
        out_shape=[jax.ShapeDtypeStruct((n_tok, width), F32), jax.ShapeDtypeStruct((n_tok, width), BF16)],
        scratch_shapes=[pltpu.VMEM((n_blk * cap * width // 128, 128), F32), pltpu.VMEM((rows * width // 128, 128), F32)],
        name="embed_norm",
        cost_estimate=pl.CostEstimate(flops=15_000_000_000, bytes_accessed=n_tok * width * 10, transcendentals=0),
        compiler_params=pltpu.CompilerParams(vmem_limit_bytes=63 * 1024 * 1024),
    )(code, *blocks, pos_rows, gain, bias)


def pack_kernel(n_blk, code_ref, tok_ref, *refs):
    out_refs = refs[:n_blk]
    stage, image = refs[n_blk:]
    n_tok, width = tok_ref.shape
    cap = out_refs[0].shape[0]
    tiles = width // 128

    def widen(g, _):
        part = tok_ref[pl.ds(pl.multiple_of(g * WIDEN, WIDEN), WIDEN), :].astype(F32)
        to_image(part, stage, pl.multiple_of(g * WIDEN * tiles, WIDEN * tiles))
        return 0

    lax.fori_loop(0, n_tok // WIDEN, widen, 0)
    for b in range(n_blk):
        pick_rows(code_ref, b * cap, stage, image, cap, tiles)

        def narrow(g, _, b=b):
            part = from_image(image, pl.multiple_of(g * WIDEN * tiles, WIDEN * tiles), WIDEN, width)
            out_refs[b][pl.ds(pl.multiple_of(g * WIDEN, WIDEN), WIDEN), :] = part.astype(BF16)
            return 0

        lax.fori_loop(0, cap // WIDEN, narrow, 0)


def pack(code, tok, cap):
    n_tok, width = tok.shape
    n_blk = code.shape[0] // cap
    return pl.pallas_call(
        functools.partial(pack_kernel, n_blk),
        in_specs=[pl.BlockSpec(memory_space=pltpu.SMEM), pl.BlockSpec(memory_space=pltpu.VMEM)],
        out_specs=[pl.BlockSpec(memory_space=pltpu.VMEM)] * n_blk,
        out_shape=[jax.ShapeDtypeStruct((cap, width), BF16)] * n_blk,
        scratch_shapes=[pltpu.VMEM((n_tok * width // 128, 128), F32), pltpu.VMEM((cap * width // 128, 128), F32)],
        name="token_pack",
        cost_estimate=pl.CostEstimate(flops=15_000_000_000, bytes_accessed=n_tok * width * 5, transcendentals=0),
        compiler_params=pltpu.CompilerParams(vmem_limit_bytes=63 * 1024 * 1024),
    )(code, tok)


def proj_kernel(c_ref, w_ref, x_ref, b_ref, gain_ref, bias_ref, x1_ref, hid_ref):
    part = x_ref.shape[0] // 2
    for i in range(2):
        at = slice(i * part, (i + 1) * part)
        x1 = x_ref[at, :] + dot_nn(c_ref[at, :], w_ref[...].reshape(c_ref.shape[1], -1)).astype(BF16).astype(F32) + b_ref[...]
        x1_ref[at, :] = x1
        normed, _ = row_stats(x1)
        hid_ref[at, :] = (normed * gain_ref[...] + bias_ref[...]).astype(BF16)


def proj_norm(ctx, w, start, x, b, gain, bias):
    n_tok, width = x.shape
    n_row = ctx.shape[1] // w.shape[0]
    rows = 512
    vec = pl.BlockSpec((1, width), lambda i: (0, 0))
    mat = pl.BlockSpec((rows, width), lambda i: (i, 0))
    return pl.pallas_call(
        proj_kernel,
        grid=(n_tok // rows,),
        in_specs=[pl.BlockSpec((rows, ctx.shape[1]), lambda i: (i, 0)), pl.BlockSpec((w.shape[0], n_row, width), lambda i: (0, start // n_row, 0)), mat, vec, vec, vec],
        out_specs=[mat, mat],
        out_shape=[jax.ShapeDtypeStruct((n_tok, width), F32), jax.ShapeDtypeStruct((n_tok, width), BF16)],
        name="proj_norm",
        cost_estimate=pl.CostEstimate(flops=2 * n_tok * ctx.shape[1] * width, bytes_accessed=n_tok * width * 12, transcendentals=0),
        compiler_params=pltpu.CompilerParams(vmem_limit_bytes=63 * 1024 * 1024),
    )(ctx, w, x, b, gain, bias)


def ffn_kernel(part, h_ref, og_ref, wu_ref, wd_ref, b_ref, act_ref, dup_ref, db_ref):
    total = jnp.zeros(db_ref.shape, F32)
    for i in range(h_ref.shape[0] // part):
        at = slice(i * part, (i + 1) * part)
        z = dot_nt(h_ref[at, :], wu_ref[0]) + b_ref[...]
        d_act = dot_nt(og_ref[at, :], wd_ref[0])
        z2 = z * z
        gate = 0.5 * jnp.tanh(z * (GELU_S + (GELU_S * GELU_A) * z2)) + 0.5
        act = z * gate
        d_up = d_act * (gate + act * (1.0 - gate) * (2.0 * GELU_S + (6.0 * GELU_S * GELU_A) * z2))
        act_ref[at, :] = act.astype(BF16)
        dup_ref[at, :] = d_up.astype(BF16)
        total = total + col_sum(d_up)
    db_ref[...] = total


def ffn(hid, og, w, b_up, part=1024):
    n_tok, width = hid.shape
    ff = b_up.shape[1]
    n_piece = w.shape[0]
    bn = ff // n_piece
    whole = pl.BlockSpec((n_tok, width), lambda i: (0, 0), pipeline_mode=pl.Buffered(1))
    ospec = pl.BlockSpec((n_tok, bn), lambda i: (0, i))
    vec = pl.BlockSpec((1, bn), lambda i: (0, i))
    return pl.pallas_call(
        functools.partial(ffn_kernel, part),
        grid=(n_piece,),
        in_specs=[whole, whole, pl.BlockSpec((1, bn, width), lambda i: (i, 0, 0)), pl.BlockSpec((1, bn, width), lambda i: (i, 1, 0)), vec],
        out_specs=[ospec, ospec, vec],
        out_shape=[jax.ShapeDtypeStruct((n_tok, ff), BF16), jax.ShapeDtypeStruct((n_tok, ff), BF16), jax.ShapeDtypeStruct((1, ff), F32)],
        name="ffn",
        cost_estimate=pl.CostEstimate(flops=4 * n_tok * ff * width, bytes_accessed=4 * n_tok * ff + 4 * ff * width, transcendentals=n_tok * ff),
        compiler_params=pltpu.CompilerParams(vmem_limit_bytes=63 * 1024 * 1024),
    )(hid, og, w, w, b_up)


def down_kernel(n_tp, me_ref, act_ref, w_ref, x1_ref, b_ref, *out_refs):
    out = x1_ref[...] + dot_nn(act_ref[...], w_ref[...].reshape(act_ref.shape[1], -1)).astype(BF16).astype(F32) + b_ref[...]
    k = me_ref[0] ^ (pl.program_id(0) % n_tp)
    seq = pl.program_id(0) // n_tp
    for j in range(n_tp):
        @pl.when(k == j)
        def _(j=j):
            out_refs[j][seq] = out.astype(BF16)


def down(me, act, w, x1, b, n_seq, n_tp):
    n_tok, width = x1.shape
    ff = act.shape[1]
    rows = n_tok // n_seq // n_tp
    part = jax.ShapeDtypeStruct((n_seq, rows, width), BF16)
    return pl.pallas_call(
        functools.partial(down_kernel, n_tp),
        grid_spec=pltpu.PrefetchScalarGridSpec(
            num_scalar_prefetch=1, grid=(n_seq * n_tp,),
            in_specs=[pl.BlockSpec((rows, ff), lambda i, m: (i, 0)),
                      pl.BlockSpec((w.shape[0], ff // w.shape[0], width), lambda i, m: (0, 1, 0), pipeline_mode=pl.Buffered(1)),
                      pl.BlockSpec((rows, width), lambda i, m: (i, 0)), pl.BlockSpec((1, width), lambda i, m: (0, 0))],
            out_specs=[pl.BlockSpec(part.shape, lambda i, m: (0, 0, 0))] * n_tp),
        out_shape=[part] * n_tp,
        name="down",
        cost_estimate=pl.CostEstimate(flops=2 * n_tok * ff * width, bytes_accessed=2 * n_tok * ff + n_tok * width * 6, transcendentals=0),
        compiler_params=pltpu.CompilerParams(vmem_limit_bytes=63 * 1024 * 1024),
    )(me, act, w, x1, b)


def back2_kernel(dup_ref, w_ref, x1_ref, og_ref, gain_ref, dr_ref, da_ref, sums_ref):
    @pl.when(pl.program_id(0) == 0)
    def _():
        sums_ref[...] = jnp.zeros(sums_ref.shape, F32)

    n_part = 2
    part = dr_ref.shape[0] // n_part
    w = w_ref[...].reshape(dup_ref.shape[1], -1)
    d_ys = [dot_nn(dup_ref[i * part:(i + 1) * part, :], w) for i in range(n_part)]
    for i in range(n_part):
        at = slice(i * part, (i + 1) * part)
        d_y = d_ys[i].astype(BF16).astype(F32)
        d_x, d_gain = norm_back(d_y, x1_ref[at, :], gain_ref[...])
        og = og_ref[at, :].astype(F32)
        d_resid = og + d_x
        dr_ref[at, :] = d_resid
        da_ref[at, :] = d_resid.astype(BF16)
        sums_ref[0:1, :] += col_sum(d_gain)
        sums_ref[1:2, :] += col_sum(d_y)
        sums_ref[2:3, :] += col_sum(d_resid)
        sums_ref[3:4, :] += col_sum(og)


def back2(d_up, w, x1, og, gain):
    n_tok, width = x1.shape
    ff = d_up.shape[1]
    rows = 256
    mat = pl.BlockSpec((rows, width), lambda i: (i, 0))
    return pl.pallas_call(
        back2_kernel,
        grid=(n_tok // rows,),
        in_specs=[pl.BlockSpec((rows, ff), lambda i: (i, 0)), pl.BlockSpec((w.shape[0], ff // w.shape[0], width), lambda i: (0, 0, 0), pipeline_mode=pl.Buffered(1)),
                  mat, mat, pl.BlockSpec((1, width), lambda i: (0, 0))],
        out_specs=[mat, mat, pl.BlockSpec((8, width), lambda i: (0, 0))],
        out_shape=[jax.ShapeDtypeStruct((n_tok, width), F32), jax.ShapeDtypeStruct((n_tok, width), BF16), jax.ShapeDtypeStruct((8, width), F32)],
        name="ffn_back",
        cost_estimate=pl.CostEstimate(flops=2 * n_tok * ff * width, bytes_accessed=2 * n_tok * ff + n_tok * width * 12, transcendentals=0),
        compiler_params=pltpu.CompilerParams(vmem_limit_bytes=63 * 1024 * 1024),
    )(d_up, w, x1, og, gain)


def back1_kernel(dq_ref, w_ref, x_ref, dr_ref, gain_ref, *refs):
    tok_ref, pos_ref, sums_ref, bsum_ref = refs[-4:]
    before_refs = refs[:-4]

    @pl.when(pl.program_id(0) == 0)
    def _():
        sums_ref[...] = before_refs[1][...] if before_refs else jnp.zeros(sums_ref.shape, F32)
        bsum_ref[...] = before_refs[2][...] if before_refs else jnp.zeros(bsum_ref.shape, F32)

    n_part = 2
    part = tok_ref.shape[0] // n_part
    d_ys = [dot_nn(dq_ref[i * part:(i + 1) * part, :], w_ref[...]) for i in range(n_part)]
    for i in range(n_part):
        at = slice(i * part, (i + 1) * part)
        d_y = d_ys[i].astype(BF16).astype(F32)
        d_x, d_gain = norm_back(d_y, x_ref[at, :], gain_ref[...])
        d_resid = dr_ref[at, :] + d_x
        tok_ref[at, :] = d_resid.astype(BF16)
        pos_ref[at, :] = before_refs[0][at, :] + d_resid if before_refs else d_resid
        sums_ref[0:1, :] += col_sum(d_gain)
        sums_ref[1:2, :] += col_sum(d_y)
        bsum_ref[0:1, :] += col_sum(dq_ref[at, :].astype(F32))


def back1(d_qkv, w_qkv, x, d_resid1, gain, at, pos_rows, earlier=None):
    seq, n_cols = d_qkv.shape
    width = x.shape[1]
    rows = 256
    steps = seq // rows
    mat = pl.BlockSpec((rows, width), lambda i: (at * steps + i, 0))
    out = pl.BlockSpec((rows, width), lambda i: (i, 0))
    few = [pl.BlockSpec((8, width), lambda i: (0, 0)), pl.BlockSpec((8, n_cols), lambda i: (0, 0))]
    return pl.pallas_call(
        back1_kernel,
        grid=(steps,),
        in_specs=[pl.BlockSpec((rows, n_cols), lambda i: (i, 0)),
                  pl.BlockSpec((n_cols, width), lambda i: (0, 0), pipeline_mode=pl.Buffered(1)),
                  mat, mat, pl.BlockSpec((1, width), lambda i: (0, 0))] + ([out] + few if earlier else []),
        out_specs=[out, out] + few,
        out_shape=[jax.ShapeDtypeStruct((seq, width), BF16), jax.ShapeDtypeStruct((pos_rows, width), F32),
                   jax.ShapeDtypeStruct((8, width), F32), jax.ShapeDtypeStruct((8, n_cols), F32)],
        name="qkv_back",
        cost_estimate=pl.CostEstimate(flops=2 * seq * n_cols * width, bytes_accessed=2 * seq * n_cols + seq * width * 12, transcendentals=0),
        compiler_params=pltpu.CompilerParams(vmem_limit_bytes=63 * 1024 * 1024),
    )(d_qkv, w_qkv, x, d_resid1, gain, *(earlier or ()))


def pieces_out_kernel(n_in, spans, me_ref, *refs):
    out_refs = refs[n_in:]
    for p in range(n_in):
        @pl.when(pl.program_id(0) == p)
        def _(p=p):
            for (start, n, turned), out_ref in zip(spans, out_refs):
                part = refs[p][start:start + n, :]
                out_ref[...] = part.T if turned else part


def pieces_out(me, pieces, spans):
    rows, width = pieces[0].shape
    n_in = len(pieces)

    def place(p, m):
        return (m[1] ^ (p // 2)) * 2 + (m[0] ^ (p % 2))

    out_specs, out_shape = [], []
    for start, n, turned in spans:
        if turned:
            out_specs.append(pl.BlockSpec((width, n), lambda p, m: (0, place(p, m))))
            out_shape.append(jax.ShapeDtypeStruct((width, n_in * n), F32))
        else:
            out_specs.append(pl.BlockSpec((n, width), lambda p, m: (place(p, m), 0)))
            out_shape.append(jax.ShapeDtypeStruct((n_in * n, width), F32))
    return pl.pallas_call(
        functools.partial(pieces_out_kernel, n_in, spans),
        grid_spec=pltpu.PrefetchScalarGridSpec(
            num_scalar_prefetch=1, grid=(n_in,),
            in_specs=[pl.BlockSpec((rows, width), lambda p, m: (0, 0), pipeline_mode=pl.Buffered(1))] * n_in,
            out_specs=out_specs),
        out_shape=out_shape,
        name="grads_out",
        cost_estimate=pl.CostEstimate(flops=8_000_000_000, bytes_accessed=n_in * rows * width * 8, transcendentals=0),
        compiler_params=pltpu.CompilerParams(vmem_limit_bytes=63 * 1024 * 1024),
    )(me, *pieces)


def assemble_kernel(n, me_ref, *refs):
    out_ref = refs[n]
    k = me_ref[0] ^ pl.program_id(0)
    for j in range(n):
        @pl.when(k == j)
        def _(j=j):
            out_ref[...] = refs[j][...].reshape(out_ref.shape)


def assemble(me, parts, out_shape, block):
    at = 1 if len(out_shape) == 4 else 0
    return pl.pallas_call(
        functools.partial(assemble_kernel, len(parts)),
        grid_spec=pltpu.PrefetchScalarGridSpec(
            num_scalar_prefetch=1, grid=(len(parts),),
            in_specs=[pl.BlockSpec(p.shape, lambda i, m: (0, 0, 0), pipeline_mode=pl.Buffered(1)) for p in parts],
            out_specs=pl.BlockSpec(block, lambda i, m: tuple(i if d == at else 0 for d in range(len(block))))),
        out_shape=jax.ShapeDtypeStruct(out_shape, parts[0].dtype),
        name="assemble",
        cost_estimate=pl.CostEstimate(flops=4_000_000_000, bytes_accessed=16 * MIB, transcendentals=0),
        compiler_params=pltpu.CompilerParams(vmem_limit_bytes=63 * 1024 * 1024),
    )(me, *parts)


LANES = 128


def accum_kernel(n_block, cap, sub_rows, width, where_ref, first_ref, *refs):
    tok_refs = refs[:n_block]
    out_ref = refs[n_block]
    n_sub = len(sub_rows)
    acc = refs[n_block + 1:n_block + 1 + n_sub]
    buf, stage, in_sem, out_sem = refs[n_block + 1 + n_sub:]
    tiles = width // LANES
    group = 8 * tiles

    def fetch(block, n):
        return pltpu.make_async_copy(tok_refs[n], buf.at[block % 2], in_sem.at[block % 2])

    def fetch_next(block):
        for n in range(n_block):
            @pl.when(block == n)
            def _(n=n):
                fetch(block, n).start()

    fetch_next(0)
    for s in range(n_sub):
        def clear(i, _, s=s):
            acc[s][pl.ds(pl.multiple_of(i * group, group), group), :] = jnp.zeros((group, LANES), F32)
            return 0

        lax.fori_loop(0, sub_rows[s] // 8, clear, 0)

    def add_rows(s, slot, n):
        codes = [where_ref[slot + j] for j in range(n)]
        at = [code >> 16 for code in codes]
        rows = [stage[pl.ds(code & 0xffff, tiles, stride=8), :] for code in codes]
        sums = [acc[s][pl.ds(a, tiles, stride=8), :] for a in at]
        for j in range(n):
            for i in range(j):
                sums[j] = jnp.where(at[i] == at[j], sums[i], sums[j])
            sums[j] = sums[j] + rows[j]
        for j in range(n):
            acc[s][pl.ds(at[j], tiles, stride=8), :] = sums[j]

    def add_block(block, _):
        fetch_next(block + 1)
        fetch(block, 0).wait()

        def widen(g, _):
            rows = buf[block % 2, pl.ds(pl.multiple_of(g * WIDEN, WIDEN), WIDEN), :].astype(F32)
            base = pl.multiple_of(g * (WIDEN // 8) * group, (WIDEN // 8) * group)
            for h in range(WIDEN // 8):
                for c in range(tiles):
                    stage[pl.ds(base + h * group + c * 8, 8), :] = rows[h * 8:(h + 1) * 8, c * LANES:(c + 1) * LANES]
            return 0

        lax.fori_loop(0, cap // WIDEN, widen, 0)

        starts = [first_ref[block * (n_sub + 1) + s] for s in range(n_sub + 1)]
        counts = [starts[s + 1] - starts[s] for s in range(n_sub)]
        both = functools.reduce(jnp.minimum, counts) // 2
        begin = [block * cap + starts[s] for s in range(n_sub)]

        def together(i, _):
            for s in range(n_sub):
                add_rows(s, begin[s] + 2 * i, 2)
            return 0

        lax.fori_loop(0, both, together, 0)
        for s in range(n_sub):
            fours = (counts[s] - 2 * both) // 4

            def alone(i, _, s=s):
                add_rows(s, begin[s] + 2 * both + 4 * i, 4)
                return 0

            lax.fori_loop(0, fours, alone, 0)

            def single(i, _, s=s):
                add_rows(s, begin[s] + i, 1)
                return 0

            lax.fori_loop(2 * both + 4 * fours, counts[s], single, 0)
        return 0

    lax.fori_loop(0, n_block, add_block, 0)
    done = 0
    copies = []
    for s in range(n_sub):
        n = sub_rows[s] * tiles
        copies.append(pltpu.make_async_copy(acc[s], out_ref.at[pl.ds(done, n), :], out_sem.at[s]))
        copies[-1].start()
        done += n
    for c in copies:
        c.wait()


def accum(tok_blocks, code, first, sub_rows, width):
    n_block = len(tok_blocks)
    cap = tok_blocks[0].shape[0]
    n_sub = len(sub_rows)
    tiles = width // LANES
    return pl.pallas_call(
        functools.partial(accum_kernel, n_block, cap, sub_rows, width),
        in_specs=[pl.BlockSpec(memory_space=pltpu.SMEM), pl.BlockSpec(memory_space=pltpu.SMEM)]
        + [pl.BlockSpec(memory_space=pl.ANY)] * n_block,
        out_specs=pl.BlockSpec(memory_space=pl.ANY),
        out_shape=jax.ShapeDtypeStruct((sum(sub_rows) * tiles, LANES), F32),
        scratch_shapes=[pltpu.VMEM((r * tiles, LANES), F32) for r in sub_rows]
        + [pltpu.VMEM((2, cap, width), BF16), pltpu.VMEM((cap * tiles, LANES), F32),
           pltpu.SemaphoreType.DMA((2,)), pltpu.SemaphoreType.DMA((n_sub,))],
        name="table_accum",
        cost_estimate=pl.CostEstimate(flops=50_000_000_000, bytes_accessed=100_000_000, transcendentals=0),
        compiler_params=pltpu.CompilerParams(vmem_limit_bytes=63 * 1024 * 1024),
    )(code, first, *tok_blocks)


def dot_tn(a, b):
    return lax.dot_general(a, b, (((0,), (0,)), ((), ())), preferred_element_type=F32)


def grad_kernel(has_plus, core_ref, a_ref, b_ref, *refs):
    out_ref = refs[-1]
    piece, width = out_ref.shape[2:]
    half = a_ref.shape[1] // 2
    g = dot_tn(a_ref[...], b_ref[...])
    for x in range(2):
        part = g[x * half:(x + 1) * half]
        out_ref[x, 0, 0:half, :] = part + refs[0][x * piece:x * piece + half, :] if has_plus else part
        if piece > half:
            out_ref[x, 0, half:, :] = jnp.zeros((piece - half, width), F32)


def grad_pieces(core, a, b, n_tp, piece, which, n_which, plus=None, into=None):
    n_tok, n_cols = a.shape
    width = b.shape[1]
    out_spec = pl.BlockSpec((2, 1, piece, width), lambda t, c: (t, which, 0, 0))
    in_specs = [pl.BlockSpec((n_tok, n_cols // (2 * n_tp)), lambda t, c: (0, 2 * t + c[0])),
                pl.BlockSpec((n_tok, width), lambda t, c: (0, 0), pipeline_mode=pl.Buffered(1))]
    args = [a, b]
    if plus is not None:
        in_specs.append(pl.BlockSpec((2 * piece, width), lambda t, c: (t, 0)))
        args.append(plus)
    shape = (2 * n_tp, n_which, piece, width)
    if into is not None:
        in_specs.append(pl.BlockSpec(memory_space=pl.ANY))
        args.append(into.reshape(shape))
    return pl.pallas_call(
        functools.partial(grad_kernel, plus is not None),
        grid_spec=pltpu.PrefetchScalarGridSpec(num_scalar_prefetch=1, grid=(n_tp,), in_specs=in_specs, out_specs=out_spec),
        out_shape=jax.ShapeDtypeStruct(shape, F32),
        input_output_aliases={} if into is None else {len(args): 0},
        name="weight_grad",
        cost_estimate=pl.CostEstimate(flops=n_tok * n_cols * width, bytes_accessed=n_tok * (n_cols + 2 * width) + 2 * n_cols * width,
                                      transcendentals=0),
        compiler_params=pltpu.CompilerParams(vmem_limit_bytes=63 * 1024 * 1024),
    )(core, *args).reshape(-1, width)


def grad_rest_kernel(spans, last, n_a2, core_ref, a1_ref, b1_ref, b2_ref, *refs):
    a2_refs, refs, out_ref = refs[:n_a2], refs[n_a2:-1], refs[-1]
    plus = refs[0] if refs else None
    piece, piece_in = out_ref.shape[0] // 2, (plus.shape[0] // 2 if refs else 0)
    rows = b2_ref.shape[0] // n_a2
    for which, (start, stop) in enumerate(spans):
        half = (a2_refs[0] if which else a1_ref).shape[1] // 2
        for i in range(0, 2 * half, 128):
            cols = slice(i, i + 128)
            if which:
                g = sum(dot_tn(a_ref[:, cols], b2_ref[n * rows:(n + 1) * rows, :]) for n, a_ref in enumerate(a2_refs))
            else:
                g = dot_tn(a1_ref[:, cols], b1_ref[...])
            for x in range(2):
                lo, hi = max(i, x * half), min(i + 128, (x + 1) * half)
                if lo < hi:
                    to = lo - x * half + start
                    part = g[lo - i:hi - i]
                    if plus is not None:
                        part = part + plus[x * piece_in + to:x * piece_in + to + hi - lo, :]
                    out_ref[x * piece + to:x * piece + to + hi - lo, :] = part
        for x in range(2):
            if stop > start + half:
                out_ref[x * piece + start + half:x * piece + stop, :] = jnp.zeros((stop - start - half, out_ref.shape[1]), F32)
    if last:
        for x in range(2):
            out_ref[x * piece + spans[-1][1]:(x + 1) * piece, :] = refs[1][x, 0] + refs[2][x * last:(x + 1) * last, :]


def grad_rest(core, a1, b1, a2, b2, n_tp, spans, plus=None, tail=None):
    n_tok, width = b1.shape
    last = tail[0].shape[2] if tail else 0
    piece = spans[-1][1] + last
    whole = pl.BlockSpec((n_tok, width), lambda t, c: (0, 0), pipeline_mode=pl.Buffered(1))
    cols = [pl.BlockSpec((a.shape[0], a.shape[1] // (2 * n_tp)), lambda t, c: (0, 2 * t + c[0])) for a in (a1, *a2)]
    in_specs, args = [cols[0], whole, whole] + cols[1:], [a1, b1, b2, *a2]
    if plus is not None:
        in_specs.append(pl.BlockSpec((plus.shape[0] // n_tp, width), lambda t, c: (t, 0)))
        args.append(plus)
    if tail:
        in_specs.append(pl.BlockSpec((2, 1, last, width), lambda t, c: (t, c[0], 0, 0)))
        in_specs.append(pl.BlockSpec((2 * last, width), lambda t, c: (t, 0)))
        args += tail
    n_cols = a1.shape[1] + a2[0].shape[1]
    return pl.pallas_call(
        functools.partial(grad_rest_kernel, spans, last, len(a2)),
        grid_spec=pltpu.PrefetchScalarGridSpec(num_scalar_prefetch=1, grid=(n_tp,), in_specs=in_specs,
                                               out_specs=pl.BlockSpec((2 * piece, width), lambda t, c: (t, 0))),
        out_shape=jax.ShapeDtypeStruct((2 * n_tp * piece, width), F32),
        name="weight_grads",
        cost_estimate=pl.CostEstimate(flops=n_tok * n_cols * width, bytes_accessed=n_tok * (n_cols + 4 * width) + 2 * n_cols * width,
                                      transcendentals=0),
        compiler_params=pltpu.CompilerParams(vmem_limit_bytes=63 * 1024 * 1024),
    )(core, *args)


POS_OFFSET = 2
SLOTS = 704
GRAD_SLOTS = 384
LOW = 32


def before(n):
    return (lax.broadcasted_iota(jnp.int32, (n, n), 1) < lax.broadcasted_iota(jnp.int32, (n, n), 0)).astype(BF16)


def rank_in_class(hot):
    n_blk, n_tok, n_cls = hot.shape
    ones = hot.astype(BF16).reshape(n_blk, n_tok // 128, 128, n_cls)
    within = jnp.einsum("ij,bnjk->bnik", before(128), ones, preferred_element_type=F32)
    sums = jnp.sum(ones.astype(F32), axis=2)
    ahead = jnp.einsum("mn,bnk->bmk", before(n_tok // 128), sums.astype(BF16), preferred_element_type=F32)
    rank = jnp.sum((within + ahead[:, :, None, :]) * ones.astype(F32), axis=3)
    return rank.reshape(n_blk, n_tok).astype(jnp.int32), jnp.sum(sums, axis=1).astype(jnp.int32)


def compact(rank, valid, value, slots):
    n_high = slots // LOW
    high = ((rank // LOW)[:, :, None] == jnp.arange(n_high)) & valid[:, :, None]
    low = ((rank % LOW)[:, :, None] == jnp.arange(LOW)).astype(F32)
    parts = jnp.concatenate([low * (value // 128).astype(F32)[:, :, None], low * (value % 128).astype(F32)[:, :, None]], axis=2)
    out = jnp.einsum("bjh,bjl->bhl", high.astype(BF16), parts.astype(BF16), preferred_element_type=F32).astype(jnp.int32)
    return (out[:, :, :LOW] * 128 + out[:, :, LOW:]).reshape(rank.shape[0], slots)


def solution(mesh):
    n_tp, n_dp = mesh.shape["tp"], mesh.shape["dp"]
    n_core = 2
    n_x = n_dp // n_core
    mesh3 = Mesh(mesh.devices.reshape(n_tp, n_x, n_core), ("tp", "xx", "cc"))
    dp = ("xx", "cc")
    tp_swap = [[(i, i ^ k) for i in range(n_tp)] for k in range(n_tp)]
    pair = [(0, 1), (1, 0)]

    def local_step(tok_ids, emb_table, pos_table, ln1_gain, ln1_bias, w_qkv, b_qkv, w_out, b_out,
                   ln2_gain, ln2_bias, w_up, b_up, w_down, b_down, out_grad):
        tp_index, x_index, c_index = lax.axis_index("tp"), lax.axis_index("xx"), lax.axis_index("cc")
        dp_index = x_index * n_core + c_index
        n_seq_dp, seq = tok_ids.shape
        n_seq = n_seq_dp // n_tp
        n_tok = n_seq * seq
        rows, width = emb_table.shape
        n_sub = 4
        sub = -(-rows // n_sub // 8) * 8
        sub_rows = (sub,) * (n_sub - 1) + (rows - (n_sub - 1) * sub,)
        seq_local = seq // n_tp
        ff = w_up.shape[1]
        gain1, bias1 = ln1_gain.astype(F32)[None], ln1_bias.astype(F32)[None]
        gain2, bias2 = ln2_gain.astype(F32)[None], ln2_bias.astype(F32)[None]

        def half(w, axis):
            n = w.shape[axis] // n_core
            return lax.dynamic_slice_in_dim(w, c_index * n, n, axis)

        def gather_rows(w):
            return lax.all_gather(w, ("tp", "cc"), axis=0, tiled=True)

        def swap(v, axis, k=1):
            return lax.ppermute(v, axis, tp_swap[k] if axis == "tp" else pair)

        def by_owner(parts):
            out = []
            for p in range(n_tp):
                k = tp_index ^ p
                out.append(jnp.where(k < 2, jnp.where(k == 0, parts[0], parts[1]), jnp.where(k == 2, parts[2], parts[3])))
            return out

        ids_all = lax.all_gather(tok_ids, dp, axis=0, tiled=True)
        ids_all, w_up, w_down, w_out, b_qkv, b_up = lax.optimization_barrier((ids_all, w_up, w_down, w_out, b_qkv, b_up))

        wqkv_t = gather_rows(jnp.transpose(half(w_qkv, 2), (1, 2, 3, 0)).reshape(-1, width))
        n_ff, n_out = ff // n_dp, w_out.shape[0] * w_out.shape[1] // n_dp

        def quarter(w, axis):
            n = w.shape[axis] // n_dp
            return lax.dynamic_slice_in_dim(w, dp_index * n, n, axis)

        own_w = jnp.concatenate([quarter(w_up, 1).T, quarter(w_down, 0), quarter(w_out.reshape(-1, width), 0)])
        w_all = lax.all_gather(own_w, ("tp", "xx", "cc"), axis=0, tiled=True)
        w_all = w_all.reshape(n_tp * n_dp, 2 * n_ff + n_out, width)
        wout_w = w_all[:, 2 * n_ff:].reshape(-1, width)
        n_pair = wqkv_t.shape[0] // (3 * 128)
        own_bias = jnp.concatenate([b_qkv.reshape(3, n_core, -1, b_qkv.shape[2]).transpose(1, 0, 2, 3).reshape(-1), b_up])
        biases = jnp.stack(by_owner([swap(own_bias, "tp", k) if k else own_bias for k in range(n_tp)]))
        bqkv_w = biases[:, :-ff].reshape(-1).astype(F32)
        bup_w = biases[:, -ff:].reshape(1, -1).astype(F32)
        pos_rows = lax.slice_in_dim(pos_table, POS_OFFSET, POS_OFFSET + seq, axis=0)

        local = ids_all - tp_index * rows
        sub_of = sum(((local >= s * sub).astype(jnp.int32) for s in range(1, n_sub)), jnp.zeros_like(local))
        owned = (local >= 0) & (local < rows)
        hot = owned[:, :, None] & (sub_of[:, :, None] == jnp.arange(n_sub))
        rank, counts = rank_in_class(hot)
        first = jnp.concatenate([jnp.zeros_like(counts[:, :1]), jnp.cumsum(counts, axis=1)], axis=1)
        rank = rank + jnp.sum(jnp.where(hot, first[:, None, :-1], 0), axis=2)
        owner_counts = jnp.stack([jnp.sum(((ids_all >= o * rows) & (ids_all < (o + 1) * rows)).astype(jnp.int32), axis=1)
                                  for o in range(n_tp)])
        grad_rounds = (jnp.max(owner_counts) + GRAD_SLOTS - 1) // GRAD_SLOTS
        rounds = (jnp.max(jnp.sum(owner_counts.reshape(n_tp, -1, n_seq), axis=2)) + SLOTS - 1) // SLOTS

        def after_first(ranks, totals):
            return (ranks + (jnp.cumsum(totals, axis=1) - totals)[:, :, None]).reshape(ranks.shape[0], -1)

        def grad_lists(r):
            at = rank - r * GRAD_SLOTS
            return compact(at, owned & (at >= 0) & (at < GRAD_SLOTS), jnp.where(owned, local, 0), GRAD_SLOTS)

        my_rank = lax.dynamic_slice_in_dim(rank, dp_index * n_seq_dp, n_seq_dp, 0)
        my_total = lax.dynamic_slice_in_dim(first[:, -1], dp_index * n_seq_dp, n_seq_dp, 0)
        my_rank = after_first(my_rank.reshape(n_tp, n_seq, seq), my_total.reshape(n_tp, n_seq))
        my_owned = lax.dynamic_slice_in_dim(owned, dp_index * n_seq_dp, n_seq_dp, 0).reshape(n_tp, n_tok)
        my_local = lax.dynamic_slice_in_dim(local, dp_index * n_seq_dp, n_seq_dp, 0).reshape(n_tp, n_tok)

        def lists(r):
            at = my_rank - r * SLOTS
            return compact(at, my_owned & (at >= 0) & (at < SLOTS), jnp.where(my_owned, my_local, 0), SLOTS)

        own_ids = lax.dynamic_slice_in_dim(ids_all, dp_index * n_seq_dp + tp_index * n_seq, n_seq, 0)
        own_owner = sum(((own_ids >= o * rows).astype(jnp.int32) for o in range(1, n_tp)), jnp.zeros_like(own_ids))
        own_local = own_ids - own_owner * rows
        own_sub = sum(((own_local >= s * sub).astype(jnp.int32) for s in range(1, n_sub)), jnp.zeros_like(own_ids))
        own_hot = (own_owner * n_sub + own_sub)[:, :, None] == jnp.arange(n_tp * n_sub)
        own_rank, own_counts = rank_in_class(own_hot)
        own_counts = own_counts.reshape(n_seq, n_tp, n_sub)
        own_first = jnp.cumsum(own_counts, axis=2) - own_counts
        own_rank = own_rank + jnp.sum(jnp.where(own_hot, own_first.reshape(n_seq, 1, -1), 0), axis=2)
        own_total = jnp.sum(own_counts, axis=2)
        own_shift = jnp.cumsum(own_total, axis=0) - own_total
        own_place = sum(jnp.where(own_owner == o, own_shift[:, o:o + 1], 0) for o in range(n_tp))
        own_place = (own_place + own_rank).reshape(-1)

        def own_lists(r, b):
            at = jnp.broadcast_to(own_rank[b] - r * GRAD_SLOTS, (n_tp, seq))
            mine = own_owner[b] == jnp.arange(n_tp)[:, None]
            return compact(at, mine & (at >= 0) & (at < GRAD_SLOTS), jnp.broadcast_to(jnp.arange(seq), (n_tp, seq)), GRAD_SLOTS)

        tiles = width // 128

        def own_places(r, b):
            own = own_lists(r, b)
            place = jnp.concatenate([lax.dynamic_index_in_dim(own, tp_index ^ k, 0, keepdims=False) for k in range(n_tp)])
            return (place // 8) * (8 * tiles) + place % 8

        places0 = [own_places(0, b) for b in range(n_seq)]

        def in_block_order(table, b):
            out = []
            for dc in range(n_core):
                for dx in range(n_x):
                    for k in range(n_tp):
                        d = (x_index ^ dx) * n_core + (c_index ^ dc)
                        out.append(lax.dynamic_index_in_dim(table, (d * n_tp + (tp_index ^ k)) * n_seq + b, 0, keepdims=False))
            return out

        def both_orders(table):
            return jnp.stack(in_block_order(table, 0) + in_block_order(table, 1))

        block_rows = both_orders(grad_lists(0))
        in_sub = sum(((block_rows >= s * sub).astype(jnp.int32) for s in range(1, n_sub)), jnp.zeros_like(block_rows))
        in_sub = block_rows - in_sub * sub
        slot = jnp.arange(GRAD_SLOTS)
        code = (((in_sub // 8) * (8 * tiles) + in_sub % 8) << 16) | ((slot // 8) * (8 * tiles) + slot % 8)
        code = code.reshape(-1)
        block_first = jnp.minimum(both_orders(first), GRAD_SLOTS).reshape(-1)

        def rows_here(r, my_lists):
            index = [lax.dynamic_index_in_dim(my_lists, tp_index ^ k, 0, keepdims=False) for k in range(n_tp)]
            first_two = jnp.take(emb_table, jnp.concatenate([index[3], index[1]]), axis=0, mode="clip")
            rest, first_two = lax.optimization_barrier((jnp.concatenate([index[2], index[0]]), first_two))
            last_two = jnp.take(emb_table, rest, axis=0, mode="clip")
            sent = [last_two[SLOTS:], first_two[SLOTS:], last_two[:SLOTS], first_two[:SLOTS]]
            got = list(sent)
            for k in range(1, n_tp):
                got[k] = swap(sent[k], "tp", k)
            at = own_place - r * SLOTS
            valid = (at >= 0) & (at < SLOTS)
            return got, jnp.where(valid, (own_owner.reshape(-1) ^ tp_index) * SLOTS + at, 0), valid

        def norm_rows(x):
            normed, _ = row_stats(x)
            return (normed * gain1 + bias1).astype(BF16)

        got0, place0, _ = rows_here(0, lists(0))
        code0 = (place0 // 8) * (8 * tiles) + place0 % 8
        og_parts = out_grad.reshape(n_tp, n_seq, seq_local, width)
        og_parts = [lax.dynamic_index_in_dim(og_parts, tp_index ^ k, 0, keepdims=False) for k in range(n_tp)]
        got0, og_parts = lax.optimization_barrier((got0, og_parts))
        resid_x, hid1 = embed(code0, got0, pos_rows, gain1, bias1, n_tok)

        def more_rows(carry):
            r, x, _ = carry
            got, place, valid = rows_here(r, lists(r))
            new = jnp.take(jnp.concatenate(got), place, axis=0, mode="clip").astype(F32) + jnp.tile(pos_rows.astype(F32), (n_seq, 1))
            x = jnp.where(valid[:, None], new, x)
            return r + 1, x, norm_rows(x)

        _, resid_x, hid1 = lax.while_loop(lambda c: c[0] < rounds, more_rows, (jnp.int32(1), resid_x, hid1))

        parts = [swap(part, "tp", k) if k else part for k, part in enumerate(og_parts)]
        me = jnp.reshape(tp_index, (1,))
        og = assemble(me, parts, (n_seq, n_tp, seq_local, width), (n_seq, 1, seq_local, width)).reshape(n_tok, width)

        qkv = (dot_nt(hid1, wqkv_t) + bqkv_w).astype(BF16)
        ctx, lse = attn_fwd(qkv, n_seq, seq, n_pair)
        resid_x1, hid2 = proj_norm(ctx, w_all, 2 * n_ff, resid_x, b_out.astype(F32)[None], gain2, bias2)
        act, d_up, d_b_up = ffn(hid2, og, w_all, bup_w)
        parts = down(me, act, w_all, resid_x1, b_down.astype(F32)[None], n_seq, n_tp)
        parts = [swap(part, "tp", k) if k else part for k, part in enumerate(parts)]
        layer_out = assemble(me, parts, (n_seq_dp, seq_local, width), (n_seq, seq_local, width))

        core = jnp.reshape(c_index, (1,))

        def piece_of(n_rows):
            return -(-n_rows // (4 * n_tp) // 24) * 24

        def every_piece(g):
            other = swap(g, "xx")
            return [g, other, swap(g, "cc"), swap(other, "cc")]

        x_and_core = jnp.stack([x_index, c_index])

        p_ff = piece_of(n_tp * ff)
        down_theirs = swap(grad_pieces(1 - core, act, og, n_tp, p_ff, 0, 1), "cc")
        up_theirs = swap(grad_pieces(1 - core, d_up, hid2, n_tp, p_ff, 0, 1), "cc")
        ff_grads = grad_pieces(core, act, og, n_tp, p_ff, 0, 2, plus=down_theirs)
        ff_grads = grad_pieces(core, d_up, hid2, n_tp, p_ff, 1, 2, plus=up_theirs, into=ff_grads)
        ff_grads = lax.psum_scatter(ff_grads, ("tp", "xx"), scatter_dimension=0, tiled=True)
        ff_grads = every_piece(ff_grads)

        d_resid1, d_attn, sums2 = back2(d_up, w_all, resid_x1, og, gain2)
        d_ctx = dot_nt(d_attn, wout_w).astype(BF16)
        n_small = n_tp * (b_qkv.size + ff) // width + 6
        p_pos = -(-(seq + n_small) // (24 * n_tp * n_dp)) * 24
        p_out = piece_of(wout_w.shape[0])
        spans = ((0, p_out), (p_out, p_out + piece_of(wqkv_t.shape[0])))

        def token_blocks(places, d_tok):
            parts = pack(places, d_tok, GRAD_SLOTS)
            blocks = [swap(part, "tp", k) if k else part for k, part in enumerate(parts)]
            other = []
            for block in blocks:
                other.append(swap(block, "xx"))
            return blocks + other + [swap(block, "cc") for block in blocks + other]

        d_qkv0 = attn_bwd(qkv, ctx, d_ctx, lse, 0, seq, n_pair)
        d_tok0, *sums0 = back1(d_qkv0, wqkv_t, resid_x, d_resid1, gain1, 0, p_pos * n_tp * n_dp)
        blocks0 = token_blocks(places0[0], d_tok0)
        d_qkv1 = attn_bwd(qkv, ctx, d_ctx, lse, 1, seq, n_pair)
        d_tok1, pos_all, sums1, sums_qkv = back1(d_qkv1, wqkv_t, resid_x, d_resid1, gain1, 1, p_pos * n_tp * n_dp, earlier=sums0)
        blocks1 = token_blocks(places0[1], d_tok1)
        d_qkvs = [d_qkv0, d_qkv1]
        rest_theirs = swap(grad_rest(1 - core, ctx, d_attn, d_qkvs, hid1, n_tp, spans), "cc")

        d_w_down, d_w_up = pieces_out(x_and_core, ff_grads, ((0, n_ff, False), (p_ff, n_ff, True)))
        image = accum(blocks0 + blocks1, code, block_first, sub_rows, width)
        d_emb = image.reshape(rows // 8, tiles, 8, 128).transpose(0, 2, 1, 3).reshape(rows, width)

        def more_grads(carry):
            r, table = carry
            at = rank - r * GRAD_SLOTS
            there = owned & (at >= 0) & (at < GRAD_SLOTS)
            dest = compact(at, there, jnp.where(owned, local, 0) + 1, GRAD_SLOTS)
            dest = jnp.where(dest == 0, rows, dest - 1)
            grads = jnp.concatenate(token_blocks(own_places(r, 0), d_tok0) + token_blocks(own_places(r, 1), d_tok1), axis=0).astype(F32)
            return r + 1, table.at[both_orders(dest).reshape(-1)].add(grads, mode="drop")

        _, d_emb = lax.while_loop(lambda c: c[0] < grad_rounds, more_grads, (jnp.int32(1), d_emb))

        small = jnp.concatenate([sums_qkv[0], d_b_up[0], sums1[:2].reshape(-1), sums2[:4].reshape(-1)]).reshape(-1, width)
        small = jnp.concatenate([small, jnp.zeros((pos_all.shape[0] - seq - n_small, width), F32)])
        pos_all = lax.dynamic_update_slice_in_dim(pos_all, small, seq, 0).reshape(n_tp * n_x, n_core, p_pos, width)
        pos_theirs = swap(lax.dynamic_index_in_dim(pos_all, 1 - c_index, 1, keepdims=False).reshape(-1, width), "cc")
        pos_both = lax.dynamic_index_in_dim(pos_all, c_index, 1, keepdims=False).reshape(-1, width) + pos_theirs
        pos_both = lax.psum_scatter(pos_both, ("tp", "xx"), scatter_dimension=0, tiled=True)
        rest = grad_rest(core, ctx, d_attn, d_qkvs, hid1, n_tp, spans, plus=rest_theirs)
        rest = lax.psum_scatter(rest, ("tp", "xx"), scatter_dimension=0, tiled=True)
        rest_w = every_piece(rest)
        whole = lax.all_gather(pos_both, ("tp", "xx", "cc"), axis=0, tiled=True)
        d_pos = jnp.pad(whole[:seq], ((POS_OFFSET, pos_table.shape[0] - seq - POS_OFFSET), (0, 0)))
        small = whole[seq:seq + n_small].reshape(-1)
        n_b = b_qkv.size
        d_b_qkv = lax.dynamic_slice_in_dim(small, tp_index * n_b, n_b).reshape(n_core, 3, -1, b_qkv.shape[2])
        d_b_qkv = d_b_qkv.transpose(1, 0, 2, 3).reshape(b_qkv.shape)
        d_b_up = lax.dynamic_slice_in_dim(small, n_tp * n_b + tp_index * ff, ff)
        d_gain1, d_bias1, d_gain2, d_bias2, d_b_out, d_b_down = small[n_tp * (n_b + ff):].reshape(6, width)

        d_w_out, d_w_qkv = pieces_out(x_and_core, rest_w, ((0, n_out, False), (p_out, n_b // n_dp, False)))
        d_w_out = d_w_out.reshape(w_out.shape)
        d_w_qkv = d_w_qkv.reshape(n_core, 3, -1, w_qkv.shape[3], width).transpose(4, 1, 0, 2, 3).reshape(w_qkv.shape)
        return (layer_out, d_emb, d_pos, d_gain1, d_bias1, d_w_qkv, d_b_qkv, d_w_out,
                d_b_out, d_gain2, d_bias2, d_w_up, d_b_up, d_w_down, d_b_down)

    rep = P()
    in_specs = (P(dp, None), P("tp", None), rep, rep, rep,
                P(None, None, "tp", None), P(None, "tp", None), P("tp", None, None), rep,
                rep, rep, P(None, "tp"), P("tp"), P("tp", None), rep,
                P(dp, "tp", None))
    out_specs = (P(dp, "tp", None), P("tp", None), rep, rep, rep,
                 P(None, None, "tp", None), P(None, "tp", None), P("tp", None, None), rep,
                 rep, rep, P(None, "tp"), P("tp"), P("tp", None), rep)

    return jax.shard_map(local_step, mesh=mesh3, in_specs=in_specs, out_specs=out_specs, check_vma=False)
```

```python
import functools

import jax
import jax.numpy as jnp
from jax import lax
from jax.experimental import pallas as pl
from jax.experimental.pallas import tpu as pltpu
from jax.sharding import Mesh, PartitionSpec as P


F32 = jnp.float32
BF16 = jnp.bfloat16
MIB = 1024 * 1024
WIDEN = 32

BLK = 256


def dot_nt(a, b):
    return lax.dot_general(a, b, (((1,), (1,)), ((), ())), preferred_element_type=F32)


def dot_nn(a, b):
    return lax.dot_general(a, b, (((1,), (0,)), ((), ())), preferred_element_type=F32)


def head_only(x, head):
    half = x.shape[1] // 2
    lane = lax.broadcasted_iota(jnp.int32, x.shape, 1)
    keep = (lane < half) if head == 0 else (lane >= half)
    return jnp.where(keep, x, jnp.zeros((), x.dtype))


def attn_fwd_kernel(qkv_ref, ctx_ref, lse_ref, ctx_t):
    seq, width = ctx_ref.shape
    half = width // 2
    scale = half ** -0.5
    q2 = qkv_ref[:, 0:width] * jnp.asarray(scale, BF16)
    v_t = qkv_ref[:, 2 * width:3 * width].T
    tasks = [(head, i) for i in range(seq // BLK) for head in range(2)]

    def scores(head, i):
        return dot_nt(qkv_ref[0:(i + 1) * BLK, width:2 * width], head_only(q2[i * BLK:(i + 1) * BLK], head))

    ready = scores(*tasks[0])
    for n, (head, i) in enumerate(tasks):
        s = ready
        if n + 1 < len(tasks):
            ready = scores(*tasks[n + 1])
        lo, hi = i * BLK, (i + 1) * BLK
        v_h = v_t[head * half:(head + 1) * half, :]
        key = lax.broadcasted_iota(jnp.int32, (BLK, BLK), 0)
        qry = lax.broadcasted_iota(jnp.int32, (BLK, BLK), 1)
        diag = jnp.where(key <= qry, s[lo:hi], -1e30)
        top = jnp.max(diag, axis=0, keepdims=True)
        if i:
            top = jnp.maximum(top, jnp.max(s[0:lo], axis=0, keepdims=True))
        p_diag = jnp.exp(diag - top)
        total = jnp.sum(p_diag, axis=0, keepdims=True)
        if i:
            p_left = jnp.exp(s[0:lo] - top)
            total = total + jnp.sum(p_left, axis=0, keepdims=True)
        inv = 1.0 / total
        acc = dot_nn(v_h[:, lo:hi], (p_diag * inv).astype(BF16))
        if i:
            acc = acc + dot_nn(v_h[:, 0:lo], (p_left * inv).astype(BF16))
        ctx_t[head * half:(head + 1) * half, lo:hi] = acc
        lse_ref[head:head + 1, lo:hi] = top + jnp.log(total)
    ctx_ref[...] = ctx_t[...].T.astype(BF16)


def attn_fwd(qkv, n_seq, seq, n_pair):
    width = 128
    return pl.pallas_call(
        attn_fwd_kernel,
        grid=(n_seq, n_pair),
        in_specs=[pl.BlockSpec((seq, 3 * width), lambda b, p: (b, p))],
        out_specs=[pl.BlockSpec((seq, width), lambda b, p: (b, p)),
                   pl.BlockSpec((None, None, 2, seq), lambda b, p: (b, p, 0, 0))],
        out_shape=[jax.ShapeDtypeStruct((n_seq * seq, n_pair * width), BF16),
                   jax.ShapeDtypeStruct((n_seq, n_pair, 2, seq), F32)],
        scratch_shapes=[pltpu.VMEM((width, seq), F32)],
        name="attn_fwd",
        cost_estimate=pl.CostEstimate(flops=n_seq * n_pair * 8 * seq * seq * 256 * 10 // 16, bytes_accessed=n_seq * seq * n_pair * width * 8,
                                      transcendentals=n_seq * n_pair * seq * seq),
        compiler_params=pltpu.CompilerParams(vmem_limit_bytes=63 * 1024 * 1024),
    )(qkv)


def attn_bwd_kernel(qkv_ref, ctx_ref, dctx_ref, lse_ref, dqkv_ref, dk_t, dv_t):
    seq, width = ctx_ref.shape
    half = width // 2
    scale = half ** -0.5
    q2 = qkv_ref[:, 0:width] * jnp.asarray(scale, BF16)
    q_t = q2.T
    do_t = dctx_ref[...].T
    lse_c = jnp.concatenate([lse_ref[...], jnp.zeros((6, seq), F32)], axis=0).T
    prod = dctx_ref[...].astype(F32) * ctx_ref[...].astype(F32)
    tasks = [(head, i) for i in range(seq // BLK) for head in range(2)]

    def scores(head, i):
        lo, hi = i * BLK, (i + 1) * BLK
        return (dot_nt(head_only(q2[lo:hi], head), qkv_ref[0:hi, width:2 * width]),
                dot_nt(head_only(dctx_ref[lo:hi, :], head), qkv_ref[0:hi, 2 * width:3 * width]))

    dq = []
    ready = scores(*tasks[0])
    for n, (head, i) in enumerate(tasks):
        s, dp = ready
        if n + 1 < len(tasks):
            ready = scores(*tasks[n + 1])
        lo, hi = i * BLK, (i + 1) * BLK
        rows = slice(head * half, (head + 1) * half)
        mean = jnp.sum(head_only(prod[lo:hi], head), axis=1, keepdims=True)
        lse = lse_c[lo:hi, head:head + 1]
        qry = lax.broadcasted_iota(jnp.int32, (BLK, BLK), 0)
        key = lax.broadcasted_iota(jnp.int32, (BLK, BLK), 1)
        p_diag = jnp.where(key <= qry, jnp.exp(s[:, lo:hi] - lse), 0.0)
        ds_diag = (p_diag * (dp[:, lo:hi] - mean)).astype(BF16)
        dv_t[rows, lo:hi] = dot_nn(do_t[rows, lo:hi], p_diag.astype(BF16))
        dk_t[rows, lo:hi] = dot_nn(q_t[rows, lo:hi], ds_diag)
        dq_h = dot_nn(ds_diag, qkv_ref[lo:hi, width:2 * width])
        if i:
            p_left = jnp.exp(s[:, 0:lo] - lse)
            ds_left = (p_left * (dp[:, 0:lo] - mean)).astype(BF16)
            dv_t[rows, 0:lo] += dot_nn(do_t[rows, lo:hi], p_left.astype(BF16))
            dk_t[rows, 0:lo] += dot_nn(q_t[rows, lo:hi], ds_left)
            dq_h = dq_h + dot_nn(ds_left, qkv_ref[0:lo, width:2 * width])
        dq.append(dq_h)
        if head == 1:
            lane = lax.broadcasted_iota(jnp.int32, (BLK, width), 1)
            dqkv_ref[lo:hi, 0:width] = (jnp.where(lane < half, dq[0], dq[1]) * scale).astype(BF16)
            dq = []
    dqkv_ref[:, width:2 * width] = dk_t[...].T.astype(BF16)
    dqkv_ref[:, 2 * width:3 * width] = dv_t[...].T.astype(BF16)


def attn_bwd(qkv, ctx, dctx, lse, at, seq, n_pair):
    width = 128
    return pl.pallas_call(
        attn_bwd_kernel,
        grid=(n_pair,),
        in_specs=[pl.BlockSpec((seq, 3 * width), lambda p: (at, p)),
                  pl.BlockSpec((seq, width), lambda p: (at, p)),
                  pl.BlockSpec((seq, width), lambda p: (at, p)),
                  pl.BlockSpec((None, None, 2, seq), lambda p: (at, p, 0, 0))],
        out_specs=pl.BlockSpec((seq, 3 * width), lambda p: (0, p)),
        out_shape=jax.ShapeDtypeStruct((seq, n_pair * 3 * width), BF16),
        scratch_shapes=[pltpu.VMEM((width, seq), F32), pltpu.VMEM((width, seq), F32)],
        name="attn_bwd",
        cost_estimate=pl.CostEstimate(flops=n_pair * 20 * seq * seq * 256 * 10 // 16, bytes_accessed=seq * n_pair * width * 16,
                                      transcendentals=n_pair * seq * seq),
        compiler_params=pltpu.CompilerParams(vmem_limit_bytes=63 * 1024 * 1024),
    )(qkv, ctx, dctx, lse)


LN_EPS = 1e-5
GELU_S = 0.7978845608028654
GELU_A = 0.044715


def row_mean(v):
    return jnp.sum(v, axis=1, keepdims=True) * (1.0 / v.shape[1])


def row_stats(v):
    centered = v - row_mean(v)
    inv_std = lax.rsqrt(row_mean(centered * centered) + LN_EPS)
    return centered * inv_std, inv_std


def norm_back(d_y, x_in, gain):
    normed, inv_std = row_stats(x_in)
    d_norm = d_y * gain
    d_x = inv_std * (d_norm - row_mean(d_norm) - normed * row_mean(d_norm * normed))
    return d_x, d_y * normed


def col_sum(v):
    return jnp.sum(v, axis=0, keepdims=True)


def to_image(rows, image, base):
    tiles = rows.shape[1] // 128
    for h in range(rows.shape[0] // 8):
        for c in range(tiles):
            image[pl.ds(base + (h * tiles + c) * 8, 8), :] = rows[h * 8:(h + 1) * 8, c * 128:(c + 1) * 128]


def from_image(image, base, n_rows, width):
    tiles = width // 128
    return jnp.concatenate([jnp.concatenate([image[pl.ds(base + (h * tiles + c) * 8, 8), :] for c in range(tiles)], axis=1)
                            for h in range(n_rows // 8)], axis=0)


def pick_rows(code_ref, first, stage, image, n_rows, tiles):
    def pick(g, _):
        base = pl.multiple_of(g * 16 * tiles, 16 * tiles)
        for j in range(16):
            row = stage[pl.ds(code_ref[first + g * 16 + j], tiles, stride=8), :]
            image[pl.ds(base + (j // 8) * 8 * tiles + j % 8, tiles, stride=8), :] = row
        return 0

    lax.fori_loop(0, n_rows // 16, pick, 0)


def embed_kernel(n_blk, cap, code_ref, *refs):
    tok_refs = refs[:n_blk]
    pos_ref, gain_ref, bias_ref, x_ref, hid_ref, stage, image = refs[n_blk:]
    rows, width = x_ref.shape
    tiles = width // 128

    @pl.when(pl.program_id(0) == 0)
    def _():
        for b in range(n_blk):
            def widen(g, _, b=b):
                part = tok_refs[b][pl.ds(pl.multiple_of(g * WIDEN, WIDEN), WIDEN), :].astype(F32)
                to_image(part, stage, pl.multiple_of((b * cap + g * WIDEN) * tiles, WIDEN * tiles))
                return 0

            lax.fori_loop(0, cap // WIDEN, widen, 0)

    pick_rows(code_ref, pl.program_id(0) * rows, stage, image, rows, tiles)
    part = 64
    for i in range(rows // part):
        at = slice(i * part, (i + 1) * part)
        x = from_image(image, i * part * tiles, part, width) + pos_ref[at, :].astype(F32)
        x_ref[at, :] = x
        normed, _ = row_stats(x)
        hid_ref[at, :] = (normed * gain_ref[...] + bias_ref[...]).astype(BF16)


def embed(code, blocks, pos_rows, gain, bias, n_tok):
    cap, width = blocks[0].shape
    seq = pos_rows.shape[0]
    rows = 256
    per_seq = seq // rows
    n_blk = len(blocks)
    vec = pl.BlockSpec((1, width), lambda i: (0, 0))
    return pl.pallas_call(
        functools.partial(embed_kernel, n_blk, cap),
        grid=(n_tok // rows,),
        in_specs=[pl.BlockSpec(memory_space=pltpu.SMEM)]
        + [pl.BlockSpec((cap, width), lambda i: (0, 0), pipeline_mode=pl.Buffered(1))] * n_blk
        + [pl.BlockSpec((rows, width), lambda i: (i % per_seq, 0)), vec, vec],
        out_specs=[pl.BlockSpec((rows, width), lambda i: (i, 0))] * 2,
        out_shape=[jax.ShapeDtypeStruct((n_tok, width), F32), jax.ShapeDtypeStruct((n_tok, width), BF16)],
        scratch_shapes=[pltpu.VMEM((n_blk * cap * width // 128, 128), F32), pltpu.VMEM((rows * width // 128, 128), F32)],
        name="embed_norm",
        cost_estimate=pl.CostEstimate(flops=15_000_000_000, bytes_accessed=n_tok * width * 10, transcendentals=0),
        compiler_params=pltpu.CompilerParams(vmem_limit_bytes=63 * 1024 * 1024),
    )(code, *blocks, pos_rows, gain, bias)


def pack_kernel(n_blk, code_ref, tok_ref, *refs):
    out_refs = refs[:n_blk]
    stage, image = refs[n_blk:]
    n_tok, width = tok_ref.shape
    cap = out_refs[0].shape[0]
    tiles = width // 128

    def widen(g, _):
        part = tok_ref[pl.ds(pl.multiple_of(g * WIDEN, WIDEN), WIDEN), :].astype(F32)
        to_image(part, stage, pl.multiple_of(g * WIDEN * tiles, WIDEN * tiles))
        return 0

    lax.fori_loop(0, n_tok // WIDEN, widen, 0)
    for b in range(n_blk):
        pick_rows(code_ref, b * cap, stage, image, cap, tiles)

        def narrow(g, _, b=b):
            part = from_image(image, pl.multiple_of(g * WIDEN * tiles, WIDEN * tiles), WIDEN, width)
            out_refs[b][pl.ds(pl.multiple_of(g * WIDEN, WIDEN), WIDEN), :] = part.astype(BF16)
            return 0

        lax.fori_loop(0, cap // WIDEN, narrow, 0)


def pack(code, tok, cap):
    n_tok, width = tok.shape
    n_blk = code.shape[0] // cap
    return pl.pallas_call(
        functools.partial(pack_kernel, n_blk),
        in_specs=[pl.BlockSpec(memory_space=pltpu.SMEM), pl.BlockSpec(memory_space=pltpu.VMEM)],
        out_specs=[pl.BlockSpec(memory_space=pltpu.VMEM)] * n_blk,
        out_shape=[jax.ShapeDtypeStruct((cap, width), BF16)] * n_blk,
        scratch_shapes=[pltpu.VMEM((n_tok * width // 128, 128), F32), pltpu.VMEM((cap * width // 128, 128), F32)],
        name="token_pack",
        cost_estimate=pl.CostEstimate(flops=15_000_000_000, bytes_accessed=n_tok * width * 5, transcendentals=0),
        compiler_params=pltpu.CompilerParams(vmem_limit_bytes=63 * 1024 * 1024),
    )(code, tok)


def proj_kernel(c_ref, w_ref, x_ref, b_ref, gain_ref, bias_ref, x1_ref, hid_ref):
    part = x_ref.shape[0] // 2
    for i in range(2):
        at = slice(i * part, (i + 1) * part)
        x1 = x_ref[at, :] + dot_nn(c_ref[at, :], w_ref[...].reshape(c_ref.shape[1], -1)).astype(BF16).astype(F32) + b_ref[...]
        x1_ref[at, :] = x1
        normed, _ = row_stats(x1)
        hid_ref[at, :] = (normed * gain_ref[...] + bias_ref[...]).astype(BF16)


def proj_norm(ctx, w, start, x, b, gain, bias):
    n_tok, width = x.shape
    n_row = ctx.shape[1] // w.shape[0]
    rows = 512
    vec = pl.BlockSpec((1, width), lambda i: (0, 0))
    mat = pl.BlockSpec((rows, width), lambda i: (i, 0))
    return pl.pallas_call(
        proj_kernel,
        grid=(n_tok // rows,),
        in_specs=[pl.BlockSpec((rows, ctx.shape[1]), lambda i: (i, 0)), pl.BlockSpec((w.shape[0], n_row, width), lambda i: (0, start // n_row, 0)), mat, vec, vec, vec],
        out_specs=[mat, mat],
        out_shape=[jax.ShapeDtypeStruct((n_tok, width), F32), jax.ShapeDtypeStruct((n_tok, width), BF16)],
        name="proj_norm",
        cost_estimate=pl.CostEstimate(flops=2 * n_tok * ctx.shape[1] * width, bytes_accessed=n_tok * width * 12, transcendentals=0),
        compiler_params=pltpu.CompilerParams(vmem_limit_bytes=63 * 1024 * 1024),
    )(ctx, w, x, b, gain, bias)


def ffn_kernel(part, h_ref, og_ref, wu_ref, wd_ref, b_ref, act_ref, dup_ref, db_ref):
    total = jnp.zeros(db_ref.shape, F32)
    for i in range(h_ref.shape[0] // part):
        at = slice(i * part, (i + 1) * part)
        z = dot_nt(h_ref[at, :], wu_ref[0]) + b_ref[...]
        d_act = dot_nt(og_ref[at, :], wd_ref[0])
        z2 = z * z
        gate = 0.5 * jnp.tanh(z * (GELU_S + (GELU_S * GELU_A) * z2)) + 0.5
        act = z * gate
        d_up = d_act * (gate + act * (1.0 - gate) * (2.0 * GELU_S + (6.0 * GELU_S * GELU_A) * z2))
        act_ref[at, :] = act.astype(BF16)
        dup_ref[at, :] = d_up.astype(BF16)
        total = total + col_sum(d_up)
    db_ref[...] = total


def ffn(hid, og, w, b_up, part=1024):
    n_tok, width = hid.shape
    ff = b_up.shape[1]
    n_piece = w.shape[0]
    bn = ff // n_piece
    whole = pl.BlockSpec((n_tok, width), lambda i: (0, 0), pipeline_mode=pl.Buffered(1))
    ospec = pl.BlockSpec((n_tok, bn), lambda i: (0, i))
    vec = pl.BlockSpec((1, bn), lambda i: (0, i))
    return pl.pallas_call(
        functools.partial(ffn_kernel, part),
        grid=(n_piece,),
        in_specs=[whole, whole, pl.BlockSpec((1, bn, width), lambda i: (i, 0, 0)), pl.BlockSpec((1, bn, width), lambda i: (i, 1, 0)), vec],
        out_specs=[ospec, ospec, vec],
        out_shape=[jax.ShapeDtypeStruct((n_tok, ff), BF16), jax.ShapeDtypeStruct((n_tok, ff), BF16), jax.ShapeDtypeStruct((1, ff), F32)],
        name="ffn",
        cost_estimate=pl.CostEstimate(flops=4 * n_tok * ff * width, bytes_accessed=4 * n_tok * ff + 4 * ff * width, transcendentals=n_tok * ff),
        compiler_params=pltpu.CompilerParams(vmem_limit_bytes=63 * 1024 * 1024),
    )(hid, og, w, w, b_up)


def down_kernel(n_tp, me_ref, act_ref, w_ref, x1_ref, b_ref, *out_refs):
    out = x1_ref[...] + dot_nn(act_ref[...], w_ref[...].reshape(act_ref.shape[1], -1)).astype(BF16).astype(F32) + b_ref[...]
    k = me_ref[0] ^ (pl.program_id(0) % n_tp)
    seq = pl.program_id(0) // n_tp
    for j in range(n_tp):
        @pl.when(k == j)
        def _(j=j):
            out_refs[j][seq] = out.astype(BF16)


def down(me, act, w, x1, b, n_seq, n_tp):
    n_tok, width = x1.shape
    ff = act.shape[1]
    rows = n_tok // n_seq // n_tp
    part = jax.ShapeDtypeStruct((n_seq, rows, width), BF16)
    return pl.pallas_call(
        functools.partial(down_kernel, n_tp),
        grid_spec=pltpu.PrefetchScalarGridSpec(
            num_scalar_prefetch=1, grid=(n_seq * n_tp,),
            in_specs=[pl.BlockSpec((rows, ff), lambda i, m: (i, 0)),
                      pl.BlockSpec((w.shape[0], ff // w.shape[0], width), lambda i, m: (0, 1, 0), pipeline_mode=pl.Buffered(1)),
                      pl.BlockSpec((rows, width), lambda i, m: (i, 0)), pl.BlockSpec((1, width), lambda i, m: (0, 0))],
            out_specs=[pl.BlockSpec(part.shape, lambda i, m: (0, 0, 0))] * n_tp),
        out_shape=[part] * n_tp,
        name="down",
        cost_estimate=pl.CostEstimate(flops=2 * n_tok * ff * width, bytes_accessed=2 * n_tok * ff + n_tok * width * 6, transcendentals=0),
        compiler_params=pltpu.CompilerParams(vmem_limit_bytes=63 * 1024 * 1024),
    )(me, act, w, x1, b)


def back2_kernel(dup_ref, w_ref, wout_ref, x1_ref, og_ref, gain_ref, dr_ref, da_ref, dc_ref, sums_ref):
    @pl.when(pl.program_id(0) == 0)
    def _():
        sums_ref[...] = jnp.zeros(sums_ref.shape, F32)

    n_part = 2
    part = dr_ref.shape[0] // n_part
    w = w_ref[...].reshape(dup_ref.shape[1], -1)
    d_ys = [dot_nn(dup_ref[i * part:(i + 1) * part, :], w) for i in range(n_part)]
    for i in range(n_part):
        at = slice(i * part, (i + 1) * part)
        d_y = d_ys[i].astype(BF16).astype(F32)
        d_x, d_gain = norm_back(d_y, x1_ref[at, :], gain_ref[...])
        og = og_ref[at, :].astype(F32)
        d_resid = og + d_x
        dr_ref[at, :] = d_resid
        d_attn = d_resid.astype(BF16)
        da_ref[at, :] = d_attn
        dc_ref[at, :] = dot_nt(d_attn, wout_ref[...].reshape(-1, d_attn.shape[1])).astype(BF16)
        sums_ref[0:1, :] += col_sum(d_gain)
        sums_ref[1:2, :] += col_sum(d_y)
        sums_ref[2:3, :] += col_sum(d_resid)
        sums_ref[3:4, :] += col_sum(og)


def back2(d_up, w, start, x1, og, gain):
    n_tok, width = x1.shape
    ff = d_up.shape[1]
    rows = 256
    n_out = (w.shape[1] - start)
    mat = pl.BlockSpec((rows, width), lambda i: (i, 0))
    return pl.pallas_call(
        back2_kernel,
        grid=(n_tok // rows,),
        in_specs=[pl.BlockSpec((rows, ff), lambda i: (i, 0)), pl.BlockSpec((w.shape[0], ff // w.shape[0], width), lambda i: (0, 0, 0), pipeline_mode=pl.Buffered(1)),
                  pl.BlockSpec((w.shape[0], n_out, width), lambda i: (0, start // n_out, 0), pipeline_mode=pl.Buffered(1)),
                  mat, mat, pl.BlockSpec((1, width), lambda i: (0, 0))],
        out_specs=[mat, mat, pl.BlockSpec((rows, w.shape[0] * n_out), lambda i: (i, 0)), pl.BlockSpec((8, width), lambda i: (0, 0))],
        out_shape=[jax.ShapeDtypeStruct((n_tok, width), F32), jax.ShapeDtypeStruct((n_tok, width), BF16),
                   jax.ShapeDtypeStruct((n_tok, w.shape[0] * n_out), BF16), jax.ShapeDtypeStruct((8, width), F32)],
        name="ffn_back",
        cost_estimate=pl.CostEstimate(flops=2 * n_tok * ff * width, bytes_accessed=2 * n_tok * ff + n_tok * width * 12, transcendentals=0),
        compiler_params=pltpu.CompilerParams(vmem_limit_bytes=63 * 1024 * 1024),
    )(d_up, w, w, x1, og, gain)


def back1_kernel(dq_ref, w_ref, x_ref, dr_ref, gain_ref, *refs):
    tok_ref, pos_ref, sums_ref, bsum_ref = refs[-4:]
    before_refs = refs[:-4]

    @pl.when(pl.program_id(0) == 0)
    def _():
        sums_ref[...] = before_refs[1][...] if before_refs else jnp.zeros(sums_ref.shape, F32)
        bsum_ref[...] = before_refs[2][...] if before_refs else jnp.zeros(bsum_ref.shape, F32)

    n_part = 2
    part = tok_ref.shape[0] // n_part
    d_ys = [dot_nn(dq_ref[i * part:(i + 1) * part, :], w_ref[...]) for i in range(n_part)]
    for i in range(n_part):
        at = slice(i * part, (i + 1) * part)
        d_y = d_ys[i].astype(BF16).astype(F32)
        d_x, d_gain = norm_back(d_y, x_ref[at, :], gain_ref[...])
        d_resid = dr_ref[at, :] + d_x
        tok_ref[at, :] = d_resid.astype(BF16)
        pos_ref[at, :] = before_refs[0][at, :] + d_resid if before_refs else d_resid
        sums_ref[0:1, :] += col_sum(d_gain)
        sums_ref[1:2, :] += col_sum(d_y)
        bsum_ref[0:1, :] += col_sum(dq_ref[at, :].astype(F32))


def back1(d_qkv, w_qkv, x, d_resid1, gain, at, pos_rows, earlier=None):
    seq, n_cols = d_qkv.shape
    width = x.shape[1]
    rows = 256
    steps = seq // rows
    mat = pl.BlockSpec((rows, width), lambda i: (at * steps + i, 0))
    out = pl.BlockSpec((rows, width), lambda i: (i, 0))
    few = [pl.BlockSpec((8, width), lambda i: (0, 0)), pl.BlockSpec((8, n_cols), lambda i: (0, 0))]
    return pl.pallas_call(
        back1_kernel,
        grid=(steps,),
        in_specs=[pl.BlockSpec((rows, n_cols), lambda i: (i, 0)),
                  pl.BlockSpec((n_cols, width), lambda i: (0, 0), pipeline_mode=pl.Buffered(1)),
                  mat, mat, pl.BlockSpec((1, width), lambda i: (0, 0))] + ([out] + few if earlier else []),
        out_specs=[out, out] + few,
        out_shape=[jax.ShapeDtypeStruct((seq, width), BF16), jax.ShapeDtypeStruct((pos_rows, width), F32),
                   jax.ShapeDtypeStruct((8, width), F32), jax.ShapeDtypeStruct((8, n_cols), F32)],
        name="qkv_back",
        cost_estimate=pl.CostEstimate(flops=2 * seq * n_cols * width, bytes_accessed=2 * seq * n_cols + seq * width * 12, transcendentals=0),
        compiler_params=pltpu.CompilerParams(vmem_limit_bytes=63 * 1024 * 1024),
    )(d_qkv, w_qkv, x, d_resid1, gain, *(earlier or ()))


def pieces_out_kernel(n_in, spans, me_ref, *refs):
    out_refs = refs[n_in:]
    for p in range(n_in):
        @pl.when(pl.program_id(0) == p)
        def _(p=p):
            for (start, n, turned), out_ref in zip(spans, out_refs):
                part = refs[p][start:start + n, :]
                out_ref[...] = part.T if turned else part


def pieces_out(me, pieces, spans):
    rows, width = pieces[0].shape
    n_in = len(pieces)

    def place(p, m):
        return (m[1] ^ (p // 2)) * 2 + (m[0] ^ (p % 2))

    out_specs, out_shape = [], []
    for start, n, turned in spans:
        if turned:
            out_specs.append(pl.BlockSpec((width, n), lambda p, m: (0, place(p, m))))
            out_shape.append(jax.ShapeDtypeStruct((width, n_in * n), F32))
        else:
            out_specs.append(pl.BlockSpec((n, width), lambda p, m: (place(p, m), 0)))
            out_shape.append(jax.ShapeDtypeStruct((n_in * n, width), F32))
    return pl.pallas_call(
        functools.partial(pieces_out_kernel, n_in, spans),
        grid_spec=pltpu.PrefetchScalarGridSpec(
            num_scalar_prefetch=1, grid=(n_in,),
            in_specs=[pl.BlockSpec((rows, width), lambda p, m: (0, 0), pipeline_mode=pl.Buffered(1))] * n_in,
            out_specs=out_specs),
        out_shape=out_shape,
        name="grads_out",
        cost_estimate=pl.CostEstimate(flops=8_000_000_000, bytes_accessed=n_in * rows * width * 8, transcendentals=0),
        compiler_params=pltpu.CompilerParams(vmem_limit_bytes=63 * 1024 * 1024),
    )(me, *pieces)


def assemble_kernel(n, me_ref, *refs):
    out_ref = refs[n]
    k = me_ref[0] ^ pl.program_id(0)
    for j in range(n):
        @pl.when(k == j)
        def _(j=j):
            out_ref[...] = refs[j][...].reshape(out_ref.shape)


def assemble(me, parts, out_shape, block):
    at = 1 if len(out_shape) == 4 else 0
    return pl.pallas_call(
        functools.partial(assemble_kernel, len(parts)),
        grid_spec=pltpu.PrefetchScalarGridSpec(
            num_scalar_prefetch=1, grid=(len(parts),),
            in_specs=[pl.BlockSpec(p.shape, lambda i, m: (0, 0, 0), pipeline_mode=pl.Buffered(1)) for p in parts],
            out_specs=pl.BlockSpec(block, lambda i, m: tuple(i if d == at else 0 for d in range(len(block))))),
        out_shape=jax.ShapeDtypeStruct(out_shape, parts[0].dtype),
        name="assemble",
        cost_estimate=pl.CostEstimate(flops=4_000_000_000, bytes_accessed=16 * MIB, transcendentals=0),
        compiler_params=pltpu.CompilerParams(vmem_limit_bytes=63 * 1024 * 1024),
    )(me, *parts)


LANES = 128


def accum_kernel(n_block, cap, sub_rows, width, where_ref, first_ref, *refs):
    tok_refs = refs[:n_block]
    out_ref = refs[n_block]
    n_sub = len(sub_rows)
    acc = refs[n_block + 1:n_block + 1 + n_sub]
    buf, stage, in_sem, out_sem = refs[n_block + 1 + n_sub:]
    tiles = width // LANES
    group = 8 * tiles

    def fetch(block, n):
        return pltpu.make_async_copy(tok_refs[n], buf.at[block % 2], in_sem.at[block % 2])

    def fetch_next(block):
        for n in range(n_block):
            @pl.when(block == n)
            def _(n=n):
                fetch(block, n).start()

    fetch_next(0)
    for s in range(n_sub):
        def clear(i, _, s=s):
            acc[s][pl.ds(pl.multiple_of(i * group, group), group), :] = jnp.zeros((group, LANES), F32)
            return 0

        lax.fori_loop(0, sub_rows[s] // 8, clear, 0)

    def add_rows(s, slot, n):
        codes = [where_ref[slot + j] for j in range(n)]
        at = [code >> 16 for code in codes]
        rows = [stage[pl.ds(code & 0xffff, tiles, stride=8), :] for code in codes]
        sums = [acc[s][pl.ds(a, tiles, stride=8), :] for a in at]
        for j in range(n):
            for i in range(j):
                sums[j] = jnp.where(at[i] == at[j], sums[i], sums[j])
            sums[j] = sums[j] + rows[j]
        for j in range(n):
            acc[s][pl.ds(at[j], tiles, stride=8), :] = sums[j]

    def add_block(block, _):
        fetch_next(block + 1)
        fetch(block, 0).wait()

        def widen(g, _):
            rows = buf[block % 2, pl.ds(pl.multiple_of(g * WIDEN, WIDEN), WIDEN), :].astype(F32)
            base = pl.multiple_of(g * (WIDEN // 8) * group, (WIDEN // 8) * group)
            for h in range(WIDEN // 8):
                for c in range(tiles):
                    stage[pl.ds(base + h * group + c * 8, 8), :] = rows[h * 8:(h + 1) * 8, c * LANES:(c + 1) * LANES]
            return 0

        lax.fori_loop(0, cap // WIDEN, widen, 0)

        starts = [first_ref[block * (n_sub + 1) + s] for s in range(n_sub + 1)]
        counts = [starts[s + 1] - starts[s] for s in range(n_sub)]
        both = functools.reduce(jnp.minimum, counts) // 2
        begin = [block * cap + starts[s] for s in range(n_sub)]

        def together(i, _):
            for s in range(n_sub):
                add_rows(s, begin[s] + 2 * i, 2)
            return 0

        lax.fori_loop(0, both, together, 0)
        for s in range(n_sub):
            fours = (counts[s] - 2 * both) // 4

            def alone(i, _, s=s):
                add_rows(s, begin[s] + 2 * both + 4 * i, 4)
                return 0

            lax.fori_loop(0, fours, alone, 0)

            def single(i, _, s=s):
                add_rows(s, begin[s] + i, 1)
                return 0

            lax.fori_loop(2 * both + 4 * fours, counts[s], single, 0)
        return 0

    lax.fori_loop(0, n_block, add_block, 0)
    done = 0
    copies = []
    for s in range(n_sub):
        n = sub_rows[s] * tiles
        copies.append(pltpu.make_async_copy(acc[s], out_ref.at[pl.ds(done, n), :], out_sem.at[s]))
        copies[-1].start()
        done += n
    for c in copies:
        c.wait()


def accum(tok_blocks, code, first, sub_rows, width):
    n_block = len(tok_blocks)
    cap = tok_blocks[0].shape[0]
    n_sub = len(sub_rows)
    tiles = width // LANES
    return pl.pallas_call(
        functools.partial(accum_kernel, n_block, cap, sub_rows, width),
        in_specs=[pl.BlockSpec(memory_space=pltpu.SMEM), pl.BlockSpec(memory_space=pltpu.SMEM)]
        + [pl.BlockSpec(memory_space=pl.ANY)] * n_block,
        out_specs=pl.BlockSpec(memory_space=pl.ANY),
        out_shape=jax.ShapeDtypeStruct((sum(sub_rows) * tiles, LANES), F32),
        scratch_shapes=[pltpu.VMEM((r * tiles, LANES), F32) for r in sub_rows]
        + [pltpu.VMEM((2, cap, width), BF16), pltpu.VMEM((cap * tiles, LANES), F32),
           pltpu.SemaphoreType.DMA((2,)), pltpu.SemaphoreType.DMA((n_sub,))],
        name="table_accum",
        cost_estimate=pl.CostEstimate(flops=50_000_000_000, bytes_accessed=100_000_000, transcendentals=0),
        compiler_params=pltpu.CompilerParams(vmem_limit_bytes=63 * 1024 * 1024),
    )(code, first, *tok_blocks)


def dot_tn(a, b):
    return lax.dot_general(a, b, (((0,), (0,)), ((), ())), preferred_element_type=F32)


def grad_kernel(has_plus, core_ref, a_ref, b_ref, *refs):
    out_ref = refs[-1]
    piece, width = out_ref.shape[2:]
    half = a_ref.shape[1] // 2
    g = dot_tn(a_ref[...], b_ref[...])
    for x in range(2):
        part = g[x * half:(x + 1) * half]
        out_ref[x, 0, 0:half, :] = part + refs[0][x * piece:x * piece + half, :] if has_plus else part
        if piece > half:
            out_ref[x, 0, half:, :] = jnp.zeros((piece - half, width), F32)


def grad_pieces(core, a, b, n_tp, piece, which, n_which, plus=None, into=None):
    n_tok, n_cols = a.shape
    width = b.shape[1]
    out_spec = pl.BlockSpec((2, 1, piece, width), lambda t, c: (t, which, 0, 0))
    in_specs = [pl.BlockSpec((n_tok, n_cols // (2 * n_tp)), lambda t, c: (0, 2 * t + c[0])),
                pl.BlockSpec((n_tok, width), lambda t, c: (0, 0), pipeline_mode=pl.Buffered(1))]
    args = [a, b]
    if plus is not None:
        in_specs.append(pl.BlockSpec((2 * piece, width), lambda t, c: (t, 0)))
        args.append(plus)
    shape = (2 * n_tp, n_which, piece, width)
    if into is not None:
        in_specs.append(pl.BlockSpec(memory_space=pl.ANY))
        args.append(into.reshape(shape))
    return pl.pallas_call(
        functools.partial(grad_kernel, plus is not None),
        grid_spec=pltpu.PrefetchScalarGridSpec(num_scalar_prefetch=1, grid=(n_tp,), in_specs=in_specs, out_specs=out_spec),
        out_shape=jax.ShapeDtypeStruct(shape, F32),
        input_output_aliases={} if into is None else {len(args): 0},
        name="weight_grad",
        cost_estimate=pl.CostEstimate(flops=n_tok * n_cols * width, bytes_accessed=n_tok * (n_cols + 2 * width) + 2 * n_cols * width,
                                      transcendentals=0),
        compiler_params=pltpu.CompilerParams(vmem_limit_bytes=63 * 1024 * 1024),
    )(core, *args).reshape(-1, width)


def grad_rest_kernel(spans, last, n_a2, core_ref, a1_ref, b1_ref, b2_ref, *refs):
    a2_refs, refs, out_ref = refs[:n_a2], refs[n_a2:-1], refs[-1]
    plus = refs[0] if refs else None
    piece, piece_in = out_ref.shape[0] // 2, (plus.shape[0] // 2 if refs else 0)
    rows = b2_ref.shape[0] // n_a2
    for which, (start, stop) in enumerate(spans):
        half = (a2_refs[0] if which else a1_ref).shape[1] // 2
        for i in range(0, 2 * half, 128):
            cols = slice(i, i + 128)
            if which:
                g = sum(dot_tn(a_ref[:, cols], b2_ref[n * rows:(n + 1) * rows, :]) for n, a_ref in enumerate(a2_refs))
            else:
                g = dot_tn(a1_ref[:, cols], b1_ref[...])
            for x in range(2):
                lo, hi = max(i, x * half), min(i + 128, (x + 1) * half)
                if lo < hi:
                    to = lo - x * half + start
                    part = g[lo - i:hi - i]
                    if plus is not None:
                        part = part + plus[x * piece_in + to:x * piece_in + to + hi - lo, :]
                    out_ref[x * piece + to:x * piece + to + hi - lo, :] = part
        for x in range(2):
            if stop > start + half:
                out_ref[x * piece + start + half:x * piece + stop, :] = jnp.zeros((stop - start - half, out_ref.shape[1]), F32)
    if last:
        for x in range(2):
            out_ref[x * piece + spans[-1][1]:(x + 1) * piece, :] = refs[1][x, 0] + refs[2][x * last:(x + 1) * last, :]


def grad_rest(core, a1, b1, a2, b2, n_tp, spans, plus=None, tail=None):
    n_tok, width = b1.shape
    last = tail[0].shape[2] if tail else 0
    piece = spans[-1][1] + last
    whole = pl.BlockSpec((n_tok, width), lambda t, c: (0, 0), pipeline_mode=pl.Buffered(1))
    cols = [pl.BlockSpec((a.shape[0], a.shape[1] // (2 * n_tp)), lambda t, c: (0, 2 * t + c[0])) for a in (a1, *a2)]
    in_specs, args = [cols[0], whole, whole] + cols[1:], [a1, b1, b2, *a2]
    if plus is not None:
        in_specs.append(pl.BlockSpec((plus.shape[0] // n_tp, width), lambda t, c: (t, 0)))
        args.append(plus)
    if tail:
        in_specs.append(pl.BlockSpec((2, 1, last, width), lambda t, c: (t, c[0], 0, 0)))
        in_specs.append(pl.BlockSpec((2 * last, width), lambda t, c: (t, 0)))
        args += tail
    n_cols = a1.shape[1] + a2[0].shape[1]
    return pl.pallas_call(
        functools.partial(grad_rest_kernel, spans, last, len(a2)),
        grid_spec=pltpu.PrefetchScalarGridSpec(num_scalar_prefetch=1, grid=(n_tp,), in_specs=in_specs,
                                               out_specs=pl.BlockSpec((2 * piece, width), lambda t, c: (t, 0))),
        out_shape=jax.ShapeDtypeStruct((2 * n_tp * piece, width), F32),
        name="weight_grads",
        cost_estimate=pl.CostEstimate(flops=n_tok * n_cols * width, bytes_accessed=n_tok * (n_cols + 4 * width) + 2 * n_cols * width,
                                      transcendentals=0),
        compiler_params=pltpu.CompilerParams(vmem_limit_bytes=63 * 1024 * 1024),
    )(core, *args)


POS_OFFSET = 2
SLOTS = 704
GRAD_SLOTS = 384
LOW = 32


def before(n):
    return (lax.broadcasted_iota(jnp.int32, (n, n), 1) < lax.broadcasted_iota(jnp.int32, (n, n), 0)).astype(BF16)


def rank_in_class(hot):
    n_blk, n_tok, n_cls = hot.shape
    ones = hot.astype(BF16).reshape(n_blk, n_tok // 128, 128, n_cls)
    within = jnp.einsum("ij,bnjk->bnik", before(128), ones, preferred_element_type=F32)
    sums = jnp.sum(ones.astype(F32), axis=2)
    ahead = jnp.einsum("mn,bnk->bmk", before(n_tok // 128), sums.astype(BF16), preferred_element_type=F32)
    rank = jnp.sum((within + ahead[:, :, None, :]) * ones.astype(F32), axis=3)
    return rank.reshape(n_blk, n_tok).astype(jnp.int32), jnp.sum(sums, axis=1).astype(jnp.int32)


def compact(rank, valid, value, slots):
    n_high = slots // LOW
    high = ((rank // LOW)[:, :, None] == jnp.arange(n_high)) & valid[:, :, None]
    low = ((rank % LOW)[:, :, None] == jnp.arange(LOW)).astype(F32)
    parts = jnp.concatenate([low * (value // 128).astype(F32)[:, :, None], low * (value % 128).astype(F32)[:, :, None]], axis=2)
    out = jnp.einsum("bjh,bjl->bhl", high.astype(BF16), parts.astype(BF16), preferred_element_type=F32).astype(jnp.int32)
    return (out[:, :, :LOW] * 128 + out[:, :, LOW:]).reshape(rank.shape[0], slots)


def solution(mesh):
    n_tp, n_dp = mesh.shape["tp"], mesh.shape["dp"]
    n_core = 2
    n_x = n_dp // n_core
    mesh3 = Mesh(mesh.devices.reshape(n_tp, n_x, n_core), ("tp", "xx", "cc"))
    dp = ("xx", "cc")
    tp_swap = [[(i, i ^ k) for i in range(n_tp)] for k in range(n_tp)]
    pair = [(0, 1), (1, 0)]

    def local_step(tok_ids, emb_table, pos_table, ln1_gain, ln1_bias, w_qkv, b_qkv, w_out, b_out,
                   ln2_gain, ln2_bias, w_up, b_up, w_down, b_down, out_grad):
        tp_index, x_index, c_index = lax.axis_index("tp"), lax.axis_index("xx"), lax.axis_index("cc")
        dp_index = x_index * n_core + c_index
        n_seq_dp, seq = tok_ids.shape
        n_seq = n_seq_dp // n_tp
        n_tok = n_seq * seq
        rows, width = emb_table.shape
        n_sub = 4
        sub = -(-rows // n_sub // 8) * 8
        sub_rows = (sub,) * (n_sub - 1) + (rows - (n_sub - 1) * sub,)
        seq_local = seq // n_tp
        ff = w_up.shape[1]
        gain1, bias1 = ln1_gain.astype(F32)[None], ln1_bias.astype(F32)[None]
        gain2, bias2 = ln2_gain.astype(F32)[None], ln2_bias.astype(F32)[None]

        def half(w, axis):
            n = w.shape[axis] // n_core
            return lax.dynamic_slice_in_dim(w, c_index * n, n, axis)

        def gather_rows(w):
            return lax.all_gather(w, ("tp", "cc"), axis=0, tiled=True)

        def swap(v, axis, k=1):
            return lax.ppermute(v, axis, tp_swap[k] if axis == "tp" else pair)

        def by_owner(parts):
            out = []
            for p in range(n_tp):
                k = tp_index ^ p
                out.append(jnp.where(k < 2, jnp.where(k == 0, parts[0], parts[1]), jnp.where(k == 2, parts[2], parts[3])))
            return out

        ids_all = lax.all_gather(tok_ids, dp, axis=0, tiled=True)
        ids_all, w_up, w_down, w_out, b_qkv, b_up = lax.optimization_barrier((ids_all, w_up, w_down, w_out, b_qkv, b_up))

        wqkv_t = gather_rows(jnp.transpose(half(w_qkv, 2), (1, 2, 3, 0)).reshape(-1, width))
        n_ff, n_out = ff // n_dp, w_out.shape[0] * w_out.shape[1] // n_dp

        def quarter(w, axis):
            n = w.shape[axis] // n_dp
            return lax.dynamic_slice_in_dim(w, dp_index * n, n, axis)

        own_w = jnp.concatenate([quarter(w_up, 1).T, quarter(w_down, 0), quarter(w_out.reshape(-1, width), 0)])
        w_all = lax.all_gather(own_w, ("tp", "xx", "cc"), axis=0, tiled=True)
        w_all = w_all.reshape(n_tp * n_dp, 2 * n_ff + n_out, width)
        n_pair = wqkv_t.shape[0] // (3 * 128)
        own_bias = jnp.concatenate([b_qkv.reshape(3, n_core, -1, b_qkv.shape[2]).transpose(1, 0, 2, 3).reshape(-1), b_up])
        biases = jnp.stack(by_owner([swap(own_bias, "tp", k) if k else own_bias for k in range(n_tp)]))
        bqkv_w = biases[:, :-ff].reshape(-1).astype(F32)
        bup_w = biases[:, -ff:].reshape(1, -1).astype(F32)
        pos_rows = lax.slice_in_dim(pos_table, POS_OFFSET, POS_OFFSET + seq, axis=0)

        local = ids_all - tp_index * rows
        sub_of = sum(((local >= s * sub).astype(jnp.int32) for s in range(1, n_sub)), jnp.zeros_like(local))
        owned = (local >= 0) & (local < rows)
        hot = owned[:, :, None] & (sub_of[:, :, None] == jnp.arange(n_sub))
        rank, counts = rank_in_class(hot)
        first = jnp.concatenate([jnp.zeros_like(counts[:, :1]), jnp.cumsum(counts, axis=1)], axis=1)
        rank = rank + jnp.sum(jnp.where(hot, first[:, None, :-1], 0), axis=2)
        owner_counts = jnp.stack([jnp.sum(((ids_all >= o * rows) & (ids_all < (o + 1) * rows)).astype(jnp.int32), axis=1)
                                  for o in range(n_tp)])
        grad_rounds = (jnp.max(owner_counts) + GRAD_SLOTS - 1) // GRAD_SLOTS
        rounds = (jnp.max(jnp.sum(owner_counts.reshape(n_tp, -1, n_seq), axis=2)) + SLOTS - 1) // SLOTS

        def after_first(ranks, totals):
            return (ranks + (jnp.cumsum(totals, axis=1) - totals)[:, :, None]).reshape(ranks.shape[0], -1)

        def grad_lists(r):
            at = rank - r * GRAD_SLOTS
            return compact(at, owned & (at >= 0) & (at < GRAD_SLOTS), jnp.where(owned, local, 0), GRAD_SLOTS)

        my_rank = lax.dynamic_slice_in_dim(rank, dp_index * n_seq_dp, n_seq_dp, 0)
        my_total = lax.dynamic_slice_in_dim(first[:, -1], dp_index * n_seq_dp, n_seq_dp, 0)
        my_rank = after_first(my_rank.reshape(n_tp, n_seq, seq), my_total.reshape(n_tp, n_seq))
        my_owned = lax.dynamic_slice_in_dim(owned, dp_index * n_seq_dp, n_seq_dp, 0).reshape(n_tp, n_tok)
        my_local = lax.dynamic_slice_in_dim(local, dp_index * n_seq_dp, n_seq_dp, 0).reshape(n_tp, n_tok)

        def lists(r):
            at = my_rank - r * SLOTS
            return compact(at, my_owned & (at >= 0) & (at < SLOTS), jnp.where(my_owned, my_local, 0), SLOTS)

        own_ids = lax.dynamic_slice_in_dim(ids_all, dp_index * n_seq_dp + tp_index * n_seq, n_seq, 0)
        own_owner = sum(((own_ids >= o * rows).astype(jnp.int32) for o in range(1, n_tp)), jnp.zeros_like(own_ids))
        own_local = own_ids - own_owner * rows
        own_sub = sum(((own_local >= s * sub).astype(jnp.int32) for s in range(1, n_sub)), jnp.zeros_like(own_ids))
        own_hot = (own_owner * n_sub + own_sub)[:, :, None] == jnp.arange(n_tp * n_sub)
        own_rank, own_counts = rank_in_class(own_hot)
        own_counts = own_counts.reshape(n_seq, n_tp, n_sub)
        own_first = jnp.cumsum(own_counts, axis=2) - own_counts
        own_rank = own_rank + jnp.sum(jnp.where(own_hot, own_first.reshape(n_seq, 1, -1), 0), axis=2)
        own_total = jnp.sum(own_counts, axis=2)
        own_shift = jnp.cumsum(own_total, axis=0) - own_total
        own_place = sum(jnp.where(own_owner == o, own_shift[:, o:o + 1], 0) for o in range(n_tp))
        own_place = (own_place + own_rank).reshape(-1)

        def own_lists(r, b):
            at = jnp.broadcast_to(own_rank[b] - r * GRAD_SLOTS, (n_tp, seq))
            mine = own_owner[b] == jnp.arange(n_tp)[:, None]
            return compact(at, mine & (at >= 0) & (at < GRAD_SLOTS), jnp.broadcast_to(jnp.arange(seq), (n_tp, seq)), GRAD_SLOTS)

        tiles = width // 128

        def own_places(r, b):
            own = own_lists(r, b)
            place = jnp.concatenate([lax.dynamic_index_in_dim(own, tp_index ^ k, 0, keepdims=False) for k in range(n_tp)])
            return (place // 8) * (8 * tiles) + place % 8

        places0 = [own_places(0, b) for b in range(n_seq)]

        def in_block_order(table, b):
            out = []
            for dc in range(n_core):
                for dx in range(n_x):
                    for k in range(n_tp):
                        d = (x_index ^ dx) * n_core + (c_index ^ dc)
                        out.append(lax.dynamic_index_in_dim(table, (d * n_tp + (tp_index ^ k)) * n_seq + b, 0, keepdims=False))
            return out

        def both_orders(table):
            return jnp.stack(in_block_order(table, 0) + in_block_order(table, 1))

        block_rows = both_orders(grad_lists(0))
        in_sub = sum(((block_rows >= s * sub).astype(jnp.int32) for s in range(1, n_sub)), jnp.zeros_like(block_rows))
        in_sub = block_rows - in_sub * sub
        slot = jnp.arange(GRAD_SLOTS)
        code = (((in_sub // 8) * (8 * tiles) + in_sub % 8) << 16) | ((slot // 8) * (8 * tiles) + slot % 8)
        code = code.reshape(-1)
        block_first = jnp.minimum(both_orders(first), GRAD_SLOTS).reshape(-1)

        def rows_here(r, my_lists):
            index = [lax.dynamic_index_in_dim(my_lists, tp_index ^ k, 0, keepdims=False) for k in range(n_tp)]
            first_two = jnp.take(emb_table, jnp.concatenate([index[3], index[1]]), axis=0, mode="clip")
            rest, first_two = lax.optimization_barrier((jnp.concatenate([index[2], index[0]]), first_two))
            last_two = jnp.take(emb_table, rest, axis=0, mode="clip")
            sent = [last_two[SLOTS:], first_two[SLOTS:], last_two[:SLOTS], first_two[:SLOTS]]
            got = list(sent)
            for k in range(1, n_tp):
                got[k] = swap(sent[k], "tp", k)
            at = own_place - r * SLOTS
            valid = (at >= 0) & (at < SLOTS)
            return got, jnp.where(valid, (own_owner.reshape(-1) ^ tp_index) * SLOTS + at, 0), valid

        def norm_rows(x):
            normed, _ = row_stats(x)
            return (normed * gain1 + bias1).astype(BF16)

        got0, place0, _ = rows_here(0, lists(0))
        code0 = (place0 // 8) * (8 * tiles) + place0 % 8
        og_parts = out_grad.reshape(n_tp, n_seq, seq_local, width)
        og_parts = [lax.dynamic_index_in_dim(og_parts, tp_index ^ k, 0, keepdims=False) for k in range(n_tp)]
        resid_x, hid1 = embed(code0, got0, pos_rows, gain1, bias1, n_tok)

        def more_rows(carry):
            r, x, _ = carry
            got, place, valid = rows_here(r, lists(r))
            new = jnp.take(jnp.concatenate(got), place, axis=0, mode="clip").astype(F32) + jnp.tile(pos_rows.astype(F32), (n_seq, 1))
            x = jnp.where(valid[:, None], new, x)
            return r + 1, x, norm_rows(x)

        _, resid_x, hid1 = lax.while_loop(lambda c: c[0] < rounds, more_rows, (jnp.int32(1), resid_x, hid1))

        parts = [swap(part, "tp", k) if k else part for k, part in enumerate(og_parts)]
        me = jnp.reshape(tp_index, (1,))
        og = assemble(me, parts, (n_seq, n_tp, seq_local, width), (n_seq, 1, seq_local, width)).reshape(n_tok, width)

        qkv = (dot_nt(hid1, wqkv_t) + bqkv_w).astype(BF16)
        ctx, lse = attn_fwd(qkv, n_seq, seq, n_pair)
        resid_x1, hid2 = proj_norm(ctx, w_all, 2 * n_ff, resid_x, b_out.astype(F32)[None], gain2, bias2)
        act, d_up, d_b_up = ffn(hid2, og, w_all, bup_w)
        parts = down(me, act, w_all, resid_x1, b_down.astype(F32)[None], n_seq, n_tp)
        parts = [swap(part, "tp", k) if k else part for k, part in enumerate(parts)]
        layer_out = assemble(me, parts, (n_seq_dp, seq_local, width), (n_seq, seq_local, width))

        core = jnp.reshape(c_index, (1,))

        def piece_of(n_rows):
            return -(-n_rows // (4 * n_tp) // 24) * 24

        def every_piece(g):
            other = swap(g, "xx")
            return [g, other, swap(g, "cc"), swap(other, "cc")]

        x_and_core = jnp.stack([x_index, c_index])

        p_ff = piece_of(n_tp * ff)
        down_theirs = swap(grad_pieces(1 - core, act, og, n_tp, p_ff, 0, 1), "cc")
        up_theirs = swap(grad_pieces(1 - core, d_up, hid2, n_tp, p_ff, 0, 1), "cc")
        d_down = grad_pieces(core, act, og, n_tp, p_ff, 0, 1, plus=down_theirs)
        d_down = lax.psum_scatter(d_down, ("tp", "xx"), scatter_dimension=0, tiled=True)
        d_upw = grad_pieces(core, d_up, hid2, n_tp, p_ff, 0, 1, plus=up_theirs)
        d_upw = lax.psum_scatter(d_upw, ("tp", "xx"), scatter_dimension=0, tiled=True)
        d_down, d_upw = every_piece(d_down), every_piece(d_upw)

        d_resid1, d_attn, d_ctx, sums2 = back2(d_up, w_all, 2 * n_ff, resid_x1, og, gain2)
        n_small = n_tp * (b_qkv.size + ff) // width + 6
        p_pos = -(-(seq + n_small) // (24 * n_tp * n_dp)) * 24
        p_out = piece_of(ctx.shape[1])
        spans = ((0, p_out), (p_out, p_out + piece_of(wqkv_t.shape[0])))

        def token_blocks(places, d_tok):
            parts = pack(places, d_tok, GRAD_SLOTS)
            blocks = [swap(part, "tp", k) if k else part for k, part in enumerate(parts)]
            other = []
            for block in blocks:
                other.append(swap(block, "xx"))
            return blocks + other + [swap(block, "cc") for block in blocks + other]

        d_qkv0 = attn_bwd(qkv, ctx, d_ctx, lse, 0, seq, n_pair)
        d_tok0, *sums0 = back1(d_qkv0, wqkv_t, resid_x, d_resid1, gain1, 0, p_pos * n_tp * n_dp)
        blocks0 = token_blocks(places0[0], d_tok0)
        d_qkv1 = attn_bwd(qkv, ctx, d_ctx, lse, 1, seq, n_pair)
        d_tok1, pos_all, sums1, sums_qkv = back1(d_qkv1, wqkv_t, resid_x, d_resid1, gain1, 1, p_pos * n_tp * n_dp, earlier=sums0)
        blocks1 = token_blocks(places0[1], d_tok1)
        d_qkvs = [d_qkv0, d_qkv1]
        rest_theirs = swap(grad_rest(1 - core, ctx, d_attn, d_qkvs, hid1, n_tp, spans), "cc")

        (d_w_down,) = pieces_out(x_and_core, d_down, ((0, n_ff, False),))
        (d_w_up,) = pieces_out(x_and_core, d_upw, ((0, n_ff, True),))
        image = accum(blocks0 + blocks1, code, block_first, sub_rows, width)
        d_emb = image.reshape(rows // 8, tiles, 8, 128).transpose(0, 2, 1, 3).reshape(rows, width)

        def more_grads(carry):
            r, table = carry
            at = rank - r * GRAD_SLOTS
            there = owned & (at >= 0) & (at < GRAD_SLOTS)
            dest = compact(at, there, jnp.where(owned, local, 0) + 1, GRAD_SLOTS)
            dest = jnp.where(dest == 0, rows, dest - 1)
            grads = jnp.concatenate(token_blocks(own_places(r, 0), d_tok0) + token_blocks(own_places(r, 1), d_tok1), axis=0).astype(F32)
            return r + 1, table.at[both_orders(dest).reshape(-1)].add(grads, mode="drop")

        _, d_emb = lax.while_loop(lambda c: c[0] < grad_rounds, more_grads, (jnp.int32(1), d_emb))

        small = jnp.concatenate([sums_qkv[0], d_b_up[0], sums1[:2].reshape(-1), sums2[:4].reshape(-1)]).reshape(-1, width)
        small = jnp.concatenate([small, jnp.zeros((pos_all.shape[0] - seq - n_small, width), F32)])
        pos_all = lax.dynamic_update_slice_in_dim(pos_all, small, seq, 0).reshape(n_tp * n_x, n_core, p_pos, width)
        pos_theirs = swap(lax.dynamic_index_in_dim(pos_all, 1 - c_index, 1, keepdims=False).reshape(-1, width), "cc")
        pos_both = lax.dynamic_index_in_dim(pos_all, c_index, 1, keepdims=False).reshape(-1, width) + pos_theirs
        pos_both = lax.psum_scatter(pos_both, ("tp", "xx"), scatter_dimension=0, tiled=True)
        rest = grad_rest(core, ctx, d_attn, d_qkvs, hid1, n_tp, spans, plus=rest_theirs)
        rest = lax.psum_scatter(rest, ("tp", "xx"), scatter_dimension=0, tiled=True)
        rest_w = every_piece(rest)
        whole = lax.all_gather(pos_both, ("tp", "xx", "cc"), axis=0, tiled=True)
        d_pos = jnp.pad(whole[:seq], ((POS_OFFSET, pos_table.shape[0] - seq - POS_OFFSET), (0, 0)))
        small = whole[seq:seq + n_small].reshape(-1)
        n_b = b_qkv.size
        d_b_qkv = lax.dynamic_slice_in_dim(small, tp_index * n_b, n_b).reshape(n_core, 3, -1, b_qkv.shape[2])
        d_b_qkv = d_b_qkv.transpose(1, 0, 2, 3).reshape(b_qkv.shape)
        d_b_up = lax.dynamic_slice_in_dim(small, n_tp * n_b + tp_index * ff, ff)
        d_gain1, d_bias1, d_gain2, d_bias2, d_b_out, d_b_down = small[n_tp * (n_b + ff):].reshape(6, width)

        d_w_out, d_w_qkv = pieces_out(x_and_core, rest_w, ((0, n_out, False), (p_out, n_b // n_dp, False)))
        d_w_out = d_w_out.reshape(w_out.shape)
        d_w_qkv = d_w_qkv.reshape(n_core, 3, -1, w_qkv.shape[3], width).transpose(4, 1, 0, 2, 3).reshape(w_qkv.shape)
        return (layer_out, d_emb, d_pos, d_gain1, d_bias1, d_w_qkv, d_b_qkv, d_w_out,
                d_b_out, d_gain2, d_bias2, d_w_up, d_b_up, d_w_down, d_b_down)

    rep = P()
    in_specs = (P(dp, None), P("tp", None), rep, rep, rep,
                P(None, None, "tp", None), P(None, "tp", None), P("tp", None, None), rep,
                rep, rep, P(None, "tp"), P("tp"), P("tp", None), rep,
                P(dp, "tp", None))
    out_specs = (P(dp, "tp", None), P("tp", None), rep, rep, rep,
                 P(None, None, "tp", None), P(None, "tp", None), P("tp", None, None), rep,
                 rep, rep, P(None, "tp"), P("tp"), P("tp", None), rep)

    return jax.shard_map(local_step, mesh=mesh3, in_specs=in_specs, out_specs=out_specs, check_vma=False)
```

```python
import functools

import jax
import jax.numpy as jnp
from jax import lax
from jax.experimental import pallas as pl
from jax.experimental.pallas import tpu as pltpu
from jax.sharding import Mesh, PartitionSpec as P


F32 = jnp.float32
BF16 = jnp.bfloat16
MIB = 1024 * 1024
DEPTH = 4
WIDEN = 32

BLK = 256


def dot_nt(a, b):
    return lax.dot_general(a, b, (((1,), (1,)), ((), ())), preferred_element_type=F32)


def dot_nn(a, b):
    return lax.dot_general(a, b, (((1,), (0,)), ((), ())), preferred_element_type=F32)


def head_only(x, head):
    half = x.shape[1] // 2
    lane = lax.broadcasted_iota(jnp.int32, x.shape, 1)
    keep = (lane < half) if head == 0 else (lane >= half)
    return jnp.where(keep, x, jnp.zeros((), x.dtype))


def attn_fwd_kernel(qkv_ref, ctx_ref, lse_ref, ctx_t):
    seq, width = ctx_ref.shape
    half = width // 2
    scale = half ** -0.5
    q2 = qkv_ref[:, 0:width] * jnp.asarray(scale, BF16)
    v_t = qkv_ref[:, 2 * width:3 * width].T
    tasks = [(head, i) for i in range(seq // BLK) for head in range(2)]

    def scores(head, i):
        return dot_nt(qkv_ref[0:(i + 1) * BLK, width:2 * width], head_only(q2[i * BLK:(i + 1) * BLK], head))

    ready = scores(*tasks[0])
    for n, (head, i) in enumerate(tasks):
        s = ready
        if n + 1 < len(tasks):
            ready = scores(*tasks[n + 1])
        lo, hi = i * BLK, (i + 1) * BLK
        v_h = v_t[head * half:(head + 1) * half, :]
        key = lax.broadcasted_iota(jnp.int32, (BLK, BLK), 0)
        qry = lax.broadcasted_iota(jnp.int32, (BLK, BLK), 1)
        diag = jnp.where(key <= qry, s[lo:hi], -1e30)
        top = jnp.max(diag, axis=0, keepdims=True)
        if i:
            top = jnp.maximum(top, jnp.max(s[0:lo], axis=0, keepdims=True))
        p_diag = jnp.exp(diag - top)
        total = jnp.sum(p_diag, axis=0, keepdims=True)
        if i:
            p_left = jnp.exp(s[0:lo] - top)
            total = total + jnp.sum(p_left, axis=0, keepdims=True)
        inv = 1.0 / total
        acc = dot_nn(v_h[:, lo:hi], (p_diag * inv).astype(BF16))
        if i:
            acc = acc + dot_nn(v_h[:, 0:lo], (p_left * inv).astype(BF16))
        ctx_t[head * half:(head + 1) * half, lo:hi] = acc
        lse_ref[head:head + 1, lo:hi] = top + jnp.log(total)
    ctx_ref[...] = ctx_t[...].T.astype(BF16)


def attn_fwd(qkv, n_seq, seq, n_pair):
    width = 128
    return pl.pallas_call(
        attn_fwd_kernel,
        grid=(n_seq, n_pair),
        in_specs=[pl.BlockSpec((seq, 3 * width), lambda b, p: (b, p))],
        out_specs=[pl.BlockSpec((seq, width), lambda b, p: (b, p)),
                   pl.BlockSpec((None, None, 2, seq), lambda b, p: (b, p, 0, 0))],
        out_shape=[jax.ShapeDtypeStruct((n_seq * seq, n_pair * width), BF16),
                   jax.ShapeDtypeStruct((n_seq, n_pair, 2, seq), F32)],
        scratch_shapes=[pltpu.VMEM((width, seq), F32)],
        name="attn_fwd",
        cost_estimate=pl.CostEstimate(flops=n_seq * n_pair * 8 * seq * seq * 256 * 10 // 16, bytes_accessed=n_seq * seq * n_pair * width * 8,
                                      transcendentals=n_seq * n_pair * seq * seq),
        compiler_params=pltpu.CompilerParams(vmem_limit_bytes=63 * 1024 * 1024),
    )(qkv)


def attn_bwd_kernel(qkv_ref, ctx_ref, dctx_ref, lse_ref, dqkv_ref, dk_t, dv_t):
    seq, width = ctx_ref.shape
    half = width // 2
    scale = half ** -0.5
    q2 = qkv_ref[:, 0:width] * jnp.asarray(scale, BF16)
    q_t = q2.T
    do_t = dctx_ref[...].T
    lse_c = jnp.concatenate([lse_ref[...], jnp.zeros((6, seq), F32)], axis=0).T
    prod = dctx_ref[...].astype(F32) * ctx_ref[...].astype(F32)
    tasks = [(head, i) for i in range(seq // BLK) for head in range(2)]

    def scores(head, i):
        lo, hi = i * BLK, (i + 1) * BLK
        return (dot_nt(head_only(q2[lo:hi], head), qkv_ref[0:hi, width:2 * width]),
                dot_nt(head_only(dctx_ref[lo:hi, :], head), qkv_ref[0:hi, 2 * width:3 * width]))

    dq = []
    ready = scores(*tasks[0])
    for n, (head, i) in enumerate(tasks):
        s, dp = ready
        if n + 1 < len(tasks):
            ready = scores(*tasks[n + 1])
        lo, hi = i * BLK, (i + 1) * BLK
        rows = slice(head * half, (head + 1) * half)
        mean = jnp.sum(head_only(prod[lo:hi], head), axis=1, keepdims=True)
        lse = lse_c[lo:hi, head:head + 1]
        qry = lax.broadcasted_iota(jnp.int32, (BLK, BLK), 0)
        key = lax.broadcasted_iota(jnp.int32, (BLK, BLK), 1)
        p_diag = jnp.where(key <= qry, jnp.exp(s[:, lo:hi] - lse), 0.0)
        ds_diag = (p_diag * (dp[:, lo:hi] - mean)).astype(BF16)
        dv_t[rows, lo:hi] = dot_nn(do_t[rows, lo:hi], p_diag.astype(BF16))
        dk_t[rows, lo:hi] = dot_nn(q_t[rows, lo:hi], ds_diag)
        dq_h = dot_nn(ds_diag, qkv_ref[lo:hi, width:2 * width])
        if i:
            p_left = jnp.exp(s[:, 0:lo] - lse)
            ds_left = (p_left * (dp[:, 0:lo] - mean)).astype(BF16)
            dv_t[rows, 0:lo] += dot_nn(do_t[rows, lo:hi], p_left.astype(BF16))
            dk_t[rows, 0:lo] += dot_nn(q_t[rows, lo:hi], ds_left)
            dq_h = dq_h + dot_nn(ds_left, qkv_ref[0:lo, width:2 * width])
        dq.append(dq_h)
        if head == 1:
            lane = lax.broadcasted_iota(jnp.int32, (BLK, width), 1)
            dqkv_ref[lo:hi, 0:width] = (jnp.where(lane < half, dq[0], dq[1]) * scale).astype(BF16)
            dq = []
    dqkv_ref[:, width:2 * width] = dk_t[...].T.astype(BF16)
    dqkv_ref[:, 2 * width:3 * width] = dv_t[...].T.astype(BF16)


def attn_bwd(qkv, ctx, dctx, lse, at, seq, n_pair):
    width = 128
    return pl.pallas_call(
        attn_bwd_kernel,
        grid=(n_pair,),
        in_specs=[pl.BlockSpec((seq, 3 * width), lambda p: (at, p)),
                  pl.BlockSpec((seq, width), lambda p: (at, p)),
                  pl.BlockSpec((seq, width), lambda p: (at, p)),
                  pl.BlockSpec((None, None, 2, seq), lambda p: (at, p, 0, 0))],
        out_specs=pl.BlockSpec((seq, 3 * width), lambda p: (0, p)),
        out_shape=jax.ShapeDtypeStruct((seq, n_pair * 3 * width), BF16),
        scratch_shapes=[pltpu.VMEM((width, seq), F32), pltpu.VMEM((width, seq), F32)],
        name="attn_bwd",
        cost_estimate=pl.CostEstimate(flops=n_pair * 20 * seq * seq * 256 * 10 // 16, bytes_accessed=seq * n_pair * width * 16,
                                      transcendentals=n_pair * seq * seq),
        compiler_params=pltpu.CompilerParams(vmem_limit_bytes=63 * 1024 * 1024),
    )(qkv, ctx, dctx, lse)


LN_EPS = 1e-5
GELU_S = 0.7978845608028654
GELU_A = 0.044715


def row_mean(v):
    return jnp.sum(v, axis=1, keepdims=True) * (1.0 / v.shape[1])


def row_stats(v):
    centered = v - row_mean(v)
    inv_std = lax.rsqrt(row_mean(centered * centered) + LN_EPS)
    return centered * inv_std, inv_std


def norm_back(d_y, x_in, gain):
    normed, inv_std = row_stats(x_in)
    d_norm = d_y * gain
    d_x = inv_std * (d_norm - row_mean(d_norm) - normed * row_mean(d_norm * normed))
    return d_x, d_y * normed


def col_sum(v):
    return jnp.sum(v, axis=0, keepdims=True)


def to_image(rows, image, base):
    tiles = rows.shape[1] // 128
    for h in range(rows.shape[0] // 8):
        for c in range(tiles):
            image[pl.ds(base + (h * tiles + c) * 8, 8), :] = rows[h * 8:(h + 1) * 8, c * 128:(c + 1) * 128]


def from_image(image, base, n_rows, width):
    tiles = width // 128
    return jnp.concatenate([jnp.concatenate([image[pl.ds(base + (h * tiles + c) * 8, 8), :] for c in range(tiles)], axis=1)
                            for h in range(n_rows // 8)], axis=0)


def pick_rows(code_ref, first, stage, image, n_rows, tiles):
    def pick(g, _):
        base = pl.multiple_of(g * 16 * tiles, 16 * tiles)
        for j in range(16):
            row = stage[pl.ds(code_ref[first + g * 16 + j], tiles, stride=8), :]
            image[pl.ds(base + (j // 8) * 8 * tiles + j % 8, tiles, stride=8), :] = row
        return 0

    lax.fori_loop(0, n_rows // 16, pick, 0)


def embed_kernel(n_blk, cap, code_ref, *refs):
    tok_refs = refs[:n_blk]
    pos_ref, gain_ref, bias_ref, x_ref, hid_ref, stage, image = refs[n_blk:]
    rows, width = x_ref.shape
    tiles = width // 128

    @pl.when(pl.program_id(0) == 0)
    def _():
        for b in range(n_blk):
            def widen(g, _, b=b):
                part = tok_refs[b][pl.ds(pl.multiple_of(g * WIDEN, WIDEN), WIDEN), :].astype(F32)
                to_image(part, stage, pl.multiple_of((b * cap + g * WIDEN) * tiles, WIDEN * tiles))
                return 0

            lax.fori_loop(0, cap // WIDEN, widen, 0)

    pick_rows(code_ref, pl.program_id(0) * rows, stage, image, rows, tiles)
    part = 64
    for i in range(rows // part):
        at = slice(i * part, (i + 1) * part)
        x = from_image(image, i * part * tiles, part, width) + pos_ref[at, :].astype(F32)
        x_ref[at, :] = x
        normed, _ = row_stats(x)
        hid_ref[at, :] = (normed * gain_ref[...] + bias_ref[...]).astype(BF16)


def embed(code, blocks, pos_rows, gain, bias, n_tok):
    cap, width = blocks[0].shape
    seq = pos_rows.shape[0]
    rows = 256
    per_seq = seq // rows
    n_blk = len(blocks)
    vec = pl.BlockSpec((1, width), lambda i: (0, 0))
    return pl.pallas_call(
        functools.partial(embed_kernel, n_blk, cap),
        grid=(n_tok // rows,),
        in_specs=[pl.BlockSpec(memory_space=pltpu.SMEM)]
        + [pl.BlockSpec((cap, width), lambda i: (0, 0), pipeline_mode=pl.Buffered(1))] * n_blk
        + [pl.BlockSpec((rows, width), lambda i: (i % per_seq, 0)), vec, vec],
        out_specs=[pl.BlockSpec((rows, width), lambda i: (i, 0))] * 2,
        out_shape=[jax.ShapeDtypeStruct((n_tok, width), F32), jax.ShapeDtypeStruct((n_tok, width), BF16)],
        scratch_shapes=[pltpu.VMEM((n_blk * cap * width // 128, 128), F32), pltpu.VMEM((rows * width // 128, 128), F32)],
        name="embed_norm",
        cost_estimate=pl.CostEstimate(flops=15_000_000_000, bytes_accessed=n_tok * width * 10, transcendentals=0),
        compiler_params=pltpu.CompilerParams(vmem_limit_bytes=63 * 1024 * 1024),
    )(code, *blocks, pos_rows, gain, bias)


def pack_kernel(n_blk, code_ref, tok_ref, *refs):
    out_refs = refs[:n_blk]
    stage, image = refs[n_blk:]
    n_tok, width = tok_ref.shape
    cap = out_refs[0].shape[0]
    tiles = width // 128

    def widen(g, _):
        part = tok_ref[pl.ds(pl.multiple_of(g * WIDEN, WIDEN), WIDEN), :].astype(F32)
        to_image(part, stage, pl.multiple_of(g * WIDEN * tiles, WIDEN * tiles))
        return 0

    lax.fori_loop(0, n_tok // WIDEN, widen, 0)
    for b in range(n_blk):
        pick_rows(code_ref, b * cap, stage, image, cap, tiles)

        def narrow(g, _, b=b):
            part = from_image(image, pl.multiple_of(g * WIDEN * tiles, WIDEN * tiles), WIDEN, width)
            out_refs[b][pl.ds(pl.multiple_of(g * WIDEN, WIDEN), WIDEN), :] = part.astype(BF16)
            return 0

        lax.fori_loop(0, cap // WIDEN, narrow, 0)


def pack(code, tok, cap):
    n_tok, width = tok.shape
    n_blk = code.shape[0] // cap
    return pl.pallas_call(
        functools.partial(pack_kernel, n_blk),
        in_specs=[pl.BlockSpec(memory_space=pltpu.SMEM), pl.BlockSpec(memory_space=pltpu.VMEM)],
        out_specs=[pl.BlockSpec(memory_space=pltpu.VMEM)] * n_blk,
        out_shape=[jax.ShapeDtypeStruct((cap, width), BF16)] * n_blk,
        scratch_shapes=[pltpu.VMEM((n_tok * width // 128, 128), F32), pltpu.VMEM((cap * width // 128, 128), F32)],
        name="token_pack",
        cost_estimate=pl.CostEstimate(flops=15_000_000_000, bytes_accessed=n_tok * width * 5, transcendentals=0),
        compiler_params=pltpu.CompilerParams(vmem_limit_bytes=63 * 1024 * 1024),
    )(code, tok)


def proj_kernel(c_ref, w_ref, x_ref, b_ref, gain_ref, bias_ref, x1_ref, hid_ref):
    part = x_ref.shape[0] // 2
    for i in range(2):
        at = slice(i * part, (i + 1) * part)
        x1 = x_ref[at, :] + dot_nn(c_ref[at, :], w_ref[...].reshape(c_ref.shape[1], -1)).astype(BF16).astype(F32) + b_ref[...]
        x1_ref[at, :] = x1
        normed, _ = row_stats(x1)
        hid_ref[at, :] = (normed * gain_ref[...] + bias_ref[...]).astype(BF16)


def proj_norm(ctx, w, start, x, b, gain, bias):
    n_tok, width = x.shape
    n_row = ctx.shape[1] // w.shape[0]
    rows = 512
    vec = pl.BlockSpec((1, width), lambda i: (0, 0))
    mat = pl.BlockSpec((rows, width), lambda i: (i, 0))
    return pl.pallas_call(
        proj_kernel,
        grid=(n_tok // rows,),
        in_specs=[pl.BlockSpec((rows, ctx.shape[1]), lambda i: (i, 0)), pl.BlockSpec((w.shape[0], n_row, width), lambda i: (0, start // n_row, 0)), mat, vec, vec, vec],
        out_specs=[mat, mat],
        out_shape=[jax.ShapeDtypeStruct((n_tok, width), F32), jax.ShapeDtypeStruct((n_tok, width), BF16)],
        name="proj_norm",
        cost_estimate=pl.CostEstimate(flops=2 * n_tok * ctx.shape[1] * width, bytes_accessed=n_tok * width * 12, transcendentals=0),
        compiler_params=pltpu.CompilerParams(vmem_limit_bytes=63 * 1024 * 1024),
    )(ctx, w, x, b, gain, bias)


def ffn_kernel(part, h_ref, og_ref, wu_ref, wd_ref, b_ref, act_ref, dup_ref, db_ref):
    total = jnp.zeros(db_ref.shape, F32)
    for i in range(h_ref.shape[0] // part):
        at = slice(i * part, (i + 1) * part)
        z = dot_nt(h_ref[at, :], wu_ref[0]) + b_ref[...]
        d_act = dot_nt(og_ref[at, :], wd_ref[0])
        z2 = z * z
        gate = 0.5 * jnp.tanh(z * (GELU_S + (GELU_S * GELU_A) * z2)) + 0.5
        act = z * gate
        d_up = d_act * (gate + act * (1.0 - gate) * (2.0 * GELU_S + (6.0 * GELU_S * GELU_A) * z2))
        act_ref[at, :] = act.astype(BF16)
        dup_ref[at, :] = d_up.astype(BF16)
        total = total + col_sum(d_up)
    db_ref[...] = total


def ffn(hid, og, w, b_up, part=1024):
    n_tok, width = hid.shape
    ff = b_up.shape[1]
    n_piece = w.shape[0]
    bn = ff // n_piece
    whole = pl.BlockSpec((n_tok, width), lambda i: (0, 0), pipeline_mode=pl.Buffered(1))
    ospec = pl.BlockSpec((n_tok, bn), lambda i: (0, i))
    vec = pl.BlockSpec((1, bn), lambda i: (0, i))
    return pl.pallas_call(
        functools.partial(ffn_kernel, part),
        grid=(n_piece,),
        in_specs=[whole, whole, pl.BlockSpec((1, bn, width), lambda i: (i, 0, 0)), pl.BlockSpec((1, bn, width), lambda i: (i, 1, 0)), vec],
        out_specs=[ospec, ospec, vec],
        out_shape=[jax.ShapeDtypeStruct((n_tok, ff), BF16), jax.ShapeDtypeStruct((n_tok, ff), BF16), jax.ShapeDtypeStruct((1, ff), F32)],
        name="ffn",
        cost_estimate=pl.CostEstimate(flops=4 * n_tok * ff * width, bytes_accessed=4 * n_tok * ff + 4 * ff * width, transcendentals=n_tok * ff),
        compiler_params=pltpu.CompilerParams(vmem_limit_bytes=63 * 1024 * 1024),
    )(hid, og, w, w, b_up)


def down_kernel(n_tp, me_ref, act_ref, w_ref, x1_ref, b_ref, *out_refs):
    out = x1_ref[...] + dot_nn(act_ref[...], w_ref[...].reshape(act_ref.shape[1], -1)).astype(BF16).astype(F32) + b_ref[...]
    k = me_ref[0] ^ (pl.program_id(0) % n_tp)
    seq = pl.program_id(0) // n_tp
    for j in range(n_tp):
        @pl.when(k == j)
        def _(j=j):
            out_refs[j][seq] = out.astype(BF16)


def down(me, act, w, x1, b, n_seq, n_tp):
    n_tok, width = x1.shape
    ff = act.shape[1]
    rows = n_tok // n_seq // n_tp
    part = jax.ShapeDtypeStruct((n_seq, rows, width), BF16)
    return pl.pallas_call(
        functools.partial(down_kernel, n_tp),
        grid_spec=pltpu.PrefetchScalarGridSpec(
            num_scalar_prefetch=1, grid=(n_seq * n_tp,),
            in_specs=[pl.BlockSpec((rows, ff), lambda i, m: (i, 0)),
                      pl.BlockSpec((w.shape[0], ff // w.shape[0], width), lambda i, m: (0, 1, 0), pipeline_mode=pl.Buffered(1)),
                      pl.BlockSpec((rows, width), lambda i, m: (i, 0)), pl.BlockSpec((1, width), lambda i, m: (0, 0))],
            out_specs=[pl.BlockSpec(part.shape, lambda i, m: (0, 0, 0))] * n_tp),
        out_shape=[part] * n_tp,
        name="down",
        cost_estimate=pl.CostEstimate(flops=2 * n_tok * ff * width, bytes_accessed=2 * n_tok * ff + n_tok * width * 6, transcendentals=0),
        compiler_params=pltpu.CompilerParams(vmem_limit_bytes=63 * 1024 * 1024),
    )(me, act, w, x1, b)


def back2_kernel(dup_ref, w_ref, wout_ref, x1_ref, og_ref, gain_ref, dr_ref, da_ref, dc_ref, sums_ref):
    @pl.when(pl.program_id(0) == 0)
    def _():
        sums_ref[...] = jnp.zeros(sums_ref.shape, F32)

    n_part = 2
    part = dr_ref.shape[0] // n_part
    w = w_ref[...].reshape(dup_ref.shape[1], -1)
    d_ys = [dot_nn(dup_ref[i * part:(i + 1) * part, :], w) for i in range(n_part)]
    for i in range(n_part):
        at = slice(i * part, (i + 1) * part)
        d_y = d_ys[i].astype(BF16).astype(F32)
        d_x, d_gain = norm_back(d_y, x1_ref[at, :], gain_ref[...])
        og = og_ref[at, :].astype(F32)
        d_resid = og + d_x
        dr_ref[at, :] = d_resid
        d_attn = d_resid.astype(BF16)
        da_ref[at, :] = d_attn
        dc_ref[at, :] = dot_nt(d_attn, wout_ref[...].reshape(-1, d_attn.shape[1])).astype(BF16)
        sums_ref[0:1, :] += col_sum(d_gain)
        sums_ref[1:2, :] += col_sum(d_y)
        sums_ref[2:3, :] += col_sum(d_resid)
        sums_ref[3:4, :] += col_sum(og)


def back2(d_up, w, start, x1, og, gain):
    n_tok, width = x1.shape
    ff = d_up.shape[1]
    rows = 256
    n_out = (w.shape[1] - start)
    mat = pl.BlockSpec((rows, width), lambda i: (i, 0))
    return pl.pallas_call(
        back2_kernel,
        grid=(n_tok // rows,),
        in_specs=[pl.BlockSpec((rows, ff), lambda i: (i, 0)), pl.BlockSpec((w.shape[0], ff // w.shape[0], width), lambda i: (0, 0, 0), pipeline_mode=pl.Buffered(1)),
                  pl.BlockSpec((w.shape[0], n_out, width), lambda i: (0, start // n_out, 0), pipeline_mode=pl.Buffered(1)),
                  mat, mat, pl.BlockSpec((1, width), lambda i: (0, 0))],
        out_specs=[mat, mat, pl.BlockSpec((rows, w.shape[0] * n_out), lambda i: (i, 0)), pl.BlockSpec((8, width), lambda i: (0, 0))],
        out_shape=[jax.ShapeDtypeStruct((n_tok, width), F32), jax.ShapeDtypeStruct((n_tok, width), BF16),
                   jax.ShapeDtypeStruct((n_tok, w.shape[0] * n_out), BF16), jax.ShapeDtypeStruct((8, width), F32)],
        name="ffn_back",
        cost_estimate=pl.CostEstimate(flops=2 * n_tok * ff * width, bytes_accessed=2 * n_tok * ff + n_tok * width * 12, transcendentals=0),
        compiler_params=pltpu.CompilerParams(vmem_limit_bytes=63 * 1024 * 1024),
    )(d_up, w, w, x1, og, gain)


def back1_kernel(dq_ref, w_ref, x_ref, dr_ref, gain_ref, *refs):
    tok_ref, pos_ref, sums_ref, bsum_ref = refs[-4:]
    before_refs = refs[:-4]

    @pl.when(pl.program_id(0) == 0)
    def _():
        sums_ref[...] = before_refs[1][...] if before_refs else jnp.zeros(sums_ref.shape, F32)
        bsum_ref[...] = before_refs[2][...] if before_refs else jnp.zeros(bsum_ref.shape, F32)

    n_part = 2
    part = tok_ref.shape[0] // n_part
    d_ys = [dot_nn(dq_ref[i * part:(i + 1) * part, :], w_ref[...]) for i in range(n_part)]
    for i in range(n_part):
        at = slice(i * part, (i + 1) * part)
        d_y = d_ys[i].astype(BF16).astype(F32)
        d_x, d_gain = norm_back(d_y, x_ref[at, :], gain_ref[...])
        d_resid = dr_ref[at, :] + d_x
        tok_ref[at, :] = d_resid.astype(BF16)
        pos_ref[at, :] = before_refs[0][at, :] + d_resid if before_refs else d_resid
        sums_ref[0:1, :] += col_sum(d_gain)
        sums_ref[1:2, :] += col_sum(d_y)
        bsum_ref[0:1, :] += col_sum(dq_ref[at, :].astype(F32))


def back1(d_qkv, w_qkv, x, d_resid1, gain, at, pos_rows, earlier=None):
    seq, n_cols = d_qkv.shape
    width = x.shape[1]
    rows = 256
    steps = seq // rows
    mat = pl.BlockSpec((rows, width), lambda i: (at * steps + i, 0))
    out = pl.BlockSpec((rows, width), lambda i: (i, 0))
    few = [pl.BlockSpec((8, width), lambda i: (0, 0)), pl.BlockSpec((8, n_cols), lambda i: (0, 0))]
    return pl.pallas_call(
        back1_kernel,
        grid=(steps,),
        in_specs=[pl.BlockSpec((rows, n_cols), lambda i: (i, 0)),
                  pl.BlockSpec((n_cols, width), lambda i: (0, 0), pipeline_mode=pl.Buffered(1)),
                  mat, mat, pl.BlockSpec((1, width), lambda i: (0, 0))] + ([out] + few if earlier else []),
        out_specs=[out, out] + few,
        out_shape=[jax.ShapeDtypeStruct((seq, width), BF16), jax.ShapeDtypeStruct((pos_rows, width), F32),
                   jax.ShapeDtypeStruct((8, width), F32), jax.ShapeDtypeStruct((8, n_cols), F32)],
        name="qkv_back",
        cost_estimate=pl.CostEstimate(flops=2 * seq * n_cols * width, bytes_accessed=2 * seq * n_cols + seq * width * 12, transcendentals=0),
        compiler_params=pltpu.CompilerParams(vmem_limit_bytes=63 * 1024 * 1024),
    )(d_qkv, w_qkv, x, d_resid1, gain, *(earlier or ()))


def pieces_out_kernel(n_in, spans, me_ref, *refs):
    out_refs = refs[n_in:]
    for p in range(n_in):
        @pl.when(pl.program_id(0) == p)
        def _(p=p):
            for (start, n, turned), out_ref in zip(spans, out_refs):
                part = refs[p][start:start + n, :]
                out_ref[...] = part.T if turned else part


def pieces_out(me, pieces, spans):
    rows, width = pieces[0].shape
    n_in = len(pieces)

    def place(p, m):
        return (m[1] ^ (p // 2)) * 2 + (m[0] ^ (p % 2))

    out_specs, out_shape = [], []
    for start, n, turned in spans:
        if turned:
            out_specs.append(pl.BlockSpec((width, n), lambda p, m: (0, place(p, m))))
            out_shape.append(jax.ShapeDtypeStruct((width, n_in * n), F32))
        else:
            out_specs.append(pl.BlockSpec((n, width), lambda p, m: (place(p, m), 0)))
            out_shape.append(jax.ShapeDtypeStruct((n_in * n, width), F32))
    return pl.pallas_call(
        functools.partial(pieces_out_kernel, n_in, spans),
        grid_spec=pltpu.PrefetchScalarGridSpec(
            num_scalar_prefetch=1, grid=(n_in,),
            in_specs=[pl.BlockSpec((rows, width), lambda p, m: (0, 0), pipeline_mode=pl.Buffered(1))] * n_in,
            out_specs=out_specs),
        out_shape=out_shape,
        name="grads_out",
        cost_estimate=pl.CostEstimate(flops=8_000_000_000, bytes_accessed=n_in * rows * width * 8, transcendentals=0),
        compiler_params=pltpu.CompilerParams(vmem_limit_bytes=63 * 1024 * 1024),
    )(me, *pieces)


def assemble_kernel(n, me_ref, *refs):
    out_ref = refs[n]
    k = me_ref[0] ^ pl.program_id(0)
    for j in range(n):
        @pl.when(k == j)
        def _(j=j):
            out_ref[...] = refs[j][...].reshape(out_ref.shape)


def assemble(me, parts, out_shape, block):
    at = 1 if len(out_shape) == 4 else 0
    return pl.pallas_call(
        functools.partial(assemble_kernel, len(parts)),
        grid_spec=pltpu.PrefetchScalarGridSpec(
            num_scalar_prefetch=1, grid=(len(parts),),
            in_specs=[pl.BlockSpec(p.shape, lambda i, m: (0, 0, 0), pipeline_mode=pl.Buffered(1)) for p in parts],
            out_specs=pl.BlockSpec(block, lambda i, m: tuple(i if d == at else 0 for d in range(len(block))))),
        out_shape=jax.ShapeDtypeStruct(out_shape, parts[0].dtype),
        name="assemble",
        cost_estimate=pl.CostEstimate(flops=4_000_000_000, bytes_accessed=16 * MIB, transcendentals=0),
        compiler_params=pltpu.CompilerParams(vmem_limit_bytes=63 * 1024 * 1024),
    )(me, *parts)


LANES = 128


def accum_kernel(n_block, cap, sub_rows, width, where_ref, first_ref, *refs):
    tok_refs = refs[:n_block]
    out_ref = refs[n_block]
    n_sub = len(sub_rows)
    acc = refs[n_block + 1:n_block + 1 + n_sub]
    buf, stage, in_sem, out_sem = refs[n_block + 1 + n_sub:]
    tiles = width // LANES
    group = 8 * tiles

    def fetch(block, n):
        return pltpu.make_async_copy(tok_refs[n], buf.at[block % DEPTH], in_sem.at[block % DEPTH])

    def fetch_next(block):
        for n in range(n_block):
            @pl.when(block == n)
            def _(n=n):
                fetch(block, n).start()

    for n in range(min(DEPTH - 1, n_block)):
        fetch(n, n).start()
    for s in range(n_sub):
        def clear(i, _, s=s):
            acc[s][pl.ds(pl.multiple_of(i * group, group), group), :] = jnp.zeros((group, LANES), F32)
            return 0

        lax.fori_loop(0, sub_rows[s] // 8, clear, 0)

    def add_rows(s, slot, n):
        codes = [where_ref[slot + j] for j in range(n)]
        at = [code >> 16 for code in codes]
        rows = [stage[pl.ds(code & 0xffff, tiles, stride=8), :] for code in codes]
        sums = [acc[s][pl.ds(a, tiles, stride=8), :] for a in at]
        for j in range(n):
            for i in range(j):
                sums[j] = jnp.where(at[i] == at[j], sums[i], sums[j])
            sums[j] = sums[j] + rows[j]
        for j in range(n):
            acc[s][pl.ds(at[j], tiles, stride=8), :] = sums[j]

    def add_block(block, _):
        fetch_next(block + DEPTH - 1)
        fetch(block, 0).wait()

        def widen(g, _):
            rows = buf[block % DEPTH, pl.ds(pl.multiple_of(g * WIDEN, WIDEN), WIDEN), :].astype(F32)
            base = pl.multiple_of(g * (WIDEN // 8) * group, (WIDEN // 8) * group)
            for h in range(WIDEN // 8):
                for c in range(tiles):
                    stage[pl.ds(base + h * group + c * 8, 8), :] = rows[h * 8:(h + 1) * 8, c * LANES:(c + 1) * LANES]
            return 0

        lax.fori_loop(0, cap // WIDEN, widen, 0)

        starts = [first_ref[block * (n_sub + 1) + s] for s in range(n_sub + 1)]
        counts = [starts[s + 1] - starts[s] for s in range(n_sub)]
        both = functools.reduce(jnp.minimum, counts) // 2
        begin = [block * cap + starts[s] for s in range(n_sub)]

        def together(i, _):
            for s in range(n_sub):
                add_rows(s, begin[s] + 2 * i, 2)
            return 0

        lax.fori_loop(0, both, together, 0)
        for s in range(n_sub):
            fours = (counts[s] - 2 * both) // 4

            def alone(i, _, s=s):
                add_rows(s, begin[s] + 2 * both + 4 * i, 4)
                return 0

            lax.fori_loop(0, fours, alone, 0)

            def single(i, _, s=s):
                add_rows(s, begin[s] + i, 1)
                return 0

            lax.fori_loop(2 * both + 4 * fours, counts[s], single, 0)
        return 0

    lax.fori_loop(0, n_block, add_block, 0)
    done = 0
    copies = []
    for s in range(n_sub):
        n = sub_rows[s] * tiles
        copies.append(pltpu.make_async_copy(acc[s], out_ref.at[pl.ds(done, n), :], out_sem.at[s]))
        copies[-1].start()
        done += n
    for c in copies:
        c.wait()


def accum(tok_blocks, code, first, sub_rows, width):
    n_block = len(tok_blocks)
    cap = tok_blocks[0].shape[0]
    n_sub = len(sub_rows)
    tiles = width // LANES
    return pl.pallas_call(
        functools.partial(accum_kernel, n_block, cap, sub_rows, width),
        in_specs=[pl.BlockSpec(memory_space=pltpu.SMEM), pl.BlockSpec(memory_space=pltpu.SMEM)]
        + [pl.BlockSpec(memory_space=pl.ANY)] * n_block,
        out_specs=pl.BlockSpec(memory_space=pl.ANY),
        out_shape=jax.ShapeDtypeStruct((sum(sub_rows) * tiles, LANES), F32),
        scratch_shapes=[pltpu.VMEM((r * tiles, LANES), F32) for r in sub_rows]
        + [pltpu.VMEM((DEPTH, cap, width), BF16), pltpu.VMEM((cap * tiles, LANES), F32),
           pltpu.SemaphoreType.DMA((DEPTH,)), pltpu.SemaphoreType.DMA((n_sub,))],
        name="table_accum",
        cost_estimate=pl.CostEstimate(flops=50_000_000_000, bytes_accessed=100_000_000, transcendentals=0),
        compiler_params=pltpu.CompilerParams(vmem_limit_bytes=63 * 1024 * 1024),
    )(code, first, *tok_blocks)


def dot_tn(a, b):
    return lax.dot_general(a, b, (((0,), (0,)), ((), ())), preferred_element_type=F32)


def grad_kernel(has_plus, core_ref, a_ref, b_ref, *refs):
    out_ref = refs[-1]
    piece, width = out_ref.shape[2:]
    half = a_ref.shape[1] // 2
    g = dot_tn(a_ref[...], b_ref[...])
    for x in range(2):
        part = g[x * half:(x + 1) * half]
        out_ref[x, 0, 0:half, :] = part + refs[0][x * piece:x * piece + half, :] if has_plus else part
        if piece > half:
            out_ref[x, 0, half:, :] = jnp.zeros((piece - half, width), F32)


def grad_pieces(core, a, b, n_tp, piece, which, n_which, plus=None, into=None):
    n_tok, n_cols = a.shape
    width = b.shape[1]
    out_spec = pl.BlockSpec((2, 1, piece, width), lambda t, c: (t, which, 0, 0))
    in_specs = [pl.BlockSpec((n_tok, n_cols // (2 * n_tp)), lambda t, c: (0, 2 * t + c[0])),
                pl.BlockSpec((n_tok, width), lambda t, c: (0, 0), pipeline_mode=pl.Buffered(1))]
    args = [a, b]
    if plus is not None:
        in_specs.append(pl.BlockSpec((2 * piece, width), lambda t, c: (t, 0)))
        args.append(plus)
    shape = (2 * n_tp, n_which, piece, width)
    if into is not None:
        in_specs.append(pl.BlockSpec(memory_space=pl.ANY))
        args.append(into.reshape(shape))
    return pl.pallas_call(
        functools.partial(grad_kernel, plus is not None),
        grid_spec=pltpu.PrefetchScalarGridSpec(num_scalar_prefetch=1, grid=(n_tp,), in_specs=in_specs, out_specs=out_spec),
        out_shape=jax.ShapeDtypeStruct(shape, F32),
        input_output_aliases={} if into is None else {len(args): 0},
        name="weight_grad",
        cost_estimate=pl.CostEstimate(flops=n_tok * n_cols * width, bytes_accessed=n_tok * (n_cols + 2 * width) + 2 * n_cols * width,
                                      transcendentals=0),
        compiler_params=pltpu.CompilerParams(vmem_limit_bytes=63 * 1024 * 1024),
    )(core, *args).reshape(-1, width)


def grad_rest_kernel(spans, last, n_a2, core_ref, a1_ref, b1_ref, b2_ref, *refs):
    a2_refs, refs, out_ref = refs[:n_a2], refs[n_a2:-1], refs[-1]
    plus = refs[0] if refs else None
    piece, piece_in = out_ref.shape[0] // 2, (plus.shape[0] // 2 if refs else 0)
    rows = b2_ref.shape[0] // n_a2
    for which, (start, stop) in enumerate(spans):
        half = (a2_refs[0] if which else a1_ref).shape[1] // 2
        for i in range(0, 2 * half, 128):
            cols = slice(i, i + 128)
            if which:
                g = sum(dot_tn(a_ref[:, cols], b2_ref[n * rows:(n + 1) * rows, :]) for n, a_ref in enumerate(a2_refs))
            else:
                g = dot_tn(a1_ref[:, cols], b1_ref[...])
            for x in range(2):
                lo, hi = max(i, x * half), min(i + 128, (x + 1) * half)
                if lo < hi:
                    to = lo - x * half + start
                    part = g[lo - i:hi - i]
                    if plus is not None:
                        part = part + plus[x * piece_in + to:x * piece_in + to + hi - lo, :]
                    out_ref[x * piece + to:x * piece + to + hi - lo, :] = part
        for x in range(2):
            if stop > start + half:
                out_ref[x * piece + start + half:x * piece + stop, :] = jnp.zeros((stop - start - half, out_ref.shape[1]), F32)
    if last:
        for x in range(2):
            out_ref[x * piece + spans[-1][1]:(x + 1) * piece, :] = refs[1][x, 0] + refs[2][x * last:(x + 1) * last, :]


def grad_rest(core, a1, b1, a2, b2, n_tp, spans, plus=None, tail=None):
    n_tok, width = b1.shape
    last = tail[0].shape[2] if tail else 0
    piece = spans[-1][1] + last
    whole = pl.BlockSpec((n_tok, width), lambda t, c: (0, 0), pipeline_mode=pl.Buffered(1))
    cols = [pl.BlockSpec((a.shape[0], a.shape[1] // (2 * n_tp)), lambda t, c: (0, 2 * t + c[0])) for a in (a1, *a2)]
    in_specs, args = [cols[0], whole, whole] + cols[1:], [a1, b1, b2, *a2]
    if plus is not None:
        in_specs.append(pl.BlockSpec((plus.shape[0] // n_tp, width), lambda t, c: (t, 0)))
        args.append(plus)
    if tail:
        in_specs.append(pl.BlockSpec((2, 1, last, width), lambda t, c: (t, c[0], 0, 0)))
        in_specs.append(pl.BlockSpec((2 * last, width), lambda t, c: (t, 0)))
        args += tail
    n_cols = a1.shape[1] + a2[0].shape[1]
    return pl.pallas_call(
        functools.partial(grad_rest_kernel, spans, last, len(a2)),
        grid_spec=pltpu.PrefetchScalarGridSpec(num_scalar_prefetch=1, grid=(n_tp,), in_specs=in_specs,
                                               out_specs=pl.BlockSpec((2 * piece, width), lambda t, c: (t, 0))),
        out_shape=jax.ShapeDtypeStruct((2 * n_tp * piece, width), F32),
        name="weight_grads",
        cost_estimate=pl.CostEstimate(flops=n_tok * n_cols * width, bytes_accessed=n_tok * (n_cols + 4 * width) + 2 * n_cols * width,
                                      transcendentals=0),
        compiler_params=pltpu.CompilerParams(vmem_limit_bytes=63 * 1024 * 1024),
    )(core, *args)


POS_OFFSET = 2
SLOTS = 704
GRAD_SLOTS = 384
LOW = 32


def before(n):
    return (lax.broadcasted_iota(jnp.int32, (n, n), 1) < lax.broadcasted_iota(jnp.int32, (n, n), 0)).astype(BF16)


def rank_in_class(hot):
    n_blk, n_tok, n_cls = hot.shape
    ones = hot.astype(BF16).reshape(n_blk, n_tok // 128, 128, n_cls)
    within = jnp.einsum("ij,bnjk->bnik", before(128), ones, preferred_element_type=F32)
    sums = jnp.sum(ones.astype(F32), axis=2)
    ahead = jnp.einsum("mn,bnk->bmk", before(n_tok // 128), sums.astype(BF16), preferred_element_type=F32)
    rank = jnp.sum((within + ahead[:, :, None, :]) * ones.astype(F32), axis=3)
    return rank.reshape(n_blk, n_tok).astype(jnp.int32), jnp.sum(sums, axis=1).astype(jnp.int32)


def compact(rank, valid, value, slots):
    n_high = slots // LOW
    high = ((rank // LOW)[:, :, None] == jnp.arange(n_high)) & valid[:, :, None]
    low = ((rank % LOW)[:, :, None] == jnp.arange(LOW)).astype(F32)
    parts = jnp.concatenate([low * (value // 128).astype(F32)[:, :, None], low * (value % 128).astype(F32)[:, :, None]], axis=2)
    out = jnp.einsum("bjh,bjl->bhl", high.astype(BF16), parts.astype(BF16), preferred_element_type=F32).astype(jnp.int32)
    return (out[:, :, :LOW] * 128 + out[:, :, LOW:]).reshape(rank.shape[0], slots)


def solution(mesh):
    n_tp, n_dp = mesh.shape["tp"], mesh.shape["dp"]
    n_core = 2
    n_x = n_dp // n_core
    mesh3 = Mesh(mesh.devices.reshape(n_tp, n_x, n_core), ("tp", "xx", "cc"))
    dp = ("xx", "cc")
    tp_swap = [[(i, i ^ k) for i in range(n_tp)] for k in range(n_tp)]
    pair = [(0, 1), (1, 0)]

    def local_step(tok_ids, emb_table, pos_table, ln1_gain, ln1_bias, w_qkv, b_qkv, w_out, b_out,
                   ln2_gain, ln2_bias, w_up, b_up, w_down, b_down, out_grad):
        tp_index, x_index, c_index = lax.axis_index("tp"), lax.axis_index("xx"), lax.axis_index("cc")
        dp_index = x_index * n_core + c_index
        n_seq_dp, seq = tok_ids.shape
        n_seq = n_seq_dp // n_tp
        n_tok = n_seq * seq
        rows, width = emb_table.shape
        n_sub = 4
        sub = -(-rows // n_sub // 8) * 8
        sub_rows = (sub,) * (n_sub - 1) + (rows - (n_sub - 1) * sub,)
        seq_local = seq // n_tp
        ff = w_up.shape[1]
        gain1, bias1 = ln1_gain.astype(F32)[None], ln1_bias.astype(F32)[None]
        gain2, bias2 = ln2_gain.astype(F32)[None], ln2_bias.astype(F32)[None]

        def half(w, axis):
            n = w.shape[axis] // n_core
            return lax.dynamic_slice_in_dim(w, c_index * n, n, axis)

        def gather_rows(w):
            return lax.all_gather(w, ("tp", "cc"), axis=0, tiled=True)

        def swap(v, axis, k=1):
            return lax.ppermute(v, axis, tp_swap[k] if axis == "tp" else pair)

        def by_owner(parts):
            out = []
            for p in range(n_tp):
                k = tp_index ^ p
                out.append(jnp.where(k < 2, jnp.where(k == 0, parts[0], parts[1]), jnp.where(k == 2, parts[2], parts[3])))
            return out

        ids_all = lax.all_gather(tok_ids, dp, axis=0, tiled=True)
        ids_all, w_up, w_down, w_out, b_qkv, b_up = lax.optimization_barrier((ids_all, w_up, w_down, w_out, b_qkv, b_up))

        wqkv_t = gather_rows(jnp.transpose(half(w_qkv, 2), (1, 2, 3, 0)).reshape(-1, width))
        n_ff, n_out = ff // n_dp, w_out.shape[0] * w_out.shape[1] // n_dp

        def quarter(w, axis):
            n = w.shape[axis] // n_dp
            return lax.dynamic_slice_in_dim(w, dp_index * n, n, axis)

        own_w = jnp.concatenate([quarter(w_up, 1).T, quarter(w_down, 0), quarter(w_out.reshape(-1, width), 0)])
        w_all = lax.all_gather(own_w, ("tp", "xx", "cc"), axis=0, tiled=True)
        w_all = w_all.reshape(n_tp * n_dp, 2 * n_ff + n_out, width)
        n_pair = wqkv_t.shape[0] // (3 * 128)
        own_bias = jnp.concatenate([b_qkv.reshape(3, n_core, -1, b_qkv.shape[2]).transpose(1, 0, 2, 3).reshape(-1), b_up])
        biases = jnp.stack(by_owner([swap(own_bias, "tp", k) if k else own_bias for k in range(n_tp)]))
        bqkv_w = biases[:, :-ff].reshape(-1).astype(F32)
        bup_w = biases[:, -ff:].reshape(1, -1).astype(F32)
        pos_rows = lax.slice_in_dim(pos_table, POS_OFFSET, POS_OFFSET + seq, axis=0)

        local = ids_all - tp_index * rows
        sub_of = sum(((local >= s * sub).astype(jnp.int32) for s in range(1, n_sub)), jnp.zeros_like(local))
        owned = (local >= 0) & (local < rows)
        hot = owned[:, :, None] & (sub_of[:, :, None] == jnp.arange(n_sub))
        rank, counts = rank_in_class(hot)
        first = jnp.concatenate([jnp.zeros_like(counts[:, :1]), jnp.cumsum(counts, axis=1)], axis=1)
        rank = rank + jnp.sum(jnp.where(hot, first[:, None, :-1], 0), axis=2)
        owner_counts = jnp.stack([jnp.sum(((ids_all >= o * rows) & (ids_all < (o + 1) * rows)).astype(jnp.int32), axis=1)
                                  for o in range(n_tp)])
        grad_rounds = (jnp.max(owner_counts) + GRAD_SLOTS - 1) // GRAD_SLOTS
        rounds = (jnp.max(jnp.sum(owner_counts.reshape(n_tp, -1, n_seq), axis=2)) + SLOTS - 1) // SLOTS

        def after_first(ranks, totals):
            return (ranks + (jnp.cumsum(totals, axis=1) - totals)[:, :, None]).reshape(ranks.shape[0], -1)

        def grad_lists(r):
            at = rank - r * GRAD_SLOTS
            return compact(at, owned & (at >= 0) & (at < GRAD_SLOTS), jnp.where(owned, local, 0), GRAD_SLOTS)

        my_rank = lax.dynamic_slice_in_dim(rank, dp_index * n_seq_dp, n_seq_dp, 0)
        my_total = lax.dynamic_slice_in_dim(first[:, -1], dp_index * n_seq_dp, n_seq_dp, 0)
        my_rank = after_first(my_rank.reshape(n_tp, n_seq, seq), my_total.reshape(n_tp, n_seq))
        my_owned = lax.dynamic_slice_in_dim(owned, dp_index * n_seq_dp, n_seq_dp, 0).reshape(n_tp, n_tok)
        my_local = lax.dynamic_slice_in_dim(local, dp_index * n_seq_dp, n_seq_dp, 0).reshape(n_tp, n_tok)

        def lists(r):
            at = my_rank - r * SLOTS
            return compact(at, my_owned & (at >= 0) & (at < SLOTS), jnp.where(my_owned, my_local, 0), SLOTS)

        own_ids = lax.dynamic_slice_in_dim(ids_all, dp_index * n_seq_dp + tp_index * n_seq, n_seq, 0)
        own_owner = sum(((own_ids >= o * rows).astype(jnp.int32) for o in range(1, n_tp)), jnp.zeros_like(own_ids))
        own_local = own_ids - own_owner * rows
        own_sub = sum(((own_local >= s * sub).astype(jnp.int32) for s in range(1, n_sub)), jnp.zeros_like(own_ids))
        own_hot = (own_owner * n_sub + own_sub)[:, :, None] == jnp.arange(n_tp * n_sub)
        own_rank, own_counts = rank_in_class(own_hot)
        own_counts = own_counts.reshape(n_seq, n_tp, n_sub)
        own_first = jnp.cumsum(own_counts, axis=2) - own_counts
        own_rank = own_rank + jnp.sum(jnp.where(own_hot, own_first.reshape(n_seq, 1, -1), 0), axis=2)
        own_total = jnp.sum(own_counts, axis=2)
        own_shift = jnp.cumsum(own_total, axis=0) - own_total
        own_place = sum(jnp.where(own_owner == o, own_shift[:, o:o + 1], 0) for o in range(n_tp))
        own_place = (own_place + own_rank).reshape(-1)

        def own_lists(r, b):
            at = jnp.broadcast_to(own_rank[b] - r * GRAD_SLOTS, (n_tp, seq))
            mine = own_owner[b] == jnp.arange(n_tp)[:, None]
            return compact(at, mine & (at >= 0) & (at < GRAD_SLOTS), jnp.broadcast_to(jnp.arange(seq), (n_tp, seq)), GRAD_SLOTS)

        tiles = width // 128

        def own_places(r, b):
            own = own_lists(r, b)
            place = jnp.concatenate([lax.dynamic_index_in_dim(own, tp_index ^ k, 0, keepdims=False) for k in range(n_tp)])
            return (place // 8) * (8 * tiles) + place % 8

        places0 = [own_places(0, b) for b in range(n_seq)]

        def in_block_order(table, b):
            out = []
            for dc in range(n_core):
                for dx in range(n_x):
                    for k in range(n_tp):
                        d = (x_index ^ dx) * n_core + (c_index ^ dc)
                        out.append(lax.dynamic_index_in_dim(table, (d * n_tp + (tp_index ^ k)) * n_seq + b, 0, keepdims=False))
            return out

        def both_orders(table):
            return jnp.stack(in_block_order(table, 0) + in_block_order(table, 1))

        block_rows = both_orders(grad_lists(0))
        in_sub = sum(((block_rows >= s * sub).astype(jnp.int32) for s in range(1, n_sub)), jnp.zeros_like(block_rows))
        in_sub = block_rows - in_sub * sub
        slot = jnp.arange(GRAD_SLOTS)
        code = (((in_sub // 8) * (8 * tiles) + in_sub % 8) << 16) | ((slot // 8) * (8 * tiles) + slot % 8)
        code = code.reshape(-1)
        block_first = jnp.minimum(both_orders(first), GRAD_SLOTS).reshape(-1)

        def rows_here(r, my_lists):
            index = [lax.dynamic_index_in_dim(my_lists, tp_index ^ k, 0, keepdims=False) for k in range(n_tp)]
            first_two = jnp.take(emb_table, jnp.concatenate([index[3], index[1]]), axis=0, mode="clip")
            rest, first_two = lax.optimization_barrier((jnp.concatenate([index[2], index[0]]), first_two))
            last_two = jnp.take(emb_table, rest, axis=0, mode="clip")
            sent = [last_two[SLOTS:], first_two[SLOTS:], last_two[:SLOTS], first_two[:SLOTS]]
            got = list(sent)
            for k in range(1, n_tp):
                got[k] = swap(sent[k], "tp", k)
            at = own_place - r * SLOTS
            valid = (at >= 0) & (at < SLOTS)
            return got, jnp.where(valid, (own_owner.reshape(-1) ^ tp_index) * SLOTS + at, 0), valid

        def norm_rows(x):
            normed, _ = row_stats(x)
            return (normed * gain1 + bias1).astype(BF16)

        got0, place0, _ = rows_here(0, lists(0))
        code0 = (place0 // 8) * (8 * tiles) + place0 % 8
        og_parts = out_grad.reshape(n_tp, n_seq, seq_local, width)
        og_parts = [lax.dynamic_index_in_dim(og_parts, tp_index ^ k, 0, keepdims=False) for k in range(n_tp)]
        got0, og_parts = lax.optimization_barrier((got0, og_parts))
        resid_x, hid1 = embed(code0, got0, pos_rows, gain1, bias1, n_tok)

        def more_rows(carry):
            r, x, _ = carry
            got, place, valid = rows_here(r, lists(r))
            new = jnp.take(jnp.concatenate(got), place, axis=0, mode="clip").astype(F32) + jnp.tile(pos_rows.astype(F32), (n_seq, 1))
            x = jnp.where(valid[:, None], new, x)
            return r + 1, x, norm_rows(x)

        _, resid_x, hid1 = lax.while_loop(lambda c: c[0] < rounds, more_rows, (jnp.int32(1), resid_x, hid1))

        parts = [swap(part, "tp", k) if k else part for k, part in enumerate(og_parts)]
        me = jnp.reshape(tp_index, (1,))
        og = assemble(me, parts, (n_seq, n_tp, seq_local, width), (n_seq, 1, seq_local, width)).reshape(n_tok, width)

        qkv = (dot_nt(hid1, wqkv_t) + bqkv_w).astype(BF16)
        ctx, lse = attn_fwd(qkv, n_seq, seq, n_pair)
        resid_x1, hid2 = proj_norm(ctx, w_all, 2 * n_ff, resid_x, b_out.astype(F32)[None], gain2, bias2)
        act, d_up, d_b_up = ffn(hid2, og, w_all, bup_w)
        parts = down(me, act, w_all, resid_x1, b_down.astype(F32)[None], n_seq, n_tp)
        parts = [swap(part, "tp", k) if k else part for k, part in enumerate(parts)]
        layer_out = assemble(me, parts, (n_seq_dp, seq_local, width), (n_seq, seq_local, width))

        core = jnp.reshape(c_index, (1,))

        def piece_of(n_rows):
            return -(-n_rows // (4 * n_tp) // 24) * 24

        def every_piece(g):
            other = swap(g, "xx")
            return [g, other, swap(g, "cc"), swap(other, "cc")]

        x_and_core = jnp.stack([x_index, c_index])

        p_ff = piece_of(n_tp * ff)
        down_theirs = swap(grad_pieces(1 - core, act, og, n_tp, p_ff, 0, 1), "cc")
        up_theirs = swap(grad_pieces(1 - core, d_up, hid2, n_tp, p_ff, 0, 1), "cc")
        ff_grads = grad_pieces(core, act, og, n_tp, p_ff, 0, 2, plus=down_theirs)
        ff_grads = grad_pieces(core, d_up, hid2, n_tp, p_ff, 1, 2, plus=up_theirs, into=ff_grads)
        ff_grads = lax.psum_scatter(ff_grads, ("tp", "xx"), scatter_dimension=0, tiled=True)
        ff_grads = every_piece(ff_grads)

        d_resid1, d_attn, d_ctx, sums2 = back2(d_up, w_all, 2 * n_ff, resid_x1, og, gain2)
        n_small = n_tp * (b_qkv.size + ff) // width + 6
        p_pos = -(-(seq + n_small) // (24 * n_tp * n_dp)) * 24
        p_out = piece_of(ctx.shape[1])
        spans = ((0, p_out), (p_out, p_out + piece_of(wqkv_t.shape[0])))

        def token_blocks(places, d_tok):
            parts = pack(places, d_tok, GRAD_SLOTS)
            blocks = [swap(part, "tp", k) if k else part for k, part in enumerate(parts)]
            other = []
            for block in blocks:
                other.append(swap(block, "xx"))
            return blocks + other + [swap(block, "cc") for block in blocks + other]

        d_qkv0 = attn_bwd(qkv, ctx, d_ctx, lse, 0, seq, n_pair)
        d_tok0, *sums0 = back1(d_qkv0, wqkv_t, resid_x, d_resid1, gain1, 0, p_pos * n_tp * n_dp)
        blocks0 = token_blocks(places0[0], d_tok0)
        d_qkv1 = attn_bwd(qkv, ctx, d_ctx, lse, 1, seq, n_pair)
        d_tok1, pos_all, sums1, sums_qkv = back1(d_qkv1, wqkv_t, resid_x, d_resid1, gain1, 1, p_pos * n_tp * n_dp, earlier=sums0)
        blocks1 = token_blocks(places0[1], d_tok1)
        d_qkvs = [d_qkv0, d_qkv1]
        rest_theirs = swap(grad_rest(1 - core, ctx, d_attn, d_qkvs, hid1, n_tp, spans), "cc")

        d_w_down, d_w_up = pieces_out(x_and_core, ff_grads, ((0, n_ff, False), (p_ff, n_ff, True)))
        image = accum(blocks0 + blocks1, code, block_first, sub_rows, width)
        d_emb = image.reshape(rows // 8, tiles, 8, 128).transpose(0, 2, 1, 3).reshape(rows, width)

        def more_grads(carry):
            r, table = carry
            at = rank - r * GRAD_SLOTS
            there = owned & (at >= 0) & (at < GRAD_SLOTS)
            dest = compact(at, there, jnp.where(owned, local, 0) + 1, GRAD_SLOTS)
            dest = jnp.where(dest == 0, rows, dest - 1)
            grads = jnp.concatenate(token_blocks(own_places(r, 0), d_tok0) + token_blocks(own_places(r, 1), d_tok1), axis=0).astype(F32)
            return r + 1, table.at[both_orders(dest).reshape(-1)].add(grads, mode="drop")

        _, d_emb = lax.while_loop(lambda c: c[0] < grad_rounds, more_grads, (jnp.int32(1), d_emb))

        small = jnp.concatenate([sums_qkv[0], d_b_up[0], sums1[:2].reshape(-1), sums2[:4].reshape(-1)]).reshape(-1, width)
        small = jnp.concatenate([small, jnp.zeros((pos_all.shape[0] - seq - n_small, width), F32)])
        pos_all = lax.dynamic_update_slice_in_dim(pos_all, small, seq, 0).reshape(n_tp * n_x, n_core, p_pos, width)
        pos_theirs = swap(lax.dynamic_index_in_dim(pos_all, 1 - c_index, 1, keepdims=False).reshape(-1, width), "cc")
        pos_both = lax.dynamic_index_in_dim(pos_all, c_index, 1, keepdims=False).reshape(-1, width) + pos_theirs
        pos_both = lax.psum_scatter(pos_both, ("tp", "xx"), scatter_dimension=0, tiled=True)
        rest = grad_rest(core, ctx, d_attn, d_qkvs, hid1, n_tp, spans, plus=rest_theirs)
        rest = lax.psum_scatter(rest, ("tp", "xx"), scatter_dimension=0, tiled=True)
        rest_w = every_piece(rest)
        whole = lax.all_gather(pos_both, ("tp", "xx", "cc"), axis=0, tiled=True)
        d_pos = jnp.pad(whole[:seq], ((POS_OFFSET, pos_table.shape[0] - seq - POS_OFFSET), (0, 0)))
        small = whole[seq:seq + n_small].reshape(-1)
        n_b = b_qkv.size
        d_b_qkv = lax.dynamic_slice_in_dim(small, tp_index * n_b, n_b).reshape(n_core, 3, -1, b_qkv.shape[2])
        d_b_qkv = d_b_qkv.transpose(1, 0, 2, 3).reshape(b_qkv.shape)
        d_b_up = lax.dynamic_slice_in_dim(small, n_tp * n_b + tp_index * ff, ff)
        d_gain1, d_bias1, d_gain2, d_bias2, d_b_out, d_b_down = small[n_tp * (n_b + ff):].reshape(6, width)

        d_w_out, d_w_qkv = pieces_out(x_and_core, rest_w, ((0, n_out, False), (p_out, n_b // n_dp, False)))
        d_w_out = d_w_out.reshape(w_out.shape)
        d_w_qkv = d_w_qkv.reshape(n_core, 3, -1, w_qkv.shape[3], width).transpose(4, 1, 0, 2, 3).reshape(w_qkv.shape)
        return (layer_out, d_emb, d_pos, d_gain1, d_bias1, d_w_qkv, d_b_qkv, d_w_out,
                d_b_out, d_gain2, d_bias2, d_w_up, d_b_up, d_w_down, d_b_down)

    rep = P()
    in_specs = (P(dp, None), P("tp", None), rep, rep, rep,
                P(None, None, "tp", None), P(None, "tp", None), P("tp", None, None), rep,
                rep, rep, P(None, "tp"), P("tp"), P("tp", None), rep,
                P(dp, "tp", None))
    out_specs = (P(dp, "tp", None), P("tp", None), rep, rep, rep,
                 P(None, None, "tp", None), P(None, "tp", None), P("tp", None, None), rep,
                 rep, rep, P(None, "tp"), P("tp"), P("tp", None), rep)

    return jax.shard_map(local_step, mesh=mesh3, in_specs=in_specs, out_specs=out_specs, check_vma=False)
```
